128 devices in a mesh: gx: 2 (over core), gy: 4 (over x), gz: 16 (over z, y).
Axes of the slice: x: 4, y: 4, z: 4, core: 2. Of those that a mesh axis runs over, the one named last changes fastest.
Arguments:
- right_side: float32 [96, 192, 768], P('gx', 'gy', 'gz'), may hold values from -6 to 6
- face_coef: float32 [3, 96, 192, 768], P(None, 'gx', 'gy', 'gz'), may hold values from 0.3 to 3
- absorption: float32 [96, 192, 768], P('gx', 'gy', 'gz'), may hold values from 0.001 to 0.01
Outputs:
- solution: float32 [96, 192, 768], P('gx', 'gy', 'gz')
- residual: float32 [96, 192, 768], P('gx', 'gy', 'gz')
- relative_norm: float32 [], replicated
The draws below stay inside these ranges and needn't reach their ends.
All inputs are finite; a program needn't handle non-finite values.
Results may differ from the reference program's by a relative error of at most 0.0003.
Values sent between devices are 32-bit elements.
No kernel may reach another device: no remote copies, remote signals or barrier semaphores. Data moves between devices by JAX's collectives and lax.ppermute only.
A program may use at most 192 MiB of HBM per device.

```python
import math
import jax
import jax.numpy as jnp
from jax import lax

LEVELS = 5
SWEEPS = 3
BOTTOM = 6
NX = 96
NY = 192
NZ = 768


def block_scale(stream_key, shape, cuts, low, top_value):
    def one(axis_at, blocks):
        draws = jax.random.uniform(jax.random.fold_in(jax.random.fold_in(stream_key, 6), axis_at), (blocks,), jnp.float32, low / len(cuts), top_value / len(cuts))
        return jnp.repeat(jnp.exp(draws), shape[axis_at] // blocks).reshape((-1,) + (1,) * (len(shape) - axis_at - 1))

    level = one(*cuts[0])
    for cut in cuts[1:]:
        level = level * one(*cut)
    return level


def noise(rng, shape, spread, bound, split=(), kind=jnp.bfloat16):
    entries = spread * jax.random.normal(rng, shape, jnp.float32)
    if split:
        entries = entries * block_scale(rng, shape, split, -0.22, 0.18)
    return jnp.clip(entries, -bound, bound).astype(kind)


def setup_inputs(seed: int = 0) -> dict:
    streams_of = jax.random.split(jax.random.key(seed), 4)
    return {
        "right_side": noise(streams_of[0], (NX, NY, NZ), 1.0, 6.0, ((0, 2), (1, 4), (2, 16)), jnp.float32),
        "face_coef": jnp.clip(jnp.exp(math.log(3.0) - 2.3025851 * jax.random.uniform(streams_of[1], (3, NX, NY, NZ), jnp.float32) ** block_scale(streams_of[1], (3, NX, NY, NZ), ((1, 2), (2, 4), (3, 16)), -0.2, 0.2)), 0.3, 3.0),
        "absorption": jnp.clip(jnp.exp(math.log(0.01) - 2.30258502 * jax.random.uniform(streams_of[2], (NX, NY, NZ), jnp.float32) ** block_scale(streams_of[2], (NX, NY, NZ), ((0, 2), (1, 4), (2, 16)), -0.2, 0.2)), 0.001, 0.01),
    }


cheb_low = 0.25
cheb_high = 2.0

def apply_stencil(field, stencil, weight, padded):
    low_x = padded[:-2, 1:-1, 1:-1]
    high_x = padded[2:, 1:-1, 1:-1]
    low_y = padded[1:-1, :-2, 1:-1]
    high_y = padded[1:-1, 2:, 1:-1]
    low_z = padded[1:-1, 1:-1, :-2]
    high_z = padded[1:-1, 1:-1, 2:]
    flux = stencil[0] * (field - low_x) + stencil[3] * (field - high_x)
    flux = flux + stencil[1] * (field - low_y) + stencil[4] * (field - high_y)
    flux = flux + stencil[2] * (field - low_z) + stencil[5] * (field - high_z)
    return stencil[6] * field + weight * flux

def inverse_diagonal(stencil, weight):
    total = stencil[0] + stencil[3] + stencil[1] + stencil[4] + stencil[2] + stencil[5]
    return 1.0 / (stencil[6] + weight * total)

def chebyshev(iterate, source, stencil, weight, sweeps, from_zero, pad_field):
    centre = 0.5 * (cheb_high + cheb_low)
    half_width = 0.5 * (cheb_high - cheb_low)
    cheb_ratio = centre / half_width
    cheb_rho = 1.0 / cheb_ratio
    scaling = inverse_diagonal(stencil, weight)
    if from_zero:
        remainder = source
    else:
        remainder = source - apply_stencil(iterate, stencil, weight, pad_field(iterate))
    update = scaling * remainder * (1.0 / centre)
    for sweep in range(sweeps):
        iterate = iterate + update
        if sweep + 1 < sweeps:
            remainder = source - apply_stencil(iterate, stencil, weight, pad_field(iterate))
            next_rho = 1.0 / (2.0 * cheb_ratio - cheb_rho)
            update = next_rho * cheb_rho * update + 2.0 * next_rho / half_width * (scaling * remainder)
            cheb_rho = next_rho
    return iterate

def conjugate(source, stencil, weight, pad_field, total):
    iterate = jnp.zeros_like(source)
    remainder = source
    search = source
    norm_now = total(remainder * remainder)
    for step in range(BOTTOM):
        applied = apply_stencil(search, stencil, weight, pad_field(search))
        step_size = norm_now / total(search * applied)
        iterate = iterate + step_size * search
        if step + 1 < BOTTOM:
            remainder = remainder - step_size * applied
            norm_next = total(remainder * remainder)
            search = remainder + norm_next / norm_now * search
            norm_now = norm_next
    return iterate

def average_cells(field):
    blocks = field.reshape(field.shape[0] // 2, 2, field.shape[1] // 2, 2, field.shape[2] // 2, 2)
    return lax.optimization_barrier(jnp.sum(blocks, axis=(1, 3, 5))) * 0.125

def average_faces(faces):
    halves = (faces.shape[1] // 2, 2, faces.shape[2] // 2, 2, faces.shape[3] // 2, 2)
    along_x = faces[0].reshape(halves)[:, 0]
    along_y = faces[1].reshape(halves)[:, :, :, 0]
    along_z = faces[2].reshape(halves)[..., 0]
    return jnp.stack([lax.optimization_barrier(jnp.sum(along_x, axis=(2, 4))), lax.optimization_barrier(jnp.sum(along_y, axis=(1, 4))), lax.optimization_barrier(jnp.sum(along_z, axis=(1, 3)))]) * 0.25

def repeat_cells(field):
    shape = field.shape
    wide = jnp.broadcast_to(field[:, None, :, None, :, None], (shape[0], 2, shape[1], 2, shape[2], 2))
    return wide.reshape(2 * shape[0], 2 * shape[1], 2 * shape[2])

def pad_zero(field):
    return jnp.pad(field, 1)

def build_stencil(faces, cells):
    high_x = jnp.pad(faces[0, 1:], ((0, 1), (0, 0), (0, 0)))
    high_y = jnp.pad(faces[1, :, 1:], ((0, 0), (0, 1), (0, 0)))
    high_z = jnp.pad(faces[2, :, :, 1:], ((0, 0), (0, 0), (0, 1)))
    return jnp.stack([faces[0], faces[1], faces[2], high_x, high_y, high_z, cells])

def reference(right_side, face_coef, absorption):
    stencils = []
    faces = face_coef
    cells = absorption
    for level in range(LEVELS):
        stencils.append(build_stencil(faces, cells))
        if level + 1 < LEVELS:
            faces = average_faces(faces)
            cells = average_cells(cells)
    sources = []
    iterates = []
    source = right_side
    for level in range(LEVELS - 1):
        weight = 0.25 ** level
        iterate = chebyshev(jnp.zeros_like(source), source, stencils[level], weight, SWEEPS, True, pad_zero)
        remainder = source - apply_stencil(iterate, stencils[level], weight, pad_zero(iterate))
        sources.append(source)
        iterates.append(iterate)
        source = average_cells(remainder)
    correction = conjugate(source, stencils[LEVELS - 1], 0.25 ** (LEVELS - 1), pad_zero, jnp.sum)
    for level in reversed(range(LEVELS - 1)):
        weight = 0.25 ** level
        iterate = iterates[level] + repeat_cells(correction)
        correction = chebyshev(iterate, sources[level], stencils[level], weight, SWEEPS, False, pad_zero)
    residual = right_side - apply_stencil(correction, stencils[0], 1.0, pad_zero(correction))
    relative_norm = jnp.sqrt(jnp.sum(residual * residual) / jnp.sum(right_side * right_side))
    return (correction, residual, relative_norm)
```

```python
import functools

import jax
import jax.numpy as jnp
from jax import lax
from jax.experimental import pallas as pl
from jax.experimental.pallas import tpu as pltpu
from jax.sharding import Mesh
from jax.sharding import PartitionSpec as P

BOTTOM = 6
ALL = ("gx", "gy", "gz_0", "gz_1")
YZ = ("gy", "gz_0", "gz_1")
GZ = ("gz_0", "gz_1")
LANES = 128
WIDTH = 8
COUNT_Y = 4
COUNT_Z = 16
COLUMNS = COUNT_Y * COUNT_Z
SIZES = (48, 24, 12, 6)
CHUNK = 24

theta = 1.125
delta = 0.875
sigma = theta / delta
rho_0 = 1.0 / sigma
rho_1 = 1.0 / (2.0 * sigma - rho_0)
rho_2 = 1.0 / (2.0 * sigma - rho_1)
FIRST = (0.0, 1.0 / theta)
LATER = ((rho_1 * rho_0, 2.0 * rho_1 / delta), (rho_2 * rho_1, 2.0 * rho_2 / delta))

vmem = pl.BlockSpec(memory_space=pltpu.VMEM)
anywhere = pl.BlockSpec(memory_space=pl.ANY)


def roll(value, by, axis):
    axis = axis % value.ndim
    by = by % value.shape[axis]
    return pltpu.roll(value, by, axis) if by else value


def iota(shape, dim):
    return lax.broadcasted_iota(jnp.int32, shape, dim % len(shape))


def exact_dot(left, right):
    return jnp.dot(
        left, right, precision=lax.Precision.HIGHEST, preferred_element_type=jnp.float32
    )


class Wrapped:
    @staticmethod
    def low_y(v):
        return roll(v, 1, -2)

    @staticmethod
    def up_y(v):
        return roll(v, -1, -2)

    @staticmethod
    def low_z(v):
        return roll(v, 1, -1)

    @staticmethod
    def up_z(v):
        return roll(v, -1, -1)


class Columns:
    def __init__(self, cells):
        self.cells = cells

    def low_y(self, v):
        lane = iota(v.shape, -1)
        last = lax.slice_in_dim(v, self.cells - 1, self.cells, axis=v.ndim - 3)
        rest = lax.slice_in_dim(v, 0, self.cells - 1, axis=v.ndim - 3)
        lane = iota(last.shape, -1)
        last = jnp.where((lane >= COUNT_Z) & (lane < COLUMNS), roll(last, COUNT_Z, -1), 0.0)
        return jnp.concatenate([last, rest], axis=v.ndim - 3)

    def up_y(self, v):
        first = lax.slice_in_dim(v, 0, 1, axis=v.ndim - 3)
        rest = lax.slice_in_dim(v, 1, self.cells, axis=v.ndim - 3)
        lane = iota(first.shape, -1)
        first = jnp.where(lane < COLUMNS - COUNT_Z, roll(first, -COUNT_Z, -1), 0.0)
        return jnp.concatenate([rest, first], axis=v.ndim - 3)

    def low_z(self, v):
        lane, row = iota(v.shape, -1), iota(v.shape, -2)
        edge = roll(roll(v, 1 - self.cells, -2), 1, -1)
        edge = jnp.where((lane % COUNT_Z != 0) & (lane < COLUMNS), edge, 0.0)
        return jnp.where(row == 0, edge, roll(v, 1, -2))

    def up_z(self, v):
        lane, row = iota(v.shape, -1), iota(v.shape, -2)
        edge = roll(roll(v, self.cells - 1, -2), -1, -1)
        edge = jnp.where((lane % COUNT_Z != COUNT_Z - 1) & (lane < COLUMNS), edge, 0.0)
        inner = jnp.where(row < self.cells - 1, roll(v, -1, -2), 0.0)
        return jnp.where(row == self.cells - 1, edge, inner)


def set_up(stack, weight, planes, move):
    stack[1, planes] = stack[1, 0]

    def body(i, carry):
        cell, face_y, face_z = stack[4, i], stack[2, i], stack[3, i]
        total = stack[1, i] + stack[1, i + 1] + face_y + move.up_y(face_y)
        total = total + face_z + move.up_z(face_z)
        stack[5, i] = jnp.where(cell > 0.0, 1.0 / (cell + weight * total), 0.0)
        return carry

    lax.fori_loop(0, planes, body, 0)


def from_zero(stack, iterate, update, planes):
    def body(i, carry):
        step = FIRST[1] * (stack[5, i] * stack[0, i])
        update[i] = step
        iterate[i] = step
        return carry

    lax.fori_loop(0, planes, body, 0)


def stencil_pass(stack, iterate, weight, planes, count, move, use, carry):
    flux = stack[1, 0] * (iterate[0] - iterate[planes - 1])

    def body(i, both):
        flux, carry = both
        v = iterate[i]
        above = stack[1, i + 1] * (iterate[i + 1] - v)
        flux_y = stack[2, i] * (v - move.low_y(v))
        flux_z = stack[3, i] * (v - move.low_z(v))
        total = (flux - above) + (flux_y - move.up_y(flux_y)) + (flux_z - move.up_z(flux_z))
        carry = use(i, v, stack[0, i] - (stack[4, i] * v + weight * total), carry)
        return above, carry

    return lax.fori_loop(0, count, body, (flux, carry))[1]


def sweep(stack, iterate, update, weight, planes, move, factors):
    keep, gain = factors
    iterate[planes] = iterate[0]

    def use(i, v, remainder, carry):
        step = gain * (stack[5, i] * remainder)
        if keep:
            step = keep * update[i] + step
        update[i] = step
        iterate[i] = v + step
        return carry

    stencil_pass(stack, iterate, weight, planes, planes, move, use, 0)


def down(stack, iterate, update, weight, planes, move):
    from_zero(stack, iterate, update, planes)
    for factors in LATER:
        sweep(stack, iterate, update, weight, planes, move, factors)


def up(stack, iterate, update, weight, planes, move):
    for factors in (FIRST,) + LATER:
        sweep(stack, iterate, update, weight, planes, move, factors)


def keep_remainder(stack, iterate, update, weight, planes, count, move):
    iterate[planes] = iterate[0]

    def use(i, v, remainder, carry):
        update[i] = remainder
        return carry

    stencil_pass(stack, iterate, weight, planes, count, move, use, 0)


def coarsen(stack, remainder, rows, pairs, out, count, size):
    half = size // 2

    def body(i, carry):
        for k in range(5):
            if k == 1:
                rows[k] = stack[1, 2 * i]
            elif k == 0:
                rows[k] = remainder[2 * i] + remainder[2 * i + 1]
            else:
                rows[k] = stack[k, 2 * i] + stack[k, 2 * i + 1]
        for k in range(5):
            pair = rows[k, pl.ds(0, half, stride=2), :]
            if k != 2:
                pair = pair + rows[k, pl.ds(1, half, stride=2), :]
            pairs[k, i, 0:half, :] = pair
        return carry

    if half % 8:
        pairs[...] = jnp.zeros(pairs.shape, jnp.float32)
    lax.fori_loop(0, count // 2, body, 0)
    fine, coarse = iota((LANES, LANES), 0), iota((LANES, LANES), 1)
    mean = jnp.where((fine // 2 == coarse) & (fine < size), 1.0, 0.0)
    even = jnp.where((fine == 2 * coarse) & (fine < size), 1.0, 0.0)
    _, planes, padded, _ = pairs.shape
    for k in range(5):
        flat = pairs[k].reshape(planes * padded, LANES)
        scale = 0.125 if k in (0, 4) else 0.25
        made = scale * exact_dot(flat, even if k == 3 else mean)
        out(k, made.reshape(planes, padded, LANES))


def spread(coarse, spare, rows, fine, row_map, plane_maps):
    planes, height, _ = spare.shape
    source, target = iota((LANES, LANES), 0), iota((LANES, LANES), 1)
    half = target // 2
    pick = jnp.where(source == jnp.where(target < LANES // 2, half, LANES // 2 + half), 1.0, 0.0)
    wide = exact_dot(coarse[0:planes].reshape(planes * height, LANES), pick)
    spare[...] = wide.reshape(planes, height, LANES)
    rows[...] = jnp.zeros(rows.shape, jnp.float32)
    for count, plane_of, target_of in plane_maps:

        def body(i, carry):
            plane = plane_of(i)
            for start, number, first in row_map:
                part = spare[plane, start : start + number, :]
                rows[pl.ds(first, number, stride=2), :] = part
                rows[pl.ds(first + 1, number, stride=2), :] = part
            both = rows[...]
            at = target_of(i)
            fine[at] = fine[at] + both
            fine[at + 1] = fine[at + 1] + both
            return carry

        lax.fori_loop(0, count, body, 0)


def places():
    gx = lax.axis_index("gx")
    gy = lax.axis_index("gy")
    gz = lax.axis_index("gz_0") * 4 + lax.axis_index("gz_1")
    return gx, gy, gz


def widen(value):
    rows, lanes = value.shape
    if lanes == LANES:
        return value
    return jnp.concatenate([value, jnp.zeros((rows, LANES - lanes), jnp.float32)], axis=1)


def y_pack(parts, size):
    lane = iota((8, LANES), 1)
    tiles = [jnp.zeros((8, LANES), jnp.float32) for _ in range(-(-5 * size // LANES))]
    for k, part in enumerate(parts):
        start = k * size
        moved = roll(part, start % LANES, -1)
        for t in range(len(tiles)):
            a, b = max(start, t * LANES) - t * LANES, min(start + size, (t + 1) * LANES) - t * LANES
            if a < b:
                tiles[t] = jnp.where((lane >= a) & (lane < b), moved, tiles[t])
    return tiles


def y_unpack(tiles, k, size):
    lane = iota((8, LANES), 1)
    start = k * size
    t = start // LANES
    value = tiles[t]
    if start + size > (t + 1) * LANES:
        value = jnp.where(lane >= start - t * LANES, value, tiles[t + 1])
    return roll(value, -start, -1)


def pack(own, beside, size, outs):
    y_even, y_odd, z_even, z_odd, ee, eo, oe, oo = outs
    _, gy, gz = places()
    even_y, even_z = gy % 2 == 0, gz % 2 == 0
    lane = iota((size, LANES), 1)

    def group(g, slots, get):
        top = jnp.zeros((size, LANES), jnp.float32)
        bottom = top
        for s in range(slots):
            high, low = [], []
            for k in range(5):
                v = get(k, s)
                at = 40 * s + 8 * k
                here = (lane >= at) & (lane < at + 8)
                top = jnp.where(here, roll(v, at - (size - 8), -1), top)
                bottom = jnp.where(here, roll(v, at, -1), bottom)
                high.append(v[size - 8 :])
                low.append(v[:8])
            for t, (h, l) in enumerate(zip(y_pack(high, size), y_pack(low, size))):
                y_even[3 * g + s, 8 * t : 8 * t + 8, :] = jnp.where(even_y, h, l)
                y_odd[3 * g + s, 8 * t : 8 * t + 8, :] = jnp.where(even_y, l, h)
        a, b = jnp.where(even_z, top, bottom), jnp.where(even_z, bottom, top)
        z_even[g] = a
        z_odd[g] = b
        ee[g] = jnp.where(even_y, a[size - 8 :], a[:8])
        eo[g] = jnp.where(even_y, b[size - 8 :], b[:8])
        oe[g] = jnp.where(even_y, a[:8], a[size - 8 :])
        oo[g] = jnp.where(even_y, b[:8], b[size - 8 :])

    def body(g, carry):
        group(g, 3, lambda k, s: own(k, 3 * g + s))
        return carry

    lax.fori_loop(0, size // 3, body, 0)
    for q in range(3):
        group(size // 3 + q, min(3, 8 - 3 * q), lambda k, s: beside(k, 3 * q + s))


def unpack(stack, own, beside, size, payloads):
    y_even, y_odd, z_even, z_odd, ee, eo, oe, oo = payloads
    gx, gy, gz = places()
    even_y, even_z = gy % 2 == 0, gz % 2 == 0
    lane, lane_8 = iota((size, LANES), 1), iota((8, LANES), 1)
    tiles = -(-5 * size // LANES)

    def join(lane, middle, low, high, at):
        sides = jnp.where(lane >= LANES - 8, roll(low, LANES - 8 - at, -1), 0.0)
        sides = jnp.where(lane < size + 8, roll(high, size - at, -1), sides)
        return jnp.where(lane < size, middle, sides)

    def group(g, slots, get, first):
        low = jnp.where(even_z, z_odd[g], z_even[g])
        high = jnp.where(even_z, z_even[g], z_odd[g])
        by_even = jnp.where(even_z, eo[g], ee[g]), jnp.where(even_z, ee[g], eo[g])
        by_odd = jnp.where(even_z, oo[g], oe[g]), jnp.where(even_z, oe[g], oo[g])
        corners = (
            [jnp.where(even_y, e, o) for e, o in zip(by_even, by_odd)],
            [jnp.where(even_y, o, e) for e, o in zip(by_even, by_odd)],
        )
        for s in range(slots):
            e, o = y_even[3 * g + s], y_odd[3 * g + s]
            ends = jnp.where(even_y, e, o), jnp.where(even_y, o, e)
            ends = [[end[8 * t : 8 * t + 8] for t in range(tiles)] for end in ends]
            for k in range(5):
                at = 40 * s + 8 * k
                stack[k, first + s, 0:size, :] = join(lane, get(k, s), low, high, at)
                for which in range(2):
                    rows = slice(size + 8 * which, size + 8 * which + 8)
                    middle = y_unpack(ends[which], k, size)
                    stack[k, first + s, rows, :] = join(lane_8, middle, *corners[which], at)

    def body(g, carry):
        group(g, 3, lambda k, s: own(k, 3 * g + s), 3 * g)
        return carry

    lax.fori_loop(0, size // 3, body, 0)
    for q in range(3):
        group(
            size // 3 + q,
            min(3, 8 - 3 * q),
            lambda k, s: beside(k, 3 * q + s),
            size + gx + 3 * q,
        )
    empty = size + 8 * (1 - gx)
    for k in range(5):
        stack[k, empty] = jnp.zeros(stack.shape[2:], jnp.float32)


def payload_shapes(size):
    groups = size // 3 + 3
    tall = 8 * (-(-5 * size // LANES))
    y = jax.ShapeDtypeStruct((size + 8, tall, LANES), jnp.float32)
    z = jax.ShapeDtypeStruct((groups, size, LANES), jnp.float32)
    c = jax.ShapeDtypeStruct((groups, 8, LANES), jnp.float32)
    return [y, y, z, z, c, c, c, c]


def partner(index, parity, count):
    if parity is None:
        return index
    other = index + 1 if index % 2 == parity else index - 1
    return other if 0 <= other < count else None


def swap(value, parity_y, parity_z):
    pairs = []
    for y in range(COUNT_Y):
        for z in range(COUNT_Z):
            to_y, to_z = partner(y, parity_y, COUNT_Y), partner(z, parity_z, COUNT_Z)
            if to_y is not None and to_z is not None:
                pairs.append((y * COUNT_Z + z, to_y * COUNT_Z + to_z))
    return lax.ppermute(value, YZ, pairs)


WAYS = ((0, None), (1, None), (None, 0), (None, 1), (0, 0), (0, 1), (1, 0), (1, 1))


def swap_cores(value):
    return lax.ppermute(value, "gx", [(0, 1), (1, 0)])


def f32(*shape):
    return jax.ShapeDtypeStruct(shape, jnp.float32)


def call(body, outs, ins, scratch, operands):
    return pl.pallas_call(
        body,
        out_shape=[shape for shape, _ in outs],
        out_specs=[spec for _, spec in outs],
        in_specs=ins,
        scratch_shapes=scratch,
        compiler_params=pltpu.CompilerParams(vmem_limit_bytes=56 * 2**20),
    )(*operands)


def edge_kernel(right, faces, cells, out, sems):
    gx = lax.axis_index("gx")
    start = (1 - gx) * (SIZES[0] - WIDTH)
    part = pl.ds(start, WIDTH)
    copies = [
        pltpu.make_async_copy(right.at[part], out.at[0], sems.at[0]),
        pltpu.make_async_copy(faces.at[0, part], out.at[1], sems.at[1]),
        pltpu.make_async_copy(faces.at[1, part], out.at[2], sems.at[2]),
        pltpu.make_async_copy(faces.at[2, part], out.at[3], sems.at[3]),
        pltpu.make_async_copy(cells.at[part], out.at[4], sems.at[4]),
    ]
    for copy in copies:
        copy.start()
    for copy in copies:
        copy.wait()


def own_inputs(right, faces, cells):
    def own(k, i):
        if k == 0:
            return widen(right[i])
        return widen(cells[i] if k == 4 else faces[k - 1, i])

    return own


def pack_0_kernel(right, faces, cells, beside, *outs):
    pack(own_inputs(right, faces, cells), lambda k, j: widen(beside[k, j]), SIZES[0], outs)


def pack_1_kernel(own, beside, *outs):
    pack(lambda k, i: own[k, i], lambda k, j: beside[k, j], SIZES[1], outs)


def start_kept(stack, kept, sem):
    copy = pltpu.make_async_copy(stack, kept, sem)
    copy.start()
    return copy


def level_0_kernel(
    right, faces, cells, beside, ye, yo, ze, zo, ee, eo, oe, oo,
    coarse, coarse_edge, kept_stack, kept_iterate,
    stack, iterate, update, rows, pairs, sems,
):
    size = SIZES[0]
    planes = size + 9
    gx = lax.axis_index("gx")
    unpack(
        stack,
        own_inputs(right, faces, cells),
        lambda k, j: widen(beside[k, j]),
        size,
        (ye, yo, ze, zo, ee, eo, oe, oo),
    )
    set_up(stack, 1.0, planes, Wrapped)
    first = start_kept(stack, kept_stack, sems.at[0])
    down(stack, iterate, update, 1.0, planes, Wrapped)
    own = pl.ds(0, planes)
    keep_remainder(stack, iterate, update, 1.0, planes, size, Wrapped)
    second = start_kept(iterate.at[own], kept_iterate.at[own], sems.at[1])

    def out(k, value):
        coarse[k] = value
        coarse_edge[k] = jnp.where(gx == 0, value[16:24], value[0:8])

    coarsen(stack, update, rows, pairs, out, size, size)
    first.wait()
    second.wait()


def level_1_kernel(
    own, beside, ye, yo, ze, zo, ee, eo, oe, oo,
    coarse, kept_stack, kept_iterate,
    stack, iterate, update, rows, pairs, made, sems,
):
    size = SIZES[1]
    planes = size + 9
    gx = lax.axis_index("gx")
    unpack(
        stack,
        lambda k, i: own[k, i],
        lambda k, j: beside[k, j],
        size,
        (ye, yo, ze, zo, ee, eo, oe, oo),
    )
    set_up(stack, 0.25, planes, Wrapped)
    first = start_kept(stack, kept_stack, sems.at[0])
    down(stack, iterate, update, 0.25, planes, Wrapped)
    keep_remainder(stack, iterate, update, 0.25, planes, size, Wrapped)
    inside = pl.ds(0, planes)
    second = start_kept(iterate.at[inside], kept_iterate.at[inside], sems.at[1])

    def out(k, value):
        made[k] = value

    coarsen(stack, update, rows, pairs, out, size, size)
    for i in range(SIZES[2]):
        line = made[0, i]
        for k in range(1, 5):
            line = line + roll(made[k, i], SIZES[2] * k, -1)
        coarse[i] = jnp.where(gx == 0, line, roll(line, LANES // 2, -1))
    first.wait()
    second.wait()


def level_2_kernel(
    own, ye, yo, ze, zo, ee, eo, oe, oo,
    payload, kept_stack, kept_iterate,
    stack, iterate, update, rows, pairs, made, lines, sems,
):
    size = SIZES[2]
    planes = 2 * size + 1
    _, gy, gz = places()
    even_y, even_z = gy % 2 == 0, gz % 2 == 0
    lane = iota((16, LANES), 1)
    bases = (0, size, LANES - size)
    for k in range(5):
        stack[k, 2 * size] = jnp.zeros(stack.shape[2:], jnp.float32)

    def body(i, carry):
        e = ee[i], eo[i]
        o = oe[i], oo[i]
        table = (
            (own[i], jnp.where(even_z, ze[i], zo[i]), jnp.where(even_z, zo[i], ze[i])),
            (
                jnp.where(even_y, ye[i], yo[i]),
                jnp.where(even_y, jnp.where(even_z, e[0], e[1]), jnp.where(even_z, o[0], o[1])),
                jnp.where(even_y, jnp.where(even_z, e[1], e[0]), jnp.where(even_z, o[1], o[0])),
            ),
            (
                jnp.where(even_y, yo[i], ye[i]),
                jnp.where(even_y, jnp.where(even_z, o[0], o[1]), jnp.where(even_z, e[0], e[1])),
                jnp.where(even_y, jnp.where(even_z, o[1], o[0]), jnp.where(even_z, e[1], e[0])),
            ),
        )
        for k in range(5):
            for h in range(2):
                source = (LANES // 2) * h + size * k
                plane = size * h + i
                stack[k, plane, 24:32, :] = jnp.zeros((8, LANES), jnp.float32)
                for a, first in enumerate((0, size, 40 - size)):
                    line = jnp.zeros((16, LANES), jnp.float32)
                    for b, base in enumerate(bases):
                        here = (lane >= base) & (lane < base + size)
                        line = jnp.where(here, roll(table[a][b], base - source, -1), line)
                    stack[k, plane, first : first + size, :] = line[:size]
        return carry

    lax.fori_loop(0, size, body, 0)
    weight = 0.0625
    set_up(stack, weight, planes, Wrapped)
    first = start_kept(stack, kept_stack, sems.at[0])
    down(stack, iterate, update, weight, planes, Wrapped)
    keep_remainder(stack, iterate, update, weight, planes, 2 * size, Wrapped)
    inside = pl.ds(0, planes)
    second = start_kept(iterate.at[inside], kept_iterate.at[inside], sems.at[1])

    def out(k, value):
        made[k * 96 : k * 96 + 96, :] = value.reshape(96, LANES)

    coarsen(stack, update, rows, pairs, out, 2 * size, size)
    line = jnp.zeros((60, LANES), jnp.float32)
    for y in range(6):
        line = line + roll(made[pl.ds(y, 60, stride=8), :], 6 * y, -1)
    lines[0:60, :] = line
    chunk = lines[0:20, :] + roll(lines[20:40, :], 40, -1) + roll(lines[40:60, :], 80, -1)
    chunk = jnp.concatenate([chunk, jnp.zeros((4, LANES), jnp.float32)], axis=0)

    def repeat(c, carry):
        payload[pl.ds(pl.multiple_of(c * CHUNK, 8), CHUNK), :] = chunk
        return carry

    lax.fori_loop(0, COLUMNS, repeat, 0)
    first.wait()
    second.wait()


def compact(value):
    row = iota(value.shape, -2)
    out = jnp.where(row == 0, value, 0.0)
    out = jnp.where(row == 1, roll(value, -1, -2), out)
    return jnp.where(row == 2, roll(value, -2, -2), out)


def bottom(source, faces, cells):
    weight = 0.25**4
    move = Columns(3)
    face_x, face_y, face_z = faces
    nothing = jnp.zeros((1,) + source.shape[1:], jnp.float32)

    def apply(v):
        flux_x = face_x * (v - jnp.concatenate([nothing, v[:-1]], axis=0))
        flux_y = face_y * (v - move.low_y(v))
        flux_z = face_z * (v - move.low_z(v))
        total = flux_x - jnp.concatenate([flux_x[1:], nothing], axis=0)
        total = total + (flux_y - move.up_y(flux_y)) + (flux_z - move.up_z(flux_z))
        return cells * v + weight * total

    def total_of(v):
        flat = jnp.sum(jnp.sum(v, axis=0), axis=0)
        one = jnp.sum(jnp.sum(flat, axis=0, keepdims=True), axis=1, keepdims=True)
        return jnp.broadcast_to(one, flat.shape)

    iterate = jnp.zeros_like(source)
    remainder = source
    search = source
    norm_now = total_of(remainder * remainder)
    for step in range(BOTTOM):
        applied = apply(search)
        size = norm_now / total_of(search * applied)
        iterate = iterate + size * search
        if step + 1 < BOTTOM:
            remainder = remainder - size * applied
            norm_next = total_of(remainder * remainder)
            search = remainder + (norm_next / norm_now) * search
            norm_now = norm_next
    return iterate


def rise_kernel(
    gathered, stack_2_in, iterate_2_in, stack_1_in, iterate_1_in, stack_0_in, iterate_0_in,
    solution_out, residual_out, sums,
    stack_0, iterate_0, update_0, rows_0, spare_1,
    stack_1, iterate_1, update_1, rows_1, spare_2,
    stack_2, iterate_2, update_2, rows_2, spare_3,
    stack_3, iterate_3, update_3, turned, table, block_3, sems,
):
    gx, gy, gz = places()
    loads = []
    for n, (source, target) in enumerate(
        (
            (stack_2_in, stack_2),
            (iterate_2_in, iterate_2),
            (stack_1_in, stack_1),
            (iterate_1_in, iterate_1),
            (stack_0_in, stack_0),
            (iterate_0_in, iterate_0),
        )
    ):
        copy = pltpu.make_async_copy(source, target, sems.at[n])
        copy.start()
        loads.append(copy)

    stack_3[...] = jnp.zeros(stack_3.shape, jnp.float32)
    blank = jnp.zeros((LANES - COLUMNS, LANES), jnp.float32)
    for r in range(20):
        part = gathered[pl.ds(r, COLUMNS, stride=CHUNK), :]
        turned[...] = jnp.transpose(jnp.concatenate([part, blank], axis=0))
        for j in range(3):
            k, x = divmod(20 * j + r, 12)
            for y in range(6):
                stack_3[k, x, y, 0:6, :] = turned[40 * j + 6 * y : 40 * j + 6 * y + 6, :]
    move = Columns(6)
    weight = 0.25**3
    set_up(stack_3, weight, 13, move)
    down(stack_3, iterate_3, update_3, weight, 13, move)
    keep_remainder(stack_3, iterate_3, update_3, weight, 13, 12, move)

    def coarse(k, x_pair, y_pair, z_pair, scale):
        planes = []
        for x in range(6):
            read = (lambda i: update_3[i]) if k == 0 else (lambda i: stack_3[k, i])
            v = read(2 * x)
            if x_pair:
                v = v + read(2 * x + 1)
            lines = []
            for y in range(3):
                line = v[2 * y]
                if y_pair:
                    line = line + v[2 * y + 1]
                if z_pair:
                    line = line + roll(line, -1, -2)
                lines.append(scale * compact(line))
            planes.append(jnp.stack(lines))
        return jnp.stack(planes)

    lowest = bottom(
        coarse(0, True, True, True, 0.125),
        (
            coarse(1, False, True, True, 0.25),
            coarse(2, True, False, True, 0.25),
            coarse(3, True, True, False, 0.25),
        ),
        coarse(4, True, True, True, 0.125),
    )
    row = iota((8, LANES), 0)
    for x in range(6):
        for y in range(3):
            line = lowest[x, y]
            wide = jnp.where(row == 0, line, 0.0)
            for to in range(1, 6):
                wide = jnp.where(row == to, roll(line, to - to // 2, -2), wide)
            for a in range(2):
                for b in range(2):
                    iterate_3[2 * x + a, 2 * y + b] = iterate_3[2 * x + a, 2 * y + b] + wide
    up(stack_3, iterate_3, update_3, weight, 13, move)

    low_rows = jnp.zeros((32, LANES), jnp.float32)
    for q in range(6):
        two = [iterate_3[2 * q + h].reshape(48, LANES) for h in range(2)]
        table[q] = jnp.transpose(jnp.concatenate(two + [low_rows], axis=0))
    block_3[...] = jnp.zeros(block_3.shape, jnp.float32)
    lane = iota((8, LANES), 1)

    def place(q, carry):
        for a, first in ((0, 0), (1, 6), (-1, 18)):
            lines = [jnp.zeros((8, LANES), jnp.float32) for _ in range(2)]
            for b, base in ((0, 0), (1, 6), (-1, LANES - 6)):
                y, z = gy + a, gz + b
                inside = (y >= 0) & (y < COUNT_Y) & (z >= 0) & (z < COUNT_Z)
                at = jnp.where(inside, y * COUNT_Z + z, 0)
                here = (lane >= base) & (lane < base + 6) & inside
                found = jnp.broadcast_to(table[q, pl.ds(at, 1), :], (8, LANES))
                for h in range(2):
                    for y_in in range(6):
                        moved = roll(found, base - 48 * h - 8 * y_in, -1)
                        lines[h] = jnp.where(here & (row == y_in), moved, lines[h])
            for h in range(2):
                block_3[2 * q + h, first : first + 6, :] = lines[h][0:6]
        return carry

    lax.fori_loop(0, 6, place, 0)

    loads[0].wait()
    loads[1].wait()
    spread(
        block_3, spare_3, rows_2, iterate_2,
        ((0, 12, 0), (18, 6, 28)),
        ((12, lambda i: i, lambda i: 2 * i),),
    )
    up(stack_2, iterate_2, update_2, 0.0625, 25, Wrapped)

    loads[2].wait()
    loads[3].wait()
    size = SIZES[1]
    spread(
        iterate_2, spare_2, rows_1, iterate_1,
        ((0, 16, 0), (36, 4, 32)),
        (
            (12, lambda i: 12 * gx + i, lambda i: 2 * i),
            (4, lambda i: 12 - 4 * gx + i, lambda i: size + gx + 2 * i),
        ),
    )
    up(stack_1, iterate_1, update_1, 0.25, size + 9, Wrapped)

    loads[4].wait()
    loads[5].wait()
    size = SIZES[0]
    spread(
        iterate_1, spare_1, rows_0, iterate_0,
        ((0, 28, 0), (36, 4, 56)),
        (
            (24, lambda i: i, lambda i: 2 * i),
            (4, lambda i: 24 + 5 * gx + i, lambda i: size + gx + 2 * i),
        ),
    )
    planes = size + 9
    up(stack_0, iterate_0, update_0, 1.0, planes, Wrapped)
    iterate_0[planes] = iterate_0[0]
    mask = iota((size, LANES), 1) < size

    def use(i, v, remainder, carry):
        solution_out[i] = v[0:size, 0:size]
        residual_out[i] = remainder[0:size, 0:size]
        mine = jnp.where(mask, remainder[0:size], 0.0)
        given = jnp.where(mask, stack_0[0, i, 0:size, :], 0.0)
        return carry[0] + mine * mine, carry[1] + given * given

    zero = jnp.zeros((size, LANES), jnp.float32)
    squares = stencil_pass(stack_0, iterate_0, 1.0, planes, size, Wrapped, use, (zero, zero))
    ones = []
    for square in squares:
        one = jnp.sum(jnp.sum(square, axis=0, keepdims=True), axis=1, keepdims=True)
        ones.append(jnp.broadcast_to(one, (8, LANES)))
    sums[...] = jnp.where(lane == 0, ones[0], jnp.where(lane == 1, ones[1], 0.0))


def shards(right, faces, cells):
    dma = pltpu.SemaphoreType.DMA
    buf = lambda *shape: pltpu.VMEM(shape, jnp.float32)
    edge = call(
        edge_kernel,
        [(f32(5, WIDTH, 48, 48), anywhere)],
        [anywhere] * 3,
        [dma((5,))],
        (right, faces, cells),
    )[0]
    beside = swap_cores(edge)
    outs = call(
        pack_0_kernel,
        [(s, vmem) for s in payload_shapes(48)],
        [vmem] * 4,
        [],
        (right, faces, cells, beside),
    )
    moved = [swap(v, *way) for v, way in zip(outs, WAYS)]
    coarse, coarse_edge, stack_0, iterate_0 = call(
        level_0_kernel,
        [
            (f32(5, 24, 24, LANES), vmem),
            (f32(5, WIDTH, 24, LANES), vmem),
            (f32(6, 58, 64, LANES), anywhere),
            (f32(58, 64, LANES), anywhere),
        ],
        [vmem] * 12,
        [
            buf(6, 58, 64, LANES),
            buf(58, 64, LANES),
            buf(58, 64, LANES),
            buf(5, 64, LANES),
            buf(5, 24, 24, LANES),
            dma((2,)),
        ],
        (right, faces, cells, beside, *moved),
    )
    beside = swap_cores(coarse_edge)
    outs = call(
        pack_1_kernel,
        [(s, vmem) for s in payload_shapes(24)],
        [vmem] * 2,
        [],
        (coarse, beside),
    )
    moved = [swap(v, *way) for v, way in zip(outs, WAYS)]
    coarse, stack_1, iterate_1 = call(
        level_1_kernel,
        [
            (f32(12, 16, LANES), vmem),
            (f32(6, 34, 40, LANES), anywhere),
            (f32(34, 40, LANES), anywhere),
        ],
        [vmem] * 10,
        [
            buf(6, 34, 40, LANES),
            buf(34, 40, LANES),
            buf(34, 40, LANES),
            buf(5, 40, LANES),
            buf(5, 12, 16, LANES),
            buf(5, 12, 16, LANES),
            dma((2,)),
        ],
        (coarse, beside, *moved),
    )
    coarse = coarse + swap_cores(coarse)
    moved = [swap(coarse, *way) for way in WAYS]
    payload, stack_2, iterate_2 = call(
        level_2_kernel,
        [
            (f32(COLUMNS * CHUNK, LANES), vmem),
            (f32(6, 26, 40, LANES), anywhere),
            (f32(26, 40, LANES), anywhere),
        ],
        [vmem] * 9,
        [
            buf(6, 26, 40, LANES),
            buf(26, 40, LANES),
            buf(26, 40, LANES),
            buf(5, 40, LANES),
            buf(5, 12, 8, LANES),
            buf(480, LANES),
            buf(64, LANES),
            dma((2,)),
        ],
        (coarse, *moved),
    )
    payload = payload.reshape(COLUMNS, CHUNK, LANES)
    gathered = lax.all_to_all(payload, YZ, 0, 0).reshape(COLUMNS * CHUNK, LANES)
    solved, residual, sums = call(
        rise_kernel,
        [(f32(48, 48, 48), vmem), (f32(48, 48, 48), vmem), (f32(8, LANES), vmem)],
        [vmem] + [anywhere] * 6,
        [
            buf(6, 58, 64, LANES), buf(58, 64, LANES), buf(58, 64, LANES), buf(64, LANES),
            buf(33, 40, LANES),
            buf(6, 34, 40, LANES), buf(34, 40, LANES), buf(34, 40, LANES), buf(40, LANES),
            buf(24, 40, LANES),
            buf(6, 26, 40, LANES), buf(26, 40, LANES), buf(26, 40, LANES), buf(40, LANES),
            buf(12, 24, LANES),
            buf(6, 14, 6, 8, LANES), buf(14, 6, 8, LANES), buf(14, 6, 8, LANES),
            buf(LANES, LANES), buf(6, LANES, LANES), buf(12, 24, LANES),
            dma((6,)),
        ],
        (gathered, stack_2, iterate_2, stack_1, iterate_1, stack_0, iterate_0),
    )
    each = jnp.broadcast_to(sums[0:1].reshape(1, 1, LANES), (128, 1, LANES))
    total = jnp.sum(lax.all_to_all(each, ALL, 0, 0), axis=(0, 1))
    return solved, residual, jnp.sqrt(total[0] / total[1])


def solution(mesh):
    torus = Mesh(
        mesh.devices.reshape(mesh.shape["gx"], mesh.shape["gy"], 4, 4), ("gx", "gy", "gz_0", "gz_1")
    )
    in_specs = (P("gx", "gy", GZ), P(None, "gx", "gy", GZ), P("gx", "gy", GZ))
    out_specs = (P("gx", "gy", GZ), P("gx", "gy", GZ), P())
    return jax.shard_map(
        shards, mesh=torus, in_specs=in_specs, out_specs=out_specs, check_vma=False
    )
```

```python
import functools

import jax
import jax.numpy as jnp
from jax import lax
from jax.experimental import pallas as pl
from jax.experimental.pallas import tpu as pltpu
from jax.sharding import Mesh
from jax.sharding import PartitionSpec as P

BOTTOM = 6
ALL = ("gx", "gy", "gz_0", "gz_1")
YZ = ("gy", "gz_0", "gz_1")
GZ = ("gz_0", "gz_1")
LANES = 128
WIDTH = 8
COUNT_Y = 4
COUNT_Z = 16
COLUMNS = COUNT_Y * COUNT_Z
SIZES = (48, 24, 12, 6)
CHUNK = 24

theta = 1.125
delta = 0.875
sigma = theta / delta
rho_0 = 1.0 / sigma
rho_1 = 1.0 / (2.0 * sigma - rho_0)
rho_2 = 1.0 / (2.0 * sigma - rho_1)
FIRST = (0.0, 1.0 / theta)
LATER = ((rho_1 * rho_0, 2.0 * rho_1 / delta), (rho_2 * rho_1, 2.0 * rho_2 / delta))

vmem = pl.BlockSpec(memory_space=pltpu.VMEM)
held_near = pl.BlockSpec(memory_space=pltpu.VMEM)
anywhere = pl.BlockSpec(memory_space=pl.ANY)


def roll(value, by, axis):
    axis = axis % value.ndim
    by = by % value.shape[axis]
    return pltpu.roll(value, by, axis) if by else value


def iota(shape, dim):
    return lax.broadcasted_iota(jnp.int32, shape, dim % len(shape))


def exact_dot(left, right):
    return jnp.dot(
        left, right, precision=lax.Precision.HIGHEST, preferred_element_type=jnp.float32
    )


class Wrapped:
    @staticmethod
    def low_y(v):
        return roll(v, 1, -2)

    @staticmethod
    def up_y(v):
        return roll(v, -1, -2)

    @staticmethod
    def low_z(v):
        return roll(v, 1, -1)

    @staticmethod
    def up_z(v):
        return roll(v, -1, -1)


class Columns:
    def __init__(self, cells):
        self.cells = cells

    def low_y(self, v):
        lane = iota(v.shape, -1)
        last = lax.slice_in_dim(v, self.cells - 1, self.cells, axis=v.ndim - 3)
        rest = lax.slice_in_dim(v, 0, self.cells - 1, axis=v.ndim - 3)
        lane = iota(last.shape, -1)
        last = jnp.where((lane >= COUNT_Z) & (lane < COLUMNS), roll(last, COUNT_Z, -1), 0.0)
        return jnp.concatenate([last, rest], axis=v.ndim - 3)

    def up_y(self, v):
        first = lax.slice_in_dim(v, 0, 1, axis=v.ndim - 3)
        rest = lax.slice_in_dim(v, 1, self.cells, axis=v.ndim - 3)
        lane = iota(first.shape, -1)
        first = jnp.where(lane < COLUMNS - COUNT_Z, roll(first, -COUNT_Z, -1), 0.0)
        return jnp.concatenate([rest, first], axis=v.ndim - 3)

    def low_z(self, v):
        lane, row = iota(v.shape, -1), iota(v.shape, -2)
        edge = roll(roll(v, 1 - self.cells, -2), 1, -1)
        edge = jnp.where((lane % COUNT_Z != 0) & (lane < COLUMNS), edge, 0.0)
        return jnp.where(row == 0, edge, roll(v, 1, -2))

    def up_z(self, v):
        lane, row = iota(v.shape, -1), iota(v.shape, -2)
        edge = roll(roll(v, self.cells - 1, -2), -1, -1)
        edge = jnp.where((lane % COUNT_Z != COUNT_Z - 1) & (lane < COLUMNS), edge, 0.0)
        inner = jnp.where(row < self.cells - 1, roll(v, -1, -2), 0.0)
        return jnp.where(row == self.cells - 1, edge, inner)


def set_up(stack, weight, planes, move):
    stack[1, planes] = stack[1, 0]

    def body(i, carry):
        cell, face_y, face_z = stack[4, i], stack[2, i], stack[3, i]
        total = stack[1, i] + stack[1, i + 1] + face_y + move.up_y(face_y)
        total = total + face_z + move.up_z(face_z)
        stack[5, i] = jnp.where(cell > 0.0, 1.0 / (cell + weight * total), 0.0)
        return carry

    lax.fori_loop(0, planes, body, 0)


def from_zero(stack, iterate, update, planes):
    def body(i, carry):
        step = FIRST[1] * (stack[5, i] * stack[0, i])
        update[i] = step
        iterate[i] = step
        return carry

    lax.fori_loop(0, planes, body, 0)


def stencil_pass(stack, iterate, weight, planes, count, move, use, carry):
    flux = stack[1, 0] * (iterate[0] - iterate[planes - 1])

    def body(i, both):
        flux, carry = both
        v = iterate[i]
        above = stack[1, i + 1] * (iterate[i + 1] - v)
        flux_y = stack[2, i] * (v - move.low_y(v))
        flux_z = stack[3, i] * (v - move.low_z(v))
        total = (flux - above) + (flux_y - move.up_y(flux_y)) + (flux_z - move.up_z(flux_z))
        carry = use(i, v, stack[0, i] - (stack[4, i] * v + weight * total), carry)
        return above, carry

    return lax.fori_loop(0, count, body, (flux, carry))[1]


def sweep(stack, iterate, update, weight, planes, move, factors):
    keep, gain = factors
    iterate[planes] = iterate[0]

    def use(i, v, remainder, carry):
        step = gain * (stack[5, i] * remainder)
        if keep:
            step = keep * update[i] + step
        update[i] = step
        iterate[i] = v + step
        return carry

    stencil_pass(stack, iterate, weight, planes, planes, move, use, 0)


def down(stack, iterate, update, weight, planes, move):
    from_zero(stack, iterate, update, planes)
    for factors in LATER:
        sweep(stack, iterate, update, weight, planes, move, factors)


def up(stack, iterate, update, weight, planes, move):
    for factors in (FIRST,) + LATER:
        sweep(stack, iterate, update, weight, planes, move, factors)


def keep_remainder(stack, iterate, update, weight, planes, count, move):
    iterate[planes] = iterate[0]

    def use(i, v, remainder, carry):
        update[i] = remainder
        return carry

    stencil_pass(stack, iterate, weight, planes, count, move, use, 0)


def coarsen(stack, remainder, rows, pairs, out, count, size):
    half = size // 2

    def body(i, carry):
        for k in range(5):
            if k == 1:
                rows[k] = stack[1, 2 * i]
            elif k == 0:
                rows[k] = remainder[2 * i] + remainder[2 * i + 1]
            else:
                rows[k] = stack[k, 2 * i] + stack[k, 2 * i + 1]
        for k in range(5):
            pair = rows[k, pl.ds(0, half, stride=2), :]
            if k != 2:
                pair = pair + rows[k, pl.ds(1, half, stride=2), :]
            pairs[k, i, 0:half, :] = pair
        return carry

    if half % 8:
        pairs[...] = jnp.zeros(pairs.shape, jnp.float32)
    lax.fori_loop(0, count // 2, body, 0)
    fine, coarse = iota((LANES, LANES), 0), iota((LANES, LANES), 1)
    mean = jnp.where((fine // 2 == coarse) & (fine < size), 1.0, 0.0)
    even = jnp.where((fine == 2 * coarse) & (fine < size), 1.0, 0.0)
    _, planes, padded, _ = pairs.shape
    for k in range(5):
        flat = pairs[k].reshape(planes * padded, LANES)
        scale = 0.125 if k in (0, 4) else 0.25
        made = scale * exact_dot(flat, even if k == 3 else mean)
        out(k, made.reshape(planes, padded, LANES))


def spread(coarse, spare, rows, base, fine, row_map, plane_maps, empty):
    planes, height, _ = spare.shape
    source, target = iota((LANES, LANES), 0), iota((LANES, LANES), 1)
    half = target // 2
    pick = jnp.where(source == jnp.where(target < LANES // 2, half, LANES // 2 + half), 1.0, 0.0)
    wide = exact_dot(coarse[0:planes].reshape(planes * height, LANES), pick)
    spare[...] = wide.reshape(planes, height, LANES)
    rows[...] = jnp.zeros(rows.shape, jnp.float32)
    fine[empty] = rows[...]
    for count, plane_of, target_of in plane_maps:

        def body(i, carry):
            plane = plane_of(i)
            for start, number, first in row_map:
                part = spare[plane, start : start + number, :]
                rows[pl.ds(first, number, stride=2), :] = part
                rows[pl.ds(first + 1, number, stride=2), :] = part
            both = rows[...]
            at = target_of(i)
            fine[at] = base[at] + both
            fine[at + 1] = base[at + 1] + both
            return carry

        lax.fori_loop(0, count, body, 0)


def places():
    gx = lax.axis_index("gx")
    gy = lax.axis_index("gy")
    gz = lax.axis_index("gz_0") * 4 + lax.axis_index("gz_1")
    return gx, gy, gz


def widen(value):
    rows, lanes = value.shape
    if lanes == LANES:
        return value
    return jnp.concatenate([value, jnp.zeros((rows, LANES - lanes), jnp.float32)], axis=1)


def y_pack(parts, size):
    lane = iota((8, LANES), 1)
    tiles = [jnp.zeros((8, LANES), jnp.float32) for _ in range(-(-5 * size // LANES))]
    for k, part in enumerate(parts):
        start = k * size
        moved = roll(part, start % LANES, -1)
        for t in range(len(tiles)):
            a, b = max(start, t * LANES) - t * LANES, min(start + size, (t + 1) * LANES) - t * LANES
            if a < b:
                tiles[t] = jnp.where((lane >= a) & (lane < b), moved, tiles[t])
    return tiles


def y_unpack(tiles, k, size):
    lane = iota((8, LANES), 1)
    start = k * size
    t = start // LANES
    value = tiles[t]
    if start + size > (t + 1) * LANES:
        value = jnp.where(lane >= start - t * LANES, value, tiles[t + 1])
    return roll(value, -start, -1)


def pack(own, beside, size, outs):
    y_even, y_odd, z_even, z_odd, ee, eo, oe, oo = outs
    _, gy, gz = places()
    even_y, even_z = gy % 2 == 0, gz % 2 == 0
    lane = iota((size, LANES), 1)

    def group(g, slots, get):
        top = jnp.zeros((size, LANES), jnp.float32)
        bottom = top
        for s in range(slots):
            high, low = [], []
            for k in range(5):
                v = get(k, s)
                at = 40 * s + 8 * k
                here = (lane >= at) & (lane < at + 8)
                top = jnp.where(here, roll(v, at - (size - 8), -1), top)
                bottom = jnp.where(here, roll(v, at, -1), bottom)
                high.append(v[size - 8 :])
                low.append(v[:8])
            for t, (h, l) in enumerate(zip(y_pack(high, size), y_pack(low, size))):
                y_even[3 * g + s, 8 * t : 8 * t + 8, :] = jnp.where(even_y, h, l)
                y_odd[3 * g + s, 8 * t : 8 * t + 8, :] = jnp.where(even_y, l, h)
        a, b = jnp.where(even_z, top, bottom), jnp.where(even_z, bottom, top)
        z_even[g] = a
        z_odd[g] = b
        ee[g] = jnp.where(even_y, a[size - 8 :], a[:8])
        eo[g] = jnp.where(even_y, b[size - 8 :], b[:8])
        oe[g] = jnp.where(even_y, a[:8], a[size - 8 :])
        oo[g] = jnp.where(even_y, b[:8], b[size - 8 :])

    def body(g, carry):
        group(g, 3, lambda k, s: own(k, 3 * g + s))
        return carry

    lax.fori_loop(0, size // 3, body, 0)
    for q in range(3):
        group(size // 3 + q, min(3, 8 - 3 * q), lambda k, s: beside(k, 3 * q + s))


def unpack(stack, own, beside, size, payloads):
    y_even, y_odd, z_even, z_odd, ee, eo, oe, oo = payloads
    gx, gy, gz = places()
    even_y, even_z = gy % 2 == 0, gz % 2 == 0
    lane, lane_8 = iota((size, LANES), 1), iota((8, LANES), 1)
    tiles = -(-5 * size // LANES)

    def join(lane, middle, low, high, at):
        sides = jnp.where(lane >= LANES - 8, roll(low, LANES - 8 - at, -1), 0.0)
        sides = jnp.where(lane < size + 8, roll(high, size - at, -1), sides)
        return jnp.where(lane < size, middle, sides)

    def group(g, slots, get, first):
        low = jnp.where(even_z, z_odd[g], z_even[g])
        high = jnp.where(even_z, z_even[g], z_odd[g])
        by_even = jnp.where(even_z, eo[g], ee[g]), jnp.where(even_z, ee[g], eo[g])
        by_odd = jnp.where(even_z, oo[g], oe[g]), jnp.where(even_z, oe[g], oo[g])
        corners = (
            [jnp.where(even_y, e, o) for e, o in zip(by_even, by_odd)],
            [jnp.where(even_y, o, e) for e, o in zip(by_even, by_odd)],
        )
        for s in range(slots):
            e, o = y_even[3 * g + s], y_odd[3 * g + s]
            ends = jnp.where(even_y, e, o), jnp.where(even_y, o, e)
            ends = [[end[8 * t : 8 * t + 8] for t in range(tiles)] for end in ends]
            for k in range(5):
                at = 40 * s + 8 * k
                stack[k, first + s, 0:size, :] = join(lane, get(k, s), low, high, at)
                for which in range(2):
                    rows = slice(size + 8 * which, size + 8 * which + 8)
                    middle = y_unpack(ends[which], k, size)
                    stack[k, first + s, rows, :] = join(lane_8, middle, *corners[which], at)

    def body(g, carry):
        group(g, 3, lambda k, s: own(k, 3 * g + s), 3 * g)
        return carry

    lax.fori_loop(0, size // 3, body, 0)
    for q in range(3):
        group(
            size // 3 + q,
            min(3, 8 - 3 * q),
            lambda k, s: beside(k, 3 * q + s),
            size + gx + 3 * q,
        )
    empty = size + 8 * (1 - gx)
    for k in range(5):
        stack[k, empty] = jnp.zeros(stack.shape[2:], jnp.float32)


def payload_shapes(size):
    groups = size // 3 + 3
    tall = 8 * (-(-5 * size // LANES))
    y = near(size + 8, tall, LANES)
    z = near(groups, size, LANES)
    c = near(groups, 8, LANES)
    return [y, y, z, z, c, c, c, c]


def partner(index, parity, count):
    if parity is None:
        return index
    other = index + 1 if index % 2 == parity else index - 1
    return other if 0 <= other < count else None


def swap(value, parity_y, parity_z):
    pairs = []
    for y in range(COUNT_Y):
        for z in range(COUNT_Z):
            to_y, to_z = partner(y, parity_y, COUNT_Y), partner(z, parity_z, COUNT_Z)
            if to_y is not None and to_z is not None:
                pairs.append((y * COUNT_Z + z, to_y * COUNT_Z + to_z))
    return lax.ppermute(value, YZ, pairs)


WAYS = ((0, None), (1, None), (None, 0), (None, 1), (0, 0), (0, 1), (1, 0), (1, 1))


def swap_cores(value):
    return lax.ppermute(value, "gx", [(0, 1), (1, 0)])


def f32(*shape):
    return jax.ShapeDtypeStruct(shape, jnp.float32)


def near(*shape):
    return pltpu.VMEM(shape, jnp.float32)


def call(body, outs, ins, scratch, operands, limit):
    held = [
        pltpu.with_memory_space_constraint(v, pltpu.VMEM) if spec is held_near else v
        for v, spec in zip(operands, ins)
    ]
    return pl.pallas_call(
        body,
        out_shape=outs,
        out_specs=[vmem] * len(outs),
        in_specs=ins,
        scratch_shapes=scratch,
        compiler_params=pltpu.CompilerParams(vmem_limit_bytes=limit * 2**20),
    )(*held)


def edge_kernel(right, faces, cells, out, sems):
    gx = lax.axis_index("gx")
    start = (1 - gx) * (SIZES[0] - WIDTH)
    part = pl.ds(start, WIDTH)
    copies = [
        pltpu.make_async_copy(right.at[part], out.at[0], sems.at[0]),
        pltpu.make_async_copy(faces.at[0, part], out.at[1], sems.at[1]),
        pltpu.make_async_copy(faces.at[1, part], out.at[2], sems.at[2]),
        pltpu.make_async_copy(faces.at[2, part], out.at[3], sems.at[3]),
        pltpu.make_async_copy(cells.at[part], out.at[4], sems.at[4]),
    ]
    for copy in copies:
        copy.start()
    for copy in copies:
        copy.wait()


def own_inputs(right, faces, cells):
    def own(k, i):
        if k == 0:
            return widen(right[i])
        return widen(cells[i] if k == 4 else faces[k - 1, i])

    return own


def pack_0_kernel(right, faces, cells, beside, *outs):
    pack(own_inputs(right, faces, cells), lambda k, j: widen(beside[k, j]), SIZES[0], outs)


def pack_1_kernel(own, beside, *outs):
    pack(lambda k, i: own[k, i], lambda k, j: beside[k, j], SIZES[1], outs)


def level_0_kernel(
    right, faces, cells, beside, ye, yo, ze, zo, ee, eo, oe, oo,
    coarse, coarse_edge, stack, iterate,
    update, rows, pairs,
):
    size = SIZES[0]
    planes = size + 9
    gx = lax.axis_index("gx")
    unpack(
        stack,
        own_inputs(right, faces, cells),
        lambda k, j: widen(beside[k, j]),
        size,
        (ye, yo, ze, zo, ee, eo, oe, oo),
    )
    set_up(stack, 1.0, planes, Wrapped)
    down(stack, iterate, update, 1.0, planes, Wrapped)
    keep_remainder(stack, iterate, update, 1.0, planes, size, Wrapped)

    def out(k, value):
        coarse[k] = value
        coarse_edge[k] = jnp.where(gx == 0, value[16:24], value[0:8])

    coarsen(stack, update, rows, pairs, out, size, size)


def level_1_kernel(
    own, beside, ye, yo, ze, zo, ee, eo, oe, oo,
    coarse, stack, iterate,
    update, rows, pairs, made,
):
    size = SIZES[1]
    planes = size + 9
    gx = lax.axis_index("gx")
    unpack(
        stack,
        lambda k, i: own[k, i],
        lambda k, j: beside[k, j],
        size,
        (ye, yo, ze, zo, ee, eo, oe, oo),
    )
    set_up(stack, 0.25, planes, Wrapped)
    down(stack, iterate, update, 0.25, planes, Wrapped)
    keep_remainder(stack, iterate, update, 0.25, planes, size, Wrapped)

    def out(k, value):
        made[k] = value

    coarsen(stack, update, rows, pairs, out, size, size)
    for i in range(SIZES[2]):
        line = made[0, i]
        for k in range(1, 5):
            line = line + roll(made[k, i], SIZES[2] * k, -1)
        coarse[i] = jnp.where(gx == 0, line, roll(line, LANES // 2, -1))


def level_2_kernel(
    own, ye, yo, ze, zo, ee, eo, oe, oo,
    payload, stack, iterate,
    update, rows, pairs, made, lines,
):
    size = SIZES[2]
    planes = 2 * size + 1
    _, gy, gz = places()
    even_y, even_z = gy % 2 == 0, gz % 2 == 0
    lane = iota((16, LANES), 1)
    bases = (0, size, LANES - size)
    for k in range(5):
        stack[k, 2 * size] = jnp.zeros(stack.shape[2:], jnp.float32)

    def body(i, carry):
        e = ee[i], eo[i]
        o = oe[i], oo[i]
        table = (
            (own[i], jnp.where(even_z, ze[i], zo[i]), jnp.where(even_z, zo[i], ze[i])),
            (
                jnp.where(even_y, ye[i], yo[i]),
                jnp.where(even_y, jnp.where(even_z, e[0], e[1]), jnp.where(even_z, o[0], o[1])),
                jnp.where(even_y, jnp.where(even_z, e[1], e[0]), jnp.where(even_z, o[1], o[0])),
            ),
            (
                jnp.where(even_y, yo[i], ye[i]),
                jnp.where(even_y, jnp.where(even_z, o[0], o[1]), jnp.where(even_z, e[0], e[1])),
                jnp.where(even_y, jnp.where(even_z, o[1], o[0]), jnp.where(even_z, e[1], e[0])),
            ),
        )
        for k in range(5):
            for h in range(2):
                source = (LANES // 2) * h + size * k
                plane = size * h + i
                stack[k, plane, 24:32, :] = jnp.zeros((8, LANES), jnp.float32)
                for a, first in enumerate((0, size, 40 - size)):
                    line = jnp.zeros((16, LANES), jnp.float32)
                    for b, base in enumerate(bases):
                        here = (lane >= base) & (lane < base + size)
                        line = jnp.where(here, roll(table[a][b], base - source, -1), line)
                    stack[k, plane, first : first + size, :] = line[:size]
        return carry

    lax.fori_loop(0, size, body, 0)
    weight = 0.0625
    set_up(stack, weight, planes, Wrapped)
    down(stack, iterate, update, weight, planes, Wrapped)
    keep_remainder(stack, iterate, update, weight, planes, 2 * size, Wrapped)

    def out(k, value):
        made[k * 96 : k * 96 + 96, :] = value.reshape(96, LANES)

    coarsen(stack, update, rows, pairs, out, 2 * size, size)
    line = jnp.zeros((60, LANES), jnp.float32)
    for y in range(6):
        line = line + roll(made[pl.ds(y, 60, stride=8), :], 6 * y, -1)
    lines[0:60, :] = line
    chunk = lines[0:20, :] + roll(lines[20:40, :], 40, -1) + roll(lines[40:60, :], 80, -1)
    chunk = jnp.concatenate([chunk, jnp.zeros((4, LANES), jnp.float32)], axis=0)

    def repeat(c, carry):
        payload[pl.ds(pl.multiple_of(c * CHUNK, 8), CHUNK), :] = chunk
        return carry

    lax.fori_loop(0, COLUMNS, repeat, 0)


def compact(value):
    row = iota(value.shape, -2)
    out = jnp.where(row == 0, value, 0.0)
    out = jnp.where(row == 1, roll(value, -1, -2), out)
    return jnp.where(row == 2, roll(value, -2, -2), out)


def bottom(source, faces, cells):
    weight = 0.25**4
    move = Columns(3)
    face_x, face_y, face_z = faces
    nothing = jnp.zeros((1,) + source.shape[1:], jnp.float32)

    def apply(v):
        flux_x = face_x * (v - jnp.concatenate([nothing, v[:-1]], axis=0))
        flux_y = face_y * (v - move.low_y(v))
        flux_z = face_z * (v - move.low_z(v))
        total = flux_x - jnp.concatenate([flux_x[1:], nothing], axis=0)
        total = total + (flux_y - move.up_y(flux_y)) + (flux_z - move.up_z(flux_z))
        return cells * v + weight * total

    def total_of(v):
        flat = jnp.sum(jnp.sum(v, axis=0), axis=0)
        one = jnp.sum(jnp.sum(flat, axis=0, keepdims=True), axis=1, keepdims=True)
        return jnp.broadcast_to(one, flat.shape)

    iterate = jnp.zeros_like(source)
    remainder = source
    search = source
    norm_now = total_of(remainder * remainder)
    for step in range(BOTTOM):
        applied = apply(search)
        size = norm_now / total_of(search * applied)
        iterate = iterate + size * search
        if step + 1 < BOTTOM:
            remainder = remainder - size * applied
            norm_next = total_of(remainder * remainder)
            search = remainder + (norm_next / norm_now) * search
            norm_now = norm_next
    return iterate


def rise_kernel(
    gathered, stack_2, base_2, stack_1, base_1, stack_0, base_0,
    solution_out, residual_out, sums,
    iterate_0, update_0, rows_0, spare_1,
    iterate_1, update_1, rows_1, spare_2,
    iterate_2, update_2, rows_2, spare_3,
    stack_3, iterate_3, update_3, turned, table, block_3,
):
    gx, gy, gz = places()

    stack_3[...] = jnp.zeros(stack_3.shape, jnp.float32)
    blank = jnp.zeros((LANES - COLUMNS, LANES), jnp.float32)
    for r in range(20):
        part = gathered[pl.ds(r, COLUMNS, stride=CHUNK), :]
        turned[...] = jnp.transpose(jnp.concatenate([part, blank], axis=0))
        for j in range(3):
            k, x = divmod(20 * j + r, 12)
            for y in range(6):
                stack_3[k, x, y, 0:6, :] = turned[40 * j + 6 * y : 40 * j + 6 * y + 6, :]
    move = Columns(6)
    weight = 0.25**3
    set_up(stack_3, weight, 13, move)
    down(stack_3, iterate_3, update_3, weight, 13, move)
    keep_remainder(stack_3, iterate_3, update_3, weight, 13, 12, move)

    def coarse(k, x_pair, y_pair, z_pair, scale):
        planes = []
        for x in range(6):
            read = (lambda i: update_3[i]) if k == 0 else (lambda i: stack_3[k, i])
            v = read(2 * x)
            if x_pair:
                v = v + read(2 * x + 1)
            lines = []
            for y in range(3):
                line = v[2 * y]
                if y_pair:
                    line = line + v[2 * y + 1]
                if z_pair:
                    line = line + roll(line, -1, -2)
                lines.append(scale * compact(line))
            planes.append(jnp.stack(lines))
        return jnp.stack(planes)

    lowest = bottom(
        coarse(0, True, True, True, 0.125),
        (
            coarse(1, False, True, True, 0.25),
            coarse(2, True, False, True, 0.25),
            coarse(3, True, True, False, 0.25),
        ),
        coarse(4, True, True, True, 0.125),
    )
    row = iota((8, LANES), 0)
    for x in range(6):
        for y in range(3):
            line = lowest[x, y]
            wide = jnp.where(row == 0, line, 0.0)
            for to in range(1, 6):
                wide = jnp.where(row == to, roll(line, to - to // 2, -2), wide)
            for a in range(2):
                for b in range(2):
                    iterate_3[2 * x + a, 2 * y + b] = iterate_3[2 * x + a, 2 * y + b] + wide
    up(stack_3, iterate_3, update_3, weight, 13, move)

    low_rows = jnp.zeros((32, LANES), jnp.float32)
    for q in range(6):
        two = [iterate_3[2 * q + h].reshape(48, LANES) for h in range(2)]
        table[q] = jnp.transpose(jnp.concatenate(two + [low_rows], axis=0))
    block_3[...] = jnp.zeros(block_3.shape, jnp.float32)
    lane = iota((8, LANES), 1)

    def place(q, carry):
        for a, first in ((0, 0), (1, 6), (-1, 18)):
            lines = [jnp.zeros((8, LANES), jnp.float32) for _ in range(2)]
            for b, base in ((0, 0), (1, 6), (-1, LANES - 6)):
                y, z = gy + a, gz + b
                inside = (y >= 0) & (y < COUNT_Y) & (z >= 0) & (z < COUNT_Z)
                at = jnp.where(inside, y * COUNT_Z + z, 0)
                here = (lane >= base) & (lane < base + 6) & inside
                found = jnp.broadcast_to(table[q, pl.ds(at, 1), :], (8, LANES))
                for h in range(2):
                    for y_in in range(6):
                        moved = roll(found, base - 48 * h - 8 * y_in, -1)
                        lines[h] = jnp.where(here & (row == y_in), moved, lines[h])
            for h in range(2):
                block_3[2 * q + h, first : first + 6, :] = lines[h][0:6]
        return carry

    lax.fori_loop(0, 6, place, 0)

    spread(
        block_3, spare_3, rows_2, base_2, iterate_2,
        ((0, 12, 0), (18, 6, 28)),
        ((12, lambda i: i, lambda i: 2 * i),),
        24,
    )
    up(stack_2, iterate_2, update_2, 0.0625, 25, Wrapped)

    size = SIZES[1]
    spread(
        iterate_2, spare_2, rows_1, base_1, iterate_1,
        ((0, 16, 0), (36, 4, 32)),
        (
            (12, lambda i: 12 * gx + i, lambda i: 2 * i),
            (4, lambda i: 12 - 4 * gx + i, lambda i: size + gx + 2 * i),
        ),
        size + 8 * (1 - gx),
    )
    up(stack_1, iterate_1, update_1, 0.25, size + 9, Wrapped)

    size = SIZES[0]
    spread(
        iterate_1, spare_1, rows_0, base_0, iterate_0,
        ((0, 28, 0), (36, 4, 56)),
        (
            (24, lambda i: i, lambda i: 2 * i),
            (4, lambda i: 24 + 5 * gx + i, lambda i: size + gx + 2 * i),
        ),
        size + 8 * (1 - gx),
    )
    planes = size + 9
    up(stack_0, iterate_0, update_0, 1.0, planes, Wrapped)
    iterate_0[planes] = iterate_0[0]
    mask = iota((size, LANES), 1) < size

    def use(i, v, remainder, carry):
        solution_out[i] = v[0:size, 0:size]
        residual_out[i] = remainder[0:size, 0:size]
        mine = jnp.where(mask, remainder[0:size], 0.0)
        given = jnp.where(mask, stack_0[0, i, 0:size, :], 0.0)
        return carry[0] + mine * mine, carry[1] + given * given

    zero = jnp.zeros((size, LANES), jnp.float32)
    squares = stencil_pass(stack_0, iterate_0, 1.0, planes, size, Wrapped, use, (zero, zero))
    ones = []
    for square in squares:
        one = jnp.sum(jnp.sum(square, axis=0, keepdims=True), axis=1, keepdims=True)
        ones.append(jnp.broadcast_to(one, (8, LANES)))
    sums[...] = jnp.where(lane == 0, ones[0], jnp.where(lane == 1, ones[1], 0.0))


def shards(right, faces, cells):
    dma = pltpu.SemaphoreType.DMA
    edge = call(edge_kernel, [near(5, WIDTH, 48, 48)], [held_near] * 3, [dma((5,))],
        (right, faces, cells), 2)[0]
    beside = swap_cores(edge)
    outs = call(pack_0_kernel, payload_shapes(48), [held_near] * 4, [],
        (right, faces, cells, beside), 6)
    moved = [swap(v, *way) for v, way in zip(outs, WAYS)]
    coarse, coarse_edge, stack_0, iterate_0 = call(
        level_0_kernel,
        [near(5, 24, 24, LANES), near(5, WIDTH, 24, LANES), near(6, 58, 64, LANES), near(58, 64, LANES)],
        [held_near] * 12,
        [near(58, 64, LANES), near(5, 64, LANES), near(5, 24, 24, LANES)],
        (right, faces, cells, beside, *moved),
        12,
    )
    beside = swap_cores(coarse_edge)
    outs = call(pack_1_kernel, payload_shapes(24), [held_near] * 2, [], (coarse, beside), 8)
    moved = [swap(v, *way) for v, way in zip(outs, WAYS)]
    coarse, stack_1, iterate_1 = call(
        level_1_kernel,
        [near(12, 16, LANES), near(6, 34, 40, LANES), near(34, 40, LANES)],
        [held_near] * 10,
        [near(34, 40, LANES), near(5, 40, LANES), near(5, 12, 16, LANES), near(5, 12, 16, LANES)],
        (coarse, beside, *moved),
        12,
    )
    coarse = coarse + swap_cores(coarse)
    moved = [swap(coarse, *way) for way in WAYS]
    payload, stack_2, iterate_2 = call(
        level_2_kernel,
        [near(COLUMNS * CHUNK, LANES), near(6, 26, 40, LANES), near(26, 40, LANES)],
        [held_near] * 9,
        [near(26, 40, LANES), near(5, 40, LANES), near(5, 12, 8, LANES), near(480, LANES), near(64, LANES)],
        (coarse, *moved),
        12,
    )
    payload = payload.reshape(COLUMNS, CHUNK, LANES)
    gathered = lax.all_to_all(payload, YZ, 0, 0).reshape(COLUMNS * CHUNK, LANES)
    solved, residual, sums = call(
        rise_kernel,
        [f32(48, 48, 48), f32(48, 48, 48), f32(8, LANES)],
        [held_near] * 7,
        [
            near(58, 64, LANES), near(58, 64, LANES), near(64, LANES), near(33, 40, LANES),
            near(34, 40, LANES), near(34, 40, LANES), near(40, LANES), near(24, 40, LANES),
            near(26, 40, LANES), near(26, 40, LANES), near(40, LANES), near(12, 24, LANES),
            near(6, 14, 6, 8, LANES), near(14, 6, 8, LANES), near(14, 6, 8, LANES),
            near(LANES, LANES), near(6, LANES, LANES), near(12, 24, LANES),
        ],
        (gathered, stack_2, iterate_2, stack_1, iterate_1, stack_0, iterate_0),
        24,
    )
    each = jnp.broadcast_to(sums[0:1].reshape(1, 1, LANES), (128, 1, LANES))
    total = jnp.sum(lax.all_to_all(each, ALL, 0, 0), axis=(0, 1))
    return solved, residual, jnp.sqrt(total[0] / total[1])


def solution(mesh):
    torus = Mesh(
        mesh.devices.reshape(mesh.shape["gx"], mesh.shape["gy"], 4, 4), ("gx", "gy", "gz_0", "gz_1")
    )
    in_specs = (P("gx", "gy", GZ), P(None, "gx", "gy", GZ), P("gx", "gy", GZ))
    out_specs = (P("gx", "gy", GZ), P("gx", "gy", GZ), P())
    return jax.shard_map(
        shards, mesh=torus, in_specs=in_specs, out_specs=out_specs, check_vma=False
    )
```

```python
import functools

import jax
import jax.numpy as jnp
from jax import lax
from jax.experimental import pallas as pl
from jax.experimental.pallas import tpu as pltpu
from jax.sharding import Mesh
from jax.sharding import PartitionSpec as P

BOTTOM = 6
ALL = ("gx", "gy", "gz_0", "gz_1")
YZ = ("gy", "gz_0", "gz_1")
GZ = ("gz_0", "gz_1")
LANES = 128
WIDTH = 8
COUNT_Y = 4
COUNT_Z = 16
COLUMNS = COUNT_Y * COUNT_Z
SIZES = (48, 24, 12, 6)
CHUNK = 24
GROUP = 3

theta = 1.125
delta = 0.875
sigma = theta / delta
rho_0 = 1.0 / sigma
rho_1 = 1.0 / (2.0 * sigma - rho_0)
rho_2 = 1.0 / (2.0 * sigma - rho_1)
FIRST = (0.0, 1.0 / theta)
LATER = ((rho_1 * rho_0, 2.0 * rho_1 / delta), (rho_2 * rho_1, 2.0 * rho_2 / delta))

vmem = pl.BlockSpec(memory_space=pltpu.VMEM)
held_near = pl.BlockSpec(memory_space=pltpu.VMEM)
anywhere = pl.BlockSpec(memory_space=pl.ANY)


def roll(value, by, axis):
    axis = axis % value.ndim
    by = by % value.shape[axis]
    return pltpu.roll(value, by, axis) if by else value


def iota(shape, dim):
    return lax.broadcasted_iota(jnp.int32, shape, dim % len(shape))


def exact_dot(left, right):
    return jnp.dot(
        left, right, precision=lax.Precision.HIGHEST, preferred_element_type=jnp.float32
    )


class Wrapped:
    @staticmethod
    def low_y(v):
        return roll(v, 1, -2)

    @staticmethod
    def up_y(v):
        return roll(v, -1, -2)

    @staticmethod
    def low_z(v):
        return roll(v, 1, -1)

    @staticmethod
    def up_z(v):
        return roll(v, -1, -1)


class Columns:
    def __init__(self, cells):
        self.cells = cells

    def low_y(self, v):
        lane = iota(v.shape, -1)
        last = lax.slice_in_dim(v, self.cells - 1, self.cells, axis=v.ndim - 3)
        rest = lax.slice_in_dim(v, 0, self.cells - 1, axis=v.ndim - 3)
        lane = iota(last.shape, -1)
        last = jnp.where((lane >= COUNT_Z) & (lane < COLUMNS), roll(last, COUNT_Z, -1), 0.0)
        return jnp.concatenate([last, rest], axis=v.ndim - 3)

    def up_y(self, v):
        first = lax.slice_in_dim(v, 0, 1, axis=v.ndim - 3)
        rest = lax.slice_in_dim(v, 1, self.cells, axis=v.ndim - 3)
        lane = iota(first.shape, -1)
        first = jnp.where(lane < COLUMNS - COUNT_Z, roll(first, -COUNT_Z, -1), 0.0)
        return jnp.concatenate([rest, first], axis=v.ndim - 3)

    def low_z(self, v):
        lane, row = iota(v.shape, -1), iota(v.shape, -2)
        edge = roll(roll(v, 1 - self.cells, -2), 1, -1)
        edge = jnp.where((lane % COUNT_Z != 0) & (lane < COLUMNS), edge, 0.0)
        return jnp.where(row == 0, edge, roll(v, 1, -2))

    def up_z(self, v):
        lane, row = iota(v.shape, -1), iota(v.shape, -2)
        edge = roll(roll(v, self.cells - 1, -2), -1, -1)
        edge = jnp.where((lane % COUNT_Z != COUNT_Z - 1) & (lane < COLUMNS), edge, 0.0)
        inner = jnp.where(row < self.cells - 1, roll(v, -1, -2), 0.0)
        return jnp.where(row == self.cells - 1, edge, inner)


def set_up(stack, weight, planes, count, move, start=None):
    stack[1, planes] = stack[1, 0]

    def moved(i):
        return [move.up_z(stack[3, i + u]) for u in range(GROUP)]

    def body(g, above_z):
        i = GROUP * g
        later = moved(jnp.minimum(i + GROUP, count - GROUP))
        for u in range(GROUP):
            at = i + u
            cell, face_y = stack[4, at], stack[2, at]
            above_y = move.up_y(face_y)
            if stack.shape[0] > 7:
                stack[7, at] = above_y
            stack[6, at] = above_z[u]
            total = stack[1, at] + stack[1, at + 1] + face_y + above_y
            total = total + stack[3, at] + above_z[u]
            inverse = jnp.where(cell > 0.0, 1.0 / (cell + weight * total), 0.0)
            stack[5, at] = inverse
            if start is not None:
                step = FIRST[1] * (inverse * stack[0, at])
                for ref in start:
                    ref[at] = step
        return later

    lax.fori_loop(0, count // GROUP, body, moved(0))


def stencil_pass(stack, iterate, weight, planes, count, move, use, carry):
    flux = stack[1, 0] * (iterate[0] - iterate[planes - 1])
    by_face = stack.shape[0] > 7

    def moved(i):
        out = []
        for u in range(GROUP):
            v = iterate[i + u]
            out += [move.low_z(v), move.up_z(v)]
            if by_face:
                out += [move.low_y(v), move.up_y(v)]
        return out

    def body(g, state):
        flux, near_by, carry = state
        i = GROUP * g
        later = moved(jnp.minimum(i + GROUP, count - GROUP))
        values = [iterate[i + u] for u in range(GROUP + 1)]
        each = len(near_by) // GROUP
        for u in range(GROUP):
            at, v = i + u, values[u]
            sides = near_by[each * u : each * u + each]
            above = stack[1, at + 1] * (values[u + 1] - v)
            total = flux - above
            flux = above
            if by_face:
                total = total + stack[2, at] * (v - sides[2]) + stack[7, at] * (v - sides[3])
            else:
                flux_y = stack[2, at] * (v - move.low_y(v))
                total = total + (flux_y - move.up_y(flux_y))
            total = total + stack[3, at] * (v - sides[0]) + stack[6, at] * (v - sides[1])
            carry = use(at, v, stack[0, at] - (stack[4, at] * v + weight * total), carry)
        return flux, later, carry

    return lax.fori_loop(0, count // GROUP, body, (flux, moved(0), carry))[2]


def sweep(stack, iterate, update, weight, planes, count, move, factors):
    keep, gain = factors
    iterate[planes] = iterate[0]

    def use(i, v, remainder, carry):
        step = gain * (stack[5, i] * remainder)
        if keep:
            step = keep * update[i] + step
        update[i] = step
        iterate[i] = v + step
        return carry

    stencil_pass(stack, iterate, weight, planes, count, move, use, 0)


def down(stack, iterate, update, weight, planes, count, move):
    set_up(stack, weight, planes, count, move, (iterate, update))
    for factors in LATER:
        sweep(stack, iterate, update, weight, planes, count, move, factors)


def up(stack, iterate, update, weight, planes, count, move):
    for factors in (FIRST,) + LATER:
        sweep(stack, iterate, update, weight, planes, count, move, factors)


def keep_remainder(stack, iterate, update, weight, planes, count, move):
    iterate[planes] = iterate[0]

    def use(i, v, remainder, carry):
        update[i] = remainder
        return carry

    stencil_pass(stack, iterate, weight, planes, count, move, use, 0)


def coarsen(stack, remainder, rows, pairs, out, count, size):
    half = size // 2

    def body(i, carry):
        for k in range(5):
            if k == 1:
                rows[k] = stack[1, 2 * i]
            elif k == 0:
                rows[k] = remainder[2 * i] + remainder[2 * i + 1]
            else:
                rows[k] = stack[k, 2 * i] + stack[k, 2 * i + 1]
        for k in range(5):
            pair = rows[k, pl.ds(0, half, stride=2), :]
            if k != 2:
                pair = pair + rows[k, pl.ds(1, half, stride=2), :]
            pairs[k, i, 0:half, :] = pair
        return carry

    if half % 8:
        pairs[...] = jnp.zeros(pairs.shape, jnp.float32)
    lax.fori_loop(0, count // 2, body, 0)
    fine, coarse = iota((LANES, LANES), 0), iota((LANES, LANES), 1)
    mean = jnp.where((fine // 2 == coarse) & (fine < size), 1.0, 0.0)
    even = jnp.where((fine == 2 * coarse) & (fine < size), 1.0, 0.0)
    _, planes, padded, _ = pairs.shape
    for k in range(5):
        flat = pairs[k].reshape(planes * padded, LANES)
        scale = 0.125 if k in (0, 4) else 0.25
        made = scale * exact_dot(flat, even if k == 3 else mean)
        out(k, made.reshape(planes, padded, LANES))


def spread(coarse, spare, rows, base, fine, row_map, plane_maps, empty):
    planes, height, _ = spare.shape
    source, target = iota((LANES, LANES), 0), iota((LANES, LANES), 1)
    half = target // 2
    pick = jnp.where(source == jnp.where(target < LANES // 2, half, LANES // 2 + half), 1.0, 0.0)
    wide = exact_dot(coarse[0:planes].reshape(planes * height, LANES), pick)
    spare[...] = wide.reshape(planes, height, LANES)
    rows[...] = jnp.zeros(rows.shape, jnp.float32)
    fine[empty] = rows[...]
    for count, plane_of, target_of in plane_maps:

        def body(i, carry):
            plane = plane_of(i)
            for start, number, first in row_map:
                part = spare[plane, start : start + number, :]
                rows[pl.ds(first, number, stride=2), :] = part
                rows[pl.ds(first + 1, number, stride=2), :] = part
            both = rows[...]
            at = target_of(i)
            fine[at] = base[at] + both
            fine[at + 1] = base[at + 1] + both
            return carry

        lax.fori_loop(0, count, body, 0)


def places():
    gx = lax.axis_index("gx")
    gy = lax.axis_index("gy")
    gz = lax.axis_index("gz_0") * 4 + lax.axis_index("gz_1")
    return gx, gy, gz


def widen(value):
    rows, lanes = value.shape
    if lanes == LANES:
        return value
    return jnp.concatenate([value, jnp.zeros((rows, LANES - lanes), jnp.float32)], axis=1)


def y_pack(parts, size):
    lane = iota((8, LANES), 1)
    tiles = [jnp.zeros((8, LANES), jnp.float32) for _ in range(-(-5 * size // LANES))]
    for k, part in enumerate(parts):
        start = k * size
        moved = roll(part, start % LANES, -1)
        for t in range(len(tiles)):
            a, b = max(start, t * LANES) - t * LANES, min(start + size, (t + 1) * LANES) - t * LANES
            if a < b:
                tiles[t] = jnp.where((lane >= a) & (lane < b), moved, tiles[t])
    return tiles


def y_unpack(tiles, k, size):
    lane = iota((8, LANES), 1)
    start = k * size
    t = start // LANES
    value = tiles[t]
    if start + size > (t + 1) * LANES:
        value = jnp.where(lane >= start - t * LANES, value, tiles[t + 1])
    return roll(value, -start, -1)


def pack(own, beside, size, outs):
    y_even, y_odd, z_even, z_odd, ee, eo, oe, oo = outs
    _, gy, gz = places()
    even_y, even_z = gy % 2 == 0, gz % 2 == 0
    lane = iota((size, LANES), 1)

    def group(g, slots, get):
        top = jnp.zeros((size, LANES), jnp.float32)
        bottom = top
        for s in range(slots):
            high, low = [], []
            for k in range(5):
                v = get(k, s)
                at = 40 * s + 8 * k
                here = (lane >= at) & (lane < at + 8)
                top = jnp.where(here, roll(v, at - (size - 8), -1), top)
                bottom = jnp.where(here, roll(v, at, -1), bottom)
                high.append(v[size - 8 :])
                low.append(v[:8])
            for t, (h, l) in enumerate(zip(y_pack(high, size), y_pack(low, size))):
                y_even[3 * g + s, 8 * t : 8 * t + 8, :] = jnp.where(even_y, h, l)
                y_odd[3 * g + s, 8 * t : 8 * t + 8, :] = jnp.where(even_y, l, h)
        a, b = jnp.where(even_z, top, bottom), jnp.where(even_z, bottom, top)
        z_even[g] = a
        z_odd[g] = b
        ee[g] = jnp.where(even_y, a[size - 8 :], a[:8])
        eo[g] = jnp.where(even_y, b[size - 8 :], b[:8])
        oe[g] = jnp.where(even_y, a[:8], a[size - 8 :])
        oo[g] = jnp.where(even_y, b[:8], b[size - 8 :])

    def body(g, carry):
        group(g, 3, lambda k, s: own(k, 3 * g + s))
        return carry

    lax.fori_loop(0, size // 3, body, 0)
    for q in range(3):
        group(size // 3 + q, min(3, 8 - 3 * q), lambda k, s: beside(k, 3 * q + s))


def unpack(stack, own, beside, size, payloads):
    y_even, y_odd, z_even, z_odd, ee, eo, oe, oo = payloads
    gx, gy, gz = places()
    even_y, even_z = gy % 2 == 0, gz % 2 == 0
    lane, lane_8 = iota((size, LANES), 1), iota((8, LANES), 1)
    tiles = -(-5 * size // LANES)

    def join(lane, middle, low, high, at):
        sides = jnp.where(lane >= LANES - 8, roll(low, LANES - 8 - at, -1), 0.0)
        sides = jnp.where(lane < size + 8, roll(high, size - at, -1), sides)
        return jnp.where(lane < size, middle, sides)

    def group(g, slots, get, first):
        low = jnp.where(even_z, z_odd[g], z_even[g])
        high = jnp.where(even_z, z_even[g], z_odd[g])
        by_even = jnp.where(even_z, eo[g], ee[g]), jnp.where(even_z, ee[g], eo[g])
        by_odd = jnp.where(even_z, oo[g], oe[g]), jnp.where(even_z, oe[g], oo[g])
        corners = (
            [jnp.where(even_y, e, o) for e, o in zip(by_even, by_odd)],
            [jnp.where(even_y, o, e) for e, o in zip(by_even, by_odd)],
        )
        for s in range(slots):
            e, o = y_even[3 * g + s], y_odd[3 * g + s]
            ends = jnp.where(even_y, e, o), jnp.where(even_y, o, e)
            ends = [[end[8 * t : 8 * t + 8] for t in range(tiles)] for end in ends]
            for k in range(5):
                at = 40 * s + 8 * k
                stack[k, first + s, 0:size, :] = join(lane, get(k, s), low, high, at)
                for which in range(2):
                    rows = slice(size + 8 * which, size + 8 * which + 8)
                    middle = y_unpack(ends[which], k, size)
                    stack[k, first + s, rows, :] = join(lane_8, middle, *corners[which], at)

    def body(g, carry):
        group(g, 3, lambda k, s: own(k, 3 * g + s), 3 * g)
        return carry

    lax.fori_loop(0, size // 3, body, 0)
    for q in range(3):
        group(
            size // 3 + q,
            min(3, 8 - 3 * q),
            lambda k, s: beside(k, 3 * q + s),
            size + gx + 3 * q,
        )
    empty = size + 8 * (1 - gx)
    for k in range(5):
        stack[k, empty] = jnp.zeros(stack.shape[2:], jnp.float32)


def payload_shapes(size):
    groups = size // 3 + 3
    tall = 8 * (-(-5 * size // LANES))
    y = near(size + 8, tall, LANES)
    z = near(groups, size, LANES)
    c = near(groups, 8, LANES)
    return [y, y, z, z, c, c, c, c]


def partner(index, parity, count):
    if parity is None:
        return index
    other = index + 1 if index % 2 == parity else index - 1
    return other if 0 <= other < count else None


def swap(value, parity_y, parity_z):
    pairs = []
    for y in range(COUNT_Y):
        for z in range(COUNT_Z):
            to_y, to_z = partner(y, parity_y, COUNT_Y), partner(z, parity_z, COUNT_Z)
            if to_y is not None and to_z is not None:
                pairs.append((y * COUNT_Z + z, to_y * COUNT_Z + to_z))
    return lax.ppermute(value, YZ, pairs)


WAYS = ((0, None), (1, None), (None, 0), (None, 1), (0, 0), (0, 1), (1, 0), (1, 1))


def swap_cores(value):
    return lax.ppermute(value, "gx", [(0, 1), (1, 0)])


def f32(*shape):
    return jax.ShapeDtypeStruct(shape, jnp.float32)


def near(*shape):
    return pltpu.VMEM(shape, jnp.float32)


def call(body, outs, ins, scratch, operands, limit):
    held = [
        pltpu.with_memory_space_constraint(v, pltpu.VMEM) if spec is held_near else v
        for v, spec in zip(operands, ins)
    ]
    return pl.pallas_call(
        body,
        out_shape=outs,
        out_specs=[vmem] * len(outs),
        in_specs=ins,
        scratch_shapes=scratch,
        compiler_params=pltpu.CompilerParams(vmem_limit_bytes=limit * 2**20),
    )(*held)


def edge_kernel(right, faces, cells, out, sems):
    gx = lax.axis_index("gx")
    start = (1 - gx) * (SIZES[0] - WIDTH)
    part = pl.ds(start, WIDTH)
    copies = [
        pltpu.make_async_copy(right.at[part], out.at[0], sems.at[0]),
        pltpu.make_async_copy(faces.at[0, part], out.at[1], sems.at[1]),
        pltpu.make_async_copy(faces.at[1, part], out.at[2], sems.at[2]),
        pltpu.make_async_copy(faces.at[2, part], out.at[3], sems.at[3]),
        pltpu.make_async_copy(cells.at[part], out.at[4], sems.at[4]),
    ]
    for copy in copies:
        copy.start()
    for copy in copies:
        copy.wait()


def own_inputs(right, faces, cells):
    def own(k, i):
        if k == 0:
            return widen(right[i])
        return widen(cells[i] if k == 4 else faces[k - 1, i])

    return own


def pack_0_kernel(right, faces, cells, beside, *outs):
    pack(own_inputs(right, faces, cells), lambda k, j: widen(beside[k, j]), SIZES[0], outs)


def pack_1_kernel(own, beside, *outs):
    pack(lambda k, i: own[k, i], lambda k, j: beside[k, j], SIZES[1], outs)


def level_0_kernel(
    right, faces, cells, beside, ye, yo, ze, zo, ee, eo, oe, oo,
    coarse, coarse_edge, stack, iterate,
    update, rows, pairs,
):
    size = SIZES[0]
    planes = size + 9
    gx = lax.axis_index("gx")
    unpack(
        stack,
        own_inputs(right, faces, cells),
        lambda k, j: widen(beside[k, j]),
        size,
        (ye, yo, ze, zo, ee, eo, oe, oo),
    )
    down(stack, iterate, update, 1.0, planes, planes, Wrapped)
    keep_remainder(stack, iterate, update, 1.0, planes, size, Wrapped)

    def out(k, value):
        coarse[k] = value
        coarse_edge[k] = jnp.where(gx == 0, value[16:24], value[0:8])

    coarsen(stack, update, rows, pairs, out, size, size)


def level_1_kernel(
    own, beside, ye, yo, ze, zo, ee, eo, oe, oo,
    coarse, stack, iterate,
    update, rows, pairs, made,
):
    size = SIZES[1]
    planes = size + 9
    gx = lax.axis_index("gx")
    unpack(
        stack,
        lambda k, i: own[k, i],
        lambda k, j: beside[k, j],
        size,
        (ye, yo, ze, zo, ee, eo, oe, oo),
    )
    down(stack, iterate, update, 0.25, planes, planes, Wrapped)
    keep_remainder(stack, iterate, update, 0.25, planes, size, Wrapped)

    def out(k, value):
        made[k] = value

    coarsen(stack, update, rows, pairs, out, size, size)
    for i in range(SIZES[2]):
        line = made[0, i]
        for k in range(1, 5):
            line = line + roll(made[k, i], SIZES[2] * k, -1)
        coarse[i] = jnp.where(gx == 0, line, roll(line, LANES // 2, -1))


def level_2_kernel(
    own, ye, yo, ze, zo, ee, eo, oe, oo,
    payload, stack, iterate,
    update, rows, pairs, made, lines,
):
    size = SIZES[2]
    planes = 2 * size + 1
    _, gy, gz = places()
    even_y, even_z = gy % 2 == 0, gz % 2 == 0
    lane = iota((16, LANES), 1)
    bases = (0, size, LANES - size)
    for k in range(5):
        stack[k, 2 * size] = jnp.zeros(stack.shape[2:], jnp.float32)

    def body(i, carry):
        e = ee[i], eo[i]
        o = oe[i], oo[i]
        table = (
            (own[i], jnp.where(even_z, ze[i], zo[i]), jnp.where(even_z, zo[i], ze[i])),
            (
                jnp.where(even_y, ye[i], yo[i]),
                jnp.where(even_y, jnp.where(even_z, e[0], e[1]), jnp.where(even_z, o[0], o[1])),
                jnp.where(even_y, jnp.where(even_z, e[1], e[0]), jnp.where(even_z, o[1], o[0])),
            ),
            (
                jnp.where(even_y, yo[i], ye[i]),
                jnp.where(even_y, jnp.where(even_z, o[0], o[1]), jnp.where(even_z, e[0], e[1])),
                jnp.where(even_y, jnp.where(even_z, o[1], o[0]), jnp.where(even_z, e[1], e[0])),
            ),
        )
        for k in range(5):
            for h in range(2):
                source = (LANES // 2) * h + size * k
                plane = size * h + i
                stack[k, plane, 24:32, :] = jnp.zeros((8, LANES), jnp.float32)
                for a, first in enumerate((0, size, 40 - size)):
                    line = jnp.zeros((16, LANES), jnp.float32)
                    for b, base in enumerate(bases):
                        here = (lane >= base) & (lane < base + size)
                        line = jnp.where(here, roll(table[a][b], base - source, -1), line)
                    stack[k, plane, first : first + size, :] = line[:size]
        return carry

    lax.fori_loop(0, size, body, 0)
    weight = 0.0625
    iterate[2 * size] = jnp.zeros(iterate.shape[1:], jnp.float32)
    down(stack, iterate, update, weight, planes, 2 * size, Wrapped)
    keep_remainder(stack, iterate, update, weight, planes, 2 * size, Wrapped)

    def out(k, value):
        made[k * 96 : k * 96 + 96, :] = value.reshape(96, LANES)

    coarsen(stack, update, rows, pairs, out, 2 * size, size)
    line = jnp.zeros((60, LANES), jnp.float32)
    for y in range(6):
        line = line + roll(made[pl.ds(y, 60, stride=8), :], 6 * y, -1)
    lines[0:60, :] = line
    chunk = lines[0:20, :] + roll(lines[20:40, :], 40, -1) + roll(lines[40:60, :], 80, -1)
    chunk = jnp.concatenate([chunk, jnp.zeros((4, LANES), jnp.float32)], axis=0)

    def repeat(c, carry):
        payload[pl.ds(pl.multiple_of(c * CHUNK, 8), CHUNK), :] = chunk
        return carry

    lax.fori_loop(0, COLUMNS, repeat, 0)


def compact(value):
    row = iota(value.shape, -2)
    out = jnp.where(row == 0, value, 0.0)
    out = jnp.where(row == 1, roll(value, -1, -2), out)
    return jnp.where(row == 2, roll(value, -2, -2), out)


def bottom(source, faces, cells):
    weight = 0.25**4
    move = Columns(3)
    face_x, face_y, face_z = faces
    nothing = jnp.zeros((1,) + source.shape[1:], jnp.float32)

    def apply(v):
        flux_x = face_x * (v - jnp.concatenate([nothing, v[:-1]], axis=0))
        flux_y = face_y * (v - move.low_y(v))
        flux_z = face_z * (v - move.low_z(v))
        total = flux_x - jnp.concatenate([flux_x[1:], nothing], axis=0)
        total = total + (flux_y - move.up_y(flux_y)) + (flux_z - move.up_z(flux_z))
        return cells * v + weight * total

    def total_of(v):
        flat = jnp.sum(jnp.sum(v, axis=0), axis=0)
        one = jnp.sum(jnp.sum(flat, axis=0, keepdims=True), axis=1, keepdims=True)
        return jnp.broadcast_to(one, flat.shape)

    iterate = jnp.zeros_like(source)
    remainder = source
    search = source
    norm_now = total_of(remainder * remainder)
    for step in range(BOTTOM):
        applied = apply(search)
        size = norm_now / total_of(search * applied)
        iterate = iterate + size * search
        if step + 1 < BOTTOM:
            remainder = remainder - size * applied
            norm_next = total_of(remainder * remainder)
            search = remainder + (norm_next / norm_now) * search
            norm_now = norm_next
    return iterate


def rise_kernel(
    gathered, stack_2, base_2, stack_1, base_1, stack_0, base_0,
    solution_out, residual_out, sums,
    iterate_0, update_0, rows_0, spare_1,
    iterate_1, update_1, rows_1, spare_2,
    iterate_2, update_2, rows_2, spare_3,
    stack_3, iterate_3, update_3, turned, table, block_3,
):
    gx, gy, gz = places()

    stack_3[...] = jnp.zeros(stack_3.shape, jnp.float32)
    blank = jnp.zeros((LANES - COLUMNS, LANES), jnp.float32)
    for r in range(20):
        part = gathered[pl.ds(r, COLUMNS, stride=CHUNK), :]
        turned[...] = jnp.transpose(jnp.concatenate([part, blank], axis=0))
        for j in range(3):
            k, x = divmod(20 * j + r, 12)
            for y in range(6):
                stack_3[k, x, y, 0:6, :] = turned[40 * j + 6 * y : 40 * j + 6 * y + 6, :]
    move = Columns(6)
    weight = 0.25**3
    iterate_3[12] = jnp.zeros(iterate_3.shape[1:], jnp.float32)
    down(stack_3, iterate_3, update_3, weight, 13, 12, move)
    keep_remainder(stack_3, iterate_3, update_3, weight, 13, 12, move)

    def coarse(k, x_pair, y_pair, z_pair, scale):
        planes = []
        for x in range(6):
            read = (lambda i: update_3[i]) if k == 0 else (lambda i: stack_3[k, i])
            v = read(2 * x)
            if x_pair:
                v = v + read(2 * x + 1)
            lines = []
            for y in range(3):
                line = v[2 * y]
                if y_pair:
                    line = line + v[2 * y + 1]
                if z_pair:
                    line = line + roll(line, -1, -2)
                lines.append(scale * compact(line))
            planes.append(jnp.stack(lines))
        return jnp.stack(planes)

    lowest = bottom(
        coarse(0, True, True, True, 0.125),
        (
            coarse(1, False, True, True, 0.25),
            coarse(2, True, False, True, 0.25),
            coarse(3, True, True, False, 0.25),
        ),
        coarse(4, True, True, True, 0.125),
    )
    row = iota((8, LANES), 0)
    for x in range(6):
        for y in range(3):
            line = lowest[x, y]
            wide = jnp.where(row == 0, line, 0.0)
            for to in range(1, 6):
                wide = jnp.where(row == to, roll(line, to - to // 2, -2), wide)
            for a in range(2):
                for b in range(2):
                    iterate_3[2 * x + a, 2 * y + b] = iterate_3[2 * x + a, 2 * y + b] + wide
    up(stack_3, iterate_3, update_3, weight, 13, 12, move)

    low_rows = jnp.zeros((32, LANES), jnp.float32)
    for q in range(6):
        two = [iterate_3[2 * q + h].reshape(48, LANES) for h in range(2)]
        table[q] = jnp.transpose(jnp.concatenate(two + [low_rows], axis=0))
    block_3[...] = jnp.zeros(block_3.shape, jnp.float32)
    lane = iota((8, LANES), 1)

    def place(q, carry):
        for a, first in ((0, 0), (1, 6), (-1, 18)):
            lines = [jnp.zeros((8, LANES), jnp.float32) for _ in range(2)]
            for b, base in ((0, 0), (1, 6), (-1, LANES - 6)):
                y, z = gy + a, gz + b
                inside = (y >= 0) & (y < COUNT_Y) & (z >= 0) & (z < COUNT_Z)
                at = jnp.where(inside, y * COUNT_Z + z, 0)
                here = (lane >= base) & (lane < base + 6) & inside
                found = jnp.broadcast_to(table[q, pl.ds(at, 1), :], (8, LANES))
                for h in range(2):
                    for y_in in range(6):
                        moved = roll(found, base - 48 * h - 8 * y_in, -1)
                        lines[h] = jnp.where(here & (row == y_in), moved, lines[h])
            for h in range(2):
                block_3[2 * q + h, first : first + 6, :] = lines[h][0:6]
        return carry

    lax.fori_loop(0, 6, place, 0)

    spread(
        block_3, spare_3, rows_2, base_2, iterate_2,
        ((0, 12, 0), (18, 6, 28)),
        ((12, lambda i: i, lambda i: 2 * i),),
        24,
    )
    up(stack_2, iterate_2, update_2, 0.0625, 25, 24, Wrapped)

    size = SIZES[1]
    spread(
        iterate_2, spare_2, rows_1, base_1, iterate_1,
        ((0, 16, 0), (36, 4, 32)),
        (
            (12, lambda i: 12 * gx + i, lambda i: 2 * i),
            (4, lambda i: 12 - 4 * gx + i, lambda i: size + gx + 2 * i),
        ),
        size + 8 * (1 - gx),
    )
    up(stack_1, iterate_1, update_1, 0.25, size + 9, size + 9, Wrapped)

    size = SIZES[0]
    spread(
        iterate_1, spare_1, rows_0, base_0, iterate_0,
        ((0, 28, 0), (36, 4, 56)),
        (
            (24, lambda i: i, lambda i: 2 * i),
            (4, lambda i: 24 + 5 * gx + i, lambda i: size + gx + 2 * i),
        ),
        size + 8 * (1 - gx),
    )
    planes = size + 9
    up(stack_0, iterate_0, update_0, 1.0, planes, planes, Wrapped)
    iterate_0[planes] = iterate_0[0]
    mask = iota((size, LANES), 1) < size

    def use(i, v, remainder, carry):
        solution_out[i] = v[0:size, 0:size]
        residual_out[i] = remainder[0:size, 0:size]
        mine = jnp.where(mask, remainder[0:size], 0.0)
        given = jnp.where(mask, stack_0[0, i, 0:size, :], 0.0)
        return carry[0] + mine * mine, carry[1] + given * given

    zero = jnp.zeros((size, LANES), jnp.float32)
    squares = stencil_pass(stack_0, iterate_0, 1.0, planes, size, Wrapped, use, (zero, zero))
    ones = []
    for square in squares:
        one = jnp.sum(jnp.sum(square, axis=0, keepdims=True), axis=1, keepdims=True)
        ones.append(jnp.broadcast_to(one, (8, LANES)))
    sums[...] = jnp.where(lane == 0, ones[0], jnp.where(lane == 1, ones[1], 0.0))


def shards(right, faces, cells):
    dma = pltpu.SemaphoreType.DMA
    edge = call(edge_kernel, [near(5, WIDTH, 48, 48)], [held_near] * 3, [dma((5,))],
        (right, faces, cells), 2)[0]
    beside = swap_cores(edge)
    outs = call(pack_0_kernel, payload_shapes(48), [held_near] * 4, [],
        (right, faces, cells, beside), 6)
    moved = [swap(v, *way) for v, way in zip(outs, WAYS)]
    coarse, coarse_edge, stack_0, iterate_0 = call(
        level_0_kernel,
        [near(5, 24, 24, LANES), near(5, WIDTH, 24, LANES), near(7, 58, 64, LANES), near(58, 64, LANES)],
        [held_near] * 12,
        [near(58, 64, LANES), near(5, 64, LANES), near(5, 24, 24, LANES)],
        (right, faces, cells, beside, *moved),
        12,
    )
    beside = swap_cores(coarse_edge)
    outs = call(pack_1_kernel, payload_shapes(24), [held_near] * 2, [], (coarse, beside), 8)
    moved = [swap(v, *way) for v, way in zip(outs, WAYS)]
    coarse, stack_1, iterate_1 = call(
        level_1_kernel,
        [near(12, 16, LANES), near(7, 34, 40, LANES), near(34, 40, LANES)],
        [held_near] * 10,
        [near(34, 40, LANES), near(5, 40, LANES), near(5, 12, 16, LANES), near(5, 12, 16, LANES)],
        (coarse, beside, *moved),
        12,
    )
    coarse = coarse + swap_cores(coarse)
    moved = [swap(coarse, *way) for way in WAYS]
    payload, stack_2, iterate_2 = call(
        level_2_kernel,
        [near(COLUMNS * CHUNK, LANES), near(7, 26, 40, LANES), near(26, 40, LANES)],
        [held_near] * 9,
        [near(26, 40, LANES), near(5, 40, LANES), near(5, 12, 8, LANES), near(480, LANES), near(64, LANES)],
        (coarse, *moved),
        12,
    )
    payload = payload.reshape(COLUMNS, CHUNK, LANES)
    gathered = lax.all_to_all(payload, YZ, 0, 0).reshape(COLUMNS * CHUNK, LANES)
    solved, residual, sums = call(
        rise_kernel,
        [f32(48, 48, 48), f32(48, 48, 48), f32(8, LANES)],
        [held_near] * 7,
        [
            near(58, 64, LANES), near(58, 64, LANES), near(64, LANES), near(33, 40, LANES),
            near(34, 40, LANES), near(34, 40, LANES), near(40, LANES), near(24, 40, LANES),
            near(26, 40, LANES), near(26, 40, LANES), near(40, LANES), near(12, 24, LANES),
            near(8, 14, 6, 8, LANES), near(14, 6, 8, LANES), near(14, 6, 8, LANES),
            near(LANES, LANES), near(6, LANES, LANES), near(12, 24, LANES),
        ],
        (gathered, stack_2, iterate_2, stack_1, iterate_1, stack_0, iterate_0),
        24,
    )
    each = jnp.broadcast_to(sums[0:1].reshape(1, 1, LANES), (128, 1, LANES))
    total = jnp.sum(lax.all_to_all(each, ALL, 0, 0), axis=(0, 1))
    return solved, residual, jnp.sqrt(total[0] / total[1])


def solution(mesh):
    torus = Mesh(
        mesh.devices.reshape(mesh.shape["gx"], mesh.shape["gy"], 4, 4), ("gx", "gy", "gz_0", "gz_1")
    )
    in_specs = (P("gx", "gy", GZ), P(None, "gx", "gy", GZ), P("gx", "gy", GZ))
    out_specs = (P("gx", "gy", GZ), P("gx", "gy", GZ), P())
    return jax.shard_map(
        shards, mesh=torus, in_specs=in_specs, out_specs=out_specs, check_vma=False
    )
```

```python
import functools

import jax
import jax.numpy as jnp
from jax import lax
from jax.experimental import pallas as pl
from jax.experimental.pallas import tpu as pltpu
from jax.sharding import Mesh
from jax.sharding import PartitionSpec as P

BOTTOM = 6
ALL = ("gx", "gy", "gz_0", "gz_1")
YZ = ("gy", "gz_0", "gz_1")
GZ = ("gz_0", "gz_1")
LANES = 128
WIDTH = 8
COUNT_Y = 4
COUNT_Z = 16
COLUMNS = COUNT_Y * COUNT_Z
SIZES = (48, 24, 12, 6)
CHUNK = 24
GROUP = 3

theta = 1.125
delta = 0.875
sigma = theta / delta
rho_0 = 1.0 / sigma
rho_1 = 1.0 / (2.0 * sigma - rho_0)
rho_2 = 1.0 / (2.0 * sigma - rho_1)
FIRST = (0.0, 1.0 / theta)
LATER = ((rho_1 * rho_0, 2.0 * rho_1 / delta), (rho_2 * rho_1, 2.0 * rho_2 / delta))

vmem = pl.BlockSpec(memory_space=pltpu.VMEM)
held_near = pl.BlockSpec(memory_space=pltpu.VMEM)
anywhere = pl.BlockSpec(memory_space=pl.ANY)


def roll(value, by, axis):
    axis = axis % value.ndim
    by = by % value.shape[axis]
    return pltpu.roll(value, by, axis) if by else value


def iota(shape, dim):
    return lax.broadcasted_iota(jnp.int32, shape, dim % len(shape))


def exact_dot(left, right):
    return jnp.dot(
        left, right, precision=lax.Precision.HIGHEST, preferred_element_type=jnp.float32
    )


class Wrapped:
    @staticmethod
    def low_y(v):
        return roll(v, 1, -2)

    @staticmethod
    def up_y(v):
        return roll(v, -1, -2)

    @staticmethod
    def low_z(v):
        return roll(v, 1, -1)

    @staticmethod
    def up_z(v):
        return roll(v, -1, -1)


class Columns:
    def __init__(self, cells):
        self.cells = cells

    def low_y(self, v):
        lane = iota(v.shape, -1)
        last = lax.slice_in_dim(v, self.cells - 1, self.cells, axis=v.ndim - 3)
        rest = lax.slice_in_dim(v, 0, self.cells - 1, axis=v.ndim - 3)
        lane = iota(last.shape, -1)
        last = jnp.where((lane >= COUNT_Z) & (lane < COLUMNS), roll(last, COUNT_Z, -1), 0.0)
        return jnp.concatenate([last, rest], axis=v.ndim - 3)

    def up_y(self, v):
        first = lax.slice_in_dim(v, 0, 1, axis=v.ndim - 3)
        rest = lax.slice_in_dim(v, 1, self.cells, axis=v.ndim - 3)
        lane = iota(first.shape, -1)
        first = jnp.where(lane < COLUMNS - COUNT_Z, roll(first, -COUNT_Z, -1), 0.0)
        return jnp.concatenate([rest, first], axis=v.ndim - 3)

    def low_z(self, v):
        lane, row = iota(v.shape, -1), iota(v.shape, -2)
        edge = roll(roll(v, 1 - self.cells, -2), 1, -1)
        edge = jnp.where((lane % COUNT_Z != 0) & (lane < COLUMNS), edge, 0.0)
        return jnp.where(row == 0, edge, roll(v, 1, -2))

    def up_z(self, v):
        lane, row = iota(v.shape, -1), iota(v.shape, -2)
        edge = roll(roll(v, self.cells - 1, -2), -1, -1)
        edge = jnp.where((lane % COUNT_Z != COUNT_Z - 1) & (lane < COLUMNS), edge, 0.0)
        inner = jnp.where(row < self.cells - 1, roll(v, -1, -2), 0.0)
        return jnp.where(row == self.cells - 1, edge, inner)


def set_up(stack, weight, planes, count, move, start=None):
    stack[1, planes] = stack[1, 0]

    def moved(i):
        return [move.up_z(stack[3, i + u]) for u in range(GROUP)]

    def body(g, above_z):
        i = GROUP * g
        later = moved(jnp.minimum(i + GROUP, count - GROUP))
        for u in range(GROUP):
            at = i + u
            cell, face_y = stack[4, at], stack[2, at]
            above_y = move.up_y(face_y)
            if stack.shape[0] > 7:
                stack[7, at] = above_y
            stack[6, at] = above_z[u]
            total = stack[1, at] + stack[1, at + 1] + face_y + above_y
            total = total + stack[3, at] + above_z[u]
            inverse = jnp.where(cell > 0.0, 1.0 / (cell + weight * total), 0.0)
            stack[5, at] = inverse
            if start is not None:
                step = FIRST[1] * (inverse * stack[0, at])
                for ref in start:
                    ref[at] = step
        return later

    lax.fori_loop(0, count // GROUP, body, moved(0))


def stencil_pass(stack, iterate, weight, planes, count, move, use, carry):
    flux = stack[1, 0] * (iterate[0] - iterate[planes - 1])
    by_face = stack.shape[0] > 7

    def moved(i):
        out = []
        for u in range(GROUP):
            v = iterate[i + u]
            out += [move.low_z(v), move.up_z(v)]
            if by_face:
                out += [move.low_y(v), move.up_y(v)]
        return out

    def body(g, state):
        flux, near_by, carry = state
        i = GROUP * g
        later = moved(jnp.minimum(i + GROUP, count - GROUP))
        values = [iterate[i + u] for u in range(GROUP + 1)]
        each = len(near_by) // GROUP
        for u in range(GROUP):
            at, v = i + u, values[u]
            sides = near_by[each * u : each * u + each]
            above = stack[1, at + 1] * (values[u + 1] - v)
            total = flux - above
            flux = above
            if by_face:
                total = total + stack[2, at] * (v - sides[2]) + stack[7, at] * (v - sides[3])
            else:
                flux_y = stack[2, at] * (v - move.low_y(v))
                total = total + (flux_y - move.up_y(flux_y))
            total = total + stack[3, at] * (v - sides[0]) + stack[6, at] * (v - sides[1])
            carry = use(at, v, stack[0, at] - (stack[4, at] * v + weight * total), carry)
        return flux, later, carry

    return lax.fori_loop(0, count // GROUP, body, (flux, moved(0), carry))[2]


def sweep(stack, iterate, update, weight, planes, count, move, factors):
    keep, gain = factors
    iterate[planes] = iterate[0]

    def use(i, v, remainder, carry):
        step = gain * (stack[5, i] * remainder)
        if keep:
            step = keep * update[i] + step
        update[i] = step
        iterate[i] = v + step
        return carry

    stencil_pass(stack, iterate, weight, planes, count, move, use, 0)


def down(stack, iterate, update, weight, planes, count, move):
    set_up(stack, weight, planes, count, move, (iterate, update))
    for factors in LATER:
        sweep(stack, iterate, update, weight, planes, count, move, factors)


def up(stack, iterate, update, weight, planes, count, move):
    for factors in (FIRST,) + LATER:
        sweep(stack, iterate, update, weight, planes, count, move, factors)


def keep_remainder(stack, iterate, update, weight, planes, count, move):
    iterate[planes] = iterate[0]

    def use(i, v, remainder, carry):
        update[i] = remainder
        return carry

    stencil_pass(stack, iterate, weight, planes, count, move, use, 0)


def coarsen(stack, remainder, rows, pairs, out, count, size):
    half = size // 2

    def body(i, carry):
        for k in range(5):
            if k == 1:
                rows[k] = stack[1, 2 * i]
            elif k == 0:
                rows[k] = remainder[2 * i] + remainder[2 * i + 1]
            else:
                rows[k] = stack[k, 2 * i] + stack[k, 2 * i + 1]
        for k in range(5):
            pair = rows[k, pl.ds(0, half, stride=2), :]
            if k != 2:
                pair = pair + rows[k, pl.ds(1, half, stride=2), :]
            pairs[k, i, 0:half, :] = pair
        return carry

    if half % 8:
        pairs[...] = jnp.zeros(pairs.shape, jnp.float32)
    lax.fori_loop(0, count // 2, body, 0)
    fine, coarse = iota((LANES, LANES), 0), iota((LANES, LANES), 1)
    mean = jnp.where((fine // 2 == coarse) & (fine < size), 1.0, 0.0)
    even = jnp.where((fine == 2 * coarse) & (fine < size), 1.0, 0.0)
    _, planes, padded, _ = pairs.shape
    for k in range(5):
        flat = pairs[k].reshape(planes * padded, LANES)
        scale = 0.125 if k in (0, 4) else 0.25
        made = scale * exact_dot(flat, even if k == 3 else mean)
        out(k, made.reshape(planes, padded, LANES))


def spread(coarse, spare, rows, base, fine, row_map, plane_maps, empty):
    planes, height, _ = spare.shape
    source, target = iota((LANES, LANES), 0), iota((LANES, LANES), 1)
    half = target // 2
    pick = jnp.where(source == jnp.where(target < LANES // 2, half, LANES // 2 + half), 1.0, 0.0)
    wide = exact_dot(coarse[0:planes].reshape(planes * height, LANES), pick)
    spare[...] = wide.reshape(planes, height, LANES)
    rows[...] = jnp.zeros(rows.shape, jnp.float32)
    fine[empty] = rows[...]
    for count, plane_of, target_of in plane_maps:

        def body(i, carry):
            plane = plane_of(i)
            for start, number, first in row_map:
                part = spare[plane, start : start + number, :]
                rows[pl.ds(first, number, stride=2), :] = part
                rows[pl.ds(first + 1, number, stride=2), :] = part
            both = rows[...]
            at = target_of(i)
            fine[at] = base[at] + both
            fine[at + 1] = base[at + 1] + both
            return carry

        lax.fori_loop(0, count, body, 0)


def places():
    gx = lax.axis_index("gx")
    gy = lax.axis_index("gy")
    gz = lax.axis_index("gz_0") * 4 + lax.axis_index("gz_1")
    return gx, gy, gz


def widen(value):
    rows, lanes = value.shape
    if lanes == LANES:
        return value
    return jnp.concatenate([value, jnp.zeros((rows, LANES - lanes), jnp.float32)], axis=1)


def y_pack(parts, size):
    lane = iota((8, LANES), 1)
    tiles = [jnp.zeros((8, LANES), jnp.float32) for _ in range(-(-5 * size // LANES))]
    for k, part in enumerate(parts):
        start = k * size
        moved = roll(part, start % LANES, -1)
        for t in range(len(tiles)):
            a, b = max(start, t * LANES) - t * LANES, min(start + size, (t + 1) * LANES) - t * LANES
            if a < b:
                tiles[t] = jnp.where((lane >= a) & (lane < b), moved, tiles[t])
    return tiles


def y_unpack(tiles, k, size):
    lane = iota((8, LANES), 1)
    start = k * size
    t = start // LANES
    value = tiles[t]
    if start + size > (t + 1) * LANES:
        value = jnp.where(lane >= start - t * LANES, value, tiles[t + 1])
    return roll(value, -start, -1)


def pack(own, beside, size, outs):
    y_even, y_odd, z_even, z_odd, ee, eo, oe, oo = outs
    _, gy, gz = places()
    even_y, even_z = gy % 2 == 0, gz % 2 == 0
    lane = iota((size, LANES), 1)

    def group(g, slots, get):
        top = jnp.zeros((size, LANES), jnp.float32)
        bottom = top
        for s in range(slots):
            high, low = [], []
            for k in range(5):
                v = get(k, s)
                at = 40 * s + 8 * k
                here = (lane >= at) & (lane < at + 8)
                top = jnp.where(here, roll(v, at - (size - 8), -1), top)
                bottom = jnp.where(here, roll(v, at, -1), bottom)
                high.append(v[size - 8 :])
                low.append(v[:8])
            for t, (h, l) in enumerate(zip(y_pack(high, size), y_pack(low, size))):
                y_even[3 * g + s, 8 * t : 8 * t + 8, :] = jnp.where(even_y, h, l)
                y_odd[3 * g + s, 8 * t : 8 * t + 8, :] = jnp.where(even_y, l, h)
        a, b = jnp.where(even_z, top, bottom), jnp.where(even_z, bottom, top)
        z_even[g] = a
        z_odd[g] = b
        ee[g] = jnp.where(even_y, a[size - 8 :], a[:8])
        eo[g] = jnp.where(even_y, b[size - 8 :], b[:8])
        oe[g] = jnp.where(even_y, a[:8], a[size - 8 :])
        oo[g] = jnp.where(even_y, b[:8], b[size - 8 :])

    def body(g, carry):
        group(g, 3, lambda k, s: own(k, 3 * g + s))
        return carry

    lax.fori_loop(0, size // 3, body, 0)
    for q in range(3):
        group(size // 3 + q, min(3, 8 - 3 * q), lambda k, s: beside(k, 3 * q + s))


def unpack(stack, own, beside, size, payloads):
    y_even, y_odd, z_even, z_odd, ee, eo, oe, oo = payloads
    gx, gy, gz = places()
    even_y, even_z = gy % 2 == 0, gz % 2 == 0
    lane, lane_8 = iota((size, LANES), 1), iota((8, LANES), 1)
    tiles = -(-5 * size // LANES)

    def join(lane, middle, low, high, at):
        sides = jnp.where(lane >= LANES - 8, roll(low, LANES - 8 - at, -1), 0.0)
        sides = jnp.where(lane < size + 8, roll(high, size - at, -1), sides)
        return jnp.where(lane < size, middle, sides)

    def group(g, slots, get, first):
        low = jnp.where(even_z, z_odd[g], z_even[g])
        high = jnp.where(even_z, z_even[g], z_odd[g])
        by_even = jnp.where(even_z, eo[g], ee[g]), jnp.where(even_z, ee[g], eo[g])
        by_odd = jnp.where(even_z, oo[g], oe[g]), jnp.where(even_z, oe[g], oo[g])
        corners = (
            [jnp.where(even_y, e, o) for e, o in zip(by_even, by_odd)],
            [jnp.where(even_y, o, e) for e, o in zip(by_even, by_odd)],
        )
        for s in range(slots):
            e, o = y_even[3 * g + s], y_odd[3 * g + s]
            ends = jnp.where(even_y, e, o), jnp.where(even_y, o, e)
            ends = [[end[8 * t : 8 * t + 8] for t in range(tiles)] for end in ends]
            for k in range(5):
                at = 40 * s + 8 * k
                stack[k, first + s, 0:size, :] = join(lane, get(k, s), low, high, at)
                for which in range(2):
                    rows = slice(size + 8 * which, size + 8 * which + 8)
                    middle = y_unpack(ends[which], k, size)
                    stack[k, first + s, rows, :] = join(lane_8, middle, *corners[which], at)

    def body(g, carry):
        group(g, 3, lambda k, s: own(k, 3 * g + s), 3 * g)
        return carry

    lax.fori_loop(0, size // 3, body, 0)
    for q in range(3):
        group(
            size // 3 + q,
            min(3, 8 - 3 * q),
            lambda k, s: beside(k, 3 * q + s),
            size + gx + 3 * q,
        )
    empty = size + 8 * (1 - gx)
    for k in range(5):
        stack[k, empty] = jnp.zeros(stack.shape[2:], jnp.float32)


def pack_y(own, beside, size, y_even, y_odd):
    _, gy, _ = places()
    even_y = gy % 2 == 0

    def plane(at, get):
        values = [get(k) for k in range(5)]
        high = y_pack([v[size - 8 :] for v in values], size)
        low = y_pack([v[:8] for v in values], size)
        for t, (h, l) in enumerate(zip(high, low)):
            y_even[at, 8 * t : 8 * t + 8, :] = jnp.where(even_y, h, l)
            y_odd[at, 8 * t : 8 * t + 8, :] = jnp.where(even_y, l, h)

    def body(g, carry):
        for u in range(8):
            plane(8 * g + u, lambda k: own(k, 8 * g + u))
        return carry

    lax.fori_loop(0, size // 8, body, 0)
    for j in range(8):
        plane(size + j, lambda k: beside(k, j))


def merge_y(stack, own, beside, size, y_even, y_odd, z_even, z_odd):
    gx, gy, gz = places()
    even_y, even_z = gy % 2 == 0, gz % 2 == 0
    rows = size + 16
    lane = iota((rows, LANES), 1)
    tiles = -(-5 * size // LANES)

    def group(g, slots, get, first):
        top = jnp.zeros((rows, LANES), jnp.float32)
        bottom = top
        for s in range(slots):
            e, o = y_even[3 * g + s], y_odd[3 * g + s]
            ends = jnp.where(even_y, e, o), jnp.where(even_y, o, e)
            ends = [[end[8 * t : 8 * t + 8] for t in range(tiles)] for end in ends]
            for k in range(5):
                parts = [get(k, s)] + [y_unpack(end, k, size) for end in ends]
                v = jnp.where(lane < size, jnp.concatenate(parts, axis=0), 0.0)
                stack[k, first + s] = v
                at = 40 * s + 8 * k
                here = (lane >= at) & (lane < at + 8)
                top = jnp.where(here, roll(v, at - (size - 8), -1), top)
                bottom = jnp.where(here, roll(v, at, -1), bottom)
        z_even[g] = jnp.where(even_z, top, bottom)
        z_odd[g] = jnp.where(even_z, bottom, top)

    def body(g, carry):
        group(g, 3, lambda k, s: own(k, 3 * g + s), 3 * g)
        return carry

    lax.fori_loop(0, size // 3, body, 0)
    for q in range(3):
        group(
            size // 3 + q,
            min(3, 8 - 3 * q),
            lambda k, s: beside(k, 3 * q + s),
            size + gx + 3 * q,
        )
    empty = size + 8 * (1 - gx)
    for k in range(5):
        stack[k, empty] = jnp.zeros(stack.shape[2:], jnp.float32)


def merge_z(stack, size, z_even, z_odd):
    gx, _, gz = places()
    even_z = gz % 2 == 0
    lane = iota((size + 16, LANES), 1)

    def group(g, slots, first):
        low = jnp.where(even_z, z_odd[g], z_even[g])
        high = jnp.where(even_z, z_even[g], z_odd[g])
        for s in range(slots):
            for k in range(5):
                at = 40 * s + 8 * k
                v = stack[k, first + s]
                v = jnp.where(lane >= LANES - 8, roll(low, LANES - 8 - at, -1), v)
                here = (lane >= size) & (lane < size + 8)
                stack[k, first + s] = jnp.where(here, roll(high, size - at, -1), v)

    def body(g, carry):
        group(g, 3, 3 * g)
        return carry

    lax.fori_loop(0, size // 3, body, 0)
    for q in range(3):
        group(size // 3 + q, min(3, 8 - 3 * q), size + gx + 3 * q)


def payload_shapes(size):
    groups = size // 3 + 3
    tall = 8 * (-(-5 * size // LANES))
    y = near(size + 8, tall, LANES)
    z = near(groups, size, LANES)
    c = near(groups, 8, LANES)
    return [y, y, z, z, c, c, c, c]


def partner(index, parity, count):
    if parity is None:
        return index
    other = index + 1 if index % 2 == parity else index - 1
    return other if 0 <= other < count else None


def swap(value, parity_y, parity_z):
    pairs = []
    for y in range(COUNT_Y):
        for z in range(COUNT_Z):
            to_y, to_z = partner(y, parity_y, COUNT_Y), partner(z, parity_z, COUNT_Z)
            if to_y is not None and to_z is not None:
                pairs.append((y * COUNT_Z + z, to_y * COUNT_Z + to_z))
    return lax.ppermute(value, YZ, pairs)


WAYS = ((0, None), (1, None), (None, 0), (None, 1), (0, 0), (0, 1), (1, 0), (1, 1))


def swap_cores(value):
    return lax.ppermute(value, "gx", [(0, 1), (1, 0)])


def f32(*shape):
    return jax.ShapeDtypeStruct(shape, jnp.float32)


def near(*shape):
    return pltpu.VMEM(shape, jnp.float32)


def call(body, outs, ins, scratch, operands, limit, aliases={}):
    held = [
        pltpu.with_memory_space_constraint(v, pltpu.VMEM) if spec is held_near else v
        for v, spec in zip(operands, ins)
    ]
    return pl.pallas_call(
        body,
        out_shape=outs,
        out_specs=[vmem] * len(outs),
        in_specs=ins,
        scratch_shapes=scratch,
        input_output_aliases=aliases,
        compiler_params=pltpu.CompilerParams(vmem_limit_bytes=limit * 2**20),
    )(*held)


def edge_kernel(right, faces, cells, out, sems):
    gx = lax.axis_index("gx")
    start = (1 - gx) * (SIZES[0] - WIDTH)
    part = pl.ds(start, WIDTH)
    copies = [
        pltpu.make_async_copy(right.at[part], out.at[0], sems.at[0]),
        pltpu.make_async_copy(faces.at[0, part], out.at[1], sems.at[1]),
        pltpu.make_async_copy(faces.at[1, part], out.at[2], sems.at[2]),
        pltpu.make_async_copy(faces.at[2, part], out.at[3], sems.at[3]),
        pltpu.make_async_copy(cells.at[part], out.at[4], sems.at[4]),
    ]
    for copy in copies:
        copy.start()
    for copy in copies:
        copy.wait()


def own_inputs(right, faces, cells):
    def own(k, i):
        if k == 0:
            return widen(right[i])
        return widen(cells[i] if k == 4 else faces[k - 1, i])

    return own


def pack_0_kernel(right, faces, cells, beside, *outs):
    pack(own_inputs(right, faces, cells), lambda k, j: widen(beside[k, j]), SIZES[0], outs)


def pack_1_kernel(own, beside, y_even, y_odd):
    pack_y(lambda k, i: own[k, i], lambda k, j: beside[k, j], SIZES[1], y_even, y_odd)


def merge_1_kernel(own, beside, y_even, y_odd, stack, z_even, z_odd):
    merge_y(
        stack,
        lambda k, i: own[k, i],
        lambda k, j: beside[k, j],
        SIZES[1],
        y_even,
        y_odd,
        z_even,
        z_odd,
    )


def level_0_kernel(
    right, faces, cells, beside, ye, yo, ze, zo, ee, eo, oe, oo,
    coarse, coarse_edge, stack, iterate,
    update, rows, pairs,
):
    size = SIZES[0]
    planes = size + 9
    gx = lax.axis_index("gx")
    unpack(
        stack,
        own_inputs(right, faces, cells),
        lambda k, j: widen(beside[k, j]),
        size,
        (ye, yo, ze, zo, ee, eo, oe, oo),
    )
    down(stack, iterate, update, 1.0, planes, planes, Wrapped)
    keep_remainder(stack, iterate, update, 1.0, planes, size, Wrapped)

    def out(k, value):
        coarse[k] = value
        coarse_edge[k] = jnp.where(gx == 0, value[16:24], value[0:8])

    coarsen(stack, update, rows, pairs, out, size, size)


def level_1_kernel(
    filled, z_even, z_odd,
    coarse, stack, iterate,
    update, rows, pairs, made,
):
    size = SIZES[1]
    planes = size + 9
    merge_z(stack, size, z_even, z_odd)
    down(stack, iterate, update, 0.25, planes, planes, Wrapped)
    keep_remainder(stack, iterate, update, 0.25, planes, size, Wrapped)

    def out(k, value):
        made[k] = value

    coarsen(stack, update, rows, pairs, out, size, size)
    for i in range(SIZES[2] // 2):
        line = made[0, 2 * i] + roll(made[0, 2 * i + 1], LANES // 2, -1)
        for h in range(2):
            for k in range(1, 5):
                line = line + roll(made[k, 2 * i + h], LANES // 2 * h + SIZES[2] * k, -1)
        coarse[i] = line


def level_2_kernel(
    mine, other,
    payload, stack, iterate,
    update, rows, pairs, made, lines,
):
    size = SIZES[2]
    planes = 2 * size + 1
    gx, gy, gz = places()
    even_y, even_z = gy % 2 == 0, gz % 2 == 0
    lane = iota((16, LANES), 1)
    bases = (0, size, LANES - size)
    half = size // 2
    for k in range(5):
        stack[k, 2 * size] = jnp.zeros(stack.shape[2:], jnp.float32)

    def body(i, carry):
        for core in range(2):

            def block(a, b):
                at = half * (3 * b + a) + i
                return jnp.where(gx == core, mine[at], other[at])

            columns = []
            for b in range(3):
                even, odd = block(1, b), block(2, b)
                columns.append(
                    (block(0, b), jnp.where(even_y, even, odd), jnp.where(even_y, odd, even))
                )
            columns = [columns[0]] + [
                [jnp.where(even_z, p, q) for p, q in zip(columns[c], columns[3 - c])] for c in (1, 2)
            ]
            for h in range(2):
                plane = size * core + 2 * i + h
                for k in range(5):
                    source = (LANES // 2) * h + size * k
                    stack[k, plane, 24:32, :] = jnp.zeros((8, LANES), jnp.float32)
                    for a, first in enumerate((0, size, 40 - size)):
                        line = jnp.zeros((16, LANES), jnp.float32)
                        for b, base in enumerate(bases):
                            here = (lane >= base) & (lane < base + size)
                            line = jnp.where(here, roll(columns[b][a], base - source, -1), line)
                        stack[k, plane, first : first + size, :] = line[:size]
        return carry

    lax.fori_loop(0, half, body, 0)
    weight = 0.0625
    iterate[2 * size] = jnp.zeros(iterate.shape[1:], jnp.float32)
    down(stack, iterate, update, weight, planes, 2 * size, Wrapped)
    keep_remainder(stack, iterate, update, weight, planes, 2 * size, Wrapped)

    def out(k, value):
        made[k * 96 : k * 96 + 96, :] = value.reshape(96, LANES)

    coarsen(stack, update, rows, pairs, out, 2 * size, size)
    line = jnp.zeros((60, LANES), jnp.float32)
    for y in range(6):
        line = line + roll(made[pl.ds(y, 60, stride=8), :], 6 * y, -1)
    lines[0:60, :] = line
    chunk = lines[0:20, :] + roll(lines[20:40, :], 40, -1) + roll(lines[40:60, :], 80, -1)
    chunk = jnp.concatenate([chunk, jnp.zeros((4, LANES), jnp.float32)], axis=0)

    def repeat(c, carry):
        payload[pl.ds(pl.multiple_of(c * CHUNK, 8), CHUNK), :] = chunk
        return carry

    lax.fori_loop(0, COLUMNS, repeat, 0)


def compact(value):
    row = iota(value.shape, -2)
    out = jnp.where(row == 0, value, 0.0)
    out = jnp.where(row == 1, roll(value, -1, -2), out)
    return jnp.where(row == 2, roll(value, -2, -2), out)


def bottom(source, faces, cells):
    weight = 0.25**4
    move = Columns(3)
    face_x, face_y, face_z = faces
    nothing = jnp.zeros((1,) + source.shape[1:], jnp.float32)

    def apply(v):
        flux_x = face_x * (v - jnp.concatenate([nothing, v[:-1]], axis=0))
        flux_y = face_y * (v - move.low_y(v))
        flux_z = face_z * (v - move.low_z(v))
        total = flux_x - jnp.concatenate([flux_x[1:], nothing], axis=0)
        total = total + (flux_y - move.up_y(flux_y)) + (flux_z - move.up_z(flux_z))
        return cells * v + weight * total

    def total_of(v):
        flat = jnp.sum(jnp.sum(v, axis=0), axis=0)
        one = jnp.sum(jnp.sum(flat, axis=0, keepdims=True), axis=1, keepdims=True)
        return jnp.broadcast_to(one, flat.shape)

    iterate = jnp.zeros_like(source)
    remainder = source
    search = source
    norm_now = total_of(remainder * remainder)
    for step in range(BOTTOM):
        applied = apply(search)
        size = norm_now / total_of(search * applied)
        iterate = iterate + size * search
        if step + 1 < BOTTOM:
            remainder = remainder - size * applied
            norm_next = total_of(remainder * remainder)
            search = remainder + (norm_next / norm_now) * search
            norm_now = norm_next
    return iterate


def rise_kernel(
    gathered, stack_2, base_2, stack_1, base_1, stack_0, base_0,
    solution_out, residual_out, sums,
    iterate_0, update_0, rows_0, spare_1,
    iterate_1, update_1, rows_1, spare_2,
    iterate_2, update_2, rows_2, spare_3,
    stack_3, iterate_3, update_3, turned, table, block_3,
):
    gx, gy, gz = places()

    stack_3[...] = jnp.zeros(stack_3.shape, jnp.float32)
    blank = jnp.zeros((LANES - COLUMNS, LANES), jnp.float32)
    for r in range(20):
        part = gathered[pl.ds(r, COLUMNS, stride=CHUNK), :]
        turned[...] = jnp.transpose(jnp.concatenate([part, blank], axis=0))
        for j in range(3):
            k, x = divmod(20 * j + r, 12)
            for y in range(6):
                stack_3[k, x, y, 0:6, :] = turned[40 * j + 6 * y : 40 * j + 6 * y + 6, :]
    move = Columns(6)
    weight = 0.25**3
    iterate_3[12] = jnp.zeros(iterate_3.shape[1:], jnp.float32)
    down(stack_3, iterate_3, update_3, weight, 13, 12, move)
    keep_remainder(stack_3, iterate_3, update_3, weight, 13, 12, move)

    def coarse(k, x_pair, y_pair, z_pair, scale):
        planes = []
        for x in range(6):
            read = (lambda i: update_3[i]) if k == 0 else (lambda i: stack_3[k, i])
            v = read(2 * x)
            if x_pair:
                v = v + read(2 * x + 1)
            lines = []
            for y in range(3):
                line = v[2 * y]
                if y_pair:
                    line = line + v[2 * y + 1]
                if z_pair:
                    line = line + roll(line, -1, -2)
                lines.append(scale * compact(line))
            planes.append(jnp.stack(lines))
        return jnp.stack(planes)

    lowest = bottom(
        coarse(0, True, True, True, 0.125),
        (
            coarse(1, False, True, True, 0.25),
            coarse(2, True, False, True, 0.25),
            coarse(3, True, True, False, 0.25),
        ),
        coarse(4, True, True, True, 0.125),
    )
    row = iota((8, LANES), 0)
    for x in range(6):
        for y in range(3):
            line = lowest[x, y]
            wide = jnp.where(row == 0, line, 0.0)
            for to in range(1, 6):
                wide = jnp.where(row == to, roll(line, to - to // 2, -2), wide)
            for a in range(2):
                for b in range(2):
                    iterate_3[2 * x + a, 2 * y + b] = iterate_3[2 * x + a, 2 * y + b] + wide
    up(stack_3, iterate_3, update_3, weight, 13, 12, move)

    low_rows = jnp.zeros((32, LANES), jnp.float32)
    for q in range(6):
        two = [iterate_3[2 * q + h].reshape(48, LANES) for h in range(2)]
        table[q] = jnp.transpose(jnp.concatenate(two + [low_rows], axis=0))
    block_3[...] = jnp.zeros(block_3.shape, jnp.float32)
    lane = iota((8, LANES), 1)

    def place(q, carry):
        for a, first in ((0, 0), (1, 6), (-1, 18)):
            lines = [jnp.zeros((8, LANES), jnp.float32) for _ in range(2)]
            for b, base in ((0, 0), (1, 6), (-1, LANES - 6)):
                y, z = gy + a, gz + b
                inside = (y >= 0) & (y < COUNT_Y) & (z >= 0) & (z < COUNT_Z)
                at = jnp.where(inside, y * COUNT_Z + z, 0)
                here = (lane >= base) & (lane < base + 6) & inside
                found = jnp.broadcast_to(table[q, pl.ds(at, 1), :], (8, LANES))
                for h in range(2):
                    for y_in in range(6):
                        moved = roll(found, base - 48 * h - 8 * y_in, -1)
                        lines[h] = jnp.where(here & (row == y_in), moved, lines[h])
            for h in range(2):
                block_3[2 * q + h, first : first + 6, :] = lines[h][0:6]
        return carry

    lax.fori_loop(0, 6, place, 0)

    spread(
        block_3, spare_3, rows_2, base_2, iterate_2,
        ((0, 12, 0), (18, 6, 28)),
        ((12, lambda i: i, lambda i: 2 * i),),
        24,
    )
    up(stack_2, iterate_2, update_2, 0.0625, 25, 24, Wrapped)

    size = SIZES[1]
    spread(
        iterate_2, spare_2, rows_1, base_1, iterate_1,
        ((0, 16, 0), (36, 4, 32)),
        (
            (12, lambda i: 12 * gx + i, lambda i: 2 * i),
            (4, lambda i: 12 - 4 * gx + i, lambda i: size + gx + 2 * i),
        ),
        size + 8 * (1 - gx),
    )
    up(stack_1, iterate_1, update_1, 0.25, size + 9, size + 9, Wrapped)

    size = SIZES[0]
    spread(
        iterate_1, spare_1, rows_0, base_0, iterate_0,
        ((0, 28, 0), (36, 4, 56)),
        (
            (24, lambda i: i, lambda i: 2 * i),
            (4, lambda i: 24 + 5 * gx + i, lambda i: size + gx + 2 * i),
        ),
        size + 8 * (1 - gx),
    )
    planes = size + 9
    up(stack_0, iterate_0, update_0, 1.0, planes, planes, Wrapped)
    iterate_0[planes] = iterate_0[0]
    mask = iota((size, LANES), 1) < size

    def use(i, v, remainder, carry):
        solution_out[i] = v[0:size, 0:size]
        residual_out[i] = remainder[0:size, 0:size]
        mine = jnp.where(mask, remainder[0:size], 0.0)
        given = jnp.where(mask, stack_0[0, i, 0:size, :], 0.0)
        return carry[0] + mine * mine, carry[1] + given * given

    zero = jnp.zeros((size, LANES), jnp.float32)
    squares = stencil_pass(stack_0, iterate_0, 1.0, planes, size, Wrapped, use, (zero, zero))
    ones = []
    for square in squares:
        one = jnp.sum(jnp.sum(square, axis=0, keepdims=True), axis=1, keepdims=True)
        ones.append(jnp.broadcast_to(one, (8, LANES)))
    sums[...] = jnp.where(lane == 0, ones[0], jnp.where(lane == 1, ones[1], 0.0))


def stack_kernel(*refs):
    out = refs[-1]
    for n, ref in enumerate(refs[:-1]):
        count = ref.shape[0]
        out[n * count : n * count + count] = ref[...]


def stacked(*parts):
    count, *rest = parts[0].shape
    return call(stack_kernel, [near(len(parts) * count, *rest)], [held_near] * 3, [], parts, 1)[0]


def shards(right, faces, cells):
    dma = pltpu.SemaphoreType.DMA
    edge = call(edge_kernel, [near(5, WIDTH, 48, 48)], [held_near] * 3, [dma((5,))],
        (right, faces, cells), 2)[0]
    beside = swap_cores(edge)
    outs = call(pack_0_kernel, payload_shapes(48), [held_near] * 4, [],
        (right, faces, cells, beside), 6)
    moved = [swap(v, *way) for v, way in zip(outs, WAYS)]
    coarse, coarse_edge, stack_0, iterate_0 = call(
        level_0_kernel,
        [near(5, 24, 24, LANES), near(5, WIDTH, 24, LANES), near(7, 58, 64, LANES), near(58, 64, LANES)],
        [held_near] * 12,
        [near(58, 64, LANES), near(5, 64, LANES), near(5, 24, 24, LANES)],
        (right, faces, cells, beside, *moved),
        12,
    )
    beside = swap_cores(coarse_edge)
    outs = call(pack_1_kernel, [near(32, 8, LANES)] * 2, [held_near] * 2, [], (coarse, beside), 4)
    y_sides = [swap(v, parity, None) for parity, v in enumerate(outs)]
    filled, *outs = call(
        merge_1_kernel,
        [near(7, 34, 40, LANES), near(11, 40, LANES), near(11, 40, LANES)],
        [held_near] * 4,
        [],
        (coarse, beside, *y_sides),
        4,
    )
    z_sides = [swap(v, None, parity) for parity, v in enumerate(outs)]
    coarse, stack_1, iterate_1 = call(
        level_1_kernel,
        [near(6, 16, LANES), near(7, 34, 40, LANES), near(34, 40, LANES)],
        [held_near] * 3,
        [near(34, 40, LANES), near(5, 40, LANES), near(5, 12, 16, LANES), near(5, 12, 16, LANES)],
        (filled, *z_sides),
        12,
        {0: 1},
    )
    column = stacked(coarse, *[swap(coarse, parity, None) for parity in (0, 1)])
    region = stacked(column, *[swap(column, None, parity) for parity in (0, 1)])
    other = swap_cores(region)
    payload, stack_2, iterate_2 = call(
        level_2_kernel,
        [near(COLUMNS * CHUNK, LANES), near(7, 26, 40, LANES), near(26, 40, LANES)],
        [held_near] * 2,
        [near(26, 40, LANES), near(5, 40, LANES), near(5, 12, 8, LANES), near(480, LANES), near(64, LANES)],
        (region, other),
        12,
    )
    payload = payload.reshape(COLUMNS, CHUNK, LANES)
    gathered = lax.all_to_all(payload, YZ, 0, 0).reshape(COLUMNS * CHUNK, LANES)
    solved, residual, sums = call(
        rise_kernel,
        [f32(48, 48, 48), f32(48, 48, 48), f32(8, LANES)],
        [held_near] * 7,
        [
            near(58, 64, LANES), near(58, 64, LANES), near(64, LANES), near(33, 40, LANES),
            near(34, 40, LANES), near(34, 40, LANES), near(40, LANES), near(24, 40, LANES),
            near(26, 40, LANES), near(26, 40, LANES), near(40, LANES), near(12, 24, LANES),
            near(8, 14, 6, 8, LANES), near(14, 6, 8, LANES), near(14, 6, 8, LANES),
            near(LANES, LANES), near(6, LANES, LANES), near(12, 24, LANES),
        ],
        (gathered, stack_2, iterate_2, stack_1, iterate_1, stack_0, iterate_0),
        24,
    )
    each = jnp.broadcast_to(sums[0:1].reshape(1, 1, LANES), (128, 1, LANES))
    total = jnp.sum(lax.all_to_all(each, ALL, 0, 0), axis=(0, 1))
    return solved, residual, jnp.sqrt(total[0] / total[1])


def solution(mesh):
    torus = Mesh(
        mesh.devices.reshape(mesh.shape["gx"], mesh.shape["gy"], 4, 4), ("gx", "gy", "gz_0", "gz_1")
    )
    in_specs = (P("gx", "gy", GZ), P(None, "gx", "gy", GZ), P("gx", "gy", GZ))
    out_specs = (P("gx", "gy", GZ), P("gx", "gy", GZ), P())
    return jax.shard_map(
        shards, mesh=torus, in_specs=in_specs, out_specs=out_specs, check_vma=False
    )
```

```python
import functools

import jax
import jax.numpy as jnp
from jax import lax
from jax.experimental import pallas as pl
from jax.experimental.pallas import tpu as pltpu
from jax.sharding import Mesh
from jax.sharding import PartitionSpec as P

BOTTOM = 6
ALL = ("gx", "gy", "gz_0", "gz_1")
YZ = ("gy", "gz_0", "gz_1")
GZ = ("gz_0", "gz_1")
LANES = 128
WIDTH = 8
COUNT_Y = 4
COUNT_Z = 16
COLUMNS = COUNT_Y * COUNT_Z
SIZES = (48, 24, 12, 6)
CHUNK = 24
GROUP = 3

theta = 1.125
delta = 0.875
sigma = theta / delta
rho_0 = 1.0 / sigma
rho_1 = 1.0 / (2.0 * sigma - rho_0)
rho_2 = 1.0 / (2.0 * sigma - rho_1)
FIRST = (0.0, 1.0 / theta)
LATER = ((rho_1 * rho_0, 2.0 * rho_1 / delta), (rho_2 * rho_1, 2.0 * rho_2 / delta))

vmem = pl.BlockSpec(memory_space=pltpu.VMEM)
held_near = pl.BlockSpec(memory_space=pltpu.VMEM)
far = pl.BlockSpec(memory_space=pltpu.HBM)


def roll(value, by, axis):
    axis = axis % value.ndim
    by = by % value.shape[axis]
    return pltpu.roll(value, by, axis) if by else value


def iota(shape, dim):
    return lax.broadcasted_iota(jnp.int32, shape, dim % len(shape))


def exact_dot(left, right):
    return jnp.dot(
        left, right, precision=lax.Precision.HIGHEST, preferred_element_type=jnp.float32
    )


class Wrapped:
    @staticmethod
    def low_y(v):
        return roll(v, 1, -2)

    @staticmethod
    def up_y(v):
        return roll(v, -1, -2)

    @staticmethod
    def low_z(v):
        return roll(v, 1, -1)

    @staticmethod
    def up_z(v):
        return roll(v, -1, -1)


class Columns:
    def __init__(self, cells):
        self.cells = cells

    def low_y(self, v):
        lane = iota(v.shape, -1)
        last = lax.slice_in_dim(v, self.cells - 1, self.cells, axis=v.ndim - 3)
        rest = lax.slice_in_dim(v, 0, self.cells - 1, axis=v.ndim - 3)
        lane = iota(last.shape, -1)
        last = jnp.where((lane >= COUNT_Z) & (lane < COLUMNS), roll(last, COUNT_Z, -1), 0.0)
        return jnp.concatenate([last, rest], axis=v.ndim - 3)

    def up_y(self, v):
        first = lax.slice_in_dim(v, 0, 1, axis=v.ndim - 3)
        rest = lax.slice_in_dim(v, 1, self.cells, axis=v.ndim - 3)
        lane = iota(first.shape, -1)
        first = jnp.where(lane < COLUMNS - COUNT_Z, roll(first, -COUNT_Z, -1), 0.0)
        return jnp.concatenate([rest, first], axis=v.ndim - 3)

    def low_z(self, v):
        lane, row = iota(v.shape, -1), iota(v.shape, -2)
        edge = roll(roll(v, 1 - self.cells, -2), 1, -1)
        edge = jnp.where((lane % COUNT_Z != 0) & (lane < COLUMNS), edge, 0.0)
        return jnp.where(row == 0, edge, roll(v, 1, -2))

    def up_z(self, v):
        lane, row = iota(v.shape, -1), iota(v.shape, -2)
        edge = roll(roll(v, self.cells - 1, -2), -1, -1)
        edge = jnp.where((lane % COUNT_Z != COUNT_Z - 1) & (lane < COLUMNS), edge, 0.0)
        inner = jnp.where(row < self.cells - 1, roll(v, -1, -2), 0.0)
        return jnp.where(row == self.cells - 1, edge, inner)


def set_up(stack, weight, planes, count, move, start=None):
    stack[1, planes] = stack[1, 0]

    def moved(i):
        return [move.up_z(stack[3, i + u]) for u in range(GROUP)]

    def body(g, above_z):
        i = GROUP * g
        later = moved(jnp.minimum(i + GROUP, count - GROUP))
        for u in range(GROUP):
            at = i + u
            cell, face_y = stack[4, at], stack[2, at]
            above_y = move.up_y(face_y)
            if stack.shape[0] > 7:
                stack[7, at] = above_y
            stack[6, at] = above_z[u]
            total = stack[1, at] + stack[1, at + 1] + face_y + above_y
            total = total + stack[3, at] + above_z[u]
            inverse = jnp.where(cell > 0.0, 1.0 / (cell + weight * total), 0.0)
            stack[5, at] = inverse
            if start is not None:
                step = FIRST[1] * (inverse * stack[0, at])
                for ref in start:
                    ref[at] = step
        return later

    lax.fori_loop(0, count // GROUP, body, moved(0))


def stencil_pass(stack, iterate, weight, planes, count, move, use, carry):
    flux = stack[1, 0] * (iterate[0] - iterate[planes - 1])
    by_face = stack.shape[0] > 7

    def moved(i):
        out = []
        for u in range(GROUP):
            v = iterate[i + u]
            out += [move.low_z(v), move.up_z(v)]
            if by_face:
                out += [move.low_y(v), move.up_y(v)]
        return out

    def body(g, state):
        flux, near_by, carry = state
        i = GROUP * g
        later = moved(jnp.minimum(i + GROUP, count - GROUP))
        values = [iterate[i + u] for u in range(GROUP + 1)]
        each = len(near_by) // GROUP
        for u in range(GROUP):
            at, v = i + u, values[u]
            sides = near_by[each * u : each * u + each]
            above = stack[1, at + 1] * (values[u + 1] - v)
            total = flux - above
            flux = above
            if by_face:
                total = total + stack[2, at] * (v - sides[2]) + stack[7, at] * (v - sides[3])
            else:
                flux_y = stack[2, at] * (v - move.low_y(v))
                total = total + (flux_y - move.up_y(flux_y))
            total = total + stack[3, at] * (v - sides[0]) + stack[6, at] * (v - sides[1])
            carry = use(at, v, stack[0, at] - (stack[4, at] * v + weight * total), carry)
        return flux, later, carry

    return lax.fori_loop(0, count // GROUP, body, (flux, moved(0), carry))[2]


def sweep(stack, iterate, update, weight, planes, count, move, factors):
    keep, gain = factors
    iterate[planes] = iterate[0]

    def use(i, v, remainder, carry):
        step = gain * (stack[5, i] * remainder)
        if keep:
            step = keep * update[i] + step
        update[i] = step
        iterate[i] = v + step
        return carry

    stencil_pass(stack, iterate, weight, planes, count, move, use, 0)


def down(stack, iterate, update, weight, planes, count, move):
    set_up(stack, weight, planes, count, move, (iterate, update))
    for factors in LATER:
        sweep(stack, iterate, update, weight, planes, count, move, factors)


def up(stack, iterate, update, weight, planes, count, move):
    for factors in (FIRST,) + LATER:
        sweep(stack, iterate, update, weight, planes, count, move, factors)


def keep_remainder(stack, iterate, update, weight, planes, count, move):
    iterate[planes] = iterate[0]

    def use(i, v, remainder, carry):
        update[i] = remainder
        return carry

    stencil_pass(stack, iterate, weight, planes, count, move, use, 0)


def coarsen(stack, remainder, rows, pairs, out, count, size):
    half = size // 2

    def body(i, carry):
        for k in range(5):
            if k == 1:
                rows[k] = stack[1, 2 * i]
            elif k == 0:
                rows[k] = remainder[2 * i] + remainder[2 * i + 1]
            else:
                rows[k] = stack[k, 2 * i] + stack[k, 2 * i + 1]
        for k in range(5):
            pair = rows[k, pl.ds(0, half, stride=2), :]
            if k != 2:
                pair = pair + rows[k, pl.ds(1, half, stride=2), :]
            pairs[k, i, 0:half, :] = pair
        return carry

    if half % 8:
        pairs[...] = jnp.zeros(pairs.shape, jnp.float32)
    lax.fori_loop(0, count // 2, body, 0)
    fine, coarse = iota((LANES, LANES), 0), iota((LANES, LANES), 1)
    mean = jnp.where((fine // 2 == coarse) & (fine < size), 1.0, 0.0)
    even = jnp.where((fine == 2 * coarse) & (fine < size), 1.0, 0.0)
    _, planes, padded, _ = pairs.shape
    for k in range(5):
        flat = pairs[k].reshape(planes * padded, LANES)
        scale = 0.125 if k in (0, 4) else 0.25
        made = scale * exact_dot(flat, even if k == 3 else mean)
        out(k, made.reshape(planes, padded, LANES))


def spread(coarse, spare, rows, base, fine, row_map, plane_maps, empty):
    planes, height, _ = spare.shape
    source, target = iota((LANES, LANES), 0), iota((LANES, LANES), 1)
    half = target // 2
    pick = jnp.where(source == jnp.where(target < LANES // 2, half, LANES // 2 + half), 1.0, 0.0)
    wide = exact_dot(coarse[0:planes].reshape(planes * height, LANES), pick)
    spare[...] = wide.reshape(planes, height, LANES)
    rows[...] = jnp.zeros(rows.shape, jnp.float32)
    fine[empty] = rows[...]
    for count, plane_of, target_of in plane_maps:

        def body(i, carry):
            plane = plane_of(i)
            for start, number, first in row_map:
                part = spare[plane, start : start + number, :]
                rows[pl.ds(first, number, stride=2), :] = part
                rows[pl.ds(first + 1, number, stride=2), :] = part
            both = rows[...]
            at = target_of(i)
            fine[at] = base[at] + both
            fine[at + 1] = base[at + 1] + both
            return carry

        lax.fori_loop(0, count, body, 0)


def places():
    gx = lax.axis_index("gx")
    gy = lax.axis_index("gy")
    gz = lax.axis_index("gz_0") * 4 + lax.axis_index("gz_1")
    return gx, gy, gz


def widen(value):
    rows, lanes = value.shape
    if lanes == LANES:
        return value
    return jnp.concatenate([value, jnp.zeros((rows, LANES - lanes), jnp.float32)], axis=1)


def y_pack(parts, size):
    lane = iota((8, LANES), 1)
    tiles = [jnp.zeros((8, LANES), jnp.float32) for _ in range(-(-5 * size // LANES))]
    for k, part in enumerate(parts):
        start = k * size
        moved = roll(part, start % LANES, -1)
        for t in range(len(tiles)):
            a, b = max(start, t * LANES) - t * LANES, min(start + size, (t + 1) * LANES) - t * LANES
            if a < b:
                tiles[t] = jnp.where((lane >= a) & (lane < b), moved, tiles[t])
    return tiles


def y_unpack(tiles, k, size):
    lane = iota((8, LANES), 1)
    start = k * size
    t = start // LANES
    value = tiles[t]
    if start + size > (t + 1) * LANES:
        value = jnp.where(lane >= start - t * LANES, value, tiles[t + 1])
    return roll(value, -start, -1)


def pack(own, beside, size, outs):
    y_even, y_odd, z_even, z_odd, ee, eo, oe, oo = outs
    _, gy, gz = places()
    even_y, even_z = gy % 2 == 0, gz % 2 == 0
    lane = iota((size, LANES), 1)

    def group(g, slots, get):
        top = jnp.zeros((size, LANES), jnp.float32)
        bottom = top
        for s in range(slots):
            high, low = [], []
            for k in range(5):
                v = get(k, s)
                at = 40 * s + 8 * k
                here = (lane >= at) & (lane < at + 8)
                top = jnp.where(here, roll(v, at - (size - 8), -1), top)
                bottom = jnp.where(here, roll(v, at, -1), bottom)
                high.append(v[size - 8 :])
                low.append(v[:8])
            for t, (h, l) in enumerate(zip(y_pack(high, size), y_pack(low, size))):
                y_even[3 * g + s, 8 * t : 8 * t + 8, :] = jnp.where(even_y, h, l)
                y_odd[3 * g + s, 8 * t : 8 * t + 8, :] = jnp.where(even_y, l, h)
        a, b = jnp.where(even_z, top, bottom), jnp.where(even_z, bottom, top)
        z_even[g] = a
        z_odd[g] = b
        ee[g] = jnp.where(even_y, a[size - 8 :], a[:8])
        eo[g] = jnp.where(even_y, b[size - 8 :], b[:8])
        oe[g] = jnp.where(even_y, a[:8], a[size - 8 :])
        oo[g] = jnp.where(even_y, b[:8], b[size - 8 :])

    def body(g, carry):
        group(g, 3, lambda k, s: own(k, 3 * g + s))
        return carry

    lax.fori_loop(0, size // 3, body, 0)
    for q in range(3):
        group(size // 3 + q, min(3, 8 - 3 * q), lambda k, s: beside(k, 3 * q + s))


def unpack(stack, own, beside, size, payloads):
    y_even, y_odd, z_even, z_odd, ee, eo, oe, oo = payloads
    gx, gy, gz = places()
    even_y, even_z = gy % 2 == 0, gz % 2 == 0
    lane, lane_8 = iota((size, LANES), 1), iota((8, LANES), 1)
    tiles = -(-5 * size // LANES)

    def join(lane, middle, low, high, at):
        sides = jnp.where(lane >= LANES - 8, roll(low, LANES - 8 - at, -1), 0.0)
        sides = jnp.where(lane < size + 8, roll(high, size - at, -1), sides)
        return jnp.where(lane < size, middle, sides)

    def group(g, slots, get, first):
        low = jnp.where(even_z, z_odd[g], z_even[g])
        high = jnp.where(even_z, z_even[g], z_odd[g])
        by_even = jnp.where(even_z, eo[g], ee[g]), jnp.where(even_z, ee[g], eo[g])
        by_odd = jnp.where(even_z, oo[g], oe[g]), jnp.where(even_z, oe[g], oo[g])
        corners = (
            [jnp.where(even_y, e, o) for e, o in zip(by_even, by_odd)],
            [jnp.where(even_y, o, e) for e, o in zip(by_even, by_odd)],
        )
        for s in range(slots):
            e, o = y_even[3 * g + s], y_odd[3 * g + s]
            ends = jnp.where(even_y, e, o), jnp.where(even_y, o, e)
            ends = [[end[8 * t : 8 * t + 8] for t in range(tiles)] for end in ends]
            for k in range(5):
                at = 40 * s + 8 * k
                stack[k, first + s, 0:size, :] = join(lane, get(k, s), low, high, at)
                for which in range(2):
                    rows = slice(size + 8 * which, size + 8 * which + 8)
                    middle = y_unpack(ends[which], k, size)
                    stack[k, first + s, rows, :] = join(lane_8, middle, *corners[which], at)

    def body(g, carry):
        group(g, 3, lambda k, s: own(k, 3 * g + s), 3 * g)
        return carry

    lax.fori_loop(0, size // 3, body, 0)
    for q in range(3):
        group(
            size // 3 + q,
            min(3, 8 - 3 * q),
            lambda k, s: beside(k, 3 * q + s),
            size + gx + 3 * q,
        )
    empty = size + 8 * (1 - gx)
    for k in range(5):
        stack[k, empty] = jnp.zeros(stack.shape[2:], jnp.float32)


def pack_y(own, beside, size, y_even, y_odd):
    _, gy, _ = places()
    even_y = gy % 2 == 0

    def plane(at, get):
        values = [get(k) for k in range(5)]
        high = y_pack([v[size - 8 :] for v in values], size)
        low = y_pack([v[:8] for v in values], size)
        for t, (h, l) in enumerate(zip(high, low)):
            y_even[at, 8 * t : 8 * t + 8, :] = jnp.where(even_y, h, l)
            y_odd[at, 8 * t : 8 * t + 8, :] = jnp.where(even_y, l, h)

    def body(g, carry):
        for u in range(8):
            plane(8 * g + u, lambda k: own(k, 8 * g + u))
        return carry

    lax.fori_loop(0, size // 8, body, 0)
    for j in range(8):
        plane(size + j, lambda k: beside(k, j))


def merge_y(stack, own, beside, size, y_even, y_odd, z_even, z_odd):
    gx, gy, gz = places()
    even_y, even_z = gy % 2 == 0, gz % 2 == 0
    rows = size + 16
    lane = iota((rows, LANES), 1)
    tiles = -(-5 * size // LANES)

    def group(g, slots, get, first):
        top = jnp.zeros((rows, LANES), jnp.float32)
        bottom = top
        for s in range(slots):
            e, o = y_even[3 * g + s], y_odd[3 * g + s]
            ends = jnp.where(even_y, e, o), jnp.where(even_y, o, e)
            ends = [[end[8 * t : 8 * t + 8] for t in range(tiles)] for end in ends]
            for k in range(5):
                parts = [get(k, s)] + [y_unpack(end, k, size) for end in ends]
                v = jnp.where(lane < size, jnp.concatenate(parts, axis=0), 0.0)
                stack[k, first + s] = v
                at = 40 * s + 8 * k
                here = (lane >= at) & (lane < at + 8)
                top = jnp.where(here, roll(v, at - (size - 8), -1), top)
                bottom = jnp.where(here, roll(v, at, -1), bottom)
        z_even[g] = jnp.where(even_z, top, bottom)
        z_odd[g] = jnp.where(even_z, bottom, top)

    def body(g, carry):
        group(g, 3, lambda k, s: own(k, 3 * g + s), 3 * g)
        return carry

    lax.fori_loop(0, size // 3, body, 0)
    for q in range(3):
        group(
            size // 3 + q,
            min(3, 8 - 3 * q),
            lambda k, s: beside(k, 3 * q + s),
            size + gx + 3 * q,
        )
    empty = size + 8 * (1 - gx)
    for k in range(5):
        stack[k, empty] = jnp.zeros(stack.shape[2:], jnp.float32)


def merge_z(stack, size, z_even, z_odd):
    gx, _, gz = places()
    even_z = gz % 2 == 0
    lane = iota((size + 16, LANES), 1)

    def group(g, slots, first):
        low = jnp.where(even_z, z_odd[g], z_even[g])
        high = jnp.where(even_z, z_even[g], z_odd[g])
        for s in range(slots):
            for k in range(5):
                at = 40 * s + 8 * k
                v = stack[k, first + s]
                v = jnp.where(lane >= LANES - 8, roll(low, LANES - 8 - at, -1), v)
                here = (lane >= size) & (lane < size + 8)
                stack[k, first + s] = jnp.where(here, roll(high, size - at, -1), v)

    def body(g, carry):
        group(g, 3, 3 * g)
        return carry

    lax.fori_loop(0, size // 3, body, 0)
    for q in range(3):
        group(size // 3 + q, min(3, 8 - 3 * q), size + gx + 3 * q)


def payload_shapes(size):
    groups = size // 3 + 3
    tall = 8 * (-(-5 * size // LANES))
    y = near(size + 8, tall, LANES)
    z = near(groups, size, LANES)
    c = near(groups, 8, LANES)
    return [y, y, z, z, c, c, c, c]


def partner(index, parity, count):
    if parity is None:
        return index
    other = index + 1 if index % 2 == parity else index - 1
    return other if 0 <= other < count else None


def swap(value, parity_y, parity_z):
    pairs = []
    for y in range(COUNT_Y):
        for z in range(COUNT_Z):
            to_y, to_z = partner(y, parity_y, COUNT_Y), partner(z, parity_z, COUNT_Z)
            if to_y is not None and to_z is not None:
                pairs.append((y * COUNT_Z + z, to_y * COUNT_Z + to_z))
    return lax.ppermute(value, YZ, pairs)


WAYS = ((0, None), (1, None), (None, 0), (None, 1), (0, 0), (0, 1), (1, 0), (1, 1))


def swap_cores(value):
    return lax.ppermute(value, "gx", [(0, 1), (1, 0)])


def f32(*shape):
    return jax.ShapeDtypeStruct(shape, jnp.float32)


def near(*shape):
    return pltpu.VMEM(shape, jnp.float32)


def call(body, outs, ins, scratch, operands, limit, aliases={}):
    held = [
        pltpu.with_memory_space_constraint(v, pltpu.VMEM) if spec is held_near else v
        for v, spec in zip(operands, ins)
    ]
    return pl.pallas_call(
        body,
        out_shape=outs,
        out_specs=[vmem] * len(outs),
        in_specs=ins,
        scratch_shapes=scratch,
        input_output_aliases=aliases,
        compiler_params=pltpu.CompilerParams(vmem_limit_bytes=limit * 2**20),
    )(*held)


def edge_kernel(right, faces, cells, out, sems):
    gx = lax.axis_index("gx")
    start = (1 - gx) * (SIZES[0] - WIDTH)
    part = pl.ds(start, WIDTH)
    copies = [
        pltpu.make_async_copy(right.at[part], out.at[0], sems.at[0]),
        pltpu.make_async_copy(faces.at[0, part], out.at[1], sems.at[1]),
        pltpu.make_async_copy(faces.at[1, part], out.at[2], sems.at[2]),
        pltpu.make_async_copy(faces.at[2, part], out.at[3], sems.at[3]),
        pltpu.make_async_copy(cells.at[part], out.at[4], sems.at[4]),
    ]
    for copy in copies:
        copy.start()
    for copy in copies:
        copy.wait()


def own_inputs(right, faces, cells):
    def own(k, i):
        if k == 0:
            return widen(right[i])
        return widen(cells[i] if k == 4 else faces[k - 1, i])

    return own


def pack_0_kernel(right, faces, cells, beside, *outs):
    pack(own_inputs(right, faces, cells), lambda k, j: widen(beside[k, j]), SIZES[0], outs)


def pack_1_kernel(own, beside, held, y_even, y_odd):
    pack_y(lambda k, i: own[k, i], lambda k, j: beside[k, j], SIZES[1], y_even, y_odd)


def merge_1_kernel(own, beside, y_even, y_odd, stack, z_even, z_odd):
    merge_y(
        stack,
        lambda k, i: own[k, i],
        lambda k, j: beside[k, j],
        SIZES[1],
        y_even,
        y_odd,
        z_even,
        z_odd,
    )


def level_0_kernel(
    right, faces, cells, beside, ye, yo, ze, zo, ee, eo, oe, oo,
    coarse, coarse_edge, stack, iterate,
    update, rows, pairs,
):
    size = SIZES[0]
    planes = size + 9
    gx = lax.axis_index("gx")
    unpack(
        stack,
        own_inputs(right, faces, cells),
        lambda k, j: widen(beside[k, j]),
        size,
        (ye, yo, ze, zo, ee, eo, oe, oo),
    )
    down(stack, iterate, update, 1.0, planes, planes, Wrapped)
    keep_remainder(stack, iterate, update, 1.0, planes, size, Wrapped)

    def out(k, value):
        coarse[k] = value
        coarse_edge[k] = jnp.where(gx == 0, value[16:24], value[0:8])

    coarsen(stack, update, rows, pairs, out, size, size)


def level_1_kernel(
    filled, z_even, z_odd, held,
    coarse, stack, iterate,
    update, rows, pairs, made,
):
    size = SIZES[1]
    planes = size + 9
    merge_z(stack, size, z_even, z_odd)
    down(stack, iterate, update, 0.25, planes, planes, Wrapped)
    keep_remainder(stack, iterate, update, 0.25, planes, size, Wrapped)

    def out(k, value):
        made[k] = value

    coarsen(stack, update, rows, pairs, out, size, size)
    for i in range(SIZES[2] // 2):
        line = made[0, 2 * i] + roll(made[0, 2 * i + 1], LANES // 2, -1)
        for h in range(2):
            for k in range(1, 5):
                line = line + roll(made[k, 2 * i + h], LANES // 2 * h + SIZES[2] * k, -1)
        coarse[i] = line


def level_2_kernel(
    mine, other, held,
    payload, stack, iterate,
    update, rows, pairs, made, lines,
):
    size = SIZES[2]
    planes = 2 * size + 1
    gx, gy, gz = places()
    even_y, even_z = gy % 2 == 0, gz % 2 == 0
    lane = iota((16, LANES), 1)
    bases = (0, size, LANES - size)
    half = size // 2
    for k in range(5):
        stack[k, 2 * size] = jnp.zeros(stack.shape[2:], jnp.float32)

    def body(i, carry):
        for core in range(2):

            def block(a, b):
                at = half * (3 * b + a) + i
                return jnp.where(gx == core, mine[at], other[at])

            columns = []
            for b in range(3):
                even, odd = block(1, b), block(2, b)
                columns.append(
                    (block(0, b), jnp.where(even_y, even, odd), jnp.where(even_y, odd, even))
                )
            columns = [columns[0]] + [
                [jnp.where(even_z, p, q) for p, q in zip(columns[c], columns[3 - c])] for c in (1, 2)
            ]
            for h in range(2):
                plane = size * core + 2 * i + h
                for k in range(5):
                    source = (LANES // 2) * h + size * k
                    stack[k, plane, 24:32, :] = jnp.zeros((8, LANES), jnp.float32)
                    for a, first in enumerate((0, size, 40 - size)):
                        line = jnp.zeros((16, LANES), jnp.float32)
                        for b, base in enumerate(bases):
                            here = (lane >= base) & (lane < base + size)
                            line = jnp.where(here, roll(columns[b][a], base - source, -1), line)
                        stack[k, plane, first : first + size, :] = line[:size]
        return carry

    lax.fori_loop(0, half, body, 0)
    weight = 0.0625
    iterate[2 * size] = jnp.zeros(iterate.shape[1:], jnp.float32)
    down(stack, iterate, update, weight, planes, 2 * size, Wrapped)
    keep_remainder(stack, iterate, update, weight, planes, 2 * size, Wrapped)

    def out(k, value):
        made[k * 96 : k * 96 + 96, :] = value.reshape(96, LANES)

    coarsen(stack, update, rows, pairs, out, 2 * size, size)
    line = jnp.zeros((60, LANES), jnp.float32)
    for y in range(6):
        line = line + roll(made[pl.ds(y, 60, stride=8), :], 6 * y, -1)
    lines[0:60, :] = line
    chunk = lines[0:20, :] + roll(lines[20:40, :], 40, -1) + roll(lines[40:60, :], 80, -1)
    chunk = jnp.concatenate([chunk, jnp.zeros((4, LANES), jnp.float32)], axis=0)

    def repeat(c, carry):
        payload[pl.ds(pl.multiple_of(c * CHUNK, 8), CHUNK), :] = chunk
        return carry

    lax.fori_loop(0, COLUMNS, repeat, 0)


def compact(value):
    row = iota(value.shape, -2)
    out = jnp.where(row == 0, value, 0.0)
    out = jnp.where(row == 1, roll(value, -1, -2), out)
    return jnp.where(row == 2, roll(value, -2, -2), out)


def bottom(source, faces, cells):
    weight = 0.25**4
    move = Columns(3)
    face_x, face_y, face_z = faces
    nothing = jnp.zeros((1,) + source.shape[1:], jnp.float32)

    def apply(v):
        flux_x = face_x * (v - jnp.concatenate([nothing, v[:-1]], axis=0))
        flux_y = face_y * (v - move.low_y(v))
        flux_z = face_z * (v - move.low_z(v))
        total = flux_x - jnp.concatenate([flux_x[1:], nothing], axis=0)
        total = total + (flux_y - move.up_y(flux_y)) + (flux_z - move.up_z(flux_z))
        return cells * v + weight * total

    def total_of(v):
        flat = jnp.sum(jnp.sum(v, axis=0), axis=0)
        one = jnp.sum(jnp.sum(flat, axis=0, keepdims=True), axis=1, keepdims=True)
        return jnp.broadcast_to(one, flat.shape)

    iterate = jnp.zeros_like(source)
    remainder = source
    search = source
    norm_now = total_of(remainder * remainder)
    for step in range(BOTTOM):
        applied = apply(search)
        size = norm_now / total_of(search * applied)
        iterate = iterate + size * search
        if step + 1 < BOTTOM:
            remainder = remainder - size * applied
            norm_next = total_of(remainder * remainder)
            search = remainder + (norm_next / norm_now) * search
            norm_now = norm_next
    return iterate


def rise_kernel(
    gathered, stack_2, base_2, stack_1, base_1, stack_0, base_0,
    solution_out, residual_out, sums,
    iterate_0, update_0, rows_0, spare_1,
    iterate_1, update_1, rows_1, spare_2,
    iterate_2, update_2, rows_2, spare_3,
    stack_3, iterate_3, update_3, turned, table, block_3,
):
    gx, gy, gz = places()

    stack_3[...] = jnp.zeros(stack_3.shape, jnp.float32)
    blank = jnp.zeros((LANES - COLUMNS, LANES), jnp.float32)
    for r in range(20):
        part = gathered[pl.ds(r, COLUMNS, stride=CHUNK), :]
        turned[...] = jnp.transpose(jnp.concatenate([part, blank], axis=0))
        for j in range(3):
            k, x = divmod(20 * j + r, 12)
            for y in range(6):
                stack_3[k, x, y, 0:6, :] = turned[40 * j + 6 * y : 40 * j + 6 * y + 6, :]
    move = Columns(6)
    weight = 0.25**3
    iterate_3[12] = jnp.zeros(iterate_3.shape[1:], jnp.float32)
    down(stack_3, iterate_3, update_3, weight, 13, 12, move)
    keep_remainder(stack_3, iterate_3, update_3, weight, 13, 12, move)

    def coarse(k, x_pair, y_pair, z_pair, scale):
        planes = []
        for x in range(6):
            read = (lambda i: update_3[i]) if k == 0 else (lambda i: stack_3[k, i])
            v = read(2 * x)
            if x_pair:
                v = v + read(2 * x + 1)
            lines = []
            for y in range(3):
                line = v[2 * y]
                if y_pair:
                    line = line + v[2 * y + 1]
                if z_pair:
                    line = line + roll(line, -1, -2)
                lines.append(scale * compact(line))
            planes.append(jnp.stack(lines))
        return jnp.stack(planes)

    lowest = bottom(
        coarse(0, True, True, True, 0.125),
        (
            coarse(1, False, True, True, 0.25),
            coarse(2, True, False, True, 0.25),
            coarse(3, True, True, False, 0.25),
        ),
        coarse(4, True, True, True, 0.125),
    )
    row = iota((8, LANES), 0)
    for x in range(6):
        for y in range(3):
            line = lowest[x, y]
            wide = jnp.where(row == 0, line, 0.0)
            for to in range(1, 6):
                wide = jnp.where(row == to, roll(line, to - to // 2, -2), wide)
            for a in range(2):
                for b in range(2):
                    iterate_3[2 * x + a, 2 * y + b] = iterate_3[2 * x + a, 2 * y + b] + wide
    up(stack_3, iterate_3, update_3, weight, 13, 12, move)

    low_rows = jnp.zeros((32, LANES), jnp.float32)
    for q in range(6):
        two = [iterate_3[2 * q + h].reshape(48, LANES) for h in range(2)]
        table[q] = jnp.transpose(jnp.concatenate(two + [low_rows], axis=0))
    block_3[...] = jnp.zeros(block_3.shape, jnp.float32)
    lane = iota((8, LANES), 1)

    def place(q, carry):
        for a, first in ((0, 0), (1, 6), (-1, 18)):
            lines = [jnp.zeros((8, LANES), jnp.float32) for _ in range(2)]
            for b, base in ((0, 0), (1, 6), (-1, LANES - 6)):
                y, z = gy + a, gz + b
                inside = (y >= 0) & (y < COUNT_Y) & (z >= 0) & (z < COUNT_Z)
                at = jnp.where(inside, y * COUNT_Z + z, 0)
                here = (lane >= base) & (lane < base + 6) & inside
                found = jnp.broadcast_to(table[q, pl.ds(at, 1), :], (8, LANES))
                for h in range(2):
                    for y_in in range(6):
                        moved = roll(found, base - 48 * h - 8 * y_in, -1)
                        lines[h] = jnp.where(here & (row == y_in), moved, lines[h])
            for h in range(2):
                block_3[2 * q + h, first : first + 6, :] = lines[h][0:6]
        return carry

    lax.fori_loop(0, 6, place, 0)

    spread(
        block_3, spare_3, rows_2, base_2, iterate_2,
        ((0, 12, 0), (18, 6, 28)),
        ((12, lambda i: i, lambda i: 2 * i),),
        24,
    )
    up(stack_2, iterate_2, update_2, 0.0625, 25, 24, Wrapped)

    size = SIZES[1]
    spread(
        iterate_2, spare_2, rows_1, base_1, iterate_1,
        ((0, 16, 0), (36, 4, 32)),
        (
            (12, lambda i: 12 * gx + i, lambda i: 2 * i),
            (4, lambda i: 12 - 4 * gx + i, lambda i: size + gx + 2 * i),
        ),
        size + 8 * (1 - gx),
    )
    up(stack_1, iterate_1, update_1, 0.25, size + 9, size + 9, Wrapped)

    size = SIZES[0]
    spread(
        iterate_1, spare_1, rows_0, base_0, iterate_0,
        ((0, 28, 0), (36, 4, 56)),
        (
            (24, lambda i: i, lambda i: 2 * i),
            (4, lambda i: 24 + 5 * gx + i, lambda i: size + gx + 2 * i),
        ),
        size + 8 * (1 - gx),
    )
    planes = size + 9
    up(stack_0, iterate_0, update_0, 1.0, planes, planes, Wrapped)
    iterate_0[planes] = iterate_0[0]
    mask = iota((size, LANES), 1) < size

    def use(i, v, remainder, carry):
        solution_out[i] = v[0:size, 0:size]
        residual_out[i] = remainder[0:size, 0:size]
        mine = jnp.where(mask, remainder[0:size], 0.0)
        given = jnp.where(mask, stack_0[0, i, 0:size, :], 0.0)
        return carry[0] + mine * mine, carry[1] + given * given

    zero = jnp.zeros((size, LANES), jnp.float32)
    squares = stencil_pass(stack_0, iterate_0, 1.0, planes, size, Wrapped, use, (zero, zero))
    ones = []
    for square in squares:
        one = jnp.sum(jnp.sum(square, axis=0, keepdims=True), axis=1, keepdims=True)
        ones.append(jnp.broadcast_to(one, (8, LANES)))
    sums[...] = jnp.where(lane == 0, ones[0], jnp.where(lane == 1, ones[1], 0.0))


def stack_kernel(*refs):
    out = refs[-1]
    for n, ref in enumerate(refs[:-1]):
        count = ref.shape[0]
        out[n * count : n * count + count] = ref[...]


def stacked(*parts):
    count, *rest = parts[0].shape
    return call(stack_kernel, [near(len(parts) * count, *rest)], [held_near] * 3, [], parts, 1)[0]


def shards(right, faces, cells):
    dma = pltpu.SemaphoreType.DMA
    edge = call(edge_kernel, [near(5, WIDTH, 48, 48)], [far] * 3, [dma((5,))],
        (right, faces, cells), 2)[0]
    beside = swap_cores(edge)
    outs = call(pack_0_kernel, payload_shapes(48), [held_near] * 4, [],
        (right, faces, cells, beside), 6)
    moved = [swap(v, *way) for v, way in zip(outs, WAYS)]
    coarse, coarse_edge, stack_0, iterate_0 = call(
        level_0_kernel,
        [near(5, 24, 24, LANES), near(5, WIDTH, 24, LANES), near(7, 58, 64, LANES), near(58, 64, LANES)],
        [held_near] * 12,
        [near(58, 64, LANES), near(5, 64, LANES), near(5, 24, 24, LANES)],
        (right, faces, cells, beside, *moved),
        12,
    )
    beside = swap_cores(coarse_edge)
    outs = call(pack_1_kernel, [near(32, 8, LANES)] * 2, [held_near] * 3, [], (coarse, beside, stack_0), 4)
    y_sides = [swap(v, parity, None) for parity, v in enumerate(outs)]
    filled, *outs = call(
        merge_1_kernel,
        [near(7, 34, 40, LANES), near(11, 40, LANES), near(11, 40, LANES)],
        [held_near] * 4,
        [],
        (coarse, beside, *y_sides),
        4,
    )
    z_sides = [swap(v, None, parity) for parity, v in enumerate(outs)]
    coarse, stack_1, iterate_1 = call(
        level_1_kernel,
        [near(6, 16, LANES), near(7, 34, 40, LANES), near(34, 40, LANES)],
        [held_near] * 4,
        [near(34, 40, LANES), near(5, 40, LANES), near(5, 12, 16, LANES), near(5, 12, 16, LANES)],
        (filled, *z_sides, stack_0),
        12,
        {0: 1},
    )
    column = stacked(coarse, *[swap(coarse, parity, None) for parity in (0, 1)])
    region = stacked(column, *[swap(column, None, parity) for parity in (0, 1)])
    other = swap_cores(region)
    payload, stack_2, iterate_2 = call(
        level_2_kernel,
        [near(COLUMNS * CHUNK, LANES), near(7, 26, 40, LANES), near(26, 40, LANES)],
        [held_near] * 3,
        [near(26, 40, LANES), near(5, 40, LANES), near(5, 12, 8, LANES), near(480, LANES), near(64, LANES)],
        (region, other, stack_0),
        12,
    )
    payload = payload.reshape(COLUMNS, CHUNK, LANES)
    gathered = lax.all_to_all(payload, YZ, 0, 0).reshape(COLUMNS * CHUNK, LANES)
    solved, residual, sums = call(
        rise_kernel,
        [f32(48, 48, 48), f32(48, 48, 48), f32(8, LANES)],
        [held_near] * 7,
        [
            near(58, 64, LANES), near(58, 64, LANES), near(64, LANES), near(33, 40, LANES),
            near(34, 40, LANES), near(34, 40, LANES), near(40, LANES), near(24, 40, LANES),
            near(26, 40, LANES), near(26, 40, LANES), near(40, LANES), near(12, 24, LANES),
            near(8, 14, 6, 8, LANES), near(14, 6, 8, LANES), near(14, 6, 8, LANES),
            near(LANES, LANES), near(6, LANES, LANES), near(12, 24, LANES),
        ],
        (gathered, stack_2, iterate_2, stack_1, iterate_1, stack_0, iterate_0),
        24,
    )
    each = jnp.broadcast_to(sums[0:1].reshape(1, 1, LANES), (128, 1, LANES))
    total = jnp.sum(lax.all_to_all(each, ALL, 0, 0), axis=(0, 1))
    return solved, residual, jnp.sqrt(total[0] / total[1])


def solution(mesh):
    torus = Mesh(
        mesh.devices.reshape(mesh.shape["gx"], mesh.shape["gy"], 4, 4), ("gx", "gy", "gz_0", "gz_1")
    )
    in_specs = (P("gx", "gy", GZ), P(None, "gx", "gy", GZ), P("gx", "gy", GZ))
    out_specs = (P("gx", "gy", GZ), P("gx", "gy", GZ), P())
    return jax.shard_map(
        shards, mesh=torus, in_specs=in_specs, out_specs=out_specs, check_vma=False
    )
```

```python
import functools

import jax
import jax.numpy as jnp
from jax import lax
from jax.experimental import pallas as pl
from jax.experimental.pallas import tpu as pltpu
from jax.sharding import Mesh
from jax.sharding import PartitionSpec as P

BOTTOM = 6
ALL = ("gx", "gy", "gz_0", "gz_1")
YZ = ("gy", "gz_0", "gz_1")
GZ = ("gz_0", "gz_1")
LANES = 128
WIDTH = 8
COUNT_Y = 4
COUNT_Z = 16
COLUMNS = COUNT_Y * COUNT_Z
SIZES = (48, 24, 12, 6)
CHUNK = 24
GROUP = 3
HALF = 30

theta = 1.125
delta = 0.875
sigma = theta / delta
rho_0 = 1.0 / sigma
rho_1 = 1.0 / (2.0 * sigma - rho_0)
rho_2 = 1.0 / (2.0 * sigma - rho_1)
FIRST = (0.0, 1.0 / theta)
LATER = ((rho_1 * rho_0, 2.0 * rho_1 / delta), (rho_2 * rho_1, 2.0 * rho_2 / delta))

vmem = pl.BlockSpec(memory_space=pltpu.VMEM)
held_near = pl.BlockSpec(memory_space=pltpu.VMEM)
far = pl.BlockSpec(memory_space=pltpu.HBM)


def roll(value, by, axis):
    axis = axis % value.ndim
    by = by % value.shape[axis]
    return pltpu.roll(value, by, axis) if by else value


def iota(shape, dim):
    return lax.broadcasted_iota(jnp.int32, shape, dim % len(shape))


def exact_dot(left, right):
    return jnp.dot(
        left, right, precision=lax.Precision.HIGHEST, preferred_element_type=jnp.float32
    )


class Wrapped:
    @staticmethod
    def turn(v):
        return v

    @staticmethod
    def low_y(v):
        return roll(v, 1, -2)

    @staticmethod
    def up_y(v):
        return roll(v, -1, -2)

    @staticmethod
    def low_z(v):
        return roll(v, 1, -1)

    @staticmethod
    def up_z(v):
        return roll(v, -1, -1)


class Halves(Wrapped):
    @staticmethod
    def turn(v):
        return roll(v, LANES // 2, -1)


class Columns:
    def __init__(self, cells):
        self.cells = cells

    def turn(self, v):
        return v

    def low_y(self, v):
        lane = iota(v.shape, -1)
        last = lax.slice_in_dim(v, self.cells - 1, self.cells, axis=v.ndim - 3)
        rest = lax.slice_in_dim(v, 0, self.cells - 1, axis=v.ndim - 3)
        lane = iota(last.shape, -1)
        last = jnp.where((lane >= COUNT_Z) & (lane < COLUMNS), roll(last, COUNT_Z, -1), 0.0)
        return jnp.concatenate([last, rest], axis=v.ndim - 3)

    def up_y(self, v):
        first = lax.slice_in_dim(v, 0, 1, axis=v.ndim - 3)
        rest = lax.slice_in_dim(v, 1, self.cells, axis=v.ndim - 3)
        lane = iota(first.shape, -1)
        first = jnp.where(lane < COLUMNS - COUNT_Z, roll(first, -COUNT_Z, -1), 0.0)
        return jnp.concatenate([rest, first], axis=v.ndim - 3)

    def low_z(self, v):
        lane, row = iota(v.shape, -1), iota(v.shape, -2)
        edge = roll(roll(v, 1 - self.cells, -2), 1, -1)
        edge = jnp.where((lane % COUNT_Z != 0) & (lane < COLUMNS), edge, 0.0)
        return jnp.where(row == 0, edge, roll(v, 1, -2))

    def up_z(self, v):
        lane, row = iota(v.shape, -1), iota(v.shape, -2)
        edge = roll(roll(v, self.cells - 1, -2), -1, -1)
        edge = jnp.where((lane % COUNT_Z != COUNT_Z - 1) & (lane < COLUMNS), edge, 0.0)
        inner = jnp.where(row < self.cells - 1, roll(v, -1, -2), 0.0)
        return jnp.where(row == self.cells - 1, edge, inner)


def set_up(stack, weight, planes, count, move, start=None):
    stack[1, planes] = move.turn(stack[1, 0])

    def moved(i):
        return [move.up_z(stack[3, i + u]) for u in range(GROUP)]

    def body(g, above_z):
        i = GROUP * g
        later = moved(jnp.minimum(i + GROUP, count - GROUP))
        for u in range(GROUP):
            at = i + u
            cell, face_y = stack[4, at], stack[2, at]
            above_y = move.up_y(face_y)
            if stack.shape[0] > 7:
                stack[7, at] = above_y
            stack[6, at] = above_z[u]
            total = stack[1, at] + stack[1, at + 1] + face_y + above_y
            total = total + stack[3, at] + above_z[u]
            inverse = jnp.where(cell > 0.0, 1.0 / (cell + weight * total), 0.0)
            stack[5, at] = inverse
            if start is not None:
                step = FIRST[1] * (inverse * stack[0, at])
                for ref in start:
                    ref[at] = step
        return later

    lax.fori_loop(0, count // GROUP, body, moved(0))


def stencil_pass(stack, iterate, weight, planes, count, move, use, carry):
    flux = stack[1, 0] * (iterate[0] - move.turn(iterate[planes - 1]))
    by_face = stack.shape[0] > 7

    def moved(i):
        out = []
        for u in range(GROUP):
            v = iterate[i + u]
            out += [move.low_z(v), move.up_z(v)]
            if by_face:
                out += [move.low_y(v), move.up_y(v)]
        return out

    def body(g, state):
        flux, near_by, carry = state
        i = GROUP * g
        later = moved(jnp.minimum(i + GROUP, count - GROUP))
        values = [iterate[i + u] for u in range(GROUP + 1)]
        each = len(near_by) // GROUP
        for u in range(GROUP):
            at, v = i + u, values[u]
            sides = near_by[each * u : each * u + each]
            above = stack[1, at + 1] * (values[u + 1] - v)
            total = flux - above
            flux = above
            if by_face:
                total = total + stack[2, at] * (v - sides[2]) + stack[7, at] * (v - sides[3])
            else:
                flux_y = stack[2, at] * (v - move.low_y(v))
                total = total + (flux_y - move.up_y(flux_y))
            total = total + stack[3, at] * (v - sides[0]) + stack[6, at] * (v - sides[1])
            carry = use(at, v, stack[0, at] - (stack[4, at] * v + weight * total), carry)
        return flux, later, carry

    return lax.fori_loop(0, count // GROUP, body, (flux, moved(0), carry))[2]


def sweep(stack, iterate, update, weight, planes, count, move, factors):
    keep, gain = factors
    iterate[planes] = move.turn(iterate[0])

    def use(i, v, remainder, carry):
        step = gain * (stack[5, i] * remainder)
        if keep:
            step = keep * update[i] + step
        update[i] = step
        iterate[i] = v + step
        return carry

    stencil_pass(stack, iterate, weight, planes, count, move, use, 0)


def down(stack, iterate, update, weight, planes, count, move):
    set_up(stack, weight, planes, count, move, (iterate, update))
    for factors in LATER:
        sweep(stack, iterate, update, weight, planes, count, move, factors)


def up(stack, iterate, update, weight, planes, count, move):
    for factors in (FIRST,) + LATER:
        sweep(stack, iterate, update, weight, planes, count, move, factors)


def keep_remainder(stack, iterate, update, weight, planes, count, move):
    iterate[planes] = move.turn(iterate[0])

    def use(i, v, remainder, carry):
        update[i] = remainder
        return carry

    stencil_pass(stack, iterate, weight, planes, count, move, use, 0)


def coarsen(stack, remainder, rows, pairs, out, count, size, period=LANES, offset=0):
    half = size // 2

    def body(i, carry):
        for k in range(5):
            if k == 1:
                rows[k] = stack[1, 2 * i]
            elif k == 0:
                rows[k] = remainder[2 * i] + remainder[2 * i + 1]
            else:
                rows[k] = stack[k, 2 * i] + stack[k, 2 * i + 1]
        for k in range(5):
            pair = rows[k, pl.ds(0, half, stride=2), :]
            if k != 2:
                pair = pair + rows[k, pl.ds(1, half, stride=2), :]
            pairs[k, i, 0:half, :] = pair
        return carry

    if half % 8:
        pairs[...] = jnp.zeros(pairs.shape, jnp.float32)
    lax.fori_loop(0, count // 2, body, 0)
    fine, coarse = iota((LANES, LANES), 0), iota((LANES, LANES), 1)
    inside = fine % period - offset
    own = (inside >= 0) & (inside < size) & (fine // period == coarse // period)
    mean = jnp.where(own & (inside // 2 == coarse % period), 1.0, 0.0)
    even = jnp.where(own & (inside == 2 * (coarse % period)), 1.0, 0.0)
    _, planes, padded, _ = pairs.shape
    for k in range(5):
        flat = pairs[k].reshape(planes * padded, LANES)
        scale = 0.125 if k in (0, 4) else 0.25
        made = scale * exact_dot(flat, even if k == 3 else mean)
        out(k, made.reshape(planes, padded, LANES))


def spread(coarse, spare, rows, base, fine, row_map, plane_maps, empty):
    planes, height, _ = spare.shape
    source, target = iota((LANES, LANES), 0), iota((LANES, LANES), 1)
    half = target // 2
    pick = jnp.where(source == jnp.where(target < LANES // 2, half, LANES // 2 + half), 1.0, 0.0)
    wide = exact_dot(coarse[0:planes].reshape(planes * height, LANES), pick)
    spare[...] = wide.reshape(planes, height, LANES)
    rows[...] = jnp.zeros(rows.shape, jnp.float32)
    fine[empty] = rows[...]
    for count, plane_of, target_of in plane_maps:

        def body(i, carry):
            plane = plane_of(i)
            for start, number, first in row_map:
                part = spare[plane, start : start + number, :]
                rows[pl.ds(first, number, stride=2), :] = part
                rows[pl.ds(first + 1, number, stride=2), :] = part
            both = rows[...]
            at = target_of(i)
            fine[at] = base[at] + both
            fine[at + 1] = base[at + 1] + both
            return carry

        lax.fori_loop(0, count, body, 0)


def spread_halves(coarse, spare, rows, base, fine, gx):
    planes, height, _ = spare.shape
    source, target = iota((LANES, LANES), 0), iota((LANES, LANES), 1)
    wanted = (target % (LANES // 2)) // 2 + (LANES - 4)
    pick = jnp.where(source == wanted % LANES, 1.0, 0.0)
    wide = exact_dot(coarse[0:planes].reshape(planes * height, LANES), pick)
    spare[...] = wide.reshape(planes, height, LANES)
    lane = iota((height, LANES), 1)

    def body(q, carry):
        j = q - 9 - 2 * gx
        there = (q < 9) | ((j >= 0) & (j < 4))
        above = jnp.where(q < 9, q + 15, 24 + 5 * gx + jnp.clip(j, 0, 3))
        both = jnp.where(lane < LANES // 2, spare[q], jnp.where(there, spare[above], 0.0))
        for start, number, first in ((0, 28, 0), (36, 4, 56)):
            part = both[start : start + number]
            rows[pl.ds(first, number, stride=2), :] = part
            rows[pl.ds(first + 1, number, stride=2), :] = part
        wide_rows = rows[...]
        fine[2 * q] = base[2 * q] + wide_rows
        fine[2 * q + 1] = base[2 * q + 1] + wide_rows
        return carry

    lax.fori_loop(0, HALF // 2, body, 0)


def places():
    gx = lax.axis_index("gx")
    gy = lax.axis_index("gy")
    gz = lax.axis_index("gz_0") * 4 + lax.axis_index("gz_1")
    return gx, gy, gz


def widen(value):
    rows, lanes = value.shape
    if lanes == LANES:
        return value
    return jnp.concatenate([value, jnp.zeros((rows, LANES - lanes), jnp.float32)], axis=1)


def y_pack(parts, size):
    lane = iota((8, LANES), 1)
    tiles = [jnp.zeros((8, LANES), jnp.float32) for _ in range(-(-5 * size // LANES))]
    for k, part in enumerate(parts):
        start = k * size
        moved = roll(part, start % LANES, -1)
        for t in range(len(tiles)):
            a, b = max(start, t * LANES) - t * LANES, min(start + size, (t + 1) * LANES) - t * LANES
            if a < b:
                tiles[t] = jnp.where((lane >= a) & (lane < b), moved, tiles[t])
    return tiles


def y_unpack(tiles, k, size, to):
    lane = iota((8, LANES), 1)
    start = k * size
    t = start // LANES
    value = tiles[t]
    if start + size > (t + 1) * LANES:
        value = jnp.where(lane >= start - t * LANES, value, tiles[t + 1])
    return roll(value, to - start, -1)


def pack(own, beside, size, outs):
    y_even, y_odd, z_even, z_odd, ee, eo, oe, oo = outs
    _, gy, gz = places()
    even_y, even_z = gy % 2 == 0, gz % 2 == 0
    lane = iota((size, LANES), 1)

    def group(g, slots, get):
        top = jnp.zeros((size, LANES), jnp.float32)
        bottom = top
        for s in range(slots):
            high, low = [], []
            for k in range(5):
                v = get(k, s)
                at = 40 * s + 8 * k
                here = (lane >= at) & (lane < at + 8)
                top = jnp.where(here, roll(v, at - (size - 8), -1), top)
                bottom = jnp.where(here, roll(v, at, -1), bottom)
                high.append(v[size - 8 :])
                low.append(v[:8])
            for t, (h, l) in enumerate(zip(y_pack(high, size), y_pack(low, size))):
                y_even[3 * g + s, 8 * t : 8 * t + 8, :] = jnp.where(even_y, h, l)
                y_odd[3 * g + s, 8 * t : 8 * t + 8, :] = jnp.where(even_y, l, h)
        a, b = jnp.where(even_z, top, bottom), jnp.where(even_z, bottom, top)
        z_even[g] = a
        z_odd[g] = b
        ee[g] = jnp.where(even_y, a[size - 8 :], a[:8])
        eo[g] = jnp.where(even_y, b[size - 8 :], b[:8])
        oe[g] = jnp.where(even_y, a[:8], a[size - 8 :])
        oo[g] = jnp.where(even_y, b[:8], b[size - 8 :])

    def body(g, carry):
        group(g, 3, lambda k, s: own(k, 3 * g + s))
        return carry

    if own is not None:
        lax.fori_loop(0, size // 3, body, 0)
    if beside is not None:
        for q in range(3):
            group(size // 3 + q, min(3, 8 - 3 * q), lambda k, s: beside(k, 3 * q + s))


def place_halves(stack, own, beside, size):
    gx, _, _ = places()

    def put(p, low, high):
        for k in range(5):
            stack[k, p, 0:size, :] = roll(low(k), 8, -1) + roll(high(k), LANES // 2 + 8, -1)
            stack[k, p, size:, :] = jnp.zeros((16, LANES), jnp.float32)

    def both(g, carry):
        for u in range(3):
            p = 3 * g + u
            put(p, lambda k: own(k, p), lambda k: own(k, p + HALF))
        return carry

    lax.fori_loop(0, (size - HALF) // 3, both, 0)

    def one(p, carry):
        j = p - (size - HALF) - 4 * gx
        there = (j >= 0) & (j < 8)
        at = jnp.clip(j, 0, 7)
        put(p, lambda k: own(k, p), lambda k: jnp.where(there, beside(k, at), 0.0))
        return carry

    lax.fori_loop(size - HALF, HALF, one, 0)


def merge_halves(stack, size, payloads):
    y_even, y_odd, z_even, z_odd, ee, eo, oe, oo = payloads
    gx, gy, gz = places()
    even_y, even_z = gy % 2 == 0, gz % 2 == 0
    lane, lane_8 = iota((size, LANES), 1), iota((8, LANES), 1)
    tiles = -(-5 * size // LANES)

    def group(g, slots, first, base):
        def sides(lane, value, low, high, at):
            here = (lane >= base) & (lane < base + 8)
            value = jnp.where(here, roll(low, base - at, -1), value)
            here = (lane >= base + 56) & (lane < base + 64)
            return jnp.where(here, roll(high, base + 56 - at, -1), value)

        low = jnp.where(even_z, z_odd[g], z_even[g])
        high = jnp.where(even_z, z_even[g], z_odd[g])
        by_even = jnp.where(even_z, eo[g], ee[g]), jnp.where(even_z, ee[g], eo[g])
        by_odd = jnp.where(even_z, oo[g], oe[g]), jnp.where(even_z, oe[g], oo[g])
        corners = (
            [jnp.where(even_y, e, o) for e, o in zip(by_even, by_odd)],
            [jnp.where(even_y, o, e) for e, o in zip(by_even, by_odd)],
        )
        for s in range(slots):
            e, o = y_even[3 * g + s], y_odd[3 * g + s]
            ends = jnp.where(even_y, e, o), jnp.where(even_y, o, e)
            ends = [[end[8 * t : 8 * t + 8] for t in range(tiles)] for end in ends]
            for k in range(5):
                at = 40 * s + 8 * k
                v = stack[k, first + s, 0:size, :]
                stack[k, first + s, 0:size, :] = sides(lane, v, low, high, at)
                for which in range(2):
                    rows = slice(size + 8 * which, size + 8 * which + 8)
                    v = stack[k, first + s, rows, :]
                    middle = y_unpack(ends[which], k, size, base + 8)
                    here = (lane_8 >= base + 8) & (lane_8 < base + 56)
                    v = jnp.where(here, middle, v)
                    stack[k, first + s, rows, :] = sides(lane_8, v, *corners[which], at)

    def body_low(g, carry):
        group(g, 3, 3 * g, 0)
        return carry

    def body_high(g, carry):
        group(g + HALF // 3, 3, 3 * g, LANES // 2)
        return carry

    lax.fori_loop(0, HALF // 3, body_low, 0)
    lax.fori_loop(0, (size - HALF) // 3, body_high, 0)
    for q in range(3):
        first = size - HALF + 4 * gx + 3 * q
        group(size // 3 + q, min(3, 8 - 3 * q), first, LANES // 2)


def y_faces(values, size, at, y_even, y_odd):
    even_y = places()[1] % 2 == 0
    high = y_pack([v[size - 8 :] for v in values], size)
    low = y_pack([v[:8] for v in values], size)
    for t, (h, l) in enumerate(zip(high, low)):
        y_even[at, 8 * t : 8 * t + 8, :] = jnp.where(even_y, h, l)
        y_odd[at, 8 * t : 8 * t + 8, :] = jnp.where(even_y, l, h)


def z_faces(planes, size):
    even_z = places()[2] % 2 == 0
    rows = planes[0][0].shape[0]
    lane = iota((rows, LANES), 1)
    top = jnp.zeros((rows, LANES), jnp.float32)
    bottom = top
    for s, values in enumerate(planes):
        for k, v in enumerate(values):
            at = 40 * s + 8 * k
            here = (lane >= at) & (lane < at + 8)
            top = jnp.where(here, roll(v, at - (size - 8), -1), top)
            bottom = jnp.where(here, roll(v, at, -1), bottom)
    return jnp.where(even_z, top, bottom), jnp.where(even_z, bottom, top)


def y_sides(source, size, slots, stack, first, y_even, y_odd):
    even_y = places()[1] % 2 == 0
    lane = iota((16, LANES), 1)
    tiles = -(-5 * size // LANES)
    planes = []
    for s in range(slots):
        e, o = y_even[3 * source + s], y_odd[3 * source + s]
        ends = jnp.where(even_y, e, o), jnp.where(even_y, o, e)
        ends = [[end[8 * t : 8 * t + 8] for t in range(tiles)] for end in ends]
        values = []
        for k in range(5):
            v = jnp.concatenate([y_unpack(end, k, size, 0) for end in ends], axis=0)
            v = jnp.where(lane < size, v, 0.0)
            stack[k, first + s, size : size + 16, :] = v
            values.append(v)
        planes.append(values)
    return planes


def merge_z(stack, size, z_even, z_odd):
    gx, _, gz = places()
    even_z = gz % 2 == 0
    lane = iota((size + 16, LANES), 1)

    def group(g, slots, first):
        low = jnp.where(even_z, z_odd[g], z_even[g])
        high = jnp.where(even_z, z_even[g], z_odd[g])
        for s in range(slots):
            for k in range(5):
                at = 40 * s + 8 * k
                v = stack[k, first + s]
                v = jnp.where(lane >= LANES - 8, roll(low, LANES - 8 - at, -1), v)
                here = (lane >= size) & (lane < size + 8)
                stack[k, first + s] = jnp.where(here, roll(high, size - at, -1), v)

    def body(g, carry):
        group(g, 3, 3 * g)
        return carry

    lax.fori_loop(0, size // 3, body, 0)
    for q in range(3):
        group(size // 3 + q, min(3, 8 - 3 * q), size + gx + 3 * q)


def payload_shapes(size):
    groups = size // 3 + 3
    tall = 8 * (-(-5 * size // LANES))
    y = near(size + 8, tall, LANES)
    z = near(groups, size, LANES)
    c = near(groups, 8, LANES)
    return [y, y, z, z, c, c, c, c]


def partner(index, parity, count):
    if parity is None:
        return index
    other = index + 1 if index % 2 == parity else index - 1
    return other if 0 <= other < count else None


def swap(value, parity_y, parity_z):
    pairs = []
    for y in range(COUNT_Y):
        for z in range(COUNT_Z):
            to_y, to_z = partner(y, parity_y, COUNT_Y), partner(z, parity_z, COUNT_Z)
            if to_y is not None and to_z is not None:
                pairs.append((y * COUNT_Z + z, to_y * COUNT_Z + to_z))
    return lax.ppermute(value, YZ, pairs)


WAYS = ((0, None), (1, None), (None, 0), (None, 1), (0, 0), (0, 1), (1, 0), (1, 1))


def swap_cores(value):
    return lax.ppermute(value, "gx", [(0, 1), (1, 0)])


def f32(*shape):
    return jax.ShapeDtypeStruct(shape, jnp.float32)


def near(*shape):
    return pltpu.VMEM(shape, jnp.float32)


def call(body, outs, ins, scratch, operands, limit, aliases={}):
    held = [
        pltpu.with_memory_space_constraint(v, pltpu.HBM if spec is far else pltpu.VMEM)
        for v, spec in zip(operands, ins)
    ]
    return pl.pallas_call(
        body,
        out_shape=outs,
        out_specs=[vmem] * len(outs),
        in_specs=ins,
        scratch_shapes=scratch,
        input_output_aliases=aliases,
        compiler_params=pltpu.CompilerParams(vmem_limit_bytes=limit * 2**20),
    )(*held)


def edge_kernel(right, faces, cells, out, sems):
    gx = lax.axis_index("gx")
    start = (1 - gx) * (SIZES[0] - WIDTH)
    part = pl.ds(start, WIDTH)
    copies = [
        pltpu.make_async_copy(right.at[part], out.at[0], sems.at[0]),
        pltpu.make_async_copy(faces.at[0, part], out.at[1], sems.at[1]),
        pltpu.make_async_copy(faces.at[1, part], out.at[2], sems.at[2]),
        pltpu.make_async_copy(faces.at[2, part], out.at[3], sems.at[3]),
        pltpu.make_async_copy(cells.at[part], out.at[4], sems.at[4]),
    ]
    for copy in copies:
        copy.start()
    for copy in copies:
        copy.wait()


def own_inputs(right, faces, cells):
    def own(k, i):
        if k == 0:
            return widen(right[i])
        return widen(cells[i] if k == 4 else faces[k - 1, i])

    return own


def pack_0_kernel(right, faces, cells, beside, *outs):
    pack(own_inputs(right, faces, cells), lambda k, j: widen(beside[k, j]), SIZES[0], outs)


def place_0_kernel(right, faces, cells, beside, stack):
    own = own_inputs(right, faces, cells)
    place_halves(stack, own, lambda k, j: widen(beside[k, j]), SIZES[0])


def own_1_kernel(own, y_even, y_odd, z_even, z_odd):
    size = SIZES[1]

    def body(g, carry):
        planes = [[own[k, 3 * g + s] for k in range(5)] for s in range(3)]
        for s in range(3):
            y_faces(planes[s], size, 3 * g + s, y_even, y_odd)
        z_even[g], z_odd[g] = z_faces(planes, size)
        return carry

    lax.fori_loop(0, size // 3, body, 0)


def beside_1_kernel(beside, own_even, own_odd, y_even, y_odd):
    size = SIZES[1]
    y_even[0:size] = own_even[...]
    y_odd[0:size] = own_odd[...]
    for j in range(8):
        y_faces([beside[k, j] for k in range(5)], size, size + j, y_even, y_odd)


def fill_1_kernel(own, beside, own_even, own_odd, stack, z_even, z_odd):
    size = SIZES[1]
    gx = lax.axis_index("gx")
    z_even[0 : size // 3] = own_even[...]
    z_odd[0 : size // 3] = own_odd[...]

    def body(i, carry):
        for k in range(5):
            stack[k, i, 0:size, :] = own[k, i]
        return carry

    lax.fori_loop(0, size, body, 0)
    for q in range(3):
        slots, first = min(3, 8 - 3 * q), size + gx + 3 * q
        planes = [[beside[k, 3 * q + s] for k in range(5)] for s in range(slots)]
        for s in range(slots):
            for k in range(5):
                stack[k, first + s, 0:size, :] = planes[s][k]
        g = size // 3 + q
        z_even[g], z_odd[g] = z_faces(planes, size)
    empty = size + 8 * (1 - gx)
    for k in range(5):
        stack[k, empty] = jnp.zeros(stack.shape[2:], jnp.float32)


def side_1_kernel(filled, y_even, y_odd, own_even, own_odd, stack, z_even, z_odd):
    size = SIZES[1]
    gx = lax.axis_index("gx")
    z_even[:, 0:size, :] = own_even[...]
    z_odd[:, 0:size, :] = own_odd[...]
    sides = pl.ds(size, 16)

    def body(g, carry):
        planes = y_sides(g, size, 3, stack, 3 * g, y_even, y_odd)
        z_even[g, sides, :], z_odd[g, sides, :] = z_faces(planes, size)
        return carry

    lax.fori_loop(0, size // 3, body, 0)
    for q in range(3):
        slots, first = min(3, 8 - 3 * q), size + gx + 3 * q
        g = size // 3 + q
        planes = y_sides(g, size, slots, stack, first, y_even, y_odd)
        z_even[g, sides, :], z_odd[g, sides, :] = z_faces(planes, size)


def level_0_kernel(
    filled, ye, yo, ze, zo, ee, eo, oe, oo,
    coarse, coarse_edge, stack, iterate,
    update, rows, pairs,
):
    size = SIZES[0]
    gx = lax.axis_index("gx")
    merge_halves(stack, size, (ye, yo, ze, zo, ee, eo, oe, oo))
    down(stack, iterate, update, 1.0, HALF, HALF, Halves)
    keep_remainder(stack, iterate, update, 1.0, HALF, HALF, Halves)

    def out(k, value):
        lane = iota(value.shape, -1)
        coarse[k, 0:15] = jnp.where(lane < 24, value, 0.0)
        second = roll(value[0:9], LANES // 2, -1)
        coarse[k, 15:24] = jnp.where(lane[0:9] < 24, second, 0.0)
        coarse_edge[k] = jnp.where(gx == 0, coarse[k, 16:24], coarse[k, 0:8])

    coarsen(stack, update, rows, pairs, out, HALF, size, LANES // 2, 8)


def level_1_kernel(
    filled, z_even, z_odd, held,
    coarse, stack, iterate,
    update, rows, pairs, made,
):
    size = SIZES[1]
    planes = size + 9
    merge_z(stack, size, z_even, z_odd)
    down(stack, iterate, update, 0.25, planes, planes, Wrapped)
    keep_remainder(stack, iterate, update, 0.25, planes, size, Wrapped)

    def out(k, value):
        made[k] = value

    coarsen(stack, update, rows, pairs, out, size, size)
    for i in range(SIZES[2] // 2):
        line = made[0, 2 * i] + roll(made[0, 2 * i + 1], LANES // 2, -1)
        for h in range(2):
            for k in range(1, 5):
                line = line + roll(made[k, 2 * i + h], LANES // 2 * h + SIZES[2] * k, -1)
        coarse[i] = line


def level_2_kernel(
    mine, other, held,
    payload, stack, iterate,
    update, rows, pairs, made, lines,
):
    size = SIZES[2]
    planes = 2 * size + 1
    gx, gy, gz = places()
    even_y, even_z = gy % 2 == 0, gz % 2 == 0
    lane = iota((16, LANES), 1)
    bases = (0, size, LANES - size)
    half = size // 2
    for k in range(5):
        stack[k, 2 * size] = jnp.zeros(stack.shape[2:], jnp.float32)

    def body(i, carry):
        for core in range(2):

            def block(a, b):
                at = half * (3 * b + a) + i
                return jnp.where(gx == core, mine[at], other[at])

            columns = []
            for b in range(3):
                even, odd = block(1, b), block(2, b)
                columns.append(
                    (block(0, b), jnp.where(even_y, even, odd), jnp.where(even_y, odd, even))
                )
            columns = [columns[0]] + [
                [jnp.where(even_z, p, q) for p, q in zip(columns[c], columns[3 - c])] for c in (1, 2)
            ]
            for h in range(2):
                plane = size * core + 2 * i + h
                for k in range(5):
                    source = (LANES // 2) * h + size * k
                    stack[k, plane, 24:32, :] = jnp.zeros((8, LANES), jnp.float32)
                    for a, first in enumerate((0, size, 40 - size)):
                        line = jnp.zeros((16, LANES), jnp.float32)
                        for b, base in enumerate(bases):
                            here = (lane >= base) & (lane < base + size)
                            line = jnp.where(here, roll(columns[b][a], base - source, -1), line)
                        stack[k, plane, first : first + size, :] = line[:size]
        return carry

    lax.fori_loop(0, half, body, 0)
    weight = 0.0625
    iterate[2 * size] = jnp.zeros(iterate.shape[1:], jnp.float32)
    down(stack, iterate, update, weight, planes, 2 * size, Wrapped)
    keep_remainder(stack, iterate, update, weight, planes, 2 * size, Wrapped)

    def out(k, value):
        made[k * 96 : k * 96 + 96, :] = value.reshape(96, LANES)

    coarsen(stack, update, rows, pairs, out, 2 * size, size)
    line = jnp.zeros((60, LANES), jnp.float32)
    for y in range(6):
        line = line + roll(made[pl.ds(y, 60, stride=8), :], 6 * y, -1)
    lines[0:60, :] = line
    chunk = lines[0:20, :] + roll(lines[20:40, :], 40, -1) + roll(lines[40:60, :], 80, -1)
    chunk = jnp.concatenate([chunk, jnp.zeros((4, LANES), jnp.float32)], axis=0)

    def repeat(c, carry):
        payload[pl.ds(pl.multiple_of(c * CHUNK, 8), CHUNK), :] = chunk
        return carry

    lax.fori_loop(0, COLUMNS, repeat, 0)


def compact(value):
    row = iota(value.shape, -2)
    out = jnp.where(row == 0, value, 0.0)
    out = jnp.where(row == 1, roll(value, -1, -2), out)
    return jnp.where(row == 2, roll(value, -2, -2), out)


def bottom(source, faces, cells):
    weight = 0.25**4
    move = Columns(3)
    face_x, face_y, face_z = faces
    nothing = jnp.zeros((1,) + source.shape[1:], jnp.float32)

    def apply(v):
        flux_x = face_x * (v - jnp.concatenate([nothing, v[:-1]], axis=0))
        flux_y = face_y * (v - move.low_y(v))
        flux_z = face_z * (v - move.low_z(v))
        total = flux_x - jnp.concatenate([flux_x[1:], nothing], axis=0)
        total = total + (flux_y - move.up_y(flux_y)) + (flux_z - move.up_z(flux_z))
        return cells * v + weight * total

    def total_of(v):
        flat = jnp.sum(jnp.sum(v, axis=0), axis=0)
        one = jnp.sum(jnp.sum(flat, axis=0, keepdims=True), axis=1, keepdims=True)
        return jnp.broadcast_to(one, flat.shape)

    iterate = jnp.zeros_like(source)
    remainder = source
    search = source
    norm_now = total_of(remainder * remainder)
    for step in range(BOTTOM):
        applied = apply(search)
        size = norm_now / total_of(search * applied)
        iterate = iterate + size * search
        if step + 1 < BOTTOM:
            remainder = remainder - size * applied
            norm_next = total_of(remainder * remainder)
            search = remainder + (norm_next / norm_now) * search
            norm_now = norm_next
    return iterate


def rise_kernel(
    gathered, stack_2, base_2, stack_1, base_1, stack_0, base_0,
    solution_out, residual_out, sums,
    iterate_0, update_0, rows_0, spare_1,
    iterate_1, update_1, rows_1, spare_2,
    iterate_2, update_2, rows_2, spare_3,
    stack_3, iterate_3, update_3, turned, table, block_3,
):
    gx, gy, gz = places()

    stack_3[...] = jnp.zeros(stack_3.shape, jnp.float32)
    blank = jnp.zeros((LANES - COLUMNS, LANES), jnp.float32)
    for r in range(20):
        part = gathered[pl.ds(r, COLUMNS, stride=CHUNK), :]
        turned[...] = jnp.transpose(jnp.concatenate([part, blank], axis=0))
        for j in range(3):
            k, x = divmod(20 * j + r, 12)
            for y in range(6):
                stack_3[k, x, y, 0:6, :] = turned[40 * j + 6 * y : 40 * j + 6 * y + 6, :]
    move = Columns(6)
    weight = 0.25**3
    iterate_3[12] = jnp.zeros(iterate_3.shape[1:], jnp.float32)
    down(stack_3, iterate_3, update_3, weight, 13, 12, move)
    keep_remainder(stack_3, iterate_3, update_3, weight, 13, 12, move)

    def coarse(k, x_pair, y_pair, z_pair, scale):
        planes = []
        for x in range(6):
            read = (lambda i: update_3[i]) if k == 0 else (lambda i: stack_3[k, i])
            v = read(2 * x)
            if x_pair:
                v = v + read(2 * x + 1)
            lines = []
            for y in range(3):
                line = v[2 * y]
                if y_pair:
                    line = line + v[2 * y + 1]
                if z_pair:
                    line = line + roll(line, -1, -2)
                lines.append(scale * compact(line))
            planes.append(jnp.stack(lines))
        return jnp.stack(planes)

    lowest = bottom(
        coarse(0, True, True, True, 0.125),
        (
            coarse(1, False, True, True, 0.25),
            coarse(2, True, False, True, 0.25),
            coarse(3, True, True, False, 0.25),
        ),
        coarse(4, True, True, True, 0.125),
    )
    row = iota((8, LANES), 0)
    for x in range(6):
        for y in range(3):
            line = lowest[x, y]
            wide = jnp.where(row == 0, line, 0.0)
            for to in range(1, 6):
                wide = jnp.where(row == to, roll(line, to - to // 2, -2), wide)
            for a in range(2):
                for b in range(2):
                    iterate_3[2 * x + a, 2 * y + b] = iterate_3[2 * x + a, 2 * y + b] + wide
    up(stack_3, iterate_3, update_3, weight, 13, 12, move)

    low_rows = jnp.zeros((32, LANES), jnp.float32)
    for q in range(6):
        two = [iterate_3[2 * q + h].reshape(48, LANES) for h in range(2)]
        table[q] = jnp.transpose(jnp.concatenate(two + [low_rows], axis=0))
    block_3[...] = jnp.zeros(block_3.shape, jnp.float32)
    lane = iota((8, LANES), 1)

    def place(q, carry):
        for a, first in ((0, 0), (1, 6), (-1, 18)):
            lines = [jnp.zeros((8, LANES), jnp.float32) for _ in range(2)]
            for b, base in ((0, 0), (1, 6), (-1, LANES - 6)):
                y, z = gy + a, gz + b
                inside = (y >= 0) & (y < COUNT_Y) & (z >= 0) & (z < COUNT_Z)
                at = jnp.where(inside, y * COUNT_Z + z, 0)
                here = (lane >= base) & (lane < base + 6) & inside
                found = jnp.broadcast_to(table[q, pl.ds(at, 1), :], (8, LANES))
                for h in range(2):
                    for y_in in range(6):
                        moved = roll(found, base - 48 * h - 8 * y_in, -1)
                        lines[h] = jnp.where(here & (row == y_in), moved, lines[h])
            for h in range(2):
                block_3[2 * q + h, first : first + 6, :] = lines[h][0:6]
        return carry

    lax.fori_loop(0, 6, place, 0)

    spread(
        block_3, spare_3, rows_2, base_2, iterate_2,
        ((0, 12, 0), (18, 6, 28)),
        ((12, lambda i: i, lambda i: 2 * i),),
        24,
    )
    up(stack_2, iterate_2, update_2, 0.0625, 25, 24, Wrapped)

    size = SIZES[1]
    spread(
        iterate_2, spare_2, rows_1, base_1, iterate_1,
        ((0, 16, 0), (36, 4, 32)),
        (
            (12, lambda i: 12 * gx + i, lambda i: 2 * i),
            (4, lambda i: 12 - 4 * gx + i, lambda i: size + gx + 2 * i),
        ),
        size + 8 * (1 - gx),
    )
    up(stack_1, iterate_1, update_1, 0.25, size + 9, size + 9, Wrapped)

    size = SIZES[0]
    spread_halves(iterate_1, spare_1, rows_0, base_0, iterate_0, gx)
    up(stack_0, iterate_0, update_0, 1.0, HALF, HALF, Halves)
    iterate_0[HALF] = Halves.turn(iterate_0[0])
    inside = iota((size, LANES), 1)
    in_low = (inside >= 8) & (inside < 56)
    in_high = (inside >= 72) & (inside < 120)

    def use(i, v, remainder, carry):
        v, remainder = v[0:size], remainder[0:size]
        solution_out[i] = roll(v, -8, -1)[:, 0:size]
        residual_out[i] = roll(remainder, -8, -1)[:, 0:size]

        @pl.when(i < size - HALF)
        def _():
            solution_out[i + HALF] = roll(v, -72, -1)[:, 0:size]
            residual_out[i + HALF] = roll(remainder, -72, -1)[:, 0:size]

        mask = in_low | (in_high & (i < size - HALF))
        mine = jnp.where(mask, remainder, 0.0)
        given = jnp.where(mask, stack_0[0, i, 0:size, :], 0.0)
        return carry[0] + mine * mine, carry[1] + given * given

    zero = jnp.zeros((size, LANES), jnp.float32)
    squares = stencil_pass(stack_0, iterate_0, 1.0, HALF, HALF, Halves, use, (zero, zero))
    ones = []
    for square in squares:
        one = jnp.sum(jnp.sum(square, axis=0, keepdims=True), axis=1, keepdims=True)
        ones.append(jnp.broadcast_to(one, (8, LANES)))
    sums[...] = jnp.where(lane == 0, ones[0], jnp.where(lane == 1, ones[1], 0.0))


def stack_kernel(*refs):
    out = refs[-1]
    for n, ref in enumerate(refs[:-1]):
        count = ref.shape[0]
        out[n * count : n * count + count] = ref[...]


def stacked(*parts):
    count, *rest = parts[0].shape
    return call(stack_kernel, [near(len(parts) * count, *rest)], [held_near] * 3, [], parts, 1)[0]


def shards(right, faces, cells):
    dma = pltpu.SemaphoreType.DMA
    edge = call(edge_kernel, [near(5, WIDTH, 48, 48)], [far] * 3, [dma((5,))],
        (right, faces, cells), 2)[0]
    beside = swap_cores(edge)
    shapes = payload_shapes(48)
    outs = call(pack_0_kernel, shapes, [held_near] * 4, [], (right, faces, cells, beside), 4)
    moved = [swap(v, *way) for v, way in zip(outs, WAYS)]
    filled = call(place_0_kernel, [near(7, 31, 64, LANES)], [held_near] * 4, [],
        (right, faces, cells, beside), 4)[0]
    coarse, coarse_edge, stack_0, iterate_0 = call(
        level_0_kernel,
        [near(5, 24, 24, LANES), near(5, WIDTH, 24, LANES), near(7, 31, 64, LANES), near(31, 64, LANES)],
        [held_near] * 9,
        [near(31, 64, LANES), near(5, 64, LANES), near(5, 15, 24, LANES)],
        (filled, *moved),
        10,
        {0: 2},
    )
    beside = swap_cores(coarse_edge)
    y_shape, z_shape = near(32, 8, LANES), near(11, 24, LANES)
    *y_own, z_even, z_odd = call(own_1_kernel, [near(24, 8, LANES)] * 2 + [near(8, 24, LANES)] * 2,
        [held_near], [], (coarse,), 4)
    outs = call(beside_1_kernel, [y_shape] * 2, [held_near] * 3, [], (beside, *y_own), 4)
    sides = [swap(v, parity, None) for parity, v in enumerate(outs)]
    filled, *z_own = call(fill_1_kernel, [near(7, 34, 40, LANES), z_shape, z_shape],
        [held_near] * 4, [], (coarse, beside, z_even, z_odd), 4)
    filled, *outs = call(side_1_kernel, [near(7, 34, 40, LANES)] + [near(11, 40, LANES)] * 2,
        [held_near] * 5, [], (filled, *sides, *z_own), 4, {0: 0})
    z_sides = [swap(v, None, parity) for parity, v in enumerate(outs)]
    coarse, stack_1, iterate_1 = call(
        level_1_kernel,
        [near(6, 16, LANES), near(7, 34, 40, LANES), near(34, 40, LANES)],
        [held_near] * 4,
        [near(34, 40, LANES), near(5, 40, LANES), near(5, 12, 16, LANES), near(5, 12, 16, LANES)],
        (filled, *z_sides, stack_0),
        12,
        {0: 1},
    )
    column = stacked(coarse, *[swap(coarse, parity, None) for parity in (0, 1)])
    region = stacked(column, *[swap(column, None, parity) for parity in (0, 1)])
    other = swap_cores(region)
    payload, stack_2, iterate_2 = call(
        level_2_kernel,
        [near(COLUMNS * CHUNK, LANES), near(7, 26, 40, LANES), near(26, 40, LANES)],
        [held_near] * 3,
        [near(26, 40, LANES), near(5, 40, LANES), near(5, 12, 8, LANES), near(480, LANES), near(64, LANES)],
        (region, other, stack_0),
        12,
    )
    payload = payload.reshape(COLUMNS, CHUNK, LANES)
    gathered = lax.all_to_all(payload, YZ, 0, 0).reshape(COLUMNS * CHUNK, LANES)
    solved, residual, sums = call(
        rise_kernel,
        [f32(48, 48, 48), f32(48, 48, 48), f32(8, LANES)],
        [held_near] * 7,
        [
            near(31, 64, LANES), near(31, 64, LANES), near(64, LANES), near(33, 40, LANES),
            near(34, 40, LANES), near(34, 40, LANES), near(40, LANES), near(24, 40, LANES),
            near(26, 40, LANES), near(26, 40, LANES), near(40, LANES), near(12, 24, LANES),
            near(8, 14, 6, 8, LANES), near(14, 6, 8, LANES), near(14, 6, 8, LANES),
            near(LANES, LANES), near(6, LANES, LANES), near(12, 24, LANES),
        ],
        (gathered, stack_2, iterate_2, stack_1, iterate_1, stack_0, iterate_0),
        24,
    )
    each = jnp.broadcast_to(sums[0:1].reshape(1, 1, LANES), (128, 1, LANES))
    total = jnp.sum(lax.all_to_all(each, ALL, 0, 0), axis=(0, 1))
    return solved, residual, jnp.sqrt(total[0] / total[1])


def solution(mesh):
    torus = Mesh(
        mesh.devices.reshape(mesh.shape["gx"], mesh.shape["gy"], 4, 4), ("gx", "gy", "gz_0", "gz_1")
    )
    in_specs = (P("gx", "gy", GZ), P(None, "gx", "gy", GZ), P("gx", "gy", GZ))
    out_specs = (P("gx", "gy", GZ), P("gx", "gy", GZ), P())
    return jax.shard_map(
        shards, mesh=torus, in_specs=in_specs, out_specs=out_specs, check_vma=False
    )
```

```python
import functools

import jax
import jax.numpy as jnp
from jax import lax
from jax.experimental import pallas as pl
from jax.experimental.pallas import tpu as pltpu
from jax.sharding import Mesh
from jax.sharding import PartitionSpec as P

BOTTOM = 6
ALL = ("gx", "gy", "gz_0", "gz_1")
YZ = ("gy", "gz_0", "gz_1")
GZ = ("gz_0", "gz_1")
LANES = 128
WIDTH = 8
COUNT_Y = 4
COUNT_Z = 16
COLUMNS = COUNT_Y * COUNT_Z
SIZES = (48, 24, 12, 6)
CHUNK = 24
HALF = 30

theta = 1.125
delta = 0.875
sigma = theta / delta
rho_0 = 1.0 / sigma
rho_1 = 1.0 / (2.0 * sigma - rho_0)
rho_2 = 1.0 / (2.0 * sigma - rho_1)
FIRST = (0.0, 1.0 / theta)
LATER = ((rho_1 * rho_0, 2.0 * rho_1 / delta), (rho_2 * rho_1, 2.0 * rho_2 / delta))

vmem = pl.BlockSpec(memory_space=pltpu.VMEM)
held_near = pl.BlockSpec(memory_space=pltpu.VMEM)
far = pl.BlockSpec(memory_space=pltpu.HBM)


def roll(value, by, axis):
    axis = axis % value.ndim
    by = by % value.shape[axis]
    return pltpu.roll(value, by, axis) if by else value


def iota(shape, dim):
    return lax.broadcasted_iota(jnp.int32, shape, dim % len(shape))


def exact_dot(values, pick):
    pick = pick.astype(jnp.bfloat16)
    total = None
    for _ in range(3):
        part = values.astype(jnp.bfloat16)
        values = values - part.astype(jnp.float32)
        made = jnp.dot(part, pick, preferred_element_type=jnp.float32)
        total = made if total is None else total + made
    return total


class Wrapped:
    group = 11

    @staticmethod
    def turn(v):
        return v

    @staticmethod
    def low_y(v):
        return roll(v, 1, -2)

    @staticmethod
    def up_y(v):
        return roll(v, -1, -2)

    @staticmethod
    def low_z(v):
        return roll(v, 1, -1)

    @staticmethod
    def up_z(v):
        return roll(v, -1, -1)


class Middle(Wrapped):
    group = 4


class Halves(Wrapped):
    group = 3

    @staticmethod
    def turn(v):
        return roll(v, LANES // 2, -1)


class Columns:
    group = 12

    def __init__(self, cells):
        self.cells = cells

    def turn(self, v):
        return v

    def low_y(self, v):
        lane = iota(v.shape, -1)
        last = lax.slice_in_dim(v, self.cells - 1, self.cells, axis=v.ndim - 3)
        rest = lax.slice_in_dim(v, 0, self.cells - 1, axis=v.ndim - 3)
        lane = iota(last.shape, -1)
        last = jnp.where((lane >= COUNT_Z) & (lane < COLUMNS), roll(last, COUNT_Z, -1), 0.0)
        return jnp.concatenate([last, rest], axis=v.ndim - 3)

    def up_y(self, v):
        first = lax.slice_in_dim(v, 0, 1, axis=v.ndim - 3)
        rest = lax.slice_in_dim(v, 1, self.cells, axis=v.ndim - 3)
        lane = iota(first.shape, -1)
        first = jnp.where(lane < COLUMNS - COUNT_Z, roll(first, -COUNT_Z, -1), 0.0)
        return jnp.concatenate([rest, first], axis=v.ndim - 3)

    def low_z(self, v):
        lane, row = iota(v.shape, -1), iota(v.shape, -2)
        edge = roll(roll(v, 1 - self.cells, -2), 1, -1)
        edge = jnp.where((lane % COUNT_Z != 0) & (lane < COLUMNS), edge, 0.0)
        return jnp.where(row == 0, edge, roll(v, 1, -2))

    def up_z(self, v):
        lane, row = iota(v.shape, -1), iota(v.shape, -2)
        edge = roll(roll(v, self.cells - 1, -2), -1, -1)
        edge = jnp.where((lane % COUNT_Z != COUNT_Z - 1) & (lane < COLUMNS), edge, 0.0)
        inner = jnp.where(row < self.cells - 1, roll(v, -1, -2), 0.0)
        return jnp.where(row == self.cells - 1, edge, inner)


def set_up(stack, weight, planes, count, move, start=None):
    stack[1, planes] = move.turn(stack[1, 0])
    size = move.group

    def moved(i):
        return [move.up_z(stack[3, i + u]) for u in range(size)]

    def body(g, above_z):
        i = size * g
        later = moved(jnp.minimum(i + size, count - size)) if count > size else above_z
        for u in range(size):
            at = i + u
            cell, face_y = stack[4, at], stack[2, at]
            above_y = move.up_y(face_y)
            if stack.shape[0] > 7:
                stack[7, at] = above_y
            stack[6, at] = above_z[u]
            total = stack[1, at] + stack[1, at + 1] + face_y + above_y
            total = total + stack[3, at] + above_z[u]
            inverse = jnp.where(cell > 0.0, 1.0 / (cell + weight * total), 0.0)
            stack[5, at] = inverse
            if start is not None:
                step = FIRST[1] * (inverse * stack[0, at])
                for ref in start:
                    ref[at] = step
        return later

    lax.fori_loop(0, count // size, body, moved(0))


def stencil_pass(stack, iterate, weight, planes, count, move, use, carry):
    flux = stack[1, 0] * (iterate[0] - move.turn(iterate[planes - 1]))
    by_face = stack.shape[0] > 7
    size = move.group

    def moved(i):
        out = []
        for u in range(size):
            v = iterate[i + u]
            out += [move.low_z(v), move.up_z(v)]
            if by_face:
                out += [move.low_y(v), move.up_y(v)]
        return out

    def body(g, state):
        flux, near_by, carry = state
        i = size * g
        later = moved(jnp.minimum(i + size, count - size)) if count > size else near_by
        values = [iterate[i + u] for u in range(size + 1)]
        each = len(near_by) // size
        for u in range(size):
            at, v = i + u, values[u]
            sides = near_by[each * u : each * u + each]
            above = stack[1, at + 1] * (values[u + 1] - v)
            total = flux - above
            flux = above
            if by_face:
                total = total + stack[2, at] * (v - sides[2]) + stack[7, at] * (v - sides[3])
            else:
                flux_y = stack[2, at] * (v - move.low_y(v))
                total = total + (flux_y - move.up_y(flux_y))
            total = total + stack[3, at] * (v - sides[0]) + stack[6, at] * (v - sides[1])
            carry = use(at, v, stack[0, at] - (stack[4, at] * v + weight * total), carry)
        return flux, later, carry

    return lax.fori_loop(0, count // size, body, (flux, moved(0), carry))[2]


def sweep(stack, iterate, update, weight, planes, count, move, factors):
    keep, gain = factors
    iterate[planes] = move.turn(iterate[0])

    def use(i, v, remainder, carry):
        step = gain * (stack[5, i] * remainder)
        if keep:
            step = keep * update[i] + step
        update[i] = step
        iterate[i] = v + step
        return carry

    stencil_pass(stack, iterate, weight, planes, count, move, use, 0)


def down(stack, iterate, update, weight, planes, count, move):
    set_up(stack, weight, planes, count, move, (iterate, update))
    for factors in LATER:
        sweep(stack, iterate, update, weight, planes, count, move, factors)


def up(stack, iterate, update, weight, planes, count, move):
    for factors in (FIRST,) + LATER:
        sweep(stack, iterate, update, weight, planes, count, move, factors)


def keep_remainder(stack, iterate, update, weight, planes, count, move):
    iterate[planes] = move.turn(iterate[0])

    def use(i, v, remainder, carry):
        update[i] = remainder
        return carry

    stencil_pass(stack, iterate, weight, planes, count, move, use, 0)


def coarsen(stack, remainder, rows, pairs, out, count, size, period=LANES, offset=0):
    half = size // 2

    def body(i, carry):
        for k in range(5):
            if k == 1:
                rows[k] = stack[1, 2 * i]
            elif k == 0:
                rows[k] = remainder[2 * i] + remainder[2 * i + 1]
            else:
                rows[k] = stack[k, 2 * i] + stack[k, 2 * i + 1]
        for k in range(5):
            pair = rows[k, pl.ds(0, half, stride=2), :]
            if k != 2:
                pair = pair + rows[k, pl.ds(1, half, stride=2), :]
            pairs[k, i, 0:half, :] = pair
        return carry

    if half % 8:
        pairs[...] = jnp.zeros(pairs.shape, jnp.float32)
    lax.fori_loop(0, count // 2, body, 0)
    fine, coarse = iota((LANES, LANES), 0), iota((LANES, LANES), 1)
    inside = fine % period - offset
    own = (inside >= 0) & (inside < size) & (fine // period == coarse // period)
    mean = jnp.where(own & (inside // 2 == coarse % period), 1.0, 0.0)
    even = jnp.where(own & (inside == 2 * (coarse % period)), 1.0, 0.0)
    _, planes, padded, _ = pairs.shape
    for k in range(5):
        flat = pairs[k].reshape(planes * padded, LANES)
        scale = 0.125 if k in (0, 4) else 0.25
        made = scale * exact_dot(flat, even if k == 3 else mean)
        out(k, made.reshape(planes, padded, LANES))


def spread(coarse, spare, rows, base, fine, row_map, plane_maps, empty):
    planes, height, _ = spare.shape
    source, target = iota((LANES, LANES), 0), iota((LANES, LANES), 1)
    half = target // 2
    pick = jnp.where(source == jnp.where(target < LANES // 2, half, LANES // 2 + half), 1.0, 0.0)
    wide = exact_dot(coarse[0:planes].reshape(planes * height, LANES), pick)
    spare[...] = wide.reshape(planes, height, LANES)
    rows[...] = jnp.zeros(rows.shape, jnp.float32)
    fine[empty] = rows[...]
    for count, plane_of, target_of in plane_maps:

        def body(i, carry):
            plane = plane_of(i)
            for start, number, first in row_map:
                part = spare[plane, start : start + number, :]
                rows[pl.ds(first, number, stride=2), :] = part
                rows[pl.ds(first + 1, number, stride=2), :] = part
            both = rows[...]
            at = target_of(i)
            fine[at] = base[at] + both
            fine[at + 1] = base[at + 1] + both
            return carry

        lax.fori_loop(0, count, body, 0)


def spread_halves(coarse, spare, rows, base, fine, gx):
    planes, height, _ = spare.shape
    source, target = iota((LANES, LANES), 0), iota((LANES, LANES), 1)
    wanted = (target % (LANES // 2)) // 2 + (LANES - 4)
    pick = jnp.where(source == wanted % LANES, 1.0, 0.0)
    wide = exact_dot(coarse[0:planes].reshape(planes * height, LANES), pick)
    spare[...] = wide.reshape(planes, height, LANES)
    lane = iota((height, LANES), 1)

    def body(q, carry):
        j = q - 9 - 2 * gx
        there = (q < 9) | ((j >= 0) & (j < 4))
        above = jnp.where(q < 9, q + 15, 24 + 5 * gx + jnp.clip(j, 0, 3))
        both = jnp.where(lane < LANES // 2, spare[q], jnp.where(there, spare[above], 0.0))
        for start, number, first in ((0, 28, 0), (36, 4, 56)):
            part = both[start : start + number]
            rows[pl.ds(first, number, stride=2), :] = part
            rows[pl.ds(first + 1, number, stride=2), :] = part
        wide_rows = rows[...]
        fine[2 * q] = base[2 * q] + wide_rows
        fine[2 * q + 1] = base[2 * q + 1] + wide_rows
        return carry

    lax.fori_loop(0, HALF // 2, body, 0)


def places():
    gx = lax.axis_index("gx")
    gy = lax.axis_index("gy")
    gz = lax.axis_index("gz_0") * 4 + lax.axis_index("gz_1")
    return gx, gy, gz


def widen(value):
    rows, lanes = value.shape
    if lanes == LANES:
        return value
    return jnp.concatenate([value, jnp.zeros((rows, LANES - lanes), jnp.float32)], axis=1)


def y_pack(parts, size):
    lane = iota((8, LANES), 1)
    tiles = [jnp.zeros((8, LANES), jnp.float32) for _ in range(-(-5 * size // LANES))]
    for k, part in enumerate(parts):
        start = k * size
        moved = roll(part, start % LANES, -1)
        for t in range(len(tiles)):
            a, b = max(start, t * LANES) - t * LANES, min(start + size, (t + 1) * LANES) - t * LANES
            if a < b:
                tiles[t] = jnp.where((lane >= a) & (lane < b), moved, tiles[t])
    return tiles


def y_unpack(tiles, k, size, to):
    lane = iota((8, LANES), 1)
    start = k * size
    t = start // LANES
    value = tiles[t]
    if start + size > (t + 1) * LANES:
        value = jnp.where(lane >= start - t * LANES, value, tiles[t + 1])
    return roll(value, to - start, -1)


def pack(own, beside, size, outs):
    y_even, y_odd, z_even, z_odd, ee, eo, oe, oo = outs
    _, gy, gz = places()
    even_y, even_z = gy % 2 == 0, gz % 2 == 0
    lane = iota((size, LANES), 1)

    def group(g, slots, get):
        top = jnp.zeros((size, LANES), jnp.float32)
        bottom = top
        for s in range(slots):
            high, low = [], []
            for k in range(5):
                v = get(k, s)
                at = 40 * s + 8 * k
                here = (lane >= at) & (lane < at + 8)
                top = jnp.where(here, roll(v, at - (size - 8), -1), top)
                bottom = jnp.where(here, roll(v, at, -1), bottom)
                high.append(v[size - 8 :])
                low.append(v[:8])
            for t, (h, l) in enumerate(zip(y_pack(high, size), y_pack(low, size))):
                y_even[3 * g + s, 8 * t : 8 * t + 8, :] = jnp.where(even_y, h, l)
                y_odd[3 * g + s, 8 * t : 8 * t + 8, :] = jnp.where(even_y, l, h)
        a, b = jnp.where(even_z, top, bottom), jnp.where(even_z, bottom, top)
        z_even[g] = a
        z_odd[g] = b
        ee[g] = jnp.where(even_y, a[size - 8 :], a[:8])
        eo[g] = jnp.where(even_y, b[size - 8 :], b[:8])
        oe[g] = jnp.where(even_y, a[:8], a[size - 8 :])
        oo[g] = jnp.where(even_y, b[:8], b[size - 8 :])

    def body(g, carry):
        group(g, 3, lambda k, s: own(k, 3 * g + s))
        return carry

    if own is not None:
        lax.fori_loop(0, size // 3, body, 0)
    if beside is not None:
        for q in range(3):
            group(size // 3 + q, min(3, 8 - 3 * q), lambda k, s: beside(k, 3 * q + s))


def place_halves(stack, own, beside, size):
    gx, _, _ = places()

    def put(p, low, high):
        for k in range(5):
            stack[k, p, 0:size, :] = roll(low(k), 8, -1) + roll(high(k), LANES // 2 + 8, -1)
            stack[k, p, size:, :] = jnp.zeros((16, LANES), jnp.float32)

    def both(g, carry):
        for u in range(3):
            p = 3 * g + u
            put(p, lambda k: own(k, p), lambda k: own(k, p + HALF))
        return carry

    lax.fori_loop(0, (size - HALF) // 3, both, 0)

    def one(p, carry):
        j = p - (size - HALF) - 4 * gx
        there = (j >= 0) & (j < 8)
        at = jnp.clip(j, 0, 7)
        put(p, lambda k: own(k, p), lambda k: jnp.where(there, beside(k, at), 0.0))
        return carry

    lax.fori_loop(size - HALF, HALF, one, 0)


def merge_halves(stack, size, payloads):
    y_even, y_odd, z_even, z_odd, ee, eo, oe, oo = payloads
    gx, gy, gz = places()
    even_y, even_z = gy % 2 == 0, gz % 2 == 0
    lane, lane_8 = iota((size, LANES), 1), iota((8, LANES), 1)
    tiles = -(-5 * size // LANES)

    def group(g, slots, first, base):
        def sides(lane, value, low, high, at):
            here = (lane >= base) & (lane < base + 8)
            value = jnp.where(here, roll(low, base - at, -1), value)
            here = (lane >= base + 56) & (lane < base + 64)
            return jnp.where(here, roll(high, base + 56 - at, -1), value)

        low = jnp.where(even_z, z_odd[g], z_even[g])
        high = jnp.where(even_z, z_even[g], z_odd[g])
        by_even = jnp.where(even_z, eo[g], ee[g]), jnp.where(even_z, ee[g], eo[g])
        by_odd = jnp.where(even_z, oo[g], oe[g]), jnp.where(even_z, oe[g], oo[g])
        corners = (
            [jnp.where(even_y, e, o) for e, o in zip(by_even, by_odd)],
            [jnp.where(even_y, o, e) for e, o in zip(by_even, by_odd)],
        )
        for s in range(slots):
            e, o = y_even[3 * g + s], y_odd[3 * g + s]
            ends = jnp.where(even_y, e, o), jnp.where(even_y, o, e)
            ends = [[end[8 * t : 8 * t + 8] for t in range(tiles)] for end in ends]
            for k in range(5):
                at = 40 * s + 8 * k
                v = stack[k, first + s, 0:size, :]
                stack[k, first + s, 0:size, :] = sides(lane, v, low, high, at)
                for which in range(2):
                    rows = slice(size + 8 * which, size + 8 * which + 8)
                    v = stack[k, first + s, rows, :]
                    middle = y_unpack(ends[which], k, size, base + 8)
                    here = (lane_8 >= base + 8) & (lane_8 < base + 56)
                    v = jnp.where(here, middle, v)
                    stack[k, first + s, rows, :] = sides(lane_8, v, *corners[which], at)

    def body_low(g, carry):
        group(g, 3, 3 * g, 0)
        return carry

    def body_high(g, carry):
        group(g + HALF // 3, 3, 3 * g, LANES // 2)
        return carry

    lax.fori_loop(0, HALF // 3, body_low, 0)
    lax.fori_loop(0, (size - HALF) // 3, body_high, 0)
    for q in range(3):
        first = size - HALF + 4 * gx + 3 * q
        group(size // 3 + q, min(3, 8 - 3 * q), first, LANES // 2)


def y_faces(values, size, at, y_even, y_odd):
    even_y = places()[1] % 2 == 0
    high = y_pack([v[size - 8 :] for v in values], size)
    low = y_pack([v[:8] for v in values], size)
    for t, (h, l) in enumerate(zip(high, low)):
        y_even[at, 8 * t : 8 * t + 8, :] = jnp.where(even_y, h, l)
        y_odd[at, 8 * t : 8 * t + 8, :] = jnp.where(even_y, l, h)


def z_faces(planes, size):
    even_z = places()[2] % 2 == 0
    rows = planes[0][0].shape[0]
    lane = iota((rows, LANES), 1)
    top = jnp.zeros((rows, LANES), jnp.float32)
    bottom = top
    for s, values in enumerate(planes):
        for k, v in enumerate(values):
            at = 40 * s + 8 * k
            here = (lane >= at) & (lane < at + 8)
            top = jnp.where(here, roll(v, at - (size - 8), -1), top)
            bottom = jnp.where(here, roll(v, at, -1), bottom)
    return jnp.where(even_z, top, bottom), jnp.where(even_z, bottom, top)


def y_sides(source, size, slots, stack, first, y_even, y_odd):
    even_y = places()[1] % 2 == 0
    lane = iota((16, LANES), 1)
    tiles = -(-5 * size // LANES)
    planes = []
    for s in range(slots):
        e, o = y_even[3 * source + s], y_odd[3 * source + s]
        ends = jnp.where(even_y, e, o), jnp.where(even_y, o, e)
        ends = [[end[8 * t : 8 * t + 8] for t in range(tiles)] for end in ends]
        values = []
        for k in range(5):
            v = jnp.concatenate([y_unpack(end, k, size, 0) for end in ends], axis=0)
            v = jnp.where(lane < size, v, 0.0)
            stack[k, first + s, size : size + 16, :] = v
            values.append(v)
        planes.append(values)
    return planes


def merge_z(stack, size, z_even, z_odd):
    gx, _, gz = places()
    even_z = gz % 2 == 0
    lane = iota((size + 16, LANES), 1)

    def group(g, slots, first):
        low = jnp.where(even_z, z_odd[g], z_even[g])
        high = jnp.where(even_z, z_even[g], z_odd[g])
        for s in range(slots):
            for k in range(5):
                at = 40 * s + 8 * k
                v = stack[k, first + s]
                v = jnp.where(lane >= LANES - 8, roll(low, LANES - 8 - at, -1), v)
                here = (lane >= size) & (lane < size + 8)
                stack[k, first + s] = jnp.where(here, roll(high, size - at, -1), v)

    def body(g, carry):
        group(g, 3, 3 * g)
        return carry

    lax.fori_loop(0, size // 3, body, 0)
    for q in range(3):
        group(size // 3 + q, min(3, 8 - 3 * q), size + gx + 3 * q)


def payload_shapes(size):
    groups = size // 3 + 3
    tall = 8 * (-(-5 * size // LANES))
    y = near(size + 8, tall, LANES)
    z = near(groups, size, LANES)
    c = near(groups, 8, LANES)
    return [y, y, z, z, c, c, c, c]


def partner(index, parity, count):
    if parity is None:
        return index
    other = index + 1 if index % 2 == parity else index - 1
    return other if 0 <= other < count else None


def swap(value, parity_y, parity_z):
    pairs = []
    for y in range(COUNT_Y):
        for z in range(COUNT_Z):
            to_y, to_z = partner(y, parity_y, COUNT_Y), partner(z, parity_z, COUNT_Z)
            if to_y is not None and to_z is not None:
                pairs.append((y * COUNT_Z + z, to_y * COUNT_Z + to_z))
    return lax.ppermute(value, YZ, pairs)


WAYS = ((0, None), (1, None), (None, 0), (None, 1), (0, 0), (0, 1), (1, 0), (1, 1))


def swap_cores(value):
    return lax.ppermute(value, "gx", [(0, 1), (1, 0)])


def f32(*shape):
    return jax.ShapeDtypeStruct(shape, jnp.float32)


def near(*shape):
    return pltpu.VMEM(shape, jnp.float32)


def call(body, outs, ins, scratch, operands, limit, aliases={}):
    held = [
        pltpu.with_memory_space_constraint(v, pltpu.HBM if spec is far else pltpu.VMEM)
        for v, spec in zip(operands, ins)
    ]
    return pl.pallas_call(
        body,
        out_shape=outs,
        out_specs=[vmem] * len(outs),
        in_specs=ins,
        scratch_shapes=scratch,
        input_output_aliases=aliases,
        compiler_params=pltpu.CompilerParams(vmem_limit_bytes=limit * 2**20),
    )(*held)


def edge_kernel(right, faces, cells, out, sems):
    gx = lax.axis_index("gx")
    start = (1 - gx) * (SIZES[0] - WIDTH)
    part = pl.ds(start, WIDTH)
    copies = [
        pltpu.make_async_copy(right.at[part], out.at[0], sems.at[0]),
        pltpu.make_async_copy(faces.at[0, part], out.at[1], sems.at[1]),
        pltpu.make_async_copy(faces.at[1, part], out.at[2], sems.at[2]),
        pltpu.make_async_copy(faces.at[2, part], out.at[3], sems.at[3]),
        pltpu.make_async_copy(cells.at[part], out.at[4], sems.at[4]),
    ]
    for copy in copies:
        copy.start()
    for copy in copies:
        copy.wait()


def own_inputs(right, faces, cells):
    def own(k, i):
        if k == 0:
            return widen(right[i])
        return widen(cells[i] if k == 4 else faces[k - 1, i])

    return own


def pack_0_kernel(right, faces, cells, beside, *outs):
    pack(own_inputs(right, faces, cells), lambda k, j: widen(beside[k, j]), SIZES[0], outs)


def place_0_kernel(right, faces, cells, beside, stack):
    own = own_inputs(right, faces, cells)
    place_halves(stack, own, lambda k, j: widen(beside[k, j]), SIZES[0])


def own_1_kernel(own, y_even, y_odd, z_even, z_odd):
    size = SIZES[1]

    def body(g, carry):
        planes = [[own[k, 3 * g + s] for k in range(5)] for s in range(3)]
        for s in range(3):
            y_faces(planes[s], size, 3 * g + s, y_even, y_odd)
        z_even[g], z_odd[g] = z_faces(planes, size)
        return carry

    lax.fori_loop(0, size // 3, body, 0)


def beside_1_kernel(beside, own_even, own_odd, y_even, y_odd):
    size = SIZES[1]
    y_even[0:size] = own_even[...]
    y_odd[0:size] = own_odd[...]
    for j in range(8):
        y_faces([beside[k, j] for k in range(5)], size, size + j, y_even, y_odd)


def fill_1_kernel(own, beside, own_even, own_odd, stack, z_even, z_odd):
    size = SIZES[1]
    gx = lax.axis_index("gx")
    z_even[0 : size // 3] = own_even[...]
    z_odd[0 : size // 3] = own_odd[...]

    def body(i, carry):
        for k in range(5):
            stack[k, i, 0:size, :] = own[k, i]
        return carry

    lax.fori_loop(0, size, body, 0)
    for q in range(3):
        slots, first = min(3, 8 - 3 * q), size + gx + 3 * q
        planes = [[beside[k, 3 * q + s] for k in range(5)] for s in range(slots)]
        for s in range(slots):
            for k in range(5):
                stack[k, first + s, 0:size, :] = planes[s][k]
        g = size // 3 + q
        z_even[g], z_odd[g] = z_faces(planes, size)
    empty = size + 8 * (1 - gx)
    for k in range(5):
        stack[k, empty] = jnp.zeros(stack.shape[2:], jnp.float32)


def side_1_kernel(filled, y_even, y_odd, own_even, own_odd, stack, z_even, z_odd):
    size = SIZES[1]
    gx = lax.axis_index("gx")
    z_even[:, 0:size, :] = own_even[...]
    z_odd[:, 0:size, :] = own_odd[...]
    sides = pl.ds(size, 16)

    def body(g, carry):
        planes = y_sides(g, size, 3, stack, 3 * g, y_even, y_odd)
        z_even[g, sides, :], z_odd[g, sides, :] = z_faces(planes, size)
        return carry

    lax.fori_loop(0, size // 3, body, 0)
    for q in range(3):
        slots, first = min(3, 8 - 3 * q), size + gx + 3 * q
        g = size // 3 + q
        planes = y_sides(g, size, slots, stack, first, y_even, y_odd)
        z_even[g, sides, :], z_odd[g, sides, :] = z_faces(planes, size)


def level_0_kernel(
    filled, ye, yo, ze, zo, ee, eo, oe, oo,
    coarse, coarse_edge, stack, iterate,
    update, rows, pairs,
):
    size = SIZES[0]
    gx = lax.axis_index("gx")
    merge_halves(stack, size, (ye, yo, ze, zo, ee, eo, oe, oo))
    down(stack, iterate, update, 1.0, HALF, HALF, Halves)
    keep_remainder(stack, iterate, update, 1.0, HALF, HALF, Halves)

    def out(k, value):
        lane = iota(value.shape, -1)
        coarse[k, 0:15] = jnp.where(lane < 24, value, 0.0)
        second = roll(value[0:9], LANES // 2, -1)
        coarse[k, 15:24] = jnp.where(lane[0:9] < 24, second, 0.0)
        coarse_edge[k] = jnp.where(gx == 0, coarse[k, 16:24], coarse[k, 0:8])

    coarsen(stack, update, rows, pairs, out, HALF, size, LANES // 2, 8)


def level_1_kernel(
    filled, z_even, z_odd, held,
    coarse, stack, iterate,
    update, rows, pairs, made,
):
    size = SIZES[1]
    planes = size + 9
    merge_z(stack, size, z_even, z_odd)
    down(stack, iterate, update, 0.25, planes, planes, Wrapped)
    keep_remainder(stack, iterate, update, 0.25, planes, planes, Wrapped)

    def out(k, value):
        made[k] = value

    coarsen(stack, update, rows, pairs, out, size, size)
    for i in range(SIZES[2] // 2):
        line = made[0, 2 * i] + roll(made[0, 2 * i + 1], LANES // 2, -1)
        for h in range(2):
            for k in range(1, 5):
                line = line + roll(made[k, 2 * i + h], LANES // 2 * h + SIZES[2] * k, -1)
        coarse[i] = line


def level_2_kernel(
    mine, other, held,
    payload, stack, iterate,
    update, rows, pairs, made, lines,
):
    size = SIZES[2]
    planes = 2 * size + 1
    gx, gy, gz = places()
    even_y, even_z = gy % 2 == 0, gz % 2 == 0
    lane = iota((16, LANES), 1)
    bases = (0, size, LANES - size)
    half = size // 2
    for k in range(5):
        stack[k, 2 * size] = jnp.zeros(stack.shape[2:], jnp.float32)

    def body(i, carry):
        for core in range(2):

            def block(a, b):
                at = half * (3 * b + a) + i
                return jnp.where(gx == core, mine[at], other[at])

            columns = []
            for b in range(3):
                even, odd = block(1, b), block(2, b)
                columns.append(
                    (block(0, b), jnp.where(even_y, even, odd), jnp.where(even_y, odd, even))
                )
            columns = [columns[0]] + [
                [jnp.where(even_z, p, q) for p, q in zip(columns[c], columns[3 - c])] for c in (1, 2)
            ]
            for h in range(2):
                plane = size * core + 2 * i + h
                for k in range(5):
                    source = (LANES // 2) * h + size * k
                    stack[k, plane, 24:32, :] = jnp.zeros((8, LANES), jnp.float32)
                    for a, first in enumerate((0, size, 40 - size)):
                        line = jnp.zeros((16, LANES), jnp.float32)
                        for b, base in enumerate(bases):
                            here = (lane >= base) & (lane < base + size)
                            line = jnp.where(here, roll(columns[b][a], base - source, -1), line)
                        stack[k, plane, first : first + size, :] = line[:size]
        return carry

    lax.fori_loop(0, half, body, 0)
    weight = 0.0625
    iterate[2 * size] = jnp.zeros(iterate.shape[1:], jnp.float32)
    down(stack, iterate, update, weight, planes, 2 * size, Middle)
    keep_remainder(stack, iterate, update, weight, planes, 2 * size, Middle)

    def out(k, value):
        made[k * 96 : k * 96 + 96, :] = value.reshape(96, LANES)

    coarsen(stack, update, rows, pairs, out, 2 * size, size)
    line = jnp.zeros((60, LANES), jnp.float32)
    for y in range(6):
        line = line + roll(made[pl.ds(y, 60, stride=8), :], 6 * y, -1)
    lines[0:60, :] = line
    chunk = lines[0:20, :] + roll(lines[20:40, :], 40, -1) + roll(lines[40:60, :], 80, -1)
    chunk = jnp.concatenate([chunk, jnp.zeros((4, LANES), jnp.float32)], axis=0)

    def repeat(c, carry):
        payload[pl.ds(pl.multiple_of(c * CHUNK, 8), CHUNK), :] = chunk
        return carry

    lax.fori_loop(0, COLUMNS, repeat, 0)


def compact(value):
    row = iota(value.shape, -2)
    out = jnp.where(row == 0, value, 0.0)
    out = jnp.where(row == 1, roll(value, -1, -2), out)
    return jnp.where(row == 2, roll(value, -2, -2), out)


def bottom(source, faces, cells):
    weight = 0.25**4
    move = Columns(3)
    face_x, face_y, face_z = faces
    nothing = jnp.zeros((1,) + source.shape[1:], jnp.float32)

    def apply(v):
        flux_x = face_x * (v - jnp.concatenate([nothing, v[:-1]], axis=0))
        flux_y = face_y * (v - move.low_y(v))
        flux_z = face_z * (v - move.low_z(v))
        total = flux_x - jnp.concatenate([flux_x[1:], nothing], axis=0)
        total = total + (flux_y - move.up_y(flux_y)) + (flux_z - move.up_z(flux_z))
        return cells * v + weight * total

    def total_of(v):
        flat = jnp.sum(jnp.sum(v, axis=0), axis=0)
        one = jnp.sum(jnp.sum(flat, axis=0, keepdims=True), axis=1, keepdims=True)
        return jnp.broadcast_to(one, flat.shape)

    iterate = jnp.zeros_like(source)
    remainder = source
    search = source
    norm_now = total_of(remainder * remainder)
    for step in range(BOTTOM):
        applied = apply(search)
        size = norm_now / total_of(search * applied)
        iterate = iterate + size * search
        if step + 1 < BOTTOM:
            remainder = remainder - size * applied
            norm_next = total_of(remainder * remainder)
            search = remainder + (norm_next / norm_now) * search
            norm_now = norm_next
    return iterate


def rise_kernel(
    gathered, stack_2, base_2, stack_1, base_1, stack_0, base_0,
    solution_out, residual_out, sums,
    iterate_0, update_0, rows_0, spare_1,
    iterate_1, update_1, rows_1, spare_2,
    iterate_2, update_2, rows_2, spare_3,
    stack_3, iterate_3, update_3, turned, table, block_3,
):
    gx, gy, gz = places()

    stack_3[...] = jnp.zeros(stack_3.shape, jnp.float32)
    blank = jnp.zeros((LANES - COLUMNS, LANES), jnp.float32)
    for r in range(20):
        part = gathered[pl.ds(r, COLUMNS, stride=CHUNK), :]
        turned[...] = jnp.transpose(jnp.concatenate([part, blank], axis=0))
        for j in range(3):
            k, x = divmod(20 * j + r, 12)
            for y in range(6):
                stack_3[k, x, y, 0:6, :] = turned[40 * j + 6 * y : 40 * j + 6 * y + 6, :]
    move = Columns(6)
    weight = 0.25**3
    iterate_3[12] = jnp.zeros(iterate_3.shape[1:], jnp.float32)
    down(stack_3, iterate_3, update_3, weight, 13, 12, move)
    keep_remainder(stack_3, iterate_3, update_3, weight, 13, 12, move)

    def coarse(k, x_pair, y_pair, z_pair, scale):
        planes = []
        for x in range(6):
            read = (lambda i: update_3[i]) if k == 0 else (lambda i: stack_3[k, i])
            v = read(2 * x)
            if x_pair:
                v = v + read(2 * x + 1)
            lines = []
            for y in range(3):
                line = v[2 * y]
                if y_pair:
                    line = line + v[2 * y + 1]
                if z_pair:
                    line = line + roll(line, -1, -2)
                lines.append(scale * compact(line))
            planes.append(jnp.stack(lines))
        return jnp.stack(planes)

    lowest = bottom(
        coarse(0, True, True, True, 0.125),
        (
            coarse(1, False, True, True, 0.25),
            coarse(2, True, False, True, 0.25),
            coarse(3, True, True, False, 0.25),
        ),
        coarse(4, True, True, True, 0.125),
    )
    row = iota((8, LANES), 0)
    for x in range(6):
        for y in range(3):
            line = lowest[x, y]
            wide = jnp.where(row == 0, line, 0.0)
            for to in range(1, 6):
                wide = jnp.where(row == to, roll(line, to - to // 2, -2), wide)
            for a in range(2):
                for b in range(2):
                    iterate_3[2 * x + a, 2 * y + b] = iterate_3[2 * x + a, 2 * y + b] + wide
    up(stack_3, iterate_3, update_3, weight, 13, 12, move)

    low_rows = jnp.zeros((32, LANES), jnp.float32)
    for q in range(6):
        two = [iterate_3[2 * q + h].reshape(48, LANES) for h in range(2)]
        table[q] = jnp.transpose(jnp.concatenate(two + [low_rows], axis=0))
    block_3[...] = jnp.zeros(block_3.shape, jnp.float32)
    lane = iota((8, LANES), 1)

    def place(q, carry):
        for a, first in ((0, 0), (1, 6), (-1, 18)):
            lines = [jnp.zeros((8, LANES), jnp.float32) for _ in range(2)]
            for b, base in ((0, 0), (1, 6), (-1, LANES - 6)):
                y, z = gy + a, gz + b
                inside = (y >= 0) & (y < COUNT_Y) & (z >= 0) & (z < COUNT_Z)
                at = jnp.where(inside, y * COUNT_Z + z, 0)
                here = (lane >= base) & (lane < base + 6) & inside
                found = jnp.broadcast_to(table[q, pl.ds(at, 1), :], (8, LANES))
                for h in range(2):
                    for y_in in range(6):
                        moved = roll(found, base - 48 * h - 8 * y_in, -1)
                        lines[h] = jnp.where(here & (row == y_in), moved, lines[h])
            for h in range(2):
                block_3[2 * q + h, first : first + 6, :] = lines[h][0:6]
        return carry

    lax.fori_loop(0, 6, place, 0)

    spread(
        block_3, spare_3, rows_2, base_2, iterate_2,
        ((0, 12, 0), (18, 6, 28)),
        ((12, lambda i: i, lambda i: 2 * i),),
        24,
    )
    up(stack_2, iterate_2, update_2, 0.0625, 25, 24, Middle)

    size = SIZES[1]
    spread(
        iterate_2, spare_2, rows_1, base_1, iterate_1,
        ((0, 16, 0), (36, 4, 32)),
        (
            (12, lambda i: 12 * gx + i, lambda i: 2 * i),
            (4, lambda i: 12 - 4 * gx + i, lambda i: size + gx + 2 * i),
        ),
        size + 8 * (1 - gx),
    )
    up(stack_1, iterate_1, update_1, 0.25, size + 9, size + 9, Wrapped)

    size = SIZES[0]
    spread_halves(iterate_1, spare_1, rows_0, base_0, iterate_0, gx)
    up(stack_0, iterate_0, update_0, 1.0, HALF, HALF, Halves)
    iterate_0[HALF] = Halves.turn(iterate_0[0])
    inside = iota((size, LANES), 1)
    in_low = (inside >= 8) & (inside < 56)
    in_high = (inside >= 72) & (inside < 120)

    def use(i, v, remainder, carry):
        v, remainder = v[0:size], remainder[0:size]
        solution_out[i] = roll(v, -8, -1)[:, 0:size]
        residual_out[i] = roll(remainder, -8, -1)[:, 0:size]

        @pl.when(i < size - HALF)
        def _():
            solution_out[i + HALF] = roll(v, -72, -1)[:, 0:size]
            residual_out[i + HALF] = roll(remainder, -72, -1)[:, 0:size]

        mask = in_low | (in_high & (i < size - HALF))
        mine = jnp.where(mask, remainder, 0.0)
        given = jnp.where(mask, stack_0[0, i, 0:size, :], 0.0)
        return carry[0] + mine * mine, carry[1] + given * given

    zero = jnp.zeros((size, LANES), jnp.float32)
    squares = stencil_pass(stack_0, iterate_0, 1.0, HALF, HALF, Halves, use, (zero, zero))
    ones = []
    for square in squares:
        one = jnp.sum(jnp.sum(square, axis=0, keepdims=True), axis=1, keepdims=True)
        ones.append(jnp.broadcast_to(one, (8, LANES)))
    sums[...] = jnp.where(lane == 0, ones[0], jnp.where(lane == 1, ones[1], 0.0))


def stack_kernel(*refs):
    out = refs[-1]
    for n, ref in enumerate(refs[:-1]):
        count = ref.shape[0]
        out[n * count : n * count + count] = ref[...]


def stacked(*parts):
    count, *rest = parts[0].shape
    return call(stack_kernel, [near(len(parts) * count, *rest)], [held_near] * 3, [], parts, 1)[0]


def shards(right, faces, cells):
    dma = pltpu.SemaphoreType.DMA
    edge = call(edge_kernel, [near(5, WIDTH, 48, 48)], [far] * 3, [dma((5,))],
        (right, faces, cells), 2)[0]
    beside = swap_cores(edge)
    shapes = payload_shapes(48)
    outs = call(pack_0_kernel, shapes, [held_near] * 4, [], (right, faces, cells, beside), 4)
    moved = [swap(v, *way) for v, way in zip(outs, WAYS)]
    filled = call(place_0_kernel, [near(7, 31, 64, LANES)], [held_near] * 4, [],
        (right, faces, cells, beside), 4)[0]
    coarse, coarse_edge, stack_0, iterate_0 = call(
        level_0_kernel,
        [near(5, 24, 24, LANES), near(5, WIDTH, 24, LANES), near(7, 31, 64, LANES), near(31, 64, LANES)],
        [held_near] * 9,
        [near(31, 64, LANES), near(5, 64, LANES), near(5, 15, 24, LANES)],
        (filled, *moved),
        10,
        {0: 2},
    )
    beside = swap_cores(coarse_edge)
    y_shape, z_shape = near(32, 8, LANES), near(11, 24, LANES)
    *y_own, z_even, z_odd = call(own_1_kernel, [near(24, 8, LANES)] * 2 + [near(8, 24, LANES)] * 2,
        [held_near], [], (coarse,), 4)
    outs = call(beside_1_kernel, [y_shape] * 2, [held_near] * 3, [], (beside, *y_own), 4)
    sides = [swap(v, parity, None) for parity, v in enumerate(outs)]
    filled, *z_own = call(fill_1_kernel, [near(7, 34, 40, LANES), z_shape, z_shape],
        [held_near] * 4, [], (coarse, beside, z_even, z_odd), 4)
    filled, *outs = call(side_1_kernel, [near(7, 34, 40, LANES)] + [near(11, 40, LANES)] * 2,
        [held_near] * 5, [], (filled, *sides, *z_own), 4, {0: 0})
    z_sides = [swap(v, None, parity) for parity, v in enumerate(outs)]
    coarse, stack_1, iterate_1 = call(
        level_1_kernel,
        [near(6, 16, LANES), near(7, 34, 40, LANES), near(34, 40, LANES)],
        [held_near] * 4,
        [near(34, 40, LANES), near(5, 40, LANES), near(5, 12, 16, LANES), near(5, 12, 16, LANES)],
        (filled, *z_sides, stack_0),
        12,
        {0: 1},
    )
    column = stacked(coarse, *[swap(coarse, parity, None) for parity in (0, 1)])
    region = stacked(column, *[swap(column, None, parity) for parity in (0, 1)])
    other = swap_cores(region)
    payload, stack_2, iterate_2 = call(
        level_2_kernel,
        [near(COLUMNS * CHUNK, LANES), near(7, 26, 40, LANES), near(26, 40, LANES)],
        [held_near] * 3,
        [near(26, 40, LANES), near(5, 40, LANES), near(5, 12, 8, LANES), near(480, LANES), near(64, LANES)],
        (region, other, stack_0),
        12,
    )
    payload = payload.reshape(COLUMNS, CHUNK, LANES)
    gathered = lax.all_to_all(payload, YZ, 0, 0).reshape(COLUMNS * CHUNK, LANES)
    solved, residual, sums = call(
        rise_kernel,
        [f32(48, 48, 48), f32(48, 48, 48), f32(8, LANES)],
        [held_near] * 7,
        [
            near(31, 64, LANES), near(31, 64, LANES), near(64, LANES), near(33, 40, LANES),
            near(34, 40, LANES), near(34, 40, LANES), near(40, LANES), near(24, 40, LANES),
            near(26, 40, LANES), near(26, 40, LANES), near(40, LANES), near(12, 24, LANES),
            near(8, 14, 6, 8, LANES), near(14, 6, 8, LANES), near(14, 6, 8, LANES),
            near(LANES, LANES), near(6, LANES, LANES), near(12, 24, LANES),
        ],
        (gathered, stack_2, iterate_2, stack_1, iterate_1, stack_0, iterate_0),
        24,
    )
    each = jnp.broadcast_to(sums[0:1].reshape(1, 1, LANES), (128, 1, LANES))
    total = jnp.sum(lax.all_to_all(each, ALL, 0, 0), axis=(0, 1))
    return solved, residual, jnp.sqrt(total[0] / total[1])


def solution(mesh):
    torus = Mesh(
        mesh.devices.reshape(mesh.shape["gx"], mesh.shape["gy"], 4, 4), ("gx", "gy", "gz_0", "gz_1")
    )
    in_specs = (P("gx", "gy", GZ), P(None, "gx", "gy", GZ), P("gx", "gy", GZ))
    out_specs = (P("gx", "gy", GZ), P("gx", "gy", GZ), P())
    return jax.shard_map(
        shards, mesh=torus, in_specs=in_specs, out_specs=out_specs, check_vma=False
    )
```

```python
import functools

import jax
import jax.numpy as jnp
from jax import lax
from jax.experimental import pallas as pl
from jax.experimental.pallas import tpu as pltpu
from jax.sharding import Mesh
from jax.sharding import PartitionSpec as P

BOTTOM = 6
ALL = ("gx", "gy", "gz_0", "gz_1")
YZ = ("gy", "gz_0", "gz_1")
GZ = ("gz_0", "gz_1")
LANES = 128
WIDTH = 8
COUNT_Y = 4
COUNT_Z = 16
COLUMNS = COUNT_Y * COUNT_Z
SIZES = (48, 24, 12, 6)
CHUNK = 24
HALF = 30

theta = 1.125
delta = 0.875
sigma = theta / delta
rho_0 = 1.0 / sigma
rho_1 = 1.0 / (2.0 * sigma - rho_0)
rho_2 = 1.0 / (2.0 * sigma - rho_1)
FIRST = (0.0, 1.0 / theta)
LATER = ((rho_1 * rho_0, 2.0 * rho_1 / delta), (rho_2 * rho_1, 2.0 * rho_2 / delta))

vmem = pl.BlockSpec(memory_space=pltpu.VMEM)
held_near = pl.BlockSpec(memory_space=pltpu.VMEM)
far = pl.BlockSpec(memory_space=pltpu.HBM)


def roll(value, by, axis):
    axis = axis % value.ndim
    by = by % value.shape[axis]
    return pltpu.roll(value, by, axis) if by else value


def iota(shape, dim):
    return lax.broadcasted_iota(jnp.int32, shape, dim % len(shape))


def exact_dot(values, pick):
    pick = pick.astype(jnp.bfloat16)
    total = None
    for _ in range(3):
        part = values.astype(jnp.bfloat16)
        values = values - part.astype(jnp.float32)
        made = jnp.dot(part, pick, preferred_element_type=jnp.float32)
        total = made if total is None else total + made
    return total


class Wrapped:
    group = 33

    @staticmethod
    def turn(v):
        return v

    @staticmethod
    def low_y(v):
        return roll(v, 1, -2)

    @staticmethod
    def up_y(v):
        return roll(v, -1, -2)

    @staticmethod
    def low_z(v):
        return roll(v, 1, -1)

    @staticmethod
    def up_z(v):
        return roll(v, -1, -1)


class Middle(Wrapped):
    group = 24


class Halves(Wrapped):
    group = 30

    @staticmethod
    def turn(v):
        return roll(v, LANES // 2, -1)


class Columns:
    group = 12

    def __init__(self, cells):
        self.cells = cells

    def turn(self, v):
        return v

    def low_y(self, v):
        lane = iota(v.shape, -1)
        last = lax.slice_in_dim(v, self.cells - 1, self.cells, axis=v.ndim - 3)
        rest = lax.slice_in_dim(v, 0, self.cells - 1, axis=v.ndim - 3)
        lane = iota(last.shape, -1)
        last = jnp.where((lane >= COUNT_Z) & (lane < COLUMNS), roll(last, COUNT_Z, -1), 0.0)
        return jnp.concatenate([last, rest], axis=v.ndim - 3)

    def up_y(self, v):
        first = lax.slice_in_dim(v, 0, 1, axis=v.ndim - 3)
        rest = lax.slice_in_dim(v, 1, self.cells, axis=v.ndim - 3)
        lane = iota(first.shape, -1)
        first = jnp.where(lane < COLUMNS - COUNT_Z, roll(first, -COUNT_Z, -1), 0.0)
        return jnp.concatenate([rest, first], axis=v.ndim - 3)

    def low_z(self, v):
        lane, row = iota(v.shape, -1), iota(v.shape, -2)
        edge = roll(roll(v, 1 - self.cells, -2), 1, -1)
        edge = jnp.where((lane % COUNT_Z != 0) & (lane < COLUMNS), edge, 0.0)
        return jnp.where(row == 0, edge, roll(v, 1, -2))

    def up_z(self, v):
        lane, row = iota(v.shape, -1), iota(v.shape, -2)
        edge = roll(roll(v, self.cells - 1, -2), -1, -1)
        edge = jnp.where((lane % COUNT_Z != COUNT_Z - 1) & (lane < COLUMNS), edge, 0.0)
        inner = jnp.where(row < self.cells - 1, roll(v, -1, -2), 0.0)
        return jnp.where(row == self.cells - 1, edge, inner)


def set_up(stack, iterate, update, weight, planes, count, move):
    stack[1, planes] = move.turn(stack[1, 0])
    size = move.group

    def body(g, carry):
        for u in range(size):
            at = size * g + u
            cell, face_y, face_z = stack[4, at], stack[2, at], stack[3, at]
            above_y, above_z = move.up_y(face_y), move.up_z(face_z)
            if stack.shape[0] > 7:
                stack[7, at] = above_y
            stack[6, at] = above_z
            total = stack[1, at] + stack[1, at + 1] + face_y + above_y + face_z + above_z
            inverse = jnp.where(cell > 0.0, 1.0 / (cell + weight * total), 0.0)
            stack[5, at] = inverse
            step = FIRST[1] * (inverse * stack[0, at])
            iterate[at] = step
            update[at] = step
        return carry

    if count == size:
        body(0, 0)
    else:
        lax.fori_loop(0, count // size, body, 0)


def stencil_pass(stack, iterate, weight, planes, count, move, use, carry):
    flux = stack[1, 0] * (iterate[0] - move.turn(iterate[planes - 1]))
    by_face = stack.shape[0] > 7
    size = move.group

    def body(g, state):
        flux, carry = state
        i = size * g
        values = [iterate[i + u] for u in range(size + 1)]
        for u in range(size):
            at, v = i + u, values[u]
            above = stack[1, at + 1] * (values[u + 1] - v)
            total = flux - above
            flux = above
            if by_face:
                total = total + stack[2, at] * (v - move.low_y(v))
                total = total + stack[7, at] * (v - move.up_y(v))
            else:
                flux_y = stack[2, at] * (v - move.low_y(v))
                total = total + (flux_y - move.up_y(flux_y))
            total = total + stack[3, at] * (v - move.low_z(v))
            total = total + stack[6, at] * (v - move.up_z(v))
            carry = use(at, v, stack[0, at] - (stack[4, at] * v + weight * total), carry)
        return flux, carry

    if count == size:
        return body(0, (flux, carry))[1]
    return lax.fori_loop(0, count // size, body, (flux, carry))[1]


def sweep(stack, iterate, update, weight, planes, count, move, factors):
    keep, gain = factors
    iterate[planes] = move.turn(iterate[0])

    def use(i, v, remainder, carry):
        step = gain * (stack[5, i] * remainder)
        if keep:
            step = keep * update[i] + step
        update[i] = step
        iterate[i] = v + step
        return carry

    stencil_pass(stack, iterate, weight, planes, count, move, use, 0)


def down(stack, iterate, update, weight, planes, count, move):
    set_up(stack, iterate, update, weight, planes, count, move)
    for factors in LATER:
        sweep(stack, iterate, update, weight, planes, count, move, factors)


def up(stack, iterate, update, weight, planes, count, move):
    for factors in (FIRST,) + LATER:
        sweep(stack, iterate, update, weight, planes, count, move, factors)


def keep_remainder(stack, iterate, update, weight, planes, count, move):
    iterate[planes] = move.turn(iterate[0])

    def use(i, v, remainder, carry):
        update[i] = remainder
        return carry

    stencil_pass(stack, iterate, weight, planes, count, move, use, 0)


def coarsen(stack, remainder, rows, pairs, out, count, size, period=LANES, offset=0):
    half = size // 2

    def body(i, carry):
        for k in range(5):
            if k == 1:
                rows[k] = stack[1, 2 * i]
            elif k == 0:
                rows[k] = remainder[2 * i] + remainder[2 * i + 1]
            else:
                rows[k] = stack[k, 2 * i] + stack[k, 2 * i + 1]
        for k in range(5):
            pair = rows[k, pl.ds(0, half, stride=2), :]
            if k != 2:
                pair = pair + rows[k, pl.ds(1, half, stride=2), :]
            pairs[k, i, 0:half, :] = pair
        return carry

    if half % 8:
        pairs[...] = jnp.zeros(pairs.shape, jnp.float32)
    lax.fori_loop(0, count // 2, body, 0)
    fine, coarse = iota((LANES, LANES), 0), iota((LANES, LANES), 1)
    inside = fine % period - offset
    own = (inside >= 0) & (inside < size) & (fine // period == coarse // period)
    mean = jnp.where(own & (inside // 2 == coarse % period), 1.0, 0.0)
    even = jnp.where(own & (inside == 2 * (coarse % period)), 1.0, 0.0)
    _, planes, padded, _ = pairs.shape
    for k in range(5):
        flat = pairs[k].reshape(planes * padded, LANES)
        scale = 0.125 if k in (0, 4) else 0.25
        made = scale * exact_dot(flat, even if k == 3 else mean)
        out(k, made.reshape(planes, padded, LANES))


def spread(coarse, spare, rows, base, fine, row_map, plane_maps, empty):
    planes, height, _ = spare.shape
    source, target = iota((LANES, LANES), 0), iota((LANES, LANES), 1)
    half = target // 2
    pick = jnp.where(source == jnp.where(target < LANES // 2, half, LANES // 2 + half), 1.0, 0.0)
    wide = exact_dot(coarse[0:planes].reshape(planes * height, LANES), pick)
    spare[...] = wide.reshape(planes, height, LANES)
    rows[...] = jnp.zeros(rows.shape, jnp.float32)
    fine[empty] = rows[...]
    for count, plane_of, target_of in plane_maps:

        def body(i, carry):
            plane = plane_of(i)
            for start, number, first in row_map:
                part = spare[plane, start : start + number, :]
                rows[pl.ds(first, number, stride=2), :] = part
                rows[pl.ds(first + 1, number, stride=2), :] = part
            both = rows[...]
            at = target_of(i)
            fine[at] = base[at] + both
            fine[at + 1] = base[at + 1] + both
            return carry

        lax.fori_loop(0, count, body, 0)


def spread_halves(coarse, spare, rows, base, fine, gx):
    planes, height, _ = spare.shape
    source, target = iota((LANES, LANES), 0), iota((LANES, LANES), 1)
    wanted = (target % (LANES // 2)) // 2 + (LANES - 4)
    pick = jnp.where(source == wanted % LANES, 1.0, 0.0)
    wide = exact_dot(coarse[0:planes].reshape(planes * height, LANES), pick)
    spare[...] = wide.reshape(planes, height, LANES)
    lane = iota((height, LANES), 1)

    def body(q, carry):
        j = q - 9 - 2 * gx
        there = (q < 9) | ((j >= 0) & (j < 4))
        above = jnp.where(q < 9, q + 15, 24 + 5 * gx + jnp.clip(j, 0, 3))
        both = jnp.where(lane < LANES // 2, spare[q], jnp.where(there, spare[above], 0.0))
        for start, number, first in ((0, 28, 0), (36, 4, 56)):
            part = both[start : start + number]
            rows[pl.ds(first, number, stride=2), :] = part
            rows[pl.ds(first + 1, number, stride=2), :] = part
        wide_rows = rows[...]
        fine[2 * q] = base[2 * q] + wide_rows
        fine[2 * q + 1] = base[2 * q + 1] + wide_rows
        return carry

    lax.fori_loop(0, HALF // 2, body, 0)


def places():
    gx = lax.axis_index("gx")
    gy = lax.axis_index("gy")
    gz = lax.axis_index("gz_0") * 4 + lax.axis_index("gz_1")
    return gx, gy, gz


def widen(value):
    rows, lanes = value.shape
    if lanes == LANES:
        return value
    return jnp.concatenate([value, jnp.zeros((rows, LANES - lanes), jnp.float32)], axis=1)


def y_pack(parts, size):
    lane = iota((8, LANES), 1)
    tiles = [jnp.zeros((8, LANES), jnp.float32) for _ in range(-(-5 * size // LANES))]
    for k, part in enumerate(parts):
        start = k * size
        moved = roll(part, start % LANES, -1)
        for t in range(len(tiles)):
            a, b = max(start, t * LANES) - t * LANES, min(start + size, (t + 1) * LANES) - t * LANES
            if a < b:
                tiles[t] = jnp.where((lane >= a) & (lane < b), moved, tiles[t])
    return tiles


def y_unpack(tiles, k, size, to):
    lane = iota((8, LANES), 1)
    start = k * size
    t = start // LANES
    value = tiles[t]
    if start + size > (t + 1) * LANES:
        value = jnp.where(lane >= start - t * LANES, value, tiles[t + 1])
    return roll(value, to - start, -1)


def pack(own, beside, size, outs):
    y_even, y_odd, z_even, z_odd, ee, eo, oe, oo = outs
    _, gy, gz = places()
    even_y, even_z = gy % 2 == 0, gz % 2 == 0
    lane = iota((size, LANES), 1)

    def group(g, slots, get):
        top = jnp.zeros((size, LANES), jnp.float32)
        bottom = top
        for s in range(slots):
            high, low = [], []
            for k in range(5):
                v = get(k, s)
                at = 40 * s + 8 * k
                here = (lane >= at) & (lane < at + 8)
                top = jnp.where(here, roll(v, at - (size - 8), -1), top)
                bottom = jnp.where(here, roll(v, at, -1), bottom)
                high.append(v[size - 8 :])
                low.append(v[:8])
            for t, (h, l) in enumerate(zip(y_pack(high, size), y_pack(low, size))):
                y_even[3 * g + s, 8 * t : 8 * t + 8, :] = jnp.where(even_y, h, l)
                y_odd[3 * g + s, 8 * t : 8 * t + 8, :] = jnp.where(even_y, l, h)
        a, b = jnp.where(even_z, top, bottom), jnp.where(even_z, bottom, top)
        z_even[g] = a
        z_odd[g] = b
        ee[g] = jnp.where(even_y, a[size - 8 :], a[:8])
        eo[g] = jnp.where(even_y, b[size - 8 :], b[:8])
        oe[g] = jnp.where(even_y, a[:8], a[size - 8 :])
        oo[g] = jnp.where(even_y, b[:8], b[size - 8 :])

    def body(g, carry):
        group(g, 3, lambda k, s: own(k, 3 * g + s))
        return carry

    if own is not None:
        lax.fori_loop(0, size // 3, body, 0)
    if beside is not None:
        for q in range(3):
            group(size // 3 + q, min(3, 8 - 3 * q), lambda k, s: beside(k, 3 * q + s))


def place_halves(stack, own, beside, size):
    gx, _, _ = places()

    def put(p, low, high):
        for k in range(5):
            stack[k, p, 0:size, :] = roll(low(k), 8, -1) + roll(high(k), LANES // 2 + 8, -1)
            stack[k, p, size:, :] = jnp.zeros((16, LANES), jnp.float32)

    def both(g, carry):
        for u in range(3):
            p = 3 * g + u
            put(p, lambda k: own(k, p), lambda k: own(k, p + HALF))
        return carry

    lax.fori_loop(0, (size - HALF) // 3, both, 0)

    def one(p, carry):
        j = p - (size - HALF) - 4 * gx
        there = (j >= 0) & (j < 8)
        at = jnp.clip(j, 0, 7)
        put(p, lambda k: own(k, p), lambda k: jnp.where(there, beside(k, at), 0.0))
        return carry

    lax.fori_loop(size - HALF, HALF, one, 0)


def merge_halves(stack, size, payloads):
    y_even, y_odd, z_even, z_odd, ee, eo, oe, oo = payloads
    gx, gy, gz = places()
    even_y, even_z = gy % 2 == 0, gz % 2 == 0
    lane, lane_8 = iota((size, LANES), 1), iota((8, LANES), 1)
    tiles = -(-5 * size // LANES)

    def group(g, slots, first, base):
        def sides(lane, value, low, high, at):
            here = (lane >= base) & (lane < base + 8)
            value = jnp.where(here, roll(low, base - at, -1), value)
            here = (lane >= base + 56) & (lane < base + 64)
            return jnp.where(here, roll(high, base + 56 - at, -1), value)

        low = jnp.where(even_z, z_odd[g], z_even[g])
        high = jnp.where(even_z, z_even[g], z_odd[g])
        by_even = jnp.where(even_z, eo[g], ee[g]), jnp.where(even_z, ee[g], eo[g])
        by_odd = jnp.where(even_z, oo[g], oe[g]), jnp.where(even_z, oe[g], oo[g])
        corners = (
            [jnp.where(even_y, e, o) for e, o in zip(by_even, by_odd)],
            [jnp.where(even_y, o, e) for e, o in zip(by_even, by_odd)],
        )
        for s in range(slots):
            e, o = y_even[3 * g + s], y_odd[3 * g + s]
            ends = jnp.where(even_y, e, o), jnp.where(even_y, o, e)
            ends = [[end[8 * t : 8 * t + 8] for t in range(tiles)] for end in ends]
            for k in range(5):
                at = 40 * s + 8 * k
                v = stack[k, first + s, 0:size, :]
                stack[k, first + s, 0:size, :] = sides(lane, v, low, high, at)
                for which in range(2):
                    rows = slice(size + 8 * which, size + 8 * which + 8)
                    v = stack[k, first + s, rows, :]
                    middle = y_unpack(ends[which], k, size, base + 8)
                    here = (lane_8 >= base + 8) & (lane_8 < base + 56)
                    v = jnp.where(here, middle, v)
                    stack[k, first + s, rows, :] = sides(lane_8, v, *corners[which], at)

    def body_low(g, carry):
        group(g, 3, 3 * g, 0)
        return carry

    def body_high(g, carry):
        group(g + HALF // 3, 3, 3 * g, LANES // 2)
        return carry

    lax.fori_loop(0, HALF // 3, body_low, 0)
    lax.fori_loop(0, (size - HALF) // 3, body_high, 0)
    for q in range(3):
        first = size - HALF + 4 * gx + 3 * q
        group(size // 3 + q, min(3, 8 - 3 * q), first, LANES // 2)


def y_faces(values, size, at, y_even, y_odd):
    even_y = places()[1] % 2 == 0
    high = y_pack([v[size - 8 :] for v in values], size)
    low = y_pack([v[:8] for v in values], size)
    for t, (h, l) in enumerate(zip(high, low)):
        y_even[at, 8 * t : 8 * t + 8, :] = jnp.where(even_y, h, l)
        y_odd[at, 8 * t : 8 * t + 8, :] = jnp.where(even_y, l, h)


def z_faces(planes, size):
    even_z = places()[2] % 2 == 0
    rows = planes[0][0].shape[0]
    lane = iota((rows, LANES), 1)
    top = jnp.zeros((rows, LANES), jnp.float32)
    bottom = top
    for s, values in enumerate(planes):
        for k, v in enumerate(values):
            at = 40 * s + 8 * k
            here = (lane >= at) & (lane < at + 8)
            top = jnp.where(here, roll(v, at - (size - 8), -1), top)
            bottom = jnp.where(here, roll(v, at, -1), bottom)
    return jnp.where(even_z, top, bottom), jnp.where(even_z, bottom, top)


def y_sides(source, size, slots, stack, first, y_even, y_odd):
    even_y = places()[1] % 2 == 0
    lane = iota((16, LANES), 1)
    tiles = -(-5 * size // LANES)
    planes = []
    for s in range(slots):
        e, o = y_even[3 * source + s], y_odd[3 * source + s]
        ends = jnp.where(even_y, e, o), jnp.where(even_y, o, e)
        ends = [[end[8 * t : 8 * t + 8] for t in range(tiles)] for end in ends]
        values = []
        for k in range(5):
            v = jnp.concatenate([y_unpack(end, k, size, 0) for end in ends], axis=0)
            v = jnp.where(lane < size, v, 0.0)
            stack[k, first + s, size : size + 16, :] = v
            values.append(v)
        planes.append(values)
    return planes


def merge_z(stack, size, z_even, z_odd):
    gx, _, gz = places()
    even_z = gz % 2 == 0
    lane = iota((size + 16, LANES), 1)

    def group(g, slots, first):
        low = jnp.where(even_z, z_odd[g], z_even[g])
        high = jnp.where(even_z, z_even[g], z_odd[g])
        for s in range(slots):
            for k in range(5):
                at = 40 * s + 8 * k
                v = stack[k, first + s]
                v = jnp.where(lane >= LANES - 8, roll(low, LANES - 8 - at, -1), v)
                here = (lane >= size) & (lane < size + 8)
                stack[k, first + s] = jnp.where(here, roll(high, size - at, -1), v)

    def body(g, carry):
        group(g, 3, 3 * g)
        return carry

    lax.fori_loop(0, size // 3, body, 0)
    for q in range(3):
        group(size // 3 + q, min(3, 8 - 3 * q), size + gx + 3 * q)


def payload_shapes(size):
    groups = size // 3 + 3
    tall = 8 * (-(-5 * size // LANES))
    y = near(size + 8, tall, LANES)
    z = near(groups, size, LANES)
    c = near(groups, 8, LANES)
    return [y, y, z, z, c, c, c, c]


def partner(index, parity, count):
    if parity is None:
        return index
    other = index + 1 if index % 2 == parity else index - 1
    return other if 0 <= other < count else None


def swap(value, parity_y, parity_z):
    pairs = []
    for y in range(COUNT_Y):
        for z in range(COUNT_Z):
            to_y, to_z = partner(y, parity_y, COUNT_Y), partner(z, parity_z, COUNT_Z)
            if to_y is not None and to_z is not None:
                pairs.append((y * COUNT_Z + z, to_y * COUNT_Z + to_z))
    return lax.ppermute(value, YZ, pairs)


WAYS = ((0, None), (1, None), (None, 0), (None, 1), (0, 0), (0, 1), (1, 0), (1, 1))


def swap_cores(value):
    return lax.ppermute(value, "gx", [(0, 1), (1, 0)])


def f32(*shape):
    return jax.ShapeDtypeStruct(shape, jnp.float32)


def near(*shape):
    return pltpu.VMEM(shape, jnp.float32)


def call(body, outs, ins, scratch, operands, limit, aliases={}):
    held = [
        pltpu.with_memory_space_constraint(v, pltpu.HBM if spec is far else pltpu.VMEM)
        for v, spec in zip(operands, ins)
    ]
    return pl.pallas_call(
        body,
        out_shape=outs,
        out_specs=[vmem] * len(outs),
        in_specs=ins,
        scratch_shapes=scratch,
        input_output_aliases=aliases,
        compiler_params=pltpu.CompilerParams(vmem_limit_bytes=limit * 2**20),
    )(*held)


def edge_kernel(right, faces, cells, out, sems):
    gx = lax.axis_index("gx")
    start = (1 - gx) * (SIZES[0] - WIDTH)
    part = pl.ds(start, WIDTH)
    copies = [
        pltpu.make_async_copy(right.at[part], out.at[0], sems.at[0]),
        pltpu.make_async_copy(faces.at[0, part], out.at[1], sems.at[1]),
        pltpu.make_async_copy(faces.at[1, part], out.at[2], sems.at[2]),
        pltpu.make_async_copy(faces.at[2, part], out.at[3], sems.at[3]),
        pltpu.make_async_copy(cells.at[part], out.at[4], sems.at[4]),
    ]
    for copy in copies:
        copy.start()
    for copy in copies:
        copy.wait()


def own_inputs(right, faces, cells):
    def own(k, i):
        if k == 0:
            return widen(right[i])
        return widen(cells[i] if k == 4 else faces[k - 1, i])

    return own


def pack_0_kernel(right, faces, cells, beside, *outs):
    pack(own_inputs(right, faces, cells), lambda k, j: widen(beside[k, j]), SIZES[0], outs)


def place_0_kernel(right, faces, cells, beside, stack):
    own = own_inputs(right, faces, cells)
    place_halves(stack, own, lambda k, j: widen(beside[k, j]), SIZES[0])


def own_1_kernel(own, y_even, y_odd, z_even, z_odd):
    size = SIZES[1]

    def body(g, carry):
        planes = [[own[k, 3 * g + s] for k in range(5)] for s in range(3)]
        for s in range(3):
            y_faces(planes[s], size, 3 * g + s, y_even, y_odd)
        z_even[g], z_odd[g] = z_faces(planes, size)
        return carry

    lax.fori_loop(0, size // 3, body, 0)


def beside_1_kernel(beside, own_even, own_odd, y_even, y_odd):
    size = SIZES[1]
    y_even[0:size] = own_even[...]
    y_odd[0:size] = own_odd[...]
    for j in range(8):
        y_faces([beside[k, j] for k in range(5)], size, size + j, y_even, y_odd)


def fill_1_kernel(own, beside, own_even, own_odd, stack, z_even, z_odd):
    size = SIZES[1]
    gx = lax.axis_index("gx")
    z_even[0 : size // 3] = own_even[...]
    z_odd[0 : size // 3] = own_odd[...]

    def body(i, carry):
        for k in range(5):
            stack[k, i, 0:size, :] = own[k, i]
        return carry

    lax.fori_loop(0, size, body, 0)
    for q in range(3):
        slots, first = min(3, 8 - 3 * q), size + gx + 3 * q
        planes = [[beside[k, 3 * q + s] for k in range(5)] for s in range(slots)]
        for s in range(slots):
            for k in range(5):
                stack[k, first + s, 0:size, :] = planes[s][k]
        g = size // 3 + q
        z_even[g], z_odd[g] = z_faces(planes, size)
    empty = size + 8 * (1 - gx)
    for k in range(5):
        stack[k, empty] = jnp.zeros(stack.shape[2:], jnp.float32)


def side_1_kernel(filled, y_even, y_odd, own_even, own_odd, stack, z_even, z_odd):
    size = SIZES[1]
    gx = lax.axis_index("gx")
    z_even[:, 0:size, :] = own_even[...]
    z_odd[:, 0:size, :] = own_odd[...]
    sides = pl.ds(size, 16)

    def body(g, carry):
        planes = y_sides(g, size, 3, stack, 3 * g, y_even, y_odd)
        z_even[g, sides, :], z_odd[g, sides, :] = z_faces(planes, size)
        return carry

    lax.fori_loop(0, size // 3, body, 0)
    for q in range(3):
        slots, first = min(3, 8 - 3 * q), size + gx + 3 * q
        g = size // 3 + q
        planes = y_sides(g, size, slots, stack, first, y_even, y_odd)
        z_even[g, sides, :], z_odd[g, sides, :] = z_faces(planes, size)


def level_0_kernel(
    filled, ye, yo, ze, zo, ee, eo, oe, oo,
    coarse, coarse_edge, stack, iterate,
    update, rows, pairs,
):
    size = SIZES[0]
    gx = lax.axis_index("gx")
    merge_halves(stack, size, (ye, yo, ze, zo, ee, eo, oe, oo))
    down(stack, iterate, update, 1.0, HALF, HALF, Halves)
    keep_remainder(stack, iterate, update, 1.0, HALF, HALF, Halves)

    def out(k, value):
        lane = iota(value.shape, -1)
        coarse[k, 0:15] = jnp.where(lane < 24, value, 0.0)
        second = roll(value[0:9], LANES // 2, -1)
        coarse[k, 15:24] = jnp.where(lane[0:9] < 24, second, 0.0)
        coarse_edge[k] = jnp.where(gx == 0, coarse[k, 16:24], coarse[k, 0:8])

    coarsen(stack, update, rows, pairs, out, HALF, size, LANES // 2, 8)


def level_1_kernel(
    filled, z_even, z_odd, held,
    coarse, stack, iterate,
    update, rows, pairs, made,
):
    size = SIZES[1]
    planes = size + 9
    merge_z(stack, size, z_even, z_odd)
    down(stack, iterate, update, 0.25, planes, planes, Wrapped)
    keep_remainder(stack, iterate, update, 0.25, planes, planes, Wrapped)

    def out(k, value):
        made[k] = value

    coarsen(stack, update, rows, pairs, out, size, size)
    for i in range(SIZES[2] // 2):
        line = made[0, 2 * i] + roll(made[0, 2 * i + 1], LANES // 2, -1)
        for h in range(2):
            for k in range(1, 5):
                line = line + roll(made[k, 2 * i + h], LANES // 2 * h + SIZES[2] * k, -1)
        coarse[i] = line


def level_2_kernel(
    mine, other, held,
    payload, stack, iterate,
    update, rows, pairs, made, lines,
):
    size = SIZES[2]
    planes = 2 * size + 1
    gx, gy, gz = places()
    even_y, even_z = gy % 2 == 0, gz % 2 == 0
    lane = iota((16, LANES), 1)
    bases = (0, size, LANES - size)
    half = size // 2
    for k in range(5):
        stack[k, 2 * size] = jnp.zeros(stack.shape[2:], jnp.float32)

    def body(i, carry):
        for core in range(2):

            def block(a, b):
                at = half * (3 * b + a) + i
                return jnp.where(gx == core, mine[at], other[at])

            columns = []
            for b in range(3):
                even, odd = block(1, b), block(2, b)
                columns.append(
                    (block(0, b), jnp.where(even_y, even, odd), jnp.where(even_y, odd, even))
                )
            columns = [columns[0]] + [
                [jnp.where(even_z, p, q) for p, q in zip(columns[c], columns[3 - c])] for c in (1, 2)
            ]
            for h in range(2):
                plane = size * core + 2 * i + h
                for k in range(5):
                    source = (LANES // 2) * h + size * k
                    stack[k, plane, 24:32, :] = jnp.zeros((8, LANES), jnp.float32)
                    for a, first in enumerate((0, size, 40 - size)):
                        line = jnp.zeros((16, LANES), jnp.float32)
                        for b, base in enumerate(bases):
                            here = (lane >= base) & (lane < base + size)
                            line = jnp.where(here, roll(columns[b][a], base - source, -1), line)
                        stack[k, plane, first : first + size, :] = line[:size]
        return carry

    lax.fori_loop(0, half, body, 0)
    weight = 0.0625
    iterate[2 * size] = jnp.zeros(iterate.shape[1:], jnp.float32)
    down(stack, iterate, update, weight, planes, 2 * size, Middle)
    keep_remainder(stack, iterate, update, weight, planes, 2 * size, Middle)

    def out(k, value):
        made[k * 96 : k * 96 + 96, :] = value.reshape(96, LANES)

    coarsen(stack, update, rows, pairs, out, 2 * size, size)
    line = jnp.zeros((60, LANES), jnp.float32)
    for y in range(6):
        line = line + roll(made[pl.ds(y, 60, stride=8), :], 6 * y, -1)
    lines[0:60, :] = line
    chunk = lines[0:20, :] + roll(lines[20:40, :], 40, -1) + roll(lines[40:60, :], 80, -1)
    chunk = jnp.concatenate([chunk, jnp.zeros((4, LANES), jnp.float32)], axis=0)

    def repeat(c, carry):
        payload[pl.ds(pl.multiple_of(c * CHUNK, 8), CHUNK), :] = chunk
        return carry

    lax.fori_loop(0, COLUMNS, repeat, 0)


def compact(value):
    row = iota(value.shape, -2)
    out = jnp.where(row == 0, value, 0.0)
    out = jnp.where(row == 1, roll(value, -1, -2), out)
    return jnp.where(row == 2, roll(value, -2, -2), out)


def bottom(source, faces, cells):
    weight = 0.25**4
    move = Columns(3)
    face_x, face_y, face_z = faces
    nothing = jnp.zeros((1,) + source.shape[1:], jnp.float32)

    def apply(v):
        flux_x = face_x * (v - jnp.concatenate([nothing, v[:-1]], axis=0))
        flux_y = face_y * (v - move.low_y(v))
        flux_z = face_z * (v - move.low_z(v))
        total = flux_x - jnp.concatenate([flux_x[1:], nothing], axis=0)
        total = total + (flux_y - move.up_y(flux_y)) + (flux_z - move.up_z(flux_z))
        return cells * v + weight * total

    def total_of(v):
        flat = jnp.sum(jnp.sum(v, axis=0), axis=0)
        one = jnp.sum(jnp.sum(flat, axis=0, keepdims=True), axis=1, keepdims=True)
        return jnp.broadcast_to(one, flat.shape)

    iterate = jnp.zeros_like(source)
    remainder = source
    search = source
    norm_now = total_of(remainder * remainder)
    for step in range(BOTTOM):
        applied = apply(search)
        size = norm_now / total_of(search * applied)
        iterate = iterate + size * search
        if step + 1 < BOTTOM:
            remainder = remainder - size * applied
            norm_next = total_of(remainder * remainder)
            search = remainder + (norm_next / norm_now) * search
            norm_now = norm_next
    return iterate


def rise_kernel(
    gathered, stack_2, base_2, stack_1, base_1, stack_0, base_0,
    solution_out, residual_out, sums,
    iterate_0, update_0, rows_0, spare_1,
    iterate_1, update_1, rows_1, spare_2,
    iterate_2, update_2, rows_2, spare_3,
    stack_3, iterate_3, update_3, turned, table, block_3,
):
    gx, gy, gz = places()

    stack_3[...] = jnp.zeros(stack_3.shape, jnp.float32)
    blank = jnp.zeros((LANES - COLUMNS, LANES), jnp.float32)
    for r in range(20):
        part = gathered[pl.ds(r, COLUMNS, stride=CHUNK), :]
        turned[...] = jnp.transpose(jnp.concatenate([part, blank], axis=0))
        for j in range(3):
            k, x = divmod(20 * j + r, 12)
            for y in range(6):
                stack_3[k, x, y, 0:6, :] = turned[40 * j + 6 * y : 40 * j + 6 * y + 6, :]
    move = Columns(6)
    weight = 0.25**3
    iterate_3[12] = jnp.zeros(iterate_3.shape[1:], jnp.float32)
    down(stack_3, iterate_3, update_3, weight, 13, 12, move)
    keep_remainder(stack_3, iterate_3, update_3, weight, 13, 12, move)

    def coarse(k, x_pair, y_pair, z_pair, scale):
        planes = []
        for x in range(6):
            read = (lambda i: update_3[i]) if k == 0 else (lambda i: stack_3[k, i])
            v = read(2 * x)
            if x_pair:
                v = v + read(2 * x + 1)
            lines = []
            for y in range(3):
                line = v[2 * y]
                if y_pair:
                    line = line + v[2 * y + 1]
                if z_pair:
                    line = line + roll(line, -1, -2)
                lines.append(scale * compact(line))
            planes.append(jnp.stack(lines))
        return jnp.stack(planes)

    lowest = bottom(
        coarse(0, True, True, True, 0.125),
        (
            coarse(1, False, True, True, 0.25),
            coarse(2, True, False, True, 0.25),
            coarse(3, True, True, False, 0.25),
        ),
        coarse(4, True, True, True, 0.125),
    )
    row = iota((8, LANES), 0)
    for x in range(6):
        for y in range(3):
            line = lowest[x, y]
            wide = jnp.where(row == 0, line, 0.0)
            for to in range(1, 6):
                wide = jnp.where(row == to, roll(line, to - to // 2, -2), wide)
            for a in range(2):
                for b in range(2):
                    iterate_3[2 * x + a, 2 * y + b] = iterate_3[2 * x + a, 2 * y + b] + wide
    up(stack_3, iterate_3, update_3, weight, 13, 12, move)

    low_rows = jnp.zeros((32, LANES), jnp.float32)
    for q in range(6):
        two = [iterate_3[2 * q + h].reshape(48, LANES) for h in range(2)]
        table[q] = jnp.transpose(jnp.concatenate(two + [low_rows], axis=0))
    block_3[...] = jnp.zeros(block_3.shape, jnp.float32)
    lane = iota((8, LANES), 1)

    def place(q, carry):
        for a, first in ((0, 0), (1, 6), (-1, 18)):
            lines = [jnp.zeros((8, LANES), jnp.float32) for _ in range(2)]
            for b, base in ((0, 0), (1, 6), (-1, LANES - 6)):
                y, z = gy + a, gz + b
                inside = (y >= 0) & (y < COUNT_Y) & (z >= 0) & (z < COUNT_Z)
                at = jnp.where(inside, y * COUNT_Z + z, 0)
                here = (lane >= base) & (lane < base + 6) & inside
                found = jnp.broadcast_to(table[q, pl.ds(at, 1), :], (8, LANES))
                for h in range(2):
                    for y_in in range(6):
                        moved = roll(found, base - 48 * h - 8 * y_in, -1)
                        lines[h] = jnp.where(here & (row == y_in), moved, lines[h])
            for h in range(2):
                block_3[2 * q + h, first : first + 6, :] = lines[h][0:6]
        return carry

    lax.fori_loop(0, 6, place, 0)

    spread(
        block_3, spare_3, rows_2, base_2, iterate_2,
        ((0, 12, 0), (18, 6, 28)),
        ((12, lambda i: i, lambda i: 2 * i),),
        24,
    )
    up(stack_2, iterate_2, update_2, 0.0625, 25, 24, Middle)

    size = SIZES[1]
    spread(
        iterate_2, spare_2, rows_1, base_1, iterate_1,
        ((0, 16, 0), (36, 4, 32)),
        (
            (12, lambda i: 12 * gx + i, lambda i: 2 * i),
            (4, lambda i: 12 - 4 * gx + i, lambda i: size + gx + 2 * i),
        ),
        size + 8 * (1 - gx),
    )
    up(stack_1, iterate_1, update_1, 0.25, size + 9, size + 9, Wrapped)

    size = SIZES[0]
    spread_halves(iterate_1, spare_1, rows_0, base_0, iterate_0, gx)
    up(stack_0, iterate_0, update_0, 1.0, HALF, HALF, Halves)
    iterate_0[HALF] = Halves.turn(iterate_0[0])
    inside = iota((size, LANES), 1)
    in_low = (inside >= 8) & (inside < 56)
    in_high = (inside >= 72) & (inside < 120)

    def use(i, v, remainder, carry):
        v, remainder = v[0:size], remainder[0:size]
        solution_out[i] = roll(v, -8, -1)[:, 0:size]
        residual_out[i] = roll(remainder, -8, -1)[:, 0:size]

        mask = in_low
        if i < size - HALF:
            solution_out[i + HALF] = roll(v, -72, -1)[:, 0:size]
            residual_out[i + HALF] = roll(remainder, -72, -1)[:, 0:size]
            mask = in_low | in_high
        mine = jnp.where(mask, remainder, 0.0)
        given = jnp.where(mask, stack_0[0, i, 0:size, :], 0.0)
        return carry[0] + mine * mine, carry[1] + given * given

    zero = jnp.zeros((size, LANES), jnp.float32)
    squares = stencil_pass(stack_0, iterate_0, 1.0, HALF, HALF, Halves, use, (zero, zero))
    ones = []
    for square in squares:
        one = jnp.sum(jnp.sum(square, axis=0, keepdims=True), axis=1, keepdims=True)
        ones.append(jnp.broadcast_to(one, (8, LANES)))
    sums[...] = jnp.where(lane == 0, ones[0], jnp.where(lane == 1, ones[1], 0.0))


def stack_kernel(*refs):
    out = refs[-1]
    for n, ref in enumerate(refs[:-1]):
        count = ref.shape[0]
        out[n * count : n * count + count] = ref[...]


def stacked(*parts):
    count, *rest = parts[0].shape
    return call(stack_kernel, [near(len(parts) * count, *rest)], [held_near] * 3, [], parts, 1)[0]


def shards(right, faces, cells):
    dma = pltpu.SemaphoreType.DMA
    edge = call(edge_kernel, [near(5, WIDTH, 48, 48)], [far] * 3, [dma((5,))],
        (right, faces, cells), 2)[0]
    beside = swap_cores(edge)
    shapes = payload_shapes(48)
    outs = call(pack_0_kernel, shapes, [held_near] * 4, [], (right, faces, cells, beside), 4)
    moved = [swap(v, *way) for v, way in zip(outs, WAYS)]
    filled = call(place_0_kernel, [near(7, 31, 64, LANES)], [held_near] * 4, [],
        (right, faces, cells, beside), 4)[0]
    coarse, coarse_edge, stack_0, iterate_0 = call(
        level_0_kernel,
        [near(5, 24, 24, LANES), near(5, WIDTH, 24, LANES), near(7, 31, 64, LANES), near(31, 64, LANES)],
        [held_near] * 9,
        [near(31, 64, LANES), near(5, 64, LANES), near(5, 15, 24, LANES)],
        (filled, *moved),
        10,
        {0: 2},
    )
    beside = swap_cores(coarse_edge)
    y_shape, z_shape = near(32, 8, LANES), near(11, 24, LANES)
    *y_own, z_even, z_odd = call(own_1_kernel, [near(24, 8, LANES)] * 2 + [near(8, 24, LANES)] * 2,
        [held_near], [], (coarse,), 4)
    outs = call(beside_1_kernel, [y_shape] * 2, [held_near] * 3, [], (beside, *y_own), 4)
    sides = [swap(v, parity, None) for parity, v in enumerate(outs)]
    filled, *z_own = call(fill_1_kernel, [near(7, 34, 40, LANES), z_shape, z_shape],
        [held_near] * 4, [], (coarse, beside, z_even, z_odd), 4)
    filled, *outs = call(side_1_kernel, [near(7, 34, 40, LANES)] + [near(11, 40, LANES)] * 2,
        [held_near] * 5, [], (filled, *sides, *z_own), 4, {0: 0})
    z_sides = [swap(v, None, parity) for parity, v in enumerate(outs)]
    coarse, stack_1, iterate_1 = call(
        level_1_kernel,
        [near(6, 16, LANES), near(7, 34, 40, LANES), near(34, 40, LANES)],
        [held_near] * 4,
        [near(34, 40, LANES), near(5, 40, LANES), near(5, 12, 16, LANES), near(5, 12, 16, LANES)],
        (filled, *z_sides, stack_0),
        12,
        {0: 1},
    )
    column = stacked(coarse, *[swap(coarse, parity, None) for parity in (0, 1)])
    region = stacked(column, *[swap(column, None, parity) for parity in (0, 1)])
    other = swap_cores(region)
    payload, stack_2, iterate_2 = call(
        level_2_kernel,
        [near(COLUMNS * CHUNK, LANES), near(7, 26, 40, LANES), near(26, 40, LANES)],
        [held_near] * 3,
        [near(26, 40, LANES), near(5, 40, LANES), near(5, 12, 8, LANES), near(480, LANES), near(64, LANES)],
        (region, other, stack_0),
        12,
    )
    payload = payload.reshape(COLUMNS, CHUNK, LANES)
    gathered = lax.all_to_all(payload, YZ, 0, 0).reshape(COLUMNS * CHUNK, LANES)
    solved, residual, sums = call(
        rise_kernel,
        [f32(48, 48, 48), f32(48, 48, 48), f32(8, LANES)],
        [held_near] * 7,
        [
            near(31, 64, LANES), near(31, 64, LANES), near(64, LANES), near(33, 40, LANES),
            near(34, 40, LANES), near(34, 40, LANES), near(40, LANES), near(24, 40, LANES),
            near(26, 40, LANES), near(26, 40, LANES), near(40, LANES), near(12, 24, LANES),
            near(8, 14, 6, 8, LANES), near(14, 6, 8, LANES), near(14, 6, 8, LANES),
            near(LANES, LANES), near(6, LANES, LANES), near(12, 24, LANES),
        ],
        (gathered, stack_2, iterate_2, stack_1, iterate_1, stack_0, iterate_0),
        24,
    )
    each = jnp.broadcast_to(sums[0:1].reshape(1, 1, LANES), (128, 1, LANES))
    total = jnp.sum(lax.all_to_all(each, ALL, 0, 0), axis=(0, 1))
    return solved, residual, jnp.sqrt(total[0] / total[1])


def solution(mesh):
    torus = Mesh(
        mesh.devices.reshape(mesh.shape["gx"], mesh.shape["gy"], 4, 4), ("gx", "gy", "gz_0", "gz_1")
    )
    in_specs = (P("gx", "gy", GZ), P(None, "gx", "gy", GZ), P("gx", "gy", GZ))
    out_specs = (P("gx", "gy", GZ), P("gx", "gy", GZ), P())
    return jax.shard_map(
        shards, mesh=torus, in_specs=in_specs, out_specs=out_specs, check_vma=False
    )
```

```python
import functools

import jax
import jax.numpy as jnp
from jax import lax
from jax.experimental import pallas as pl
from jax.experimental.pallas import tpu as pltpu
from jax.sharding import Mesh
from jax.sharding import PartitionSpec as P

BOTTOM = 6
ALL = ("gx", "gy", "gz_0", "gz_1")
YZ = ("gy", "gz_0", "gz_1")
GZ = ("gz_0", "gz_1")
LANES = 128
WIDTH = 8
COUNT_Y = 4
COUNT_Z = 16
COLUMNS = COUNT_Y * COUNT_Z
SIZES = (48, 24, 12, 6)
CHUNK = 24
HALF = 30

theta = 1.125
delta = 0.875
sigma = theta / delta
rho_0 = 1.0 / sigma
rho_1 = 1.0 / (2.0 * sigma - rho_0)
rho_2 = 1.0 / (2.0 * sigma - rho_1)
FIRST = (0.0, 1.0 / theta)
LATER = ((rho_1 * rho_0, 2.0 * rho_1 / delta), (rho_2 * rho_1, 2.0 * rho_2 / delta))

vmem = pl.BlockSpec(memory_space=pltpu.VMEM)
held_near = pl.BlockSpec(memory_space=pltpu.VMEM)
far = pl.BlockSpec(memory_space=pltpu.HBM)


def roll(value, by, axis):
    axis = axis % value.ndim
    by = by % value.shape[axis]
    return pltpu.roll(value, by, axis) if by else value


def iota(shape, dim):
    return lax.broadcasted_iota(jnp.int32, shape, dim % len(shape))


def exact_dot(values, pick):
    pick = pick.astype(jnp.bfloat16)
    total = None
    for _ in range(3):
        part = values.astype(jnp.bfloat16)
        values = values - part.astype(jnp.float32)
        made = jnp.dot(part, pick, preferred_element_type=jnp.float32)
        total = made if total is None else total + made
    return total


class Wrapped:
    group = 33

    @staticmethod
    def turn(v):
        return v

    @staticmethod
    def low_y(v):
        return roll(v, 1, -2)

    @staticmethod
    def up_y(v):
        return roll(v, -1, -2)

    @staticmethod
    def low_z(v):
        return roll(v, 1, -1)

    @staticmethod
    def up_z(v):
        return roll(v, -1, -1)


class Middle(Wrapped):
    group = 24


class Halves(Wrapped):
    group = 30

    @staticmethod
    def turn(v):
        return roll(v, LANES // 2, -1)


class Columns:
    group = 12

    def __init__(self, cells):
        self.cells = cells

    def turn(self, v):
        return v

    def low_y(self, v):
        lane = iota(v.shape, -1)
        last = lax.slice_in_dim(v, self.cells - 1, self.cells, axis=v.ndim - 3)
        rest = lax.slice_in_dim(v, 0, self.cells - 1, axis=v.ndim - 3)
        lane = iota(last.shape, -1)
        last = jnp.where((lane >= COUNT_Z) & (lane < COLUMNS), roll(last, COUNT_Z, -1), 0.0)
        return jnp.concatenate([last, rest], axis=v.ndim - 3)

    def up_y(self, v):
        first = lax.slice_in_dim(v, 0, 1, axis=v.ndim - 3)
        rest = lax.slice_in_dim(v, 1, self.cells, axis=v.ndim - 3)
        lane = iota(first.shape, -1)
        first = jnp.where(lane < COLUMNS - COUNT_Z, roll(first, -COUNT_Z, -1), 0.0)
        return jnp.concatenate([rest, first], axis=v.ndim - 3)

    def low_z(self, v):
        lane, row = iota(v.shape, -1), iota(v.shape, -2)
        edge = roll(roll(v, 1 - self.cells, -2), 1, -1)
        edge = jnp.where((lane % COUNT_Z != 0) & (lane < COLUMNS), edge, 0.0)
        return jnp.where(row == 0, edge, roll(v, 1, -2))

    def up_z(self, v):
        lane, row = iota(v.shape, -1), iota(v.shape, -2)
        edge = roll(roll(v, self.cells - 1, -2), -1, -1)
        edge = jnp.where((lane % COUNT_Z != COUNT_Z - 1) & (lane < COLUMNS), edge, 0.0)
        inner = jnp.where(row < self.cells - 1, roll(v, -1, -2), 0.0)
        return jnp.where(row == self.cells - 1, edge, inner)


def set_up(stack, iterate, update, weight, planes, count, move):
    stack[1, planes] = move.turn(stack[1, 0])
    size = move.group

    def body(g, carry):
        for u in range(size):
            at = size * g + u
            cell, face_y, face_z = stack[4, at], stack[2, at], stack[3, at]
            above_y, above_z = move.up_y(face_y), move.up_z(face_z)
            if stack.shape[0] > 7:
                stack[7, at] = above_y
            stack[6, at] = above_z
            total = stack[1, at] + stack[1, at + 1] + face_y + above_y + face_z + above_z
            inverse = jnp.where(cell > 0.0, 1.0 / (cell + weight * total), 0.0)
            stack[5, at] = inverse
            step = FIRST[1] * (inverse * stack[0, at])
            iterate[at] = step
            update[at] = step
        return carry

    if count == size:
        body(0, 0)
    else:
        lax.fori_loop(0, count // size, body, 0)


def stencil_pass(stack, iterate, weight, planes, count, move, use, carry):
    flux = stack[1, 0] * (iterate[0] - move.turn(iterate[planes - 1]))
    by_face = stack.shape[0] > 7
    size = move.group

    def body(g, state):
        flux, carry = state
        i = size * g
        values = [iterate[i + u] for u in range(size + 1)]
        for u in range(size):
            at, v = i + u, values[u]
            above = stack[1, at + 1] * (values[u + 1] - v)
            total = flux - above
            flux = above
            if by_face:
                total = total + stack[2, at] * (v - move.low_y(v))
                total = total + stack[7, at] * (v - move.up_y(v))
            else:
                flux_y = stack[2, at] * (v - move.low_y(v))
                total = total + (flux_y - move.up_y(flux_y))
            total = total + stack[3, at] * (v - move.low_z(v))
            total = total + stack[6, at] * (v - move.up_z(v))
            carry = use(at, v, stack[0, at] - (stack[4, at] * v + weight * total), carry)
        return flux, carry

    if count == size:
        return body(0, (flux, carry))[1]
    return lax.fori_loop(0, count // size, body, (flux, carry))[1]


def sweep(stack, iterate, update, weight, planes, count, move, factors):
    keep, gain = factors
    iterate[planes] = move.turn(iterate[0])

    def use(i, v, remainder, carry):
        step = gain * (stack[5, i] * remainder)
        if keep:
            step = keep * update[i] + step
        update[i] = step
        iterate[i] = v + step
        return carry

    stencil_pass(stack, iterate, weight, planes, count, move, use, 0)


def down(stack, iterate, update, weight, planes, count, move):
    set_up(stack, iterate, update, weight, planes, count, move)
    for factors in LATER:
        sweep(stack, iterate, update, weight, planes, count, move, factors)


def up(stack, iterate, update, weight, planes, count, move):
    for factors in (FIRST,) + LATER:
        sweep(stack, iterate, update, weight, planes, count, move, factors)


def keep_remainder(stack, iterate, update, weight, planes, count, move):
    iterate[planes] = move.turn(iterate[0])

    def use(i, v, remainder, carry):
        update[i] = remainder
        return carry

    stencil_pass(stack, iterate, weight, planes, count, move, use, 0)


def coarsen(stack, remainder, rows, pairs, out, count, size, period=LANES, offset=0):
    half = size // 2

    def body(i, carry):
        for k in range(5):
            if k == 1:
                rows[k] = stack[1, 2 * i]
            elif k == 0:
                rows[k] = remainder[2 * i] + remainder[2 * i + 1]
            else:
                rows[k] = stack[k, 2 * i] + stack[k, 2 * i + 1]
        for k in range(5):
            pair = rows[k, pl.ds(0, half, stride=2), :]
            if k != 2:
                pair = pair + rows[k, pl.ds(1, half, stride=2), :]
            pairs[k, i, 0:half, :] = pair
        return carry

    if half % 8:
        pairs[...] = jnp.zeros(pairs.shape, jnp.float32)
    lax.fori_loop(0, count // 2, body, 0)
    fine, coarse = iota((LANES, LANES), 0), iota((LANES, LANES), 1)
    inside = fine % period - offset
    own = (inside >= 0) & (inside < size) & (fine // period == coarse // period)
    mean = jnp.where(own & (inside // 2 == coarse % period), 1.0, 0.0)
    even = jnp.where(own & (inside == 2 * (coarse % period)), 1.0, 0.0)
    _, planes, padded, _ = pairs.shape
    for k in range(5):
        flat = pairs[k].reshape(planes * padded, LANES)
        scale = 0.125 if k in (0, 4) else 0.25
        made = scale * exact_dot(flat, even if k == 3 else mean)
        out(k, made.reshape(planes, padded, LANES))


def spread(coarse, spare, rows, base, fine, row_map, plane_maps, empty):
    planes, height, _ = spare.shape
    source, target = iota((LANES, LANES), 0), iota((LANES, LANES), 1)
    half = target // 2
    pick = jnp.where(source == jnp.where(target < LANES // 2, half, LANES // 2 + half), 1.0, 0.0)
    wide = exact_dot(coarse[0:planes].reshape(planes * height, LANES), pick)
    spare[...] = wide.reshape(planes, height, LANES)
    rows[...] = jnp.zeros(rows.shape, jnp.float32)
    fine[empty] = rows[...]
    for count, plane_of, target_of in plane_maps:

        def body(i, carry):
            plane = plane_of(i)
            for start, number, first in row_map:
                part = spare[plane, start : start + number, :]
                rows[pl.ds(first, number, stride=2), :] = part
                rows[pl.ds(first + 1, number, stride=2), :] = part
            both = rows[...]
            at = target_of(i)
            fine[at] = base[at] + both
            fine[at + 1] = base[at + 1] + both
            return carry

        lax.fori_loop(0, count, body, 0)


def spread_halves(coarse, spare, rows, base, fine, gx):
    planes, height, _ = spare.shape
    source, target = iota((LANES, LANES), 0), iota((LANES, LANES), 1)
    wanted = (target % (LANES // 2)) // 2 + (LANES - 4)
    pick = jnp.where(source == wanted % LANES, 1.0, 0.0)
    wide = exact_dot(coarse[0:planes].reshape(planes * height, LANES), pick)
    spare[...] = wide.reshape(planes, height, LANES)
    lane = iota((height, LANES), 1)

    def body(q, carry):
        j = q - 9 - 2 * gx
        there = (q < 9) | ((j >= 0) & (j < 4))
        above = jnp.where(q < 9, q + 15, 24 + 5 * gx + jnp.clip(j, 0, 3))
        both = jnp.where(lane < LANES // 2, spare[q], jnp.where(there, spare[above], 0.0))
        for start, number, first in ((0, 28, 0), (36, 4, 56)):
            part = both[start : start + number]
            rows[pl.ds(first, number, stride=2), :] = part
            rows[pl.ds(first + 1, number, stride=2), :] = part
        wide_rows = rows[...]
        fine[2 * q] = base[2 * q] + wide_rows
        fine[2 * q + 1] = base[2 * q + 1] + wide_rows
        return carry

    lax.fori_loop(0, HALF // 2, body, 0)


def places():
    gx = lax.axis_index("gx")
    gy = lax.axis_index("gy")
    gz = lax.axis_index("gz_0") * 4 + lax.axis_index("gz_1")
    return gx, gy, gz


def widen(value):
    rows, lanes = value.shape
    if lanes == LANES:
        return value
    return jnp.concatenate([value, jnp.zeros((rows, LANES - lanes), jnp.float32)], axis=1)


def y_pack(parts, size):
    lane = iota((8, LANES), 1)
    tiles = [jnp.zeros((8, LANES), jnp.float32) for _ in range(-(-5 * size // LANES))]
    for k, part in enumerate(parts):
        start = k * size
        moved = roll(part, start % LANES, -1)
        for t in range(len(tiles)):
            a, b = max(start, t * LANES) - t * LANES, min(start + size, (t + 1) * LANES) - t * LANES
            if a < b:
                tiles[t] = jnp.where((lane >= a) & (lane < b), moved, tiles[t])
    return tiles


def y_unpack(tiles, k, size, to):
    lane = iota((8, LANES), 1)
    start = k * size
    t = start // LANES
    value = tiles[t]
    if start + size > (t + 1) * LANES:
        value = jnp.where(lane >= start - t * LANES, value, tiles[t + 1])
    return roll(value, to - start, -1)


def place_halves(stack, own, beside, size):
    gx, _, _ = places()

    def put(p, low, high):
        for k in range(5):
            stack[k, p, 0:size, :] = roll(low(k), 8, -1) + roll(high(k), LANES // 2 + 8, -1)
            stack[k, p, size:, :] = jnp.zeros((16, LANES), jnp.float32)

    def both(g, carry):
        for u in range(3):
            p = 3 * g + u
            put(p, lambda k: own(k, p), lambda k: own(k, p + HALF))
        return carry

    lax.fori_loop(0, (size - HALF) // 3, both, 0)

    def one(p, carry):
        j = p - (size - HALF) - 4 * gx
        there = (j >= 0) & (j < 8)
        at = jnp.clip(j, 0, 7)
        put(p, lambda k: own(k, p), lambda k: jnp.where(there, beside(k, at), 0.0))
        return carry

    lax.fori_loop(size - HALF, HALF, one, 0)


def each_group(size, group):
    gx = lax.axis_index("gx")

    def low(g, carry):
        group(g, 3, 3 * g, 0)
        return carry

    def high(g, carry):
        group(g + HALF // 3, 3, 3 * g, LANES // 2)
        return carry

    lax.fori_loop(0, HALF // 3, low, 0)
    lax.fori_loop(0, (size - HALF) // 3, high, 0)
    for q in range(3):
        first = size - HALF + 4 * gx + 3 * q
        group(size // 3 + q, min(3, 8 - 3 * q), first, LANES // 2)


def merge_halves(stack, size, z_even, z_odd, c_even, c_odd):
    even_z = places()[2] % 2 == 0
    lane = iota((size + 16, LANES), 1)

    def group(g, slots, first, base):
        even = jnp.concatenate([z_even[g], c_even[g]], axis=0)
        odd = jnp.concatenate([z_odd[g], c_odd[g]], axis=0)
        low, high = jnp.where(even_z, odd, even), jnp.where(even_z, even, odd)
        at_low = (lane >= base) & (lane < base + 8)
        at_high = (lane >= base + 56) & (lane < base + 64)
        for s in range(slots):
            for k in range(5):
                at = 40 * s + 8 * k
                v = stack[k, first + s]
                v = jnp.where(at_low, roll(low, base - at, -1), v)
                stack[k, first + s] = jnp.where(at_high, roll(high, base + 56 - at, -1), v)

    each_group(size, group)


def y_faces(values, size, at, y_even, y_odd):
    even_y = places()[1] % 2 == 0
    high = y_pack([v[size - 8 :] for v in values], size)
    low = y_pack([v[:8] for v in values], size)
    for t, (h, l) in enumerate(zip(high, low)):
        y_even[at, 8 * t : 8 * t + 8, :] = jnp.where(even_y, h, l)
        y_odd[at, 8 * t : 8 * t + 8, :] = jnp.where(even_y, l, h)


def z_faces(planes, size):
    even_z = places()[2] % 2 == 0
    rows = planes[0][0].shape[0]
    lane = iota((rows, LANES), 1)
    top = jnp.zeros((rows, LANES), jnp.float32)
    bottom = top
    for s, values in enumerate(planes):
        for k, v in enumerate(values):
            at = 40 * s + 8 * k
            here = (lane >= at) & (lane < at + 8)
            top = jnp.where(here, roll(v, at - (size - 8), -1), top)
            bottom = jnp.where(here, roll(v, at, -1), bottom)
    return jnp.where(even_z, top, bottom), jnp.where(even_z, bottom, top)


def y_sides(source, size, slots, keep, y_even, y_odd):
    even_y = places()[1] % 2 == 0
    lane = iota((16, LANES), 1)
    tiles = -(-5 * size // LANES)
    planes = []
    for s in range(slots):
        e, o = y_even[3 * source + s], y_odd[3 * source + s]
        ends = jnp.where(even_y, e, o), jnp.where(even_y, o, e)
        ends = [[end[8 * t : 8 * t + 8] for t in range(tiles)] for end in ends]
        values = []
        for k in range(5):
            v = jnp.concatenate([y_unpack(end, k, size, 0) for end in ends], axis=0)
            v = jnp.where(lane < size, v, 0.0)
            keep(k, s, v)
            values.append(v)
        planes.append(values)
    return planes


def merge_z(stack, size, z_even, z_odd):
    gx, _, gz = places()
    even_z = gz % 2 == 0
    lane = iota((size + 16, LANES), 1)

    def group(g, slots, first):
        low = jnp.where(even_z, z_odd[g], z_even[g])
        high = jnp.where(even_z, z_even[g], z_odd[g])
        for s in range(slots):
            for k in range(5):
                at = 40 * s + 8 * k
                v = stack[k, first + s]
                v = jnp.where(lane >= LANES - 8, roll(low, LANES - 8 - at, -1), v)
                here = (lane >= size) & (lane < size + 8)
                stack[k, first + s] = jnp.where(here, roll(high, size - at, -1), v)

    def body(g, carry):
        group(g, 3, 3 * g)
        return carry

    lax.fori_loop(0, size // 3, body, 0)
    for q in range(3):
        group(size // 3 + q, min(3, 8 - 3 * q), size + gx + 3 * q)


def partner(index, parity, count):
    if parity is None:
        return index
    other = index + 1 if index % 2 == parity else index - 1
    return other if 0 <= other < count else None


def swap(value, parity_y, parity_z):
    pairs = []
    for y in range(COUNT_Y):
        for z in range(COUNT_Z):
            to_y, to_z = partner(y, parity_y, COUNT_Y), partner(z, parity_z, COUNT_Z)
            if to_y is not None and to_z is not None:
                pairs.append((y * COUNT_Z + z, to_y * COUNT_Z + to_z))
    return lax.ppermute(value, YZ, pairs)


def swap_cores(value):
    return lax.ppermute(value, "gx", [(0, 1), (1, 0)])


def f32(*shape):
    return jax.ShapeDtypeStruct(shape, jnp.float32)


def near(*shape):
    return pltpu.VMEM(shape, jnp.float32)


def call(body, outs, ins, scratch, operands, limit, aliases={}):
    held = [
        pltpu.with_memory_space_constraint(v, pltpu.HBM if spec is far else pltpu.VMEM)
        for v, spec in zip(operands, ins)
    ]
    return pl.pallas_call(
        body,
        out_shape=outs,
        out_specs=[vmem] * len(outs),
        in_specs=ins,
        scratch_shapes=scratch,
        input_output_aliases=aliases,
        compiler_params=pltpu.CompilerParams(vmem_limit_bytes=limit * 2**20),
    )(*held)


def edge_kernel(right, faces, cells, out, sems):
    gx = lax.axis_index("gx")
    start = (1 - gx) * (SIZES[0] - WIDTH)
    part = pl.ds(start, WIDTH)
    copies = [
        pltpu.make_async_copy(right.at[part], out.at[0], sems.at[0]),
        pltpu.make_async_copy(faces.at[0, part], out.at[1], sems.at[1]),
        pltpu.make_async_copy(faces.at[1, part], out.at[2], sems.at[2]),
        pltpu.make_async_copy(faces.at[2, part], out.at[3], sems.at[3]),
        pltpu.make_async_copy(cells.at[part], out.at[4], sems.at[4]),
    ]
    for copy in copies:
        copy.start()
    for copy in copies:
        copy.wait()


def own_inputs(right, faces, cells):
    def own(k, i):
        if k == 0:
            return widen(right[i])
        return widen(cells[i] if k == 4 else faces[k - 1, i])

    return own


def pack_y_0_kernel(right, faces, cells, beside, y_even, y_odd):
    size = SIZES[0]
    own = own_inputs(right, faces, cells)

    def body(g, carry):
        for u in range(4):
            y_faces([own(k, 4 * g + u) for k in range(5)], size, 4 * g + u, y_even, y_odd)
        return carry

    lax.fori_loop(0, size // 4, body, 0)
    for j in range(8):
        y_faces([widen(beside[k, j]) for k in range(5)], size, size + j, y_even, y_odd)


def pack_z_0_kernel(right, faces, cells, beside, z_even, z_odd):
    size = SIZES[0]
    own = own_inputs(right, faces, cells)

    def body(g, carry):
        planes = [[own(k, 3 * g + s) for k in range(5)] for s in range(3)]
        z_even[g], z_odd[g] = z_faces(planes, size)
        return carry

    lax.fori_loop(0, size // 3, body, 0)
    for q in range(3):
        slots = range(min(3, 8 - 3 * q))
        planes = [[widen(beside[k, 3 * q + s]) for k in range(5)] for s in slots]
        g = size // 3 + q
        z_even[g], z_odd[g] = z_faces(planes, size)


def side_0_kernel(filled, y_even, y_odd, stack, c_even, c_odd):
    size = SIZES[0]
    rows = slice(size, size + 16)

    def group(g, slots, first, base):
        def keep(k, s, v):
            moved = roll(v, base + 8, -1)
            if base:
                moved = moved + stack[k, first + s, rows, :]
            stack[k, first + s, rows, :] = moved

        planes = y_sides(g, size, slots, keep, y_even, y_odd)
        c_even[g], c_odd[g] = z_faces(planes, size)

    each_group(size, group)


def place_0_kernel(right, faces, cells, beside, stack):
    own = own_inputs(right, faces, cells)
    place_halves(stack, own, lambda k, j: widen(beside[k, j]), SIZES[0])


def own_1_kernel(own, y_even, y_odd, z_even, z_odd):
    size = SIZES[1]

    def body(g, carry):
        planes = [[own[k, 3 * g + s] for k in range(5)] for s in range(3)]
        for s in range(3):
            y_faces(planes[s], size, 3 * g + s, y_even, y_odd)
        z_even[g], z_odd[g] = z_faces(planes, size)
        return carry

    lax.fori_loop(0, size // 3, body, 0)


def beside_1_kernel(beside, own_even, own_odd, y_even, y_odd):
    size = SIZES[1]
    y_even[0:size] = own_even[...]
    y_odd[0:size] = own_odd[...]
    for j in range(8):
        y_faces([beside[k, j] for k in range(5)], size, size + j, y_even, y_odd)


def fill_1_kernel(own, beside, own_even, own_odd, stack, z_even, z_odd):
    size = SIZES[1]
    gx = lax.axis_index("gx")
    z_even[0 : size // 3] = own_even[...]
    z_odd[0 : size // 3] = own_odd[...]

    def body(i, carry):
        for k in range(5):
            stack[k, i, 0:size, :] = own[k, i]
        return carry

    lax.fori_loop(0, size, body, 0)
    for q in range(3):
        slots, first = min(3, 8 - 3 * q), size + gx + 3 * q
        planes = [[beside[k, 3 * q + s] for k in range(5)] for s in range(slots)]
        for s in range(slots):
            for k in range(5):
                stack[k, first + s, 0:size, :] = planes[s][k]
        g = size // 3 + q
        z_even[g], z_odd[g] = z_faces(planes, size)
    empty = size + 8 * (1 - gx)
    for k in range(5):
        stack[k, empty] = jnp.zeros(stack.shape[2:], jnp.float32)


def side_1_kernel(filled, y_even, y_odd, own_even, own_odd, stack, z_even, z_odd):
    size = SIZES[1]
    gx = lax.axis_index("gx")
    z_even[:, 0:size, :] = own_even[...]
    z_odd[:, 0:size, :] = own_odd[...]
    sides = pl.ds(size, 16)

    def keep_at(first):
        def keep(k, s, v):
            stack[k, first + s, size : size + 16, :] = v

        return keep

    def body(g, carry):
        planes = y_sides(g, size, 3, keep_at(3 * g), y_even, y_odd)
        z_even[g, sides, :], z_odd[g, sides, :] = z_faces(planes, size)
        return carry

    lax.fori_loop(0, size // 3, body, 0)
    for q in range(3):
        slots, first = min(3, 8 - 3 * q), size + gx + 3 * q
        g = size // 3 + q
        planes = y_sides(g, size, slots, keep_at(first), y_even, y_odd)
        z_even[g, sides, :], z_odd[g, sides, :] = z_faces(planes, size)


def level_0_kernel(
    filled, z_even, z_odd, c_even, c_odd,
    coarse, coarse_edge, stack, iterate,
    update, rows, pairs,
):
    size = SIZES[0]
    gx = lax.axis_index("gx")
    merge_halves(stack, size, z_even, z_odd, c_even, c_odd)
    down(stack, iterate, update, 1.0, HALF, HALF, Halves)
    keep_remainder(stack, iterate, update, 1.0, HALF, HALF, Halves)

    def out(k, value):
        lane = iota(value.shape, -1)
        coarse[k, 0:15] = jnp.where(lane < 24, value, 0.0)
        second = roll(value[0:9], LANES // 2, -1)
        coarse[k, 15:24] = jnp.where(lane[0:9] < 24, second, 0.0)
        coarse_edge[k] = jnp.where(gx == 0, coarse[k, 16:24], coarse[k, 0:8])

    coarsen(stack, update, rows, pairs, out, HALF, size, LANES // 2, 8)


def level_1_kernel(
    filled, z_even, z_odd, held,
    coarse, stack, iterate,
    update, rows, pairs, made,
):
    size = SIZES[1]
    planes = size + 9
    merge_z(stack, size, z_even, z_odd)
    down(stack, iterate, update, 0.25, planes, planes, Wrapped)
    keep_remainder(stack, iterate, update, 0.25, planes, planes, Wrapped)

    def out(k, value):
        made[k] = value

    coarsen(stack, update, rows, pairs, out, size, size)
    for i in range(SIZES[2] // 2):
        line = made[0, 2 * i] + roll(made[0, 2 * i + 1], LANES // 2, -1)
        for h in range(2):
            for k in range(1, 5):
                line = line + roll(made[k, 2 * i + h], LANES // 2 * h + SIZES[2] * k, -1)
        coarse[i] = line


def level_2_kernel(
    mine, other, held,
    payload, stack, iterate,
    update, rows, pairs, made, lines,
):
    size = SIZES[2]
    planes = 2 * size + 1
    gx, gy, gz = places()
    even_y, even_z = gy % 2 == 0, gz % 2 == 0
    lane = iota((16, LANES), 1)
    bases = (0, size, LANES - size)
    half = size // 2
    for k in range(5):
        stack[k, 2 * size] = jnp.zeros(stack.shape[2:], jnp.float32)

    def body(i, carry):
        for core in range(2):

            def block(a, b):
                at = half * (3 * b + a) + i
                return jnp.where(gx == core, mine[at], other[at])

            columns = []
            for b in range(3):
                even, odd = block(1, b), block(2, b)
                columns.append(
                    (block(0, b), jnp.where(even_y, even, odd), jnp.where(even_y, odd, even))
                )
            columns = [columns[0]] + [
                [jnp.where(even_z, p, q) for p, q in zip(columns[c], columns[3 - c])] for c in (1, 2)
            ]
            for h in range(2):
                plane = size * core + 2 * i + h
                for k in range(5):
                    source = (LANES // 2) * h + size * k
                    stack[k, plane, 24:32, :] = jnp.zeros((8, LANES), jnp.float32)
                    for a, first in enumerate((0, size, 40 - size)):
                        line = jnp.zeros((16, LANES), jnp.float32)
                        for b, base in enumerate(bases):
                            here = (lane >= base) & (lane < base + size)
                            line = jnp.where(here, roll(columns[b][a], base - source, -1), line)
                        stack[k, plane, first : first + size, :] = line[:size]
        return carry

    lax.fori_loop(0, half, body, 0)
    weight = 0.0625
    iterate[2 * size] = jnp.zeros(iterate.shape[1:], jnp.float32)
    down(stack, iterate, update, weight, planes, 2 * size, Middle)
    keep_remainder(stack, iterate, update, weight, planes, 2 * size, Middle)

    def out(k, value):
        made[k * 96 : k * 96 + 96, :] = value.reshape(96, LANES)

    coarsen(stack, update, rows, pairs, out, 2 * size, size)
    line = jnp.zeros((60, LANES), jnp.float32)
    for y in range(6):
        line = line + roll(made[pl.ds(y, 60, stride=8), :], 6 * y, -1)
    lines[0:60, :] = line
    chunk = lines[0:20, :] + roll(lines[20:40, :], 40, -1) + roll(lines[40:60, :], 80, -1)
    chunk = jnp.concatenate([chunk, jnp.zeros((4, LANES), jnp.float32)], axis=0)

    def repeat(c, carry):
        payload[pl.ds(pl.multiple_of(c * CHUNK, 8), CHUNK), :] = chunk
        return carry

    lax.fori_loop(0, COLUMNS, repeat, 0)


def compact(value):
    row = iota(value.shape, -2)
    out = jnp.where(row == 0, value, 0.0)
    out = jnp.where(row == 1, roll(value, -1, -2), out)
    return jnp.where(row == 2, roll(value, -2, -2), out)


def bottom(source, faces, cells):
    weight = 0.25**4
    move = Columns(3)
    face_x, face_y, face_z = faces
    nothing = jnp.zeros((1,) + source.shape[1:], jnp.float32)

    def apply(v):
        flux_x = face_x * (v - jnp.concatenate([nothing, v[:-1]], axis=0))
        flux_y = face_y * (v - move.low_y(v))
        flux_z = face_z * (v - move.low_z(v))
        total = flux_x - jnp.concatenate([flux_x[1:], nothing], axis=0)
        total = total + (flux_y - move.up_y(flux_y)) + (flux_z - move.up_z(flux_z))
        return cells * v + weight * total

    def total_of(v):
        flat = jnp.sum(jnp.sum(v, axis=0), axis=0)
        one = jnp.sum(jnp.sum(flat, axis=0, keepdims=True), axis=1, keepdims=True)
        return jnp.broadcast_to(one, flat.shape)

    iterate = jnp.zeros_like(source)
    remainder = source
    search = source
    norm_now = total_of(remainder * remainder)
    for step in range(BOTTOM):
        applied = apply(search)
        size = norm_now / total_of(search * applied)
        iterate = iterate + size * search
        if step + 1 < BOTTOM:
            remainder = remainder - size * applied
            norm_next = total_of(remainder * remainder)
            search = remainder + (norm_next / norm_now) * search
            norm_now = norm_next
    return iterate


def rise_kernel(
    gathered, stack_2, base_2, stack_1, base_1, stack_0, base_0,
    solution_out, residual_out, sums,
    iterate_0, update_0, rows_0, spare_1,
    iterate_1, update_1, rows_1, spare_2,
    iterate_2, update_2, rows_2, spare_3,
    stack_3, iterate_3, update_3, turned, table, block_3,
):
    gx, gy, gz = places()

    stack_3[...] = jnp.zeros(stack_3.shape, jnp.float32)
    blank = jnp.zeros((LANES - COLUMNS, LANES), jnp.float32)
    for r in range(20):
        part = gathered[pl.ds(r, COLUMNS, stride=CHUNK), :]
        turned[...] = jnp.transpose(jnp.concatenate([part, blank], axis=0))
        for j in range(3):
            k, x = divmod(20 * j + r, 12)
            for y in range(6):
                stack_3[k, x, y, 0:6, :] = turned[40 * j + 6 * y : 40 * j + 6 * y + 6, :]
    move = Columns(6)
    weight = 0.25**3
    iterate_3[12] = jnp.zeros(iterate_3.shape[1:], jnp.float32)
    down(stack_3, iterate_3, update_3, weight, 13, 12, move)
    keep_remainder(stack_3, iterate_3, update_3, weight, 13, 12, move)

    def coarse(k, x_pair, y_pair, z_pair, scale):
        planes = []
        for x in range(6):
            read = (lambda i: update_3[i]) if k == 0 else (lambda i: stack_3[k, i])
            v = read(2 * x)
            if x_pair:
                v = v + read(2 * x + 1)
            lines = []
            for y in range(3):
                line = v[2 * y]
                if y_pair:
                    line = line + v[2 * y + 1]
                if z_pair:
                    line = line + roll(line, -1, -2)
                lines.append(scale * compact(line))
            planes.append(jnp.stack(lines))
        return jnp.stack(planes)

    lowest = bottom(
        coarse(0, True, True, True, 0.125),
        (
            coarse(1, False, True, True, 0.25),
            coarse(2, True, False, True, 0.25),
            coarse(3, True, True, False, 0.25),
        ),
        coarse(4, True, True, True, 0.125),
    )
    row = iota((8, LANES), 0)
    for x in range(6):
        for y in range(3):
            line = lowest[x, y]
            wide = jnp.where(row == 0, line, 0.0)
            for to in range(1, 6):
                wide = jnp.where(row == to, roll(line, to - to // 2, -2), wide)
            for a in range(2):
                for b in range(2):
                    iterate_3[2 * x + a, 2 * y + b] = iterate_3[2 * x + a, 2 * y + b] + wide
    up(stack_3, iterate_3, update_3, weight, 13, 12, move)

    low_rows = jnp.zeros((32, LANES), jnp.float32)
    for q in range(6):
        two = [iterate_3[2 * q + h].reshape(48, LANES) for h in range(2)]
        table[q] = jnp.transpose(jnp.concatenate(two + [low_rows], axis=0))
    block_3[...] = jnp.zeros(block_3.shape, jnp.float32)
    lane = iota((8, LANES), 1)

    def place(q, carry):
        for a, first in ((0, 0), (1, 6), (-1, 18)):
            lines = [jnp.zeros((8, LANES), jnp.float32) for _ in range(2)]
            for b, base in ((0, 0), (1, 6), (-1, LANES - 6)):
                y, z = gy + a, gz + b
                inside = (y >= 0) & (y < COUNT_Y) & (z >= 0) & (z < COUNT_Z)
                at = jnp.where(inside, y * COUNT_Z + z, 0)
                here = (lane >= base) & (lane < base + 6) & inside
                found = jnp.broadcast_to(table[q, pl.ds(at, 1), :], (8, LANES))
                for h in range(2):
                    for y_in in range(6):
                        moved = roll(found, base - 48 * h - 8 * y_in, -1)
                        lines[h] = jnp.where(here & (row == y_in), moved, lines[h])
            for h in range(2):
                block_3[2 * q + h, first : first + 6, :] = lines[h][0:6]
        return carry

    lax.fori_loop(0, 6, place, 0)

    spread(
        block_3, spare_3, rows_2, base_2, iterate_2,
        ((0, 12, 0), (18, 6, 28)),
        ((12, lambda i: i, lambda i: 2 * i),),
        24,
    )
    up(stack_2, iterate_2, update_2, 0.0625, 25, 24, Middle)

    size = SIZES[1]
    spread(
        iterate_2, spare_2, rows_1, base_1, iterate_1,
        ((0, 16, 0), (36, 4, 32)),
        (
            (12, lambda i: 12 * gx + i, lambda i: 2 * i),
            (4, lambda i: 12 - 4 * gx + i, lambda i: size + gx + 2 * i),
        ),
        size + 8 * (1 - gx),
    )
    up(stack_1, iterate_1, update_1, 0.25, size + 9, size + 9, Wrapped)

    size = SIZES[0]
    spread_halves(iterate_1, spare_1, rows_0, base_0, iterate_0, gx)
    up(stack_0, iterate_0, update_0, 1.0, HALF, HALF, Halves)
    iterate_0[HALF] = Halves.turn(iterate_0[0])
    inside = iota((size, LANES), 1)
    in_low = (inside >= 8) & (inside < 56)
    in_high = (inside >= 72) & (inside < 120)

    def use(i, v, remainder, carry):
        v, remainder = v[0:size], remainder[0:size]
        solution_out[i] = roll(v, -8, -1)[:, 0:size]
        residual_out[i] = roll(remainder, -8, -1)[:, 0:size]

        mask = in_low
        if i < size - HALF:
            solution_out[i + HALF] = roll(v, -72, -1)[:, 0:size]
            residual_out[i + HALF] = roll(remainder, -72, -1)[:, 0:size]
            mask = in_low | in_high
        mine = jnp.where(mask, remainder, 0.0)
        given = jnp.where(mask, stack_0[0, i, 0:size, :], 0.0)
        return carry[0] + mine * mine, carry[1] + given * given

    zero = jnp.zeros((size, LANES), jnp.float32)
    squares = stencil_pass(stack_0, iterate_0, 1.0, HALF, HALF, Halves, use, (zero, zero))
    ones = []
    for square in squares:
        one = jnp.sum(jnp.sum(square, axis=0, keepdims=True), axis=1, keepdims=True)
        ones.append(jnp.broadcast_to(one, (8, LANES)))
    sums[...] = jnp.where(lane == 0, ones[0], jnp.where(lane == 1, ones[1], 0.0))


def stack_kernel(*refs):
    out = refs[-1]
    for n, ref in enumerate(refs[:-1]):
        count = ref.shape[0]
        out[n * count : n * count + count] = ref[...]


def stacked(*parts):
    count, *rest = parts[0].shape
    return call(stack_kernel, [near(len(parts) * count, *rest)], [held_near] * 3, [], parts, 1)[0]


def shards(right, faces, cells):
    dma = pltpu.SemaphoreType.DMA
    edge = call(edge_kernel, [near(5, WIDTH, 48, 48)], [far] * 3, [dma((5,))],
        (right, faces, cells), 2)[0]
    beside = swap_cores(edge)
    given = (right, faces, cells, beside)
    outs = call(pack_y_0_kernel, [near(56, 16, LANES)] * 2, [held_near] * 4, [], given, 4)
    sides = [swap(v, parity, None) for parity, v in enumerate(outs)]
    outs = call(pack_z_0_kernel, [near(19, 48, LANES)] * 2, [held_near] * 4, [], given, 4)
    ends = [swap(v, None, parity) for parity, v in enumerate(outs)]
    filled = call(place_0_kernel, [near(7, 31, 64, LANES)], [held_near] * 4, [], given, 4)[0]
    filled, *outs = call(side_0_kernel, [near(7, 31, 64, LANES)] + [near(19, 16, LANES)] * 2,
        [held_near] * 3, [], (filled, *sides), 4, {0: 0})
    corners = [swap(v, None, parity) for parity, v in enumerate(outs)]
    coarse, coarse_edge, stack_0, iterate_0 = call(
        level_0_kernel,
        [near(5, 24, 24, LANES), near(5, WIDTH, 24, LANES), near(7, 31, 64, LANES), near(31, 64, LANES)],
        [held_near] * 5,
        [near(31, 64, LANES), near(5, 64, LANES), near(5, 15, 24, LANES)],
        (filled, *ends, *corners),
        10,
        {0: 2},
    )
    beside = swap_cores(coarse_edge)
    y_shape, z_shape = near(32, 8, LANES), near(11, 24, LANES)
    *y_own, z_even, z_odd = call(own_1_kernel, [near(24, 8, LANES)] * 2 + [near(8, 24, LANES)] * 2,
        [held_near], [], (coarse,), 4)
    outs = call(beside_1_kernel, [y_shape] * 2, [held_near] * 3, [], (beside, *y_own), 4)
    sides = [swap(v, parity, None) for parity, v in enumerate(outs)]
    filled, *z_own = call(fill_1_kernel, [near(7, 34, 40, LANES), z_shape, z_shape],
        [held_near] * 4, [], (coarse, beside, z_even, z_odd), 4)
    filled, *outs = call(side_1_kernel, [near(7, 34, 40, LANES)] + [near(11, 40, LANES)] * 2,
        [held_near] * 5, [], (filled, *sides, *z_own), 4, {0: 0})
    z_sides = [swap(v, None, parity) for parity, v in enumerate(outs)]
    coarse, stack_1, iterate_1 = call(
        level_1_kernel,
        [near(6, 16, LANES), near(7, 34, 40, LANES), near(34, 40, LANES)],
        [held_near] * 4,
        [near(34, 40, LANES), near(5, 40, LANES), near(5, 12, 16, LANES), near(5, 12, 16, LANES)],
        (filled, *z_sides, stack_0),
        12,
        {0: 1},
    )
    column = stacked(coarse, *[swap(coarse, parity, None) for parity in (0, 1)])
    region = stacked(column, *[swap(column, None, parity) for parity in (0, 1)])
    other = swap_cores(region)
    payload, stack_2, iterate_2 = call(
        level_2_kernel,
        [near(COLUMNS * CHUNK, LANES), near(7, 26, 40, LANES), near(26, 40, LANES)],
        [held_near] * 3,
        [near(26, 40, LANES), near(5, 40, LANES), near(5, 12, 8, LANES), near(480, LANES), near(64, LANES)],
        (region, other, stack_0),
        12,
    )
    payload = payload.reshape(COLUMNS, CHUNK, LANES)
    gathered = lax.all_to_all(payload, YZ, 0, 0).reshape(COLUMNS * CHUNK, LANES)
    solved, residual, sums = call(
        rise_kernel,
        [f32(48, 48, 48), f32(48, 48, 48), f32(8, LANES)],
        [held_near] * 7,
        [
            near(31, 64, LANES), near(31, 64, LANES), near(64, LANES), near(33, 40, LANES),
            near(34, 40, LANES), near(34, 40, LANES), near(40, LANES), near(24, 40, LANES),
            near(26, 40, LANES), near(26, 40, LANES), near(40, LANES), near(12, 24, LANES),
            near(8, 14, 6, 8, LANES), near(14, 6, 8, LANES), near(14, 6, 8, LANES),
            near(LANES, LANES), near(6, LANES, LANES), near(12, 24, LANES),
        ],
        (gathered, stack_2, iterate_2, stack_1, iterate_1, stack_0, iterate_0),
        24,
    )
    each = jnp.broadcast_to(sums[0:1].reshape(1, 1, LANES), (128, 1, LANES))
    total = jnp.sum(lax.all_to_all(each, ALL, 0, 0), axis=(0, 1))
    return solved, residual, jnp.sqrt(total[0] / total[1])


def solution(mesh):
    torus = Mesh(
        mesh.devices.reshape(mesh.shape["gx"], mesh.shape["gy"], 4, 4), ("gx", "gy", "gz_0", "gz_1")
    )
    in_specs = (P("gx", "gy", GZ), P(None, "gx", "gy", GZ), P("gx", "gy", GZ))
    out_specs = (P("gx", "gy", GZ), P("gx", "gy", GZ), P())
    return jax.shard_map(
        shards, mesh=torus, in_specs=in_specs, out_specs=out_specs, check_vma=False
    )
```

```python
import functools

import jax
import jax.numpy as jnp
from jax import lax
from jax.experimental import pallas as pl
from jax.experimental.pallas import tpu as pltpu
from jax.sharding import Mesh
from jax.sharding import PartitionSpec as P

BOTTOM = 6
ALL = ("gx", "gy", "gz_0", "gz_1")
YZ = ("gy", "gz_0", "gz_1")
GZ = ("gz_0", "gz_1")
LANES = 128
WIDTH = 8
COUNT_Y = 4
COUNT_Z = 16
COLUMNS = COUNT_Y * COUNT_Z
SIZES = (48, 24, 12, 6)
CHUNK = 24
HALF = 30

theta = 1.125
delta = 0.875
sigma = theta / delta
rho_0 = 1.0 / sigma
rho_1 = 1.0 / (2.0 * sigma - rho_0)
rho_2 = 1.0 / (2.0 * sigma - rho_1)
FIRST = (0.0, 1.0 / theta)
LATER = ((rho_1 * rho_0, 2.0 * rho_1 / delta), (rho_2 * rho_1, 2.0 * rho_2 / delta))

vmem = pl.BlockSpec(memory_space=pltpu.VMEM)
held_near = pl.BlockSpec(memory_space=pltpu.VMEM)
far = pl.BlockSpec(memory_space=pltpu.HBM)


def roll(value, by, axis):
    axis = axis % value.ndim
    by = by % value.shape[axis]
    return pltpu.roll(value, by, axis) if by else value


def iota(shape, dim):
    return lax.broadcasted_iota(jnp.int32, shape, dim % len(shape))


def exact_dot(values, pick):
    pick = pick.astype(jnp.bfloat16)
    total = None
    for _ in range(3):
        part = values.astype(jnp.bfloat16)
        values = values - part.astype(jnp.float32)
        made = jnp.dot(part, pick, preferred_element_type=jnp.float32)
        total = made if total is None else total + made
    return total


class Wrapped:
    group = 33

    @staticmethod
    def turn(v):
        return v

    @staticmethod
    def low_y(v):
        return roll(v, 1, -2)

    @staticmethod
    def up_y(v):
        return roll(v, -1, -2)

    @staticmethod
    def low_z(v):
        return roll(v, 1, -1)

    @staticmethod
    def up_z(v):
        return roll(v, -1, -1)


class Middle(Wrapped):
    group = 24


class Halves(Wrapped):
    group = 30

    @staticmethod
    def turn(v):
        return roll(v, LANES // 2, -1)


class Columns:
    group = 12

    def __init__(self, cells):
        self.cells = cells

    def turn(self, v):
        return v

    def low_y(self, v):
        lane = iota(v.shape, -1)
        last = lax.slice_in_dim(v, self.cells - 1, self.cells, axis=v.ndim - 3)
        rest = lax.slice_in_dim(v, 0, self.cells - 1, axis=v.ndim - 3)
        lane = iota(last.shape, -1)
        last = jnp.where((lane >= COUNT_Z) & (lane < COLUMNS), roll(last, COUNT_Z, -1), 0.0)
        return jnp.concatenate([last, rest], axis=v.ndim - 3)

    def up_y(self, v):
        first = lax.slice_in_dim(v, 0, 1, axis=v.ndim - 3)
        rest = lax.slice_in_dim(v, 1, self.cells, axis=v.ndim - 3)
        lane = iota(first.shape, -1)
        first = jnp.where(lane < COLUMNS - COUNT_Z, roll(first, -COUNT_Z, -1), 0.0)
        return jnp.concatenate([rest, first], axis=v.ndim - 3)

    def low_z(self, v):
        lane, row = iota(v.shape, -1), iota(v.shape, -2)
        edge = roll(roll(v, 1 - self.cells, -2), 1, -1)
        edge = jnp.where((lane % COUNT_Z != 0) & (lane < COLUMNS), edge, 0.0)
        return jnp.where(row == 0, edge, roll(v, 1, -2))

    def up_z(self, v):
        lane, row = iota(v.shape, -1), iota(v.shape, -2)
        edge = roll(roll(v, self.cells - 1, -2), -1, -1)
        edge = jnp.where((lane % COUNT_Z != COUNT_Z - 1) & (lane < COLUMNS), edge, 0.0)
        inner = jnp.where(row < self.cells - 1, roll(v, -1, -2), 0.0)
        return jnp.where(row == self.cells - 1, edge, inner)


def set_up(stack, iterate, update, weight, planes, count, move):
    stack[1, planes] = move.turn(stack[1, 0])
    size = move.group

    def body(g, carry):
        for u in range(size):
            at = size * g + u
            cell, face_y, face_z = stack[4, at], stack[2, at], stack[3, at]
            above_y, above_z = move.up_y(face_y), move.up_z(face_z)
            if stack.shape[0] > 7:
                stack[7, at] = above_y
            stack[6, at] = above_z
            total = stack[1, at] + stack[1, at + 1] + face_y + above_y + face_z + above_z
            inverse = jnp.where(cell > 0.0, 1.0 / (cell + weight * total), 0.0)
            stack[5, at] = inverse
            step = FIRST[1] * (inverse * stack[0, at])
            iterate[at] = step
            update[at] = step
        return carry

    if count == size:
        body(0, 0)
    else:
        lax.fori_loop(0, count // size, body, 0)


def stencil_pass(stack, iterate, weight, planes, count, move, use, carry):
    flux = stack[1, 0] * (iterate[0] - move.turn(iterate[planes - 1]))
    by_face = stack.shape[0] > 7
    size = move.group

    def body(g, state):
        flux, carry = state
        i = size * g
        values = [iterate[i + u] for u in range(size + 1)]
        for u in range(size):
            at, v = i + u, values[u]
            above = stack[1, at + 1] * (values[u + 1] - v)
            total = flux - above
            flux = above
            if by_face:
                total = total + stack[2, at] * (v - move.low_y(v))
                total = total + stack[7, at] * (v - move.up_y(v))
            else:
                flux_y = stack[2, at] * (v - move.low_y(v))
                total = total + (flux_y - move.up_y(flux_y))
            total = total + stack[3, at] * (v - move.low_z(v))
            total = total + stack[6, at] * (v - move.up_z(v))
            carry = use(at, v, stack[0, at] - (stack[4, at] * v + weight * total), carry)
        return flux, carry

    if count == size:
        return body(0, (flux, carry))[1]
    return lax.fori_loop(0, count // size, body, (flux, carry))[1]


def sweep(stack, iterate, update, weight, planes, count, move, factors):
    keep, gain = factors
    iterate[planes] = move.turn(iterate[0])

    def use(i, v, remainder, carry):
        step = gain * (stack[5, i] * remainder)
        if keep:
            step = keep * update[i] + step
        update[i] = step
        iterate[i] = v + step
        return carry

    stencil_pass(stack, iterate, weight, planes, count, move, use, 0)


def down(stack, iterate, update, weight, planes, count, move):
    set_up(stack, iterate, update, weight, planes, count, move)
    for factors in LATER:
        sweep(stack, iterate, update, weight, planes, count, move, factors)


def up(stack, iterate, update, weight, planes, count, move):
    for factors in (FIRST,) + LATER:
        sweep(stack, iterate, update, weight, planes, count, move, factors)


def keep_remainder(stack, iterate, update, weight, planes, count, move):
    iterate[planes] = move.turn(iterate[0])

    def use(i, v, remainder, carry):
        update[i] = remainder
        return carry

    stencil_pass(stack, iterate, weight, planes, count, move, use, 0)


def coarsen(stack, remainder, rows, pairs, out, count, size, period=LANES, offset=0):
    half = size // 2

    def body(i, carry):
        for k in range(5):
            if k == 1:
                rows[k] = stack[1, 2 * i]
            elif k == 0:
                rows[k] = remainder[2 * i] + remainder[2 * i + 1]
            else:
                rows[k] = stack[k, 2 * i] + stack[k, 2 * i + 1]
        for k in range(5):
            pair = rows[k, pl.ds(0, half, stride=2), :]
            if k != 2:
                pair = pair + rows[k, pl.ds(1, half, stride=2), :]
            pairs[k, i, 0:half, :] = pair
        return carry

    if half % 8:
        pairs[...] = jnp.zeros(pairs.shape, jnp.float32)
    lax.fori_loop(0, count // 2, body, 0)
    fine, coarse = iota((LANES, LANES), 0), iota((LANES, LANES), 1)
    inside = fine % period - offset
    own = (inside >= 0) & (inside < size) & (fine // period == coarse // period)
    mean = jnp.where(own & (inside // 2 == coarse % period), 1.0, 0.0)
    even = jnp.where(own & (inside == 2 * (coarse % period)), 1.0, 0.0)
    _, planes, padded, _ = pairs.shape
    for k in range(5):
        flat = pairs[k].reshape(planes * padded, LANES)
        scale = 0.125 if k in (0, 4) else 0.25
        made = scale * exact_dot(flat, even if k == 3 else mean)
        out(k, made.reshape(planes, padded, LANES))


def spread(coarse, spare, rows, base, fine, row_map, plane_maps, empty):
    planes, height, _ = spare.shape
    source, target = iota((LANES, LANES), 0), iota((LANES, LANES), 1)
    half = target // 2
    pick = jnp.where(source == jnp.where(target < LANES // 2, half, LANES // 2 + half), 1.0, 0.0)
    wide = exact_dot(coarse[0:planes].reshape(planes * height, LANES), pick)
    spare[...] = wide.reshape(planes, height, LANES)
    rows[...] = jnp.zeros(rows.shape, jnp.float32)
    fine[empty] = rows[...]
    for count, plane_of, target_of in plane_maps:

        def body(i, carry):
            plane = plane_of(i)
            for start, number, first in row_map:
                part = spare[plane, start : start + number, :]
                rows[pl.ds(first, number, stride=2), :] = part
                rows[pl.ds(first + 1, number, stride=2), :] = part
            both = rows[...]
            at = target_of(i)
            fine[at] = base[at] + both
            fine[at + 1] = base[at + 1] + both
            return carry

        lax.fori_loop(0, count, body, 0)


def spread_halves(coarse, spare, rows, base, fine, gx):
    planes, height, _ = spare.shape
    source, target = iota((LANES, LANES), 0), iota((LANES, LANES), 1)
    wanted = (target % (LANES // 2)) // 2 + (LANES - 4)
    pick = jnp.where(source == wanted % LANES, 1.0, 0.0)
    wide = exact_dot(coarse[0:planes].reshape(planes * height, LANES), pick)
    spare[...] = wide.reshape(planes, height, LANES)
    lane = iota((height, LANES), 1)

    def body(q, carry):
        j = q - 9 - 2 * gx
        there = (q < 9) | ((j >= 0) & (j < 4))
        above = jnp.where(q < 9, q + 15, 24 + 5 * gx + jnp.clip(j, 0, 3))
        both = jnp.where(lane < LANES // 2, spare[q], jnp.where(there, spare[above], 0.0))
        for start, number, first in ((0, 28, 0), (36, 4, 56)):
            part = both[start : start + number]
            rows[pl.ds(first, number, stride=2), :] = part
            rows[pl.ds(first + 1, number, stride=2), :] = part
        wide_rows = rows[...]
        fine[2 * q] = base[2 * q] + wide_rows
        fine[2 * q + 1] = base[2 * q + 1] + wide_rows
        return carry

    lax.fori_loop(0, HALF // 2, body, 0)


def places():
    gx = lax.axis_index("gx")
    gy = lax.axis_index("gy")
    gz = lax.axis_index("gz_0") * 4 + lax.axis_index("gz_1")
    return gx, gy, gz


def widen(value):
    rows, lanes = value.shape
    if lanes == LANES:
        return value
    return jnp.concatenate([value, jnp.zeros((rows, LANES - lanes), jnp.float32)], axis=1)


def y_pack(parts, size):
    lane = iota((8, LANES), 1)
    tiles = [jnp.zeros((8, LANES), jnp.float32) for _ in range(-(-5 * size // LANES))]
    for k, part in enumerate(parts):
        start = k * size
        moved = roll(part, start % LANES, -1)
        for t in range(len(tiles)):
            a, b = max(start, t * LANES) - t * LANES, min(start + size, (t + 1) * LANES) - t * LANES
            if a < b:
                tiles[t] = jnp.where((lane >= a) & (lane < b), moved, tiles[t])
    return tiles


def y_value(tiles, k, size):
    start = k * size
    t = start // LANES
    value = tiles[t]
    if start + size > (t + 1) * LANES:
        value = jnp.where(iota(value.shape, 1) >= start - t * LANES, value, tiles[t + 1])
    return value


def y_start(k, size):
    return k * size % LANES


def y_unpack(tiles, k, size, to):
    return roll(y_value(tiles, k, size), to - y_start(k, size), -1)


def y_rows(at, size, y_even, y_odd):
    even_y = places()[1] % 2 == 0
    e, o = y_even[at], y_odd[at]
    ends = jnp.where(even_y, e, o), jnp.where(even_y, o, e)
    tiles = [
        jnp.concatenate([end[8 * t : 8 * t + 8] for end in ends], axis=0)
        for t in range(-(-5 * size // LANES))
    ]
    return [y_value(tiles, k, size) for k in range(5)]


def place_halves(stack, own, beside, size, y_even, y_odd):
    gx, _, _ = places()
    lane = iota((16, LANES), 1)
    in_low = (lane >= 8) & (lane < size + 8)
    in_high = (lane >= LANES // 2 + 8) & (lane < LANES // 2 + size + 8)

    def put(p, low, high, other, there):
        near_low = y_rows(p, size, y_even, y_odd)
        near_high = y_rows(other, size, y_even, y_odd)
        for k in range(5):
            stack[k, p, 0:size, :] = roll(low(k), 8, -1) + roll(high(k), LANES // 2 + 8, -1)
            start = y_start(k, size)
            second = jnp.where(in_high & there, roll(near_high[k], LANES // 2 + 8 - start, -1), 0.0)
            stack[k, p, size:, :] = jnp.where(in_low, roll(near_low[k], 8 - start, -1), second)

    def both(g, carry):
        for u in range(3):
            p = 3 * g + u
            put(p, lambda k: own(k, p), lambda k: own(k, p + HALF), p + HALF, True)
        return carry

    lax.fori_loop(0, (size - HALF) // 3, both, 0)

    def mixed(g, carry):
        for u in range(3):
            p = size - HALF + 3 * g + u
            j = 3 * g + u - 4 * gx
            there = (j >= 0) & (j < 8)
            at = jnp.clip(j, 0, 7)
            second = lambda k: jnp.where(there, beside(k, at), 0.0)
            put(p, lambda k: own(k, p), second, size + at, there)
        return carry

    lax.fori_loop(0, (2 * HALF - size) // 3, mixed, 0)


def each_group(size, group):
    gx = lax.axis_index("gx")

    def low(g, carry):
        group(g, 3, 3 * g, 0)
        return carry

    def high(g, carry):
        group(g + HALF // 3, 3, 3 * g, LANES // 2)
        return carry

    lax.fori_loop(0, HALF // 3, low, 0)
    lax.fori_loop(0, (size - HALF) // 3, high, 0)
    for q in range(3):
        first = size - HALF + 4 * gx + 3 * q
        group(size // 3 + q, min(3, 8 - 3 * q), first, LANES // 2)


def merge_halves(stack, size, z_even, z_odd, c_even, c_odd):
    even_z = places()[2] % 2 == 0
    lane = iota((size + 16, LANES), 1)

    def group(g, slots, first, base):
        even = jnp.concatenate([z_even[g], c_even[g]], axis=0)
        odd = jnp.concatenate([z_odd[g], c_odd[g]], axis=0)
        low, high = jnp.where(even_z, odd, even), jnp.where(even_z, even, odd)
        at_low = (lane >= base) & (lane < base + 8)
        at_high = (lane >= base + 56) & (lane < base + 64)
        for s in range(slots):
            for k in range(5):
                at = 40 * s + 8 * k
                v = stack[k, first + s]
                v = jnp.where(at_low, roll(low, base - at, -1), v)
                stack[k, first + s] = jnp.where(at_high, roll(high, base + 56 - at, -1), v)

    each_group(size, group)


def y_faces(values, size, at, y_even, y_odd):
    even_y = places()[1] % 2 == 0
    high = y_pack([v[size - 8 :] for v in values], size)
    low = y_pack([v[:8] for v in values], size)
    for t, (h, l) in enumerate(zip(high, low)):
        y_even[at, 8 * t : 8 * t + 8, :] = jnp.where(even_y, h, l)
        y_odd[at, 8 * t : 8 * t + 8, :] = jnp.where(even_y, l, h)


def z_faces(planes, size, starts=(0,) * 5):
    even_z = places()[2] % 2 == 0
    rows = planes[0][0].shape[0]
    lane = iota((rows, LANES), 1)
    top = jnp.zeros((rows, LANES), jnp.float32)
    bottom = top
    for s, values in enumerate(planes):
        for k, v in enumerate(values):
            at = 40 * s + 8 * k
            here = (lane >= at) & (lane < at + 8)
            top = jnp.where(here, roll(v, at - starts[k] - (size - 8), -1), top)
            bottom = jnp.where(here, roll(v, at - starts[k], -1), bottom)
    return jnp.where(even_z, top, bottom), jnp.where(even_z, bottom, top)


def y_sides(source, size, slots, keep, y_even, y_odd):
    even_y = places()[1] % 2 == 0
    lane = iota((16, LANES), 1)
    tiles = -(-5 * size // LANES)
    planes = []
    for s in range(slots):
        e, o = y_even[3 * source + s], y_odd[3 * source + s]
        ends = jnp.where(even_y, e, o), jnp.where(even_y, o, e)
        ends = [[end[8 * t : 8 * t + 8] for t in range(tiles)] for end in ends]
        values = []
        for k in range(5):
            v = jnp.concatenate([y_unpack(end, k, size, 0) for end in ends], axis=0)
            v = jnp.where(lane < size, v, 0.0)
            keep(k, s, v)
            values.append(v)
        planes.append(values)
    return planes


def merge_z(stack, size, z_even, z_odd):
    gx, _, gz = places()
    even_z = gz % 2 == 0
    lane = iota((size + 16, LANES), 1)

    def group(g, slots, first):
        low = jnp.where(even_z, z_odd[g], z_even[g])
        high = jnp.where(even_z, z_even[g], z_odd[g])
        for s in range(slots):
            for k in range(5):
                at = 40 * s + 8 * k
                v = stack[k, first + s]
                v = jnp.where(lane >= LANES - 8, roll(low, LANES - 8 - at, -1), v)
                here = (lane >= size) & (lane < size + 8)
                stack[k, first + s] = jnp.where(here, roll(high, size - at, -1), v)

    def body(g, carry):
        group(g, 3, 3 * g)
        return carry

    lax.fori_loop(0, size // 3, body, 0)
    for q in range(3):
        group(size // 3 + q, min(3, 8 - 3 * q), size + gx + 3 * q)


def partner(index, parity, count):
    if parity is None:
        return index
    other = index + 1 if index % 2 == parity else index - 1
    return other if 0 <= other < count else None


def swap(value, parity_y, parity_z):
    pairs = []
    for y in range(COUNT_Y):
        for z in range(COUNT_Z):
            to_y, to_z = partner(y, parity_y, COUNT_Y), partner(z, parity_z, COUNT_Z)
            if to_y is not None and to_z is not None:
                pairs.append((y * COUNT_Z + z, to_y * COUNT_Z + to_z))
    return lax.ppermute(value, YZ, pairs)


def swap_cores(value):
    return lax.ppermute(value, "gx", [(0, 1), (1, 0)])


def f32(*shape):
    return jax.ShapeDtypeStruct(shape, jnp.float32)


def near(*shape):
    return pltpu.VMEM(shape, jnp.float32)


def call(body, outs, ins, scratch, operands, limit, aliases={}):
    held = [
        pltpu.with_memory_space_constraint(v, pltpu.HBM if spec is far else pltpu.VMEM)
        for v, spec in zip(operands, ins)
    ]
    return pl.pallas_call(
        body,
        out_shape=outs,
        out_specs=[vmem] * len(outs),
        in_specs=ins,
        scratch_shapes=scratch,
        input_output_aliases=aliases,
        compiler_params=pltpu.CompilerParams(vmem_limit_bytes=limit * 2**20),
    )(*held)


def edge_kernel(right, faces, cells, out, sems):
    gx = lax.axis_index("gx")
    start = (1 - gx) * (SIZES[0] - WIDTH)
    part = pl.ds(start, WIDTH)
    copies = [
        pltpu.make_async_copy(right.at[part], out.at[0], sems.at[0]),
        pltpu.make_async_copy(faces.at[0, part], out.at[1], sems.at[1]),
        pltpu.make_async_copy(faces.at[1, part], out.at[2], sems.at[2]),
        pltpu.make_async_copy(faces.at[2, part], out.at[3], sems.at[3]),
        pltpu.make_async_copy(cells.at[part], out.at[4], sems.at[4]),
    ]
    for copy in copies:
        copy.start()
    for copy in copies:
        copy.wait()


def own_inputs(right, faces, cells):
    def own(k, i):
        if k == 0:
            return widen(right[i])
        return widen(cells[i] if k == 4 else faces[k - 1, i])

    return own


def pack_y_0_kernel(right, faces, cells, beside, y_even, y_odd):
    size = SIZES[0]
    own = own_inputs(right, faces, cells)

    def body(g, carry):
        for u in range(4):
            y_faces([own(k, 4 * g + u) for k in range(5)], size, 4 * g + u, y_even, y_odd)
        return carry

    lax.fori_loop(0, size // 4, body, 0)
    for j in range(8):
        y_faces([widen(beside[k, j]) for k in range(5)], size, size + j, y_even, y_odd)


def pack_z_0_kernel(right, faces, cells, beside, z_even, z_odd):
    size = SIZES[0]
    own = own_inputs(right, faces, cells)

    def body(h, carry):
        for u in range(2):
            g = 2 * h + u
            planes = [[own(k, 3 * g + s) for k in range(5)] for s in range(3)]
            z_even[g], z_odd[g] = z_faces(planes, size)
        return carry

    lax.fori_loop(0, size // 6, body, 0)
    for q in range(3):
        slots = range(min(3, 8 - 3 * q))
        planes = [[widen(beside[k, 3 * q + s]) for k in range(5)] for s in slots]
        g = size // 3 + q
        z_even[g], z_odd[g] = z_faces(planes, size)


def corner_0_kernel(y_even, y_odd, c_even, c_odd):
    size = SIZES[0]
    starts = [y_start(k, size) for k in range(5)]

    def group(g, slots):
        planes = [y_rows(3 * g + s, size, y_even, y_odd) for s in range(slots)]
        c_even[g], c_odd[g] = z_faces(planes, size, starts)

    def body(h, carry):
        for u in range(3):
            group(3 * h + u, 3)
        return carry

    lax.fori_loop(0, 6, body, 0)
    group(18, 2)


def place_0_kernel(right, faces, cells, beside, y_even, y_odd, stack):
    own = own_inputs(right, faces, cells)
    place_halves(stack, own, lambda k, j: widen(beside[k, j]), SIZES[0], y_even, y_odd)


def own_1_kernel(own, y_even, y_odd, z_even, z_odd):
    size = SIZES[1]

    def body(g, carry):
        planes = [[own[k, 3 * g + s] for k in range(5)] for s in range(3)]
        for s in range(3):
            y_faces(planes[s], size, 3 * g + s, y_even, y_odd)
        z_even[g], z_odd[g] = z_faces(planes, size)
        return carry

    lax.fori_loop(0, size // 3, body, 0)


def beside_1_kernel(beside, own_even, own_odd, y_even, y_odd):
    size = SIZES[1]
    y_even[0:size] = own_even[...]
    y_odd[0:size] = own_odd[...]
    for j in range(8):
        y_faces([beside[k, j] for k in range(5)], size, size + j, y_even, y_odd)


def fill_1_kernel(own, beside, own_even, own_odd, stack, z_even, z_odd):
    size = SIZES[1]
    gx = lax.axis_index("gx")
    z_even[0 : size // 3] = own_even[...]
    z_odd[0 : size // 3] = own_odd[...]

    def body(i, carry):
        for k in range(5):
            stack[k, i, 0:size, :] = own[k, i]
        return carry

    lax.fori_loop(0, size, body, 0)
    for q in range(3):
        slots, first = min(3, 8 - 3 * q), size + gx + 3 * q
        planes = [[beside[k, 3 * q + s] for k in range(5)] for s in range(slots)]
        for s in range(slots):
            for k in range(5):
                stack[k, first + s, 0:size, :] = planes[s][k]
        g = size // 3 + q
        z_even[g], z_odd[g] = z_faces(planes, size)
    empty = size + 8 * (1 - gx)
    for k in range(5):
        stack[k, empty] = jnp.zeros(stack.shape[2:], jnp.float32)


def side_1_kernel(filled, y_even, y_odd, own_even, own_odd, stack, z_even, z_odd):
    size = SIZES[1]
    gx = lax.axis_index("gx")
    z_even[:, 0:size, :] = own_even[...]
    z_odd[:, 0:size, :] = own_odd[...]
    sides = pl.ds(size, 16)

    def keep_at(first):
        def keep(k, s, v):
            stack[k, first + s, size : size + 16, :] = v

        return keep

    def body(g, carry):
        planes = y_sides(g, size, 3, keep_at(3 * g), y_even, y_odd)
        z_even[g, sides, :], z_odd[g, sides, :] = z_faces(planes, size)
        return carry

    lax.fori_loop(0, size // 3, body, 0)
    for q in range(3):
        slots, first = min(3, 8 - 3 * q), size + gx + 3 * q
        g = size // 3 + q
        planes = y_sides(g, size, slots, keep_at(first), y_even, y_odd)
        z_even[g, sides, :], z_odd[g, sides, :] = z_faces(planes, size)


def level_0_kernel(
    filled, z_even, z_odd, c_even, c_odd,
    coarse, coarse_edge, stack, iterate,
    update, rows, pairs,
):
    size = SIZES[0]
    gx = lax.axis_index("gx")
    merge_halves(stack, size, z_even, z_odd, c_even, c_odd)
    down(stack, iterate, update, 1.0, HALF, HALF, Halves)
    keep_remainder(stack, iterate, update, 1.0, HALF, HALF, Halves)

    def out(k, value):
        lane = iota(value.shape, -1)
        coarse[k, 0:15] = jnp.where(lane < 24, value, 0.0)
        second = roll(value[0:9], LANES // 2, -1)
        coarse[k, 15:24] = jnp.where(lane[0:9] < 24, second, 0.0)
        coarse_edge[k] = jnp.where(gx == 0, coarse[k, 16:24], coarse[k, 0:8])

    coarsen(stack, update, rows, pairs, out, HALF, size, LANES // 2, 8)


def level_1_kernel(
    filled, z_even, z_odd, held,
    coarse, stack, iterate,
    update, rows, pairs, made,
):
    size = SIZES[1]
    planes = size + 9
    merge_z(stack, size, z_even, z_odd)
    down(stack, iterate, update, 0.25, planes, planes, Wrapped)
    keep_remainder(stack, iterate, update, 0.25, planes, planes, Wrapped)

    def out(k, value):
        made[k] = value

    coarsen(stack, update, rows, pairs, out, size, size)
    for i in range(SIZES[2] // 2):
        line = made[0, 2 * i] + roll(made[0, 2 * i + 1], LANES // 2, -1)
        for h in range(2):
            for k in range(1, 5):
                line = line + roll(made[k, 2 * i + h], LANES // 2 * h + SIZES[2] * k, -1)
        coarse[i] = line


def level_2_kernel(
    mine, other, held,
    payload, stack, iterate,
    update, rows, pairs, made, lines,
):
    size = SIZES[2]
    planes = 2 * size + 1
    gx, gy, gz = places()
    even_y, even_z = gy % 2 == 0, gz % 2 == 0
    lane = iota((16, LANES), 1)
    bases = (0, size, LANES - size)
    half = size // 2
    for k in range(5):
        stack[k, 2 * size] = jnp.zeros(stack.shape[2:], jnp.float32)

    def body(i, carry):
        for core in range(2):

            def block(a, b):
                at = half * (3 * b + a) + i
                return jnp.where(gx == core, mine[at], other[at])

            columns = []
            for b in range(3):
                even, odd = block(1, b), block(2, b)
                columns.append(
                    (block(0, b), jnp.where(even_y, even, odd), jnp.where(even_y, odd, even))
                )
            columns = [columns[0]] + [
                [jnp.where(even_z, p, q) for p, q in zip(columns[c], columns[3 - c])] for c in (1, 2)
            ]
            for h in range(2):
                plane = size * core + 2 * i + h
                for k in range(5):
                    source = (LANES // 2) * h + size * k
                    stack[k, plane, 24:32, :] = jnp.zeros((8, LANES), jnp.float32)
                    for a, first in enumerate((0, size, 40 - size)):
                        line = jnp.zeros((16, LANES), jnp.float32)
                        for b, base in enumerate(bases):
                            here = (lane >= base) & (lane < base + size)
                            line = jnp.where(here, roll(columns[b][a], base - source, -1), line)
                        stack[k, plane, first : first + size, :] = line[:size]
        return carry

    lax.fori_loop(0, half, body, 0)
    weight = 0.0625
    iterate[2 * size] = jnp.zeros(iterate.shape[1:], jnp.float32)
    down(stack, iterate, update, weight, planes, 2 * size, Middle)
    keep_remainder(stack, iterate, update, weight, planes, 2 * size, Middle)

    def out(k, value):
        made[k * 96 : k * 96 + 96, :] = value.reshape(96, LANES)

    coarsen(stack, update, rows, pairs, out, 2 * size, size)
    line = jnp.zeros((60, LANES), jnp.float32)
    for y in range(6):
        line = line + roll(made[pl.ds(y, 60, stride=8), :], 6 * y, -1)
    lines[0:60, :] = line
    chunk = lines[0:20, :] + roll(lines[20:40, :], 40, -1) + roll(lines[40:60, :], 80, -1)
    chunk = jnp.concatenate([chunk, jnp.zeros((4, LANES), jnp.float32)], axis=0)

    def repeat(c, carry):
        payload[pl.ds(pl.multiple_of(c * CHUNK, 8), CHUNK), :] = chunk
        return carry

    lax.fori_loop(0, COLUMNS, repeat, 0)


def compact(value):
    row = iota(value.shape, -2)
    out = jnp.where(row == 0, value, 0.0)
    out = jnp.where(row == 1, roll(value, -1, -2), out)
    return jnp.where(row == 2, roll(value, -2, -2), out)


def bottom(source, faces, cells):
    weight = 0.25**4
    move = Columns(3)
    face_x, face_y, face_z = faces
    nothing = jnp.zeros((1,) + source.shape[1:], jnp.float32)

    def apply(v):
        flux_x = face_x * (v - jnp.concatenate([nothing, v[:-1]], axis=0))
        flux_y = face_y * (v - move.low_y(v))
        flux_z = face_z * (v - move.low_z(v))
        total = flux_x - jnp.concatenate([flux_x[1:], nothing], axis=0)
        total = total + (flux_y - move.up_y(flux_y)) + (flux_z - move.up_z(flux_z))
        return cells * v + weight * total

    def total_of(v):
        flat = jnp.sum(jnp.sum(v, axis=0), axis=0)
        one = jnp.sum(jnp.sum(flat, axis=0, keepdims=True), axis=1, keepdims=True)
        return jnp.broadcast_to(one, flat.shape)

    iterate = jnp.zeros_like(source)
    remainder = source
    search = source
    norm_now = total_of(remainder * remainder)
    for step in range(BOTTOM):
        applied = apply(search)
        size = norm_now / total_of(search * applied)
        iterate = iterate + size * search
        if step + 1 < BOTTOM:
            remainder = remainder - size * applied
            norm_next = total_of(remainder * remainder)
            search = remainder + (norm_next / norm_now) * search
            norm_now = norm_next
    return iterate


def rise_kernel(
    gathered, stack_2, base_2, stack_1, base_1, stack_0, base_0,
    solution_out, residual_out, sums,
    iterate_0, update_0, rows_0, spare_1,
    iterate_1, update_1, rows_1, spare_2,
    iterate_2, update_2, rows_2, spare_3,
    stack_3, iterate_3, update_3, turned, table, block_3,
):
    gx, gy, gz = places()

    stack_3[...] = jnp.zeros(stack_3.shape, jnp.float32)
    blank = jnp.zeros((LANES - COLUMNS, LANES), jnp.float32)
    for r in range(20):
        part = gathered[pl.ds(r, COLUMNS, stride=CHUNK), :]
        turned[...] = jnp.transpose(jnp.concatenate([part, blank], axis=0))
        for j in range(3):
            k, x = divmod(20 * j + r, 12)
            for y in range(6):
                stack_3[k, x, y, 0:6, :] = turned[40 * j + 6 * y : 40 * j + 6 * y + 6, :]
    move = Columns(6)
    weight = 0.25**3
    iterate_3[12] = jnp.zeros(iterate_3.shape[1:], jnp.float32)
    down(stack_3, iterate_3, update_3, weight, 13, 12, move)
    keep_remainder(stack_3, iterate_3, update_3, weight, 13, 12, move)

    def coarse(k, x_pair, y_pair, z_pair, scale):
        planes = []
        for x in range(6):
            read = (lambda i: update_3[i]) if k == 0 else (lambda i: stack_3[k, i])
            v = read(2 * x)
            if x_pair:
                v = v + read(2 * x + 1)
            lines = []
            for y in range(3):
                line = v[2 * y]
                if y_pair:
                    line = line + v[2 * y + 1]
                if z_pair:
                    line = line + roll(line, -1, -2)
                lines.append(scale * compact(line))
            planes.append(jnp.stack(lines))
        return jnp.stack(planes)

    lowest = bottom(
        coarse(0, True, True, True, 0.125),
        (
            coarse(1, False, True, True, 0.25),
            coarse(2, True, False, True, 0.25),
            coarse(3, True, True, False, 0.25),
        ),
        coarse(4, True, True, True, 0.125),
    )
    row = iota((8, LANES), 0)
    for x in range(6):
        for y in range(3):
            line = lowest[x, y]
            wide = jnp.where(row == 0, line, 0.0)
            for to in range(1, 6):
                wide = jnp.where(row == to, roll(line, to - to // 2, -2), wide)
            for a in range(2):
                for b in range(2):
                    iterate_3[2 * x + a, 2 * y + b] = iterate_3[2 * x + a, 2 * y + b] + wide
    up(stack_3, iterate_3, update_3, weight, 13, 12, move)

    low_rows = jnp.zeros((32, LANES), jnp.float32)
    for q in range(6):
        two = [iterate_3[2 * q + h].reshape(48, LANES) for h in range(2)]
        table[q] = jnp.transpose(jnp.concatenate(two + [low_rows], axis=0))
    block_3[...] = jnp.zeros(block_3.shape, jnp.float32)
    lane = iota((8, LANES), 1)

    def place(q, carry):
        for a, first in ((0, 0), (1, 6), (-1, 18)):
            lines = [jnp.zeros((8, LANES), jnp.float32) for _ in range(2)]
            for b, base in ((0, 0), (1, 6), (-1, LANES - 6)):
                y, z = gy + a, gz + b
                inside = (y >= 0) & (y < COUNT_Y) & (z >= 0) & (z < COUNT_Z)
                at = jnp.where(inside, y * COUNT_Z + z, 0)
                here = (lane >= base) & (lane < base + 6) & inside
                found = jnp.broadcast_to(table[q, pl.ds(at, 1), :], (8, LANES))
                for h in range(2):
                    for y_in in range(6):
                        moved = roll(found, base - 48 * h - 8 * y_in, -1)
                        lines[h] = jnp.where(here & (row == y_in), moved, lines[h])
            for h in range(2):
                block_3[2 * q + h, first : first + 6, :] = lines[h][0:6]
        return carry

    lax.fori_loop(0, 6, place, 0)

    spread(
        block_3, spare_3, rows_2, base_2, iterate_2,
        ((0, 12, 0), (18, 6, 28)),
        ((12, lambda i: i, lambda i: 2 * i),),
        24,
    )
    up(stack_2, iterate_2, update_2, 0.0625, 25, 24, Middle)

    size = SIZES[1]
    spread(
        iterate_2, spare_2, rows_1, base_1, iterate_1,
        ((0, 16, 0), (36, 4, 32)),
        (
            (12, lambda i: 12 * gx + i, lambda i: 2 * i),
            (4, lambda i: 12 - 4 * gx + i, lambda i: size + gx + 2 * i),
        ),
        size + 8 * (1 - gx),
    )
    up(stack_1, iterate_1, update_1, 0.25, size + 9, size + 9, Wrapped)

    size = SIZES[0]
    spread_halves(iterate_1, spare_1, rows_0, base_0, iterate_0, gx)
    up(stack_0, iterate_0, update_0, 1.0, HALF, HALF, Halves)
    iterate_0[HALF] = Halves.turn(iterate_0[0])
    inside = iota((size, LANES), 1)
    in_low = (inside >= 8) & (inside < 56)
    in_high = (inside >= 72) & (inside < 120)

    def use(i, v, remainder, carry):
        v, remainder = v[0:size], remainder[0:size]
        solution_out[i] = roll(v, -8, -1)[:, 0:size]
        residual_out[i] = roll(remainder, -8, -1)[:, 0:size]

        mask = in_low
        if i < size - HALF:
            solution_out[i + HALF] = roll(v, -72, -1)[:, 0:size]
            residual_out[i + HALF] = roll(remainder, -72, -1)[:, 0:size]
            mask = in_low | in_high
        mine = jnp.where(mask, remainder, 0.0)
        given = jnp.where(mask, stack_0[0, i, 0:size, :], 0.0)
        return carry[0] + mine * mine, carry[1] + given * given

    zero = jnp.zeros((size, LANES), jnp.float32)
    squares = stencil_pass(stack_0, iterate_0, 1.0, HALF, HALF, Halves, use, (zero, zero))
    ones = []
    for square in squares:
        one = jnp.sum(jnp.sum(square, axis=0, keepdims=True), axis=1, keepdims=True)
        ones.append(jnp.broadcast_to(one, (8, LANES)))
    sums[...] = jnp.where(lane == 0, ones[0], jnp.where(lane == 1, ones[1], 0.0))


def stack_kernel(*refs):
    out = refs[-1]
    for n, ref in enumerate(refs[:-1]):
        count = ref.shape[0]
        out[n * count : n * count + count] = ref[...]


def stacked(*parts):
    count, *rest = parts[0].shape
    return call(stack_kernel, [near(len(parts) * count, *rest)], [held_near] * 3, [], parts, 1)[0]


def shards(right, faces, cells):
    dma = pltpu.SemaphoreType.DMA
    edge = call(edge_kernel, [near(5, WIDTH, 48, 48)], [far] * 3, [dma((5,))],
        (right, faces, cells), 2)[0]
    beside = swap_cores(edge)
    given = (right, faces, cells, beside)
    outs = call(pack_y_0_kernel, [near(56, 16, LANES)] * 2, [held_near] * 4, [], given, 4)
    sides = [swap(v, parity, None) for parity, v in enumerate(outs)]
    outs = call(pack_z_0_kernel, [near(19, 48, LANES)] * 2, [held_near] * 4, [], given, 4)
    ends = [swap(v, None, parity) for parity, v in enumerate(outs)]
    outs = call(corner_0_kernel, [near(19, 16, LANES)] * 2, [held_near] * 2, [], sides, 4)
    corners = [swap(v, None, parity) for parity, v in enumerate(outs)]
    filled = call(place_0_kernel, [near(7, 31, 64, LANES)], [held_near] * 6, [],
        (*given, *sides), 4)[0]
    coarse, coarse_edge, stack_0, iterate_0 = call(
        level_0_kernel,
        [near(5, 24, 24, LANES), near(5, WIDTH, 24, LANES), near(7, 31, 64, LANES), near(31, 64, LANES)],
        [held_near] * 5,
        [near(31, 64, LANES), near(5, 64, LANES), near(5, 15, 24, LANES)],
        (filled, *ends, *corners),
        10,
        {0: 2},
    )
    beside = swap_cores(coarse_edge)
    y_shape, z_shape = near(32, 8, LANES), near(11, 24, LANES)
    *y_own, z_even, z_odd = call(own_1_kernel, [near(24, 8, LANES)] * 2 + [near(8, 24, LANES)] * 2,
        [held_near], [], (coarse,), 4)
    outs = call(beside_1_kernel, [y_shape] * 2, [held_near] * 3, [], (beside, *y_own), 4)
    sides = [swap(v, parity, None) for parity, v in enumerate(outs)]
    filled, *z_own = call(fill_1_kernel, [near(7, 34, 40, LANES), z_shape, z_shape],
        [held_near] * 4, [], (coarse, beside, z_even, z_odd), 4)
    filled, *outs = call(side_1_kernel, [near(7, 34, 40, LANES)] + [near(11, 40, LANES)] * 2,
        [held_near] * 5, [], (filled, *sides, *z_own), 4, {0: 0})
    z_sides = [swap(v, None, parity) for parity, v in enumerate(outs)]
    coarse, stack_1, iterate_1 = call(
        level_1_kernel,
        [near(6, 16, LANES), near(7, 34, 40, LANES), near(34, 40, LANES)],
        [held_near] * 4,
        [near(34, 40, LANES), near(5, 40, LANES), near(5, 12, 16, LANES), near(5, 12, 16, LANES)],
        (filled, *z_sides, stack_0),
        12,
        {0: 1},
    )
    column = stacked(coarse, *[swap(coarse, parity, None) for parity in (0, 1)])
    region = stacked(column, *[swap(column, None, parity) for parity in (0, 1)])
    other = swap_cores(region)
    payload, stack_2, iterate_2 = call(
        level_2_kernel,
        [near(COLUMNS * CHUNK, LANES), near(7, 26, 40, LANES), near(26, 40, LANES)],
        [held_near] * 3,
        [near(26, 40, LANES), near(5, 40, LANES), near(5, 12, 8, LANES), near(480, LANES), near(64, LANES)],
        (region, other, stack_0),
        12,
    )
    payload = payload.reshape(COLUMNS, CHUNK, LANES)
    gathered = lax.all_to_all(payload, YZ, 0, 0).reshape(COLUMNS * CHUNK, LANES)
    solved, residual, sums = call(
        rise_kernel,
        [f32(48, 48, 48), f32(48, 48, 48), f32(8, LANES)],
        [held_near] * 7,
        [
            near(31, 64, LANES), near(31, 64, LANES), near(64, LANES), near(33, 40, LANES),
            near(34, 40, LANES), near(34, 40, LANES), near(40, LANES), near(24, 40, LANES),
            near(26, 40, LANES), near(26, 40, LANES), near(40, LANES), near(12, 24, LANES),
            near(8, 14, 6, 8, LANES), near(14, 6, 8, LANES), near(14, 6, 8, LANES),
            near(LANES, LANES), near(6, LANES, LANES), near(12, 24, LANES),
        ],
        (gathered, stack_2, iterate_2, stack_1, iterate_1, stack_0, iterate_0),
        24,
    )
    each = jnp.broadcast_to(sums[0:1].reshape(1, 1, LANES), (128, 1, LANES))
    total = jnp.sum(lax.all_to_all(each, ALL, 0, 0), axis=(0, 1))
    return solved, residual, jnp.sqrt(total[0] / total[1])


def solution(mesh):
    torus = Mesh(
        mesh.devices.reshape(mesh.shape["gx"], mesh.shape["gy"], 4, 4), ("gx", "gy", "gz_0", "gz_1")
    )
    in_specs = (P("gx", "gy", GZ), P(None, "gx", "gy", GZ), P("gx", "gy", GZ))
    out_specs = (P("gx", "gy", GZ), P("gx", "gy", GZ), P())
    return jax.shard_map(
        shards, mesh=torus, in_specs=in_specs, out_specs=out_specs, check_vma=False
    )
```

```python
import functools

import jax
import jax.numpy as jnp
from jax import lax
from jax.experimental import pallas as pl
from jax.experimental.pallas import tpu as pltpu
from jax.sharding import Mesh
from jax.sharding import PartitionSpec as P

BOTTOM = 6
ALL = ("gx", "gy", "gz_0", "gz_1")
YZ = ("gy", "gz_0", "gz_1")
GZ = ("gz_0", "gz_1")
LANES = 128
WIDTH = 8
COUNT_Y = 4
COUNT_Z = 16
COLUMNS = COUNT_Y * COUNT_Z
SIZES = (48, 24, 12, 6)
CHUNK = 24
HALF = 30

theta = 1.125
delta = 0.875
sigma = theta / delta
rho_0 = 1.0 / sigma
rho_1 = 1.0 / (2.0 * sigma - rho_0)
rho_2 = 1.0 / (2.0 * sigma - rho_1)
FIRST = (0.0, 1.0 / theta)
LATER = ((rho_1 * rho_0, 2.0 * rho_1 / delta), (rho_2 * rho_1, 2.0 * rho_2 / delta))

vmem = pl.BlockSpec(memory_space=pltpu.VMEM)
held_near = pl.BlockSpec(memory_space=pltpu.VMEM)
far = pl.BlockSpec(memory_space=pltpu.HBM)


def roll(value, by, axis):
    axis = axis % value.ndim
    by = by % value.shape[axis]
    return pltpu.roll(value, by, axis) if by else value


def iota(shape, dim):
    return lax.broadcasted_iota(jnp.int32, shape, dim % len(shape))


def exact_dot(values, pick):
    pick = pick.astype(jnp.bfloat16)
    total = None
    for _ in range(3):
        part = values.astype(jnp.bfloat16)
        values = values - part.astype(jnp.float32)
        made = jnp.dot(part, pick, preferred_element_type=jnp.float32)
        total = made if total is None else total + made
    return total


class Wrapped:
    group = 33

    @staticmethod
    def turn(v):
        return v

    @staticmethod
    def low_y(v):
        return roll(v, 1, -2)

    @staticmethod
    def up_y(v):
        return roll(v, -1, -2)

    @staticmethod
    def low_z(v):
        return roll(v, 1, -1)

    @staticmethod
    def up_z(v):
        return roll(v, -1, -1)


class Middle(Wrapped):
    group = 24


class Halves(Wrapped):
    group = 30

    @staticmethod
    def turn(v):
        return roll(v, LANES // 2, -1)


class Columns:
    group = 12

    def __init__(self, cells):
        self.cells = cells

    def turn(self, v):
        return v

    def low_y(self, v):
        lane = iota(v.shape, -1)
        last = lax.slice_in_dim(v, self.cells - 1, self.cells, axis=v.ndim - 3)
        rest = lax.slice_in_dim(v, 0, self.cells - 1, axis=v.ndim - 3)
        lane = iota(last.shape, -1)
        last = jnp.where((lane >= COUNT_Z) & (lane < COLUMNS), roll(last, COUNT_Z, -1), 0.0)
        return jnp.concatenate([last, rest], axis=v.ndim - 3)

    def up_y(self, v):
        first = lax.slice_in_dim(v, 0, 1, axis=v.ndim - 3)
        rest = lax.slice_in_dim(v, 1, self.cells, axis=v.ndim - 3)
        lane = iota(first.shape, -1)
        first = jnp.where(lane < COLUMNS - COUNT_Z, roll(first, -COUNT_Z, -1), 0.0)
        return jnp.concatenate([rest, first], axis=v.ndim - 3)

    def low_z(self, v):
        lane, row = iota(v.shape, -1), iota(v.shape, -2)
        edge = roll(roll(v, 1 - self.cells, -2), 1, -1)
        edge = jnp.where((lane % COUNT_Z != 0) & (lane < COLUMNS), edge, 0.0)
        return jnp.where(row == 0, edge, roll(v, 1, -2))

    def up_z(self, v):
        lane, row = iota(v.shape, -1), iota(v.shape, -2)
        edge = roll(roll(v, self.cells - 1, -2), -1, -1)
        edge = jnp.where((lane % COUNT_Z != COUNT_Z - 1) & (lane < COLUMNS), edge, 0.0)
        inner = jnp.where(row < self.cells - 1, roll(v, -1, -2), 0.0)
        return jnp.where(row == self.cells - 1, edge, inner)


def set_up(stack, iterate, update, weight, planes, count, move):
    stack[1, planes] = move.turn(stack[1, 0])
    size = move.group

    def body(g, carry):
        for u in range(size):
            at = size * g + u
            cell, face_y, face_z = stack[4, at], stack[2, at], stack[3, at]
            above_y, above_z = move.up_y(face_y), move.up_z(face_z)
            if stack.shape[0] > 7:
                stack[7, at] = above_y
            stack[6, at] = above_z
            total = stack[1, at] + stack[1, at + 1] + face_y + above_y + face_z + above_z
            inverse = jnp.where(cell > 0.0, 1.0 / (cell + weight * total), 0.0)
            stack[5, at] = inverse
            step = FIRST[1] * (inverse * stack[0, at])
            iterate[at] = step
            update[at] = step
        return carry

    if count == size:
        body(0, 0)
    else:
        lax.fori_loop(0, count // size, body, 0)


def stencil_pass(stack, iterate, weight, planes, count, move, use, carry):
    flux = stack[1, 0] * (iterate[0] - move.turn(iterate[planes - 1]))
    by_face = stack.shape[0] > 7
    size = move.group

    def body(g, state):
        flux, carry = state
        i = size * g
        values = [iterate[i + u] for u in range(size + 1)]
        for u in range(size):
            at, v = i + u, values[u]
            above = stack[1, at + 1] * (values[u + 1] - v)
            total = flux - above
            flux = above
            if by_face:
                total = total + stack[2, at] * (v - move.low_y(v))
                total = total + stack[7, at] * (v - move.up_y(v))
            else:
                flux_y = stack[2, at] * (v - move.low_y(v))
                total = total + (flux_y - move.up_y(flux_y))
            total = total + stack[3, at] * (v - move.low_z(v))
            total = total + stack[6, at] * (v - move.up_z(v))
            carry = use(at, v, stack[0, at] - (stack[4, at] * v + weight * total), carry)
        return flux, carry

    if count == size:
        return body(0, (flux, carry))[1]
    return lax.fori_loop(0, count // size, body, (flux, carry))[1]


def sweep(stack, iterate, update, weight, planes, count, move, factors):
    keep, gain = factors
    iterate[planes] = move.turn(iterate[0])

    def use(i, v, remainder, carry):
        step = gain * (stack[5, i] * remainder)
        if keep:
            step = keep * update[i] + step
        update[i] = step
        iterate[i] = v + step
        return carry

    stencil_pass(stack, iterate, weight, planes, count, move, use, 0)


def down(stack, iterate, update, weight, planes, count, move):
    set_up(stack, iterate, update, weight, planes, count, move)
    for factors in LATER:
        sweep(stack, iterate, update, weight, planes, count, move, factors)


def up(stack, iterate, update, weight, planes, count, move):
    for factors in (FIRST,) + LATER:
        sweep(stack, iterate, update, weight, planes, count, move, factors)


def keep_remainder(stack, iterate, update, weight, planes, count, move):
    iterate[planes] = move.turn(iterate[0])

    def use(i, v, remainder, carry):
        update[i] = remainder
        return carry

    stencil_pass(stack, iterate, weight, planes, count, move, use, 0)


def coarsen(stack, remainder, rows, pairs, out, count, size, period=LANES, offset=0):
    half = size // 2

    def body(i, carry):
        for k in range(5):
            if k == 1:
                rows[k] = stack[1, 2 * i]
            elif k == 0:
                rows[k] = remainder[2 * i] + remainder[2 * i + 1]
            else:
                rows[k] = stack[k, 2 * i] + stack[k, 2 * i + 1]
        for k in range(5):
            pair = rows[k, pl.ds(0, half, stride=2), :]
            if k != 2:
                pair = pair + rows[k, pl.ds(1, half, stride=2), :]
            pairs[k, i, 0:half, :] = pair
        return carry

    if half % 8:
        pairs[...] = jnp.zeros(pairs.shape, jnp.float32)
    lax.fori_loop(0, count // 2, body, 0)
    fine, coarse = iota((LANES, LANES), 0), iota((LANES, LANES), 1)
    inside = fine % period - offset
    own = (inside >= 0) & (inside < size) & (fine // period == coarse // period)
    mean = jnp.where(own & (inside // 2 == coarse % period), 1.0, 0.0)
    even = jnp.where(own & (inside == 2 * (coarse % period)), 1.0, 0.0)
    _, planes, padded, _ = pairs.shape
    for k in range(5):
        flat = pairs[k].reshape(planes * padded, LANES)
        scale = 0.125 if k in (0, 4) else 0.25
        made = scale * exact_dot(flat, even if k == 3 else mean)
        out(k, made.reshape(planes, padded, LANES))


def spread(coarse, spare, rows, base, fine, row_map, plane_maps, empty):
    planes, height, _ = spare.shape
    source, target = iota((LANES, LANES), 0), iota((LANES, LANES), 1)
    half = target // 2
    pick = jnp.where(source == jnp.where(target < LANES // 2, half, LANES // 2 + half), 1.0, 0.0)
    wide = exact_dot(coarse[0:planes].reshape(planes * height, LANES), pick)
    spare[...] = wide.reshape(planes, height, LANES)
    rows[...] = jnp.zeros(rows.shape, jnp.float32)
    fine[empty] = rows[...]
    for count, plane_of, target_of in plane_maps:

        def body(i, carry):
            plane = plane_of(i)
            for start, number, first in row_map:
                part = spare[plane, start : start + number, :]
                rows[pl.ds(first, number, stride=2), :] = part
                rows[pl.ds(first + 1, number, stride=2), :] = part
            both = rows[...]
            at = target_of(i)
            fine[at] = base[at] + both
            fine[at + 1] = base[at + 1] + both
            return carry

        lax.fori_loop(0, count, body, 0)


def spread_halves(coarse, spare, rows, base, fine, gx):
    planes, height, _ = spare.shape
    source, target = iota((LANES, LANES), 0), iota((LANES, LANES), 1)
    wanted = (target % (LANES // 2)) // 2 + (LANES - 4)
    pick = jnp.where(source == wanted % LANES, 1.0, 0.0)
    wide = exact_dot(coarse[0:planes].reshape(planes * height, LANES), pick)
    spare[...] = wide.reshape(planes, height, LANES)
    lane = iota((height, LANES), 1)

    def body(q, carry):
        j = q - 9 - 2 * gx
        there = (q < 9) | ((j >= 0) & (j < 4))
        above = jnp.where(q < 9, q + 15, 24 + 5 * gx + jnp.clip(j, 0, 3))
        both = jnp.where(lane < LANES // 2, spare[q], jnp.where(there, spare[above], 0.0))
        for start, number, first in ((0, 28, 0), (36, 4, 56)):
            part = both[start : start + number]
            rows[pl.ds(first, number, stride=2), :] = part
            rows[pl.ds(first + 1, number, stride=2), :] = part
        wide_rows = rows[...]
        fine[2 * q] = base[2 * q] + wide_rows
        fine[2 * q + 1] = base[2 * q + 1] + wide_rows
        return carry

    lax.fori_loop(0, HALF // 2, body, 0)


def places():
    gx = lax.axis_index("gx")
    gy = lax.axis_index("gy")
    gz = lax.axis_index("gz_0") * 4 + lax.axis_index("gz_1")
    return gx, gy, gz


def widen(value):
    rows, lanes = value.shape
    if lanes == LANES:
        return value
    return jnp.concatenate([value, jnp.zeros((rows, LANES - lanes), jnp.float32)], axis=1)


def y_pack(parts, size):
    lane = iota((8, LANES), 1)
    tiles = [jnp.zeros((8, LANES), jnp.float32) for _ in range(-(-5 * size // LANES))]
    for k, part in enumerate(parts):
        start = k * size
        moved = roll(part, start % LANES, -1)
        for t in range(len(tiles)):
            a, b = max(start, t * LANES) - t * LANES, min(start + size, (t + 1) * LANES) - t * LANES
            if a < b:
                tiles[t] = jnp.where((lane >= a) & (lane < b), moved, tiles[t])
    return tiles


def y_value(tiles, k, size):
    start = k * size
    t = start // LANES
    value = tiles[t]
    if start + size > (t + 1) * LANES:
        value = jnp.where(iota(value.shape, 1) >= start - t * LANES, value, tiles[t + 1])
    return value


def y_start(k, size):
    return k * size % LANES


def y_unpack(tiles, k, size, to):
    return roll(y_value(tiles, k, size), to - y_start(k, size), -1)


def y_rows(at, size, y_even, y_odd):
    even_y = places()[1] % 2 == 0
    e, o = y_even[at], y_odd[at]
    ends = jnp.where(even_y, e, o), jnp.where(even_y, o, e)
    tiles = [
        jnp.concatenate([end[8 * t : 8 * t + 8] for end in ends], axis=0)
        for t in range(-(-5 * size // LANES))
    ]
    return [y_value(tiles, k, size) for k in range(5)]


def place_halves(stack, own, beside, size, y_even, y_odd):
    gx, _, _ = places()
    lane = iota((16, LANES), 1)
    in_low = (lane >= 8) & (lane < size + 8)
    in_high = (lane >= LANES // 2 + 8) & (lane < LANES // 2 + size + 8)

    def put(p, low, high, other, there):
        near_low = y_rows(p, size, y_even, y_odd)
        near_high = y_rows(other, size, y_even, y_odd)
        for k in range(5):
            stack[k, p, 0:size, :] = roll(low(k), 8, -1) + roll(high(k), LANES // 2 + 8, -1)
            start = y_start(k, size)
            second = jnp.where(in_high & there, roll(near_high[k], LANES // 2 + 8 - start, -1), 0.0)
            stack[k, p, size:, :] = jnp.where(in_low, roll(near_low[k], 8 - start, -1), second)

    def both(g, carry):
        for u in range(3):
            p = 3 * g + u
            put(p, lambda k: own(k, p), lambda k: own(k, p + HALF), p + HALF, True)
        return carry

    lax.fori_loop(0, (size - HALF) // 3, both, 0)

    def mixed(g, carry):
        for u in range(3):
            p = size - HALF + 3 * g + u
            j = 3 * g + u - 4 * gx
            there = (j >= 0) & (j < 8)
            at = jnp.clip(j, 0, 7)
            second = lambda k: jnp.where(there, beside(k, at), 0.0)
            put(p, lambda k: own(k, p), second, size + at, there)
        return carry

    lax.fori_loop(0, (2 * HALF - size) // 3, mixed, 0)


def each_group(size, group):
    gx = lax.axis_index("gx")

    def low(h, carry):
        for g in (2 * h, 2 * h + 1):
            group(g, 3, 3 * g, 0)
        return carry

    def high(h, carry):
        for g in (2 * h, 2 * h + 1):
            group(g + HALF // 3, 3, 3 * g, LANES // 2)
        return carry

    lax.fori_loop(0, HALF // 6, low, 0)
    lax.fori_loop(0, (size - HALF) // 6, high, 0)
    for q in range(3):
        first = size - HALF + 4 * gx + 3 * q
        group(size // 3 + q, min(3, 8 - 3 * q), first, LANES // 2)


def merge_halves(stack, size, z_even, z_odd, c_even, c_odd):
    even_z = places()[2] % 2 == 0
    lane = iota((size + 16, LANES), 1)

    def group(g, slots, first, base):
        even = jnp.concatenate([z_even[g], c_even[g]], axis=0)
        odd = jnp.concatenate([z_odd[g], c_odd[g]], axis=0)
        low, high = jnp.where(even_z, odd, even), jnp.where(even_z, even, odd)
        at_low = (lane >= base) & (lane < base + 8)
        at_high = (lane >= base + 56) & (lane < base + 64)
        for s in range(slots):
            for k in range(5):
                at = 40 * s + 8 * k
                v = stack[k, first + s]
                v = jnp.where(at_low, roll(low, base - at, -1), v)
                stack[k, first + s] = jnp.where(at_high, roll(high, base + 56 - at, -1), v)

    each_group(size, group)


def y_faces(values, size, at, y_even, y_odd):
    even_y = places()[1] % 2 == 0
    high = y_pack([v[size - 8 :] for v in values], size)
    low = y_pack([v[:8] for v in values], size)
    for t, (h, l) in enumerate(zip(high, low)):
        y_even[at, 8 * t : 8 * t + 8, :] = jnp.where(even_y, h, l)
        y_odd[at, 8 * t : 8 * t + 8, :] = jnp.where(even_y, l, h)


def z_faces(planes, size, starts=(0,) * 5):
    even_z = places()[2] % 2 == 0
    rows = planes[0][0].shape[0]
    lane = iota((rows, LANES), 1)
    top = jnp.zeros((rows, LANES), jnp.float32)
    bottom = top
    for s, values in enumerate(planes):
        for k, v in enumerate(values):
            at = 40 * s + 8 * k
            here = (lane >= at) & (lane < at + 8)
            top = jnp.where(here, roll(v, at - starts[k] - (size - 8), -1), top)
            bottom = jnp.where(here, roll(v, at - starts[k], -1), bottom)
    return jnp.where(even_z, top, bottom), jnp.where(even_z, bottom, top)


def y_sides(source, size, slots, keep, y_even, y_odd):
    even_y = places()[1] % 2 == 0
    lane = iota((16, LANES), 1)
    tiles = -(-5 * size // LANES)
    planes = []
    for s in range(slots):
        e, o = y_even[3 * source + s], y_odd[3 * source + s]
        ends = jnp.where(even_y, e, o), jnp.where(even_y, o, e)
        ends = [[end[8 * t : 8 * t + 8] for t in range(tiles)] for end in ends]
        values = []
        for k in range(5):
            v = jnp.concatenate([y_unpack(end, k, size, 0) for end in ends], axis=0)
            v = jnp.where(lane < size, v, 0.0)
            keep(k, s, v)
            values.append(v)
        planes.append(values)
    return planes


def merge_z(stack, size, z_even, z_odd):
    gx, _, gz = places()
    even_z = gz % 2 == 0
    lane = iota((size + 16, LANES), 1)

    def group(g, slots, first):
        low = jnp.where(even_z, z_odd[g], z_even[g])
        high = jnp.where(even_z, z_even[g], z_odd[g])
        for s in range(slots):
            for k in range(5):
                at = 40 * s + 8 * k
                v = stack[k, first + s]
                v = jnp.where(lane >= LANES - 8, roll(low, LANES - 8 - at, -1), v)
                here = (lane >= size) & (lane < size + 8)
                stack[k, first + s] = jnp.where(here, roll(high, size - at, -1), v)

    def body(h, carry):
        for g in (2 * h, 2 * h + 1):
            group(g, 3, 3 * g)
        return carry

    lax.fori_loop(0, size // 6, body, 0)
    for q in range(3):
        group(size // 3 + q, min(3, 8 - 3 * q), size + gx + 3 * q)


def partner(index, parity, count):
    if parity is None:
        return index
    other = index + 1 if index % 2 == parity else index - 1
    return other if 0 <= other < count else None


def swap(value, parity_y, parity_z):
    pairs = []
    for y in range(COUNT_Y):
        for z in range(COUNT_Z):
            to_y, to_z = partner(y, parity_y, COUNT_Y), partner(z, parity_z, COUNT_Z)
            if to_y is not None and to_z is not None:
                pairs.append((y * COUNT_Z + z, to_y * COUNT_Z + to_z))
    return lax.ppermute(value, YZ, pairs)


def swap_cores(value):
    return lax.ppermute(value, "gx", [(0, 1), (1, 0)])


def f32(*shape):
    return jax.ShapeDtypeStruct(shape, jnp.float32)


def near(*shape):
    return pltpu.VMEM(shape, jnp.float32)


def call(body, outs, ins, scratch, operands, limit, aliases={}):
    held = [
        pltpu.with_memory_space_constraint(v, pltpu.HBM if spec is far else pltpu.VMEM)
        for v, spec in zip(operands, ins)
    ]
    return pl.pallas_call(
        body,
        out_shape=outs,
        out_specs=[vmem] * len(outs),
        in_specs=ins,
        scratch_shapes=scratch,
        input_output_aliases=aliases,
        compiler_params=pltpu.CompilerParams(vmem_limit_bytes=limit * 2**20),
    )(*held)


def edge_kernel(right, faces, cells, out, sems):
    gx = lax.axis_index("gx")
    start = (1 - gx) * (SIZES[0] - WIDTH)
    part = pl.ds(start, WIDTH)
    copies = [
        pltpu.make_async_copy(right.at[part], out.at[0], sems.at[0]),
        pltpu.make_async_copy(faces.at[0, part], out.at[1], sems.at[1]),
        pltpu.make_async_copy(faces.at[1, part], out.at[2], sems.at[2]),
        pltpu.make_async_copy(faces.at[2, part], out.at[3], sems.at[3]),
        pltpu.make_async_copy(cells.at[part], out.at[4], sems.at[4]),
    ]
    for copy in copies:
        copy.start()
    for copy in copies:
        copy.wait()


def own_inputs(right, faces, cells):
    def own(k, i):
        if k == 0:
            return widen(right[i])
        return widen(cells[i] if k == 4 else faces[k - 1, i])

    return own


def pack_y_0_kernel(right, faces, cells, beside, y_even, y_odd):
    size = SIZES[0]
    own = own_inputs(right, faces, cells)

    def body(g, carry):
        for u in range(4):
            y_faces([own(k, 4 * g + u) for k in range(5)], size, 4 * g + u, y_even, y_odd)
        return carry

    lax.fori_loop(0, size // 4, body, 0)
    for j in range(8):
        y_faces([widen(beside[k, j]) for k in range(5)], size, size + j, y_even, y_odd)


def pack_z_0_kernel(right, faces, cells, beside, z_even, z_odd):
    size = SIZES[0]
    own = own_inputs(right, faces, cells)

    def body(h, carry):
        for u in range(2):
            g = 2 * h + u
            planes = [[own(k, 3 * g + s) for k in range(5)] for s in range(3)]
            z_even[g], z_odd[g] = z_faces(planes, size)
        return carry

    lax.fori_loop(0, size // 6, body, 0)
    for q in range(3):
        slots = range(min(3, 8 - 3 * q))
        planes = [[widen(beside[k, 3 * q + s]) for k in range(5)] for s in slots]
        g = size // 3 + q
        z_even[g], z_odd[g] = z_faces(planes, size)


def corner_0_kernel(y_even, y_odd, c_even, c_odd):
    size = SIZES[0]
    starts = [y_start(k, size) for k in range(5)]

    def group(g, slots):
        planes = [y_rows(3 * g + s, size, y_even, y_odd) for s in range(slots)]
        c_even[g], c_odd[g] = z_faces(planes, size, starts)

    def body(h, carry):
        for u in range(3):
            group(3 * h + u, 3)
        return carry

    lax.fori_loop(0, 6, body, 0)
    group(18, 2)


def place_0_kernel(right, faces, cells, beside, y_even, y_odd, stack):
    own = own_inputs(right, faces, cells)
    place_halves(stack, own, lambda k, j: widen(beside[k, j]), SIZES[0], y_even, y_odd)


def own_1_kernel(own, y_even, y_odd, z_even, z_odd):
    size = SIZES[1]

    def body(g, carry):
        planes = [[own[k, 3 * g + s] for k in range(5)] for s in range(3)]
        for s in range(3):
            y_faces(planes[s], size, 3 * g + s, y_even, y_odd)
        z_even[g], z_odd[g] = z_faces(planes, size)
        return carry

    lax.fori_loop(0, size // 3, body, 0)


def beside_1_kernel(beside, own_even, own_odd, y_even, y_odd):
    size = SIZES[1]
    y_even[0:size] = own_even[...]
    y_odd[0:size] = own_odd[...]
    for j in range(8):
        y_faces([beside[k, j] for k in range(5)], size, size + j, y_even, y_odd)


def fill_1_kernel(own, beside, own_even, own_odd, stack, z_even, z_odd):
    size = SIZES[1]
    gx = lax.axis_index("gx")
    z_even[0 : size // 3] = own_even[...]
    z_odd[0 : size // 3] = own_odd[...]

    def body(i, carry):
        for k in range(5):
            stack[k, i, 0:size, :] = own[k, i]
        return carry

    lax.fori_loop(0, size, body, 0)
    for q in range(3):
        slots, first = min(3, 8 - 3 * q), size + gx + 3 * q
        planes = [[beside[k, 3 * q + s] for k in range(5)] for s in range(slots)]
        for s in range(slots):
            for k in range(5):
                stack[k, first + s, 0:size, :] = planes[s][k]
        g = size // 3 + q
        z_even[g], z_odd[g] = z_faces(planes, size)
    empty = size + 8 * (1 - gx)
    for k in range(5):
        stack[k, empty] = jnp.zeros(stack.shape[2:], jnp.float32)


def side_1_kernel(filled, y_even, y_odd, own_even, own_odd, stack, z_even, z_odd):
    size = SIZES[1]
    gx = lax.axis_index("gx")
    z_even[:, 0:size, :] = own_even[...]
    z_odd[:, 0:size, :] = own_odd[...]
    sides = pl.ds(size, 16)

    def keep_at(first):
        def keep(k, s, v):
            stack[k, first + s, size : size + 16, :] = v

        return keep

    def body(h, carry):
        for g in (2 * h, 2 * h + 1):
            planes = y_sides(g, size, 3, keep_at(3 * g), y_even, y_odd)
            z_even[g, sides, :], z_odd[g, sides, :] = z_faces(planes, size)
        return carry

    lax.fori_loop(0, size // 6, body, 0)
    for q in range(3):
        slots, first = min(3, 8 - 3 * q), size + gx + 3 * q
        g = size // 3 + q
        planes = y_sides(g, size, slots, keep_at(first), y_even, y_odd)
        z_even[g, sides, :], z_odd[g, sides, :] = z_faces(planes, size)


def level_0_kernel(
    filled, z_even, z_odd, c_even, c_odd,
    coarse, coarse_edge, stack, iterate,
    update, rows, pairs,
):
    size = SIZES[0]
    gx = lax.axis_index("gx")
    merge_halves(stack, size, z_even, z_odd, c_even, c_odd)
    down(stack, iterate, update, 1.0, HALF, HALF, Halves)
    keep_remainder(stack, iterate, update, 1.0, HALF, HALF, Halves)

    def out(k, value):
        lane = iota(value.shape, -1)
        coarse[k, 0:15] = jnp.where(lane < 24, value, 0.0)
        second = roll(value[0:9], LANES // 2, -1)
        coarse[k, 15:24] = jnp.where(lane[0:9] < 24, second, 0.0)
        coarse_edge[k] = jnp.where(gx == 0, coarse[k, 16:24], coarse[k, 0:8])

    coarsen(stack, update, rows, pairs, out, HALF, size, LANES // 2, 8)


def level_1_kernel(
    filled, z_even, z_odd, held,
    coarse, stack, iterate,
    update, rows, pairs, made,
):
    size = SIZES[1]
    planes = size + 9
    merge_z(stack, size, z_even, z_odd)
    down(stack, iterate, update, 0.25, planes, planes, Wrapped)
    keep_remainder(stack, iterate, update, 0.25, planes, planes, Wrapped)

    def out(k, value):
        made[k] = value

    coarsen(stack, update, rows, pairs, out, size, size)
    for i in range(SIZES[2] // 2):
        line = made[0, 2 * i] + roll(made[0, 2 * i + 1], LANES // 2, -1)
        for h in range(2):
            for k in range(1, 5):
                line = line + roll(made[k, 2 * i + h], LANES // 2 * h + SIZES[2] * k, -1)
        coarse[i] = line


def level_2_kernel(
    mine, other, held,
    payload, stack, iterate,
    update, rows, pairs, made, lines,
):
    size = SIZES[2]
    planes = 2 * size + 1
    gx, gy, gz = places()
    even_y, even_z = gy % 2 == 0, gz % 2 == 0
    lane = iota((16, LANES), 1)
    bases = (0, size, LANES - size)
    half = size // 2
    for k in range(5):
        stack[k, 2 * size] = jnp.zeros(stack.shape[2:], jnp.float32)

    def body(i, carry):
        for core in range(2):

            def block(a, b):
                at = half * (3 * b + a) + i
                return jnp.where(gx == core, mine[at], other[at])

            columns = []
            for b in range(3):
                even, odd = block(1, b), block(2, b)
                columns.append(
                    (block(0, b), jnp.where(even_y, even, odd), jnp.where(even_y, odd, even))
                )
            columns = [columns[0]] + [
                [jnp.where(even_z, p, q) for p, q in zip(columns[c], columns[3 - c])] for c in (1, 2)
            ]
            for h in range(2):
                plane = size * core + 2 * i + h
                for k in range(5):
                    source = (LANES // 2) * h + size * k
                    stack[k, plane, 24:32, :] = jnp.zeros((8, LANES), jnp.float32)
                    for a, first in enumerate((0, size, 40 - size)):
                        line = jnp.zeros((16, LANES), jnp.float32)
                        for b, base in enumerate(bases):
                            here = (lane >= base) & (lane < base + size)
                            line = jnp.where(here, roll(columns[b][a], base - source, -1), line)
                        stack[k, plane, first : first + size, :] = line[:size]
        return carry

    lax.fori_loop(0, half, body, 0)
    weight = 0.0625
    iterate[2 * size] = jnp.zeros(iterate.shape[1:], jnp.float32)
    down(stack, iterate, update, weight, planes, 2 * size, Middle)
    keep_remainder(stack, iterate, update, weight, planes, 2 * size, Middle)

    def out(k, value):
        made[k * 96 : k * 96 + 96, :] = value.reshape(96, LANES)

    coarsen(stack, update, rows, pairs, out, 2 * size, size)
    line = jnp.zeros((60, LANES), jnp.float32)
    for y in range(6):
        line = line + roll(made[pl.ds(y, 60, stride=8), :], 6 * y, -1)
    lines[0:60, :] = line
    chunk = lines[0:20, :] + roll(lines[20:40, :], 40, -1) + roll(lines[40:60, :], 80, -1)
    chunk = jnp.concatenate([chunk, jnp.zeros((4, LANES), jnp.float32)], axis=0)

    def repeat(c, carry):
        payload[pl.ds(pl.multiple_of(c * CHUNK, 8), CHUNK), :] = chunk
        return carry

    lax.fori_loop(0, COLUMNS, repeat, 0)


def compact(value):
    row = iota(value.shape, -2)
    out = jnp.where(row == 0, value, 0.0)
    out = jnp.where(row == 1, roll(value, -1, -2), out)
    return jnp.where(row == 2, roll(value, -2, -2), out)


def bottom(source, faces, cells):
    weight = 0.25**4
    move = Columns(3)
    face_x, face_y, face_z = faces
    nothing = jnp.zeros((1,) + source.shape[1:], jnp.float32)

    def apply(v):
        flux_x = face_x * (v - jnp.concatenate([nothing, v[:-1]], axis=0))
        flux_y = face_y * (v - move.low_y(v))
        flux_z = face_z * (v - move.low_z(v))
        total = flux_x - jnp.concatenate([flux_x[1:], nothing], axis=0)
        total = total + (flux_y - move.up_y(flux_y)) + (flux_z - move.up_z(flux_z))
        return cells * v + weight * total

    def total_of(v):
        flat = jnp.sum(jnp.sum(v, axis=0), axis=0)
        one = jnp.sum(jnp.sum(flat, axis=0, keepdims=True), axis=1, keepdims=True)
        return jnp.broadcast_to(one, flat.shape)

    iterate = jnp.zeros_like(source)
    remainder = source
    search = source
    norm_now = total_of(remainder * remainder)
    for step in range(BOTTOM):
        applied = apply(search)
        size = norm_now / total_of(search * applied)
        iterate = iterate + size * search
        if step + 1 < BOTTOM:
            remainder = remainder - size * applied
            norm_next = total_of(remainder * remainder)
            search = remainder + (norm_next / norm_now) * search
            norm_now = norm_next
    return iterate


def rise_kernel(
    gathered, stack_2, base_2, stack_1, base_1, stack_0, base_0,
    solution_out, residual_out, sums,
    iterate_0, update_0, rows_0, spare_1,
    iterate_1, update_1, rows_1, spare_2,
    iterate_2, update_2, rows_2, spare_3,
    stack_3, iterate_3, update_3, turned, table, block_3,
):
    gx, gy, gz = places()

    stack_3[...] = jnp.zeros(stack_3.shape, jnp.float32)
    blank = jnp.zeros((LANES - COLUMNS, LANES), jnp.float32)
    for r in range(20):
        part = gathered[pl.ds(r, COLUMNS, stride=CHUNK), :]
        turned[...] = jnp.transpose(jnp.concatenate([part, blank], axis=0))
        for j in range(3):
            k, x = divmod(20 * j + r, 12)
            for y in range(6):
                stack_3[k, x, y, 0:6, :] = turned[40 * j + 6 * y : 40 * j + 6 * y + 6, :]
    move = Columns(6)
    weight = 0.25**3
    iterate_3[12] = jnp.zeros(iterate_3.shape[1:], jnp.float32)
    down(stack_3, iterate_3, update_3, weight, 13, 12, move)
    keep_remainder(stack_3, iterate_3, update_3, weight, 13, 12, move)

    def coarse(k, x_pair, y_pair, z_pair, scale):
        planes = []
        for x in range(6):
            read = (lambda i: update_3[i]) if k == 0 else (lambda i: stack_3[k, i])
            v = read(2 * x)
            if x_pair:
                v = v + read(2 * x + 1)
            lines = []
            for y in range(3):
                line = v[2 * y]
                if y_pair:
                    line = line + v[2 * y + 1]
                if z_pair:
                    line = line + roll(line, -1, -2)
                lines.append(scale * compact(line))
            planes.append(jnp.stack(lines))
        return jnp.stack(planes)

    lowest = bottom(
        coarse(0, True, True, True, 0.125),
        (
            coarse(1, False, True, True, 0.25),
            coarse(2, True, False, True, 0.25),
            coarse(3, True, True, False, 0.25),
        ),
        coarse(4, True, True, True, 0.125),
    )
    row = iota((8, LANES), 0)
    for x in range(6):
        for y in range(3):
            line = lowest[x, y]
            wide = jnp.where(row == 0, line, 0.0)
            for to in range(1, 6):
                wide = jnp.where(row == to, roll(line, to - to // 2, -2), wide)
            for a in range(2):
                for b in range(2):
                    iterate_3[2 * x + a, 2 * y + b] = iterate_3[2 * x + a, 2 * y + b] + wide
    up(stack_3, iterate_3, update_3, weight, 13, 12, move)

    low_rows = jnp.zeros((32, LANES), jnp.float32)
    for q in range(6):
        two = [iterate_3[2 * q + h].reshape(48, LANES) for h in range(2)]
        table[q] = jnp.transpose(jnp.concatenate(two + [low_rows], axis=0))
    block_3[...] = jnp.zeros(block_3.shape, jnp.float32)
    lane = iota((8, LANES), 1)

    def place(q, carry):
        for a, first in ((0, 0), (1, 6), (-1, 18)):
            lines = [jnp.zeros((8, LANES), jnp.float32) for _ in range(2)]
            for b, base in ((0, 0), (1, 6), (-1, LANES - 6)):
                y, z = gy + a, gz + b
                inside = (y >= 0) & (y < COUNT_Y) & (z >= 0) & (z < COUNT_Z)
                at = jnp.where(inside, y * COUNT_Z + z, 0)
                here = (lane >= base) & (lane < base + 6) & inside
                found = jnp.broadcast_to(table[q, pl.ds(at, 1), :], (8, LANES))
                for h in range(2):
                    for y_in in range(6):
                        moved = roll(found, base - 48 * h - 8 * y_in, -1)
                        lines[h] = jnp.where(here & (row == y_in), moved, lines[h])
            for h in range(2):
                block_3[2 * q + h, first : first + 6, :] = lines[h][0:6]
        return carry

    lax.fori_loop(0, 6, place, 0)

    spread(
        block_3, spare_3, rows_2, base_2, iterate_2,
        ((0, 12, 0), (18, 6, 28)),
        ((12, lambda i: i, lambda i: 2 * i),),
        24,
    )
    up(stack_2, iterate_2, update_2, 0.0625, 25, 24, Middle)

    size = SIZES[1]
    spread(
        iterate_2, spare_2, rows_1, base_1, iterate_1,
        ((0, 16, 0), (36, 4, 32)),
        (
            (12, lambda i: 12 * gx + i, lambda i: 2 * i),
            (4, lambda i: 12 - 4 * gx + i, lambda i: size + gx + 2 * i),
        ),
        size + 8 * (1 - gx),
    )
    up(stack_1, iterate_1, update_1, 0.25, size + 9, size + 9, Wrapped)

    size = SIZES[0]
    spread_halves(iterate_1, spare_1, rows_0, base_0, iterate_0, gx)
    up(stack_0, iterate_0, update_0, 1.0, HALF, HALF, Halves)
    iterate_0[HALF] = Halves.turn(iterate_0[0])
    inside = iota((size, LANES), 1)
    in_low = (inside >= 8) & (inside < 56)
    in_high = (inside >= 72) & (inside < 120)

    def use(i, v, remainder, carry):
        v, remainder = v[0:size], remainder[0:size]
        solution_out[i] = roll(v, -8, -1)[:, 0:size]
        residual_out[i] = roll(remainder, -8, -1)[:, 0:size]

        mask = in_low
        if i < size - HALF:
            solution_out[i + HALF] = roll(v, -72, -1)[:, 0:size]
            residual_out[i + HALF] = roll(remainder, -72, -1)[:, 0:size]
            mask = in_low | in_high
        mine = jnp.where(mask, remainder, 0.0)
        given = jnp.where(mask, stack_0[0, i, 0:size, :], 0.0)
        return carry[0] + mine * mine, carry[1] + given * given

    zero = jnp.zeros((size, LANES), jnp.float32)
    squares = stencil_pass(stack_0, iterate_0, 1.0, HALF, HALF, Halves, use, (zero, zero))
    ones = []
    for square in squares:
        one = jnp.sum(jnp.sum(square, axis=0, keepdims=True), axis=1, keepdims=True)
        ones.append(jnp.broadcast_to(one, (8, LANES)))
    sums[...] = jnp.where(lane == 0, ones[0], jnp.where(lane == 1, ones[1], 0.0))


def stack_kernel(*refs):
    out = refs[-1]
    for n, ref in enumerate(refs[:-1]):
        count = ref.shape[0]
        out[n * count : n * count + count] = ref[...]


def stacked(*parts):
    count, *rest = parts[0].shape
    return call(stack_kernel, [near(len(parts) * count, *rest)], [held_near] * 3, [], parts, 1)[0]


def shards(right, faces, cells):
    dma = pltpu.SemaphoreType.DMA
    edge = call(edge_kernel, [near(5, WIDTH, 48, 48)], [far] * 3, [dma((5,))],
        (right, faces, cells), 2)[0]
    beside = swap_cores(edge)
    given = (right, faces, cells, beside)
    outs = call(pack_y_0_kernel, [near(56, 16, LANES)] * 2, [held_near] * 4, [], given, 4)
    sides = [swap(v, parity, None) for parity, v in enumerate(outs)]
    outs = call(pack_z_0_kernel, [near(19, 48, LANES)] * 2, [held_near] * 4, [], given, 4)
    ends = [swap(v, None, parity) for parity, v in enumerate(outs)]
    outs = call(corner_0_kernel, [near(19, 16, LANES)] * 2, [held_near] * 2, [], sides, 4)
    corners = [swap(v, None, parity) for parity, v in enumerate(outs)]
    filled = call(place_0_kernel, [near(7, 31, 64, LANES)], [held_near] * 6, [],
        (*given, *sides), 4)[0]
    coarse, coarse_edge, stack_0, iterate_0 = call(
        level_0_kernel,
        [near(5, 24, 24, LANES), near(5, WIDTH, 24, LANES), near(7, 31, 64, LANES), near(31, 64, LANES)],
        [held_near] * 5,
        [near(31, 64, LANES), near(5, 64, LANES), near(5, 15, 24, LANES)],
        (filled, *ends, *corners),
        10,
        {0: 2},
    )
    beside = swap_cores(coarse_edge)
    y_shape, z_shape = near(32, 8, LANES), near(11, 24, LANES)
    *y_own, z_even, z_odd = call(own_1_kernel, [near(24, 8, LANES)] * 2 + [near(8, 24, LANES)] * 2,
        [held_near], [], (coarse,), 4)
    outs = call(beside_1_kernel, [y_shape] * 2, [held_near] * 3, [], (beside, *y_own), 4)
    sides = [swap(v, parity, None) for parity, v in enumerate(outs)]
    filled, *z_own = call(fill_1_kernel, [near(7, 34, 40, LANES), z_shape, z_shape],
        [held_near] * 4, [], (coarse, beside, z_even, z_odd), 4)
    filled, *outs = call(side_1_kernel, [near(7, 34, 40, LANES)] + [near(11, 40, LANES)] * 2,
        [held_near] * 5, [], (filled, *sides, *z_own), 4, {0: 0})
    z_sides = [swap(v, None, parity) for parity, v in enumerate(outs)]
    coarse, stack_1, iterate_1 = call(
        level_1_kernel,
        [near(6, 16, LANES), near(7, 34, 40, LANES), near(34, 40, LANES)],
        [held_near] * 4,
        [near(34, 40, LANES), near(5, 40, LANES), near(5, 12, 16, LANES), near(5, 12, 16, LANES)],
        (filled, *z_sides, stack_0),
        12,
        {0: 1},
    )
    column = stacked(coarse, *[swap(coarse, parity, None) for parity in (0, 1)])
    region = stacked(column, *[swap(column, None, parity) for parity in (0, 1)])
    other = swap_cores(region)
    payload, stack_2, iterate_2 = call(
        level_2_kernel,
        [near(COLUMNS * CHUNK, LANES), near(7, 26, 40, LANES), near(26, 40, LANES)],
        [held_near] * 3,
        [near(26, 40, LANES), near(5, 40, LANES), near(5, 12, 8, LANES), near(480, LANES), near(64, LANES)],
        (region, other, stack_0),
        12,
    )
    payload = payload.reshape(COLUMNS, CHUNK, LANES)
    gathered = lax.all_to_all(payload, YZ, 0, 0).reshape(COLUMNS * CHUNK, LANES)
    solved, residual, sums = call(
        rise_kernel,
        [f32(48, 48, 48), f32(48, 48, 48), f32(8, LANES)],
        [held_near] * 7,
        [
            near(31, 64, LANES), near(31, 64, LANES), near(64, LANES), near(33, 40, LANES),
            near(34, 40, LANES), near(34, 40, LANES), near(40, LANES), near(24, 40, LANES),
            near(26, 40, LANES), near(26, 40, LANES), near(40, LANES), near(12, 24, LANES),
            near(8, 14, 6, 8, LANES), near(14, 6, 8, LANES), near(14, 6, 8, LANES),
            near(LANES, LANES), near(6, LANES, LANES), near(12, 24, LANES),
        ],
        (gathered, stack_2, iterate_2, stack_1, iterate_1, stack_0, iterate_0),
        24,
    )
    each = jnp.broadcast_to(sums[0:1].reshape(1, 1, LANES), (128, 1, LANES))
    total = jnp.sum(lax.all_to_all(each, ALL, 0, 0), axis=(0, 1))
    return solved, residual, jnp.sqrt(total[0] / total[1])


def solution(mesh):
    torus = Mesh(
        mesh.devices.reshape(mesh.shape["gx"], mesh.shape["gy"], 4, 4), ("gx", "gy", "gz_0", "gz_1")
    )
    in_specs = (P("gx", "gy", GZ), P(None, "gx", "gy", GZ), P("gx", "gy", GZ))
    out_specs = (P("gx", "gy", GZ), P("gx", "gy", GZ), P())
    return jax.shard_map(
        shards, mesh=torus, in_specs=in_specs, out_specs=out_specs, check_vma=False
    )
```

```python
import functools

import jax
import jax.numpy as jnp
from jax import lax
from jax.experimental import pallas as pl
from jax.experimental.pallas import tpu as pltpu
from jax.sharding import Mesh
from jax.sharding import PartitionSpec as P

BOTTOM = 6
ALL = ("gx", "gy", "gz_0", "gz_1")
YZ = ("gy", "gz_0", "gz_1")
GZ = ("gz_0", "gz_1")
LANES = 128
WIDTH = 8
COUNT_Y = 4
COUNT_Z = 16
COLUMNS = COUNT_Y * COUNT_Z
SIZES = (48, 24, 12, 6)
CHUNK = 24
HALF = 30

theta = 1.125
delta = 0.875
sigma = theta / delta
rho_0 = 1.0 / sigma
rho_1 = 1.0 / (2.0 * sigma - rho_0)
rho_2 = 1.0 / (2.0 * sigma - rho_1)
FIRST = (0.0, 1.0 / theta)
LATER = ((rho_1 * rho_0, 2.0 * rho_1 / delta), (rho_2 * rho_1, 2.0 * rho_2 / delta))

vmem = pl.BlockSpec(memory_space=pltpu.VMEM)
held_near = pl.BlockSpec(memory_space=pltpu.VMEM)
far = pl.BlockSpec(memory_space=pltpu.HBM)


def roll(value, by, axis):
    axis = axis % value.ndim
    by = by % value.shape[axis]
    return pltpu.roll(value, by, axis) if by else value


def iota(shape, dim):
    return lax.broadcasted_iota(jnp.int32, shape, dim % len(shape))


def exact_dot(values, pick):
    pick = pick.astype(jnp.bfloat16)
    total = None
    for _ in range(3):
        part = values.astype(jnp.bfloat16)
        values = values - part.astype(jnp.float32)
        made = jnp.dot(part, pick, preferred_element_type=jnp.float32)
        total = made if total is None else total + made
    return total


class Wrapped:
    group = 33

    @staticmethod
    def turn(v):
        return v

    @staticmethod
    def low_y(v):
        return roll(v, 1, -2)

    @staticmethod
    def up_y(v):
        return roll(v, -1, -2)

    @staticmethod
    def low_z(v):
        return roll(v, 1, -1)

    @staticmethod
    def up_z(v):
        return roll(v, -1, -1)


class Middle(Wrapped):
    group = 24


class Halves(Wrapped):
    group = 30

    @staticmethod
    def turn(v):
        return roll(v, LANES // 2, -1)


class Columns:
    group = 12

    def __init__(self, cells):
        self.cells = cells

    def turn(self, v):
        return v

    def low_y(self, v):
        lane = iota(v.shape, -1)
        last = lax.slice_in_dim(v, self.cells - 1, self.cells, axis=v.ndim - 3)
        rest = lax.slice_in_dim(v, 0, self.cells - 1, axis=v.ndim - 3)
        lane = iota(last.shape, -1)
        last = jnp.where((lane >= COUNT_Z) & (lane < COLUMNS), roll(last, COUNT_Z, -1), 0.0)
        return jnp.concatenate([last, rest], axis=v.ndim - 3)

    def up_y(self, v):
        first = lax.slice_in_dim(v, 0, 1, axis=v.ndim - 3)
        rest = lax.slice_in_dim(v, 1, self.cells, axis=v.ndim - 3)
        lane = iota(first.shape, -1)
        first = jnp.where(lane < COLUMNS - COUNT_Z, roll(first, -COUNT_Z, -1), 0.0)
        return jnp.concatenate([rest, first], axis=v.ndim - 3)

    def low_z(self, v):
        lane, row = iota(v.shape, -1), iota(v.shape, -2)
        edge = roll(roll(v, 1 - self.cells, -2), 1, -1)
        edge = jnp.where((lane % COUNT_Z != 0) & (lane < COLUMNS), edge, 0.0)
        return jnp.where(row == 0, edge, roll(v, 1, -2))

    def up_z(self, v):
        lane, row = iota(v.shape, -1), iota(v.shape, -2)
        edge = roll(roll(v, self.cells - 1, -2), -1, -1)
        edge = jnp.where((lane % COUNT_Z != COUNT_Z - 1) & (lane < COLUMNS), edge, 0.0)
        inner = jnp.where(row < self.cells - 1, roll(v, -1, -2), 0.0)
        return jnp.where(row == self.cells - 1, edge, inner)


def set_up(stack, iterate, update, weight, planes, count, move):
    stack[1, planes] = move.turn(stack[1, 0])
    size = move.group

    def body(g, carry):
        for u in range(size):
            at = size * g + u
            cell, face_y, face_z = stack[4, at], stack[2, at], stack[3, at]
            above_y, above_z = move.up_y(face_y), move.up_z(face_z)
            if stack.shape[0] > 7:
                stack[7, at] = above_y
            stack[6, at] = above_z
            total = stack[1, at] + stack[1, at + 1] + face_y + above_y + face_z + above_z
            inverse = jnp.where(cell > 0.0, 1.0 / (cell + weight * total), 0.0)
            stack[5, at] = inverse
            step = FIRST[1] * (inverse * stack[0, at])
            iterate[at] = step
            update[at] = step
        return carry

    if count == size:
        body(0, 0)
    else:
        lax.fori_loop(0, count // size, body, 0)


def stencil_pass(stack, iterate, weight, planes, count, move, use, carry):
    flux = stack[1, 0] * (iterate[0] - move.turn(iterate[planes - 1]))
    by_face = stack.shape[0] > 7
    size = move.group

    def body(g, state):
        flux, carry = state
        i = size * g
        values = [iterate[i + u] for u in range(size + 1)]
        for u in range(size):
            at, v = i + u, values[u]
            above = stack[1, at + 1] * (values[u + 1] - v)
            total = flux - above
            flux = above
            if by_face:
                total = total + stack[2, at] * (v - move.low_y(v))
                total = total + stack[7, at] * (v - move.up_y(v))
            else:
                flux_y = stack[2, at] * (v - move.low_y(v))
                total = total + (flux_y - move.up_y(flux_y))
            total = total + stack[3, at] * (v - move.low_z(v))
            total = total + stack[6, at] * (v - move.up_z(v))
            carry = use(at, v, stack[0, at] - (stack[4, at] * v + weight * total), carry)
        return flux, carry

    if count == size:
        return body(0, (flux, carry))[1]
    return lax.fori_loop(0, count // size, body, (flux, carry))[1]


def sweep(stack, iterate, update, weight, planes, count, move, factors):
    keep, gain = factors
    iterate[planes] = move.turn(iterate[0])

    def use(i, v, remainder, carry):
        step = gain * (stack[5, i] * remainder)
        if keep:
            step = keep * update[i] + step
        update[i] = step
        iterate[i] = v + step
        return carry

    stencil_pass(stack, iterate, weight, planes, count, move, use, 0)


def down(stack, iterate, update, weight, planes, count, move):
    set_up(stack, iterate, update, weight, planes, count, move)
    for factors in LATER:
        sweep(stack, iterate, update, weight, planes, count, move, factors)


def up(stack, iterate, update, weight, planes, count, move):
    for factors in (FIRST,) + LATER:
        sweep(stack, iterate, update, weight, planes, count, move, factors)


def keep_remainder(stack, iterate, update, weight, planes, count, move):
    iterate[planes] = move.turn(iterate[0])

    def use(i, v, remainder, carry):
        update[i] = remainder
        return carry

    stencil_pass(stack, iterate, weight, planes, count, move, use, 0)


def coarsen(stack, remainder, rows, pairs, out, count, size, period=LANES, offset=0):
    half = size // 2

    def body(i, carry):
        for k in range(5):
            if k == 1:
                rows[k] = stack[1, 2 * i]
            elif k == 0:
                rows[k] = remainder[2 * i] + remainder[2 * i + 1]
            else:
                rows[k] = stack[k, 2 * i] + stack[k, 2 * i + 1]
        for k in range(5):
            pair = rows[k, pl.ds(0, half, stride=2), :]
            if k != 2:
                pair = pair + rows[k, pl.ds(1, half, stride=2), :]
            pairs[k, i, 0:half, :] = pair
        return carry

    if half % 8:
        pairs[...] = jnp.zeros(pairs.shape, jnp.float32)
    lax.fori_loop(0, count // 2, body, 0)
    fine, coarse = iota((LANES, LANES), 0), iota((LANES, LANES), 1)
    inside = fine % period - offset
    own = (inside >= 0) & (inside < size) & (fine // period == coarse // period)
    mean = jnp.where(own & (inside // 2 == coarse % period), 1.0, 0.0)
    even = jnp.where(own & (inside == 2 * (coarse % period)), 1.0, 0.0)
    _, planes, padded, _ = pairs.shape
    for k in range(5):
        flat = pairs[k].reshape(planes * padded, LANES)
        scale = 0.125 if k in (0, 4) else 0.25
        made = scale * exact_dot(flat, even if k == 3 else mean)
        out(k, made.reshape(planes, padded, LANES))


def spread(coarse, spare, rows, base, fine, row_map, plane_maps, empty):
    planes, height, _ = spare.shape
    source, target = iota((LANES, LANES), 0), iota((LANES, LANES), 1)
    half = target // 2
    pick = jnp.where(source == jnp.where(target < LANES // 2, half, LANES // 2 + half), 1.0, 0.0)
    wide = exact_dot(coarse[0:planes].reshape(planes * height, LANES), pick)
    spare[...] = wide.reshape(planes, height, LANES)
    rows[...] = jnp.zeros(rows.shape, jnp.float32)
    fine[empty] = rows[...]
    for count, plane_of, target_of in plane_maps:

        def body(i, carry):
            plane = plane_of(i)
            for start, number, first in row_map:
                part = spare[plane, start : start + number, :]
                rows[pl.ds(first, number, stride=2), :] = part
                rows[pl.ds(first + 1, number, stride=2), :] = part
            both = rows[...]
            at = target_of(i)
            fine[at] = base[at] + both
            fine[at + 1] = base[at + 1] + both
            return carry

        lax.fori_loop(0, count, body, 0)


def spread_halves(coarse, spare, rows, base, fine, gx):
    planes, height, _ = spare.shape
    source, target = iota((LANES, LANES), 0), iota((LANES, LANES), 1)
    wanted = (target % (LANES // 2)) // 2 + (LANES - 4)
    pick = jnp.where(source == wanted % LANES, 1.0, 0.0)
    wide = exact_dot(coarse[0:planes].reshape(planes * height, LANES), pick)
    spare[...] = wide.reshape(planes, height, LANES)
    lane = iota((height, LANES), 1)

    def body(q, carry):
        j = q - 9 - 2 * gx
        there = (q < 9) | ((j >= 0) & (j < 4))
        above = jnp.where(q < 9, q + 15, 24 + 5 * gx + jnp.clip(j, 0, 3))
        both = jnp.where(lane < LANES // 2, spare[q], jnp.where(there, spare[above], 0.0))
        for start, number, first in ((0, 28, 0), (36, 4, 56)):
            part = both[start : start + number]
            rows[pl.ds(first, number, stride=2), :] = part
            rows[pl.ds(first + 1, number, stride=2), :] = part
        wide_rows = rows[...]
        fine[2 * q] = base[2 * q] + wide_rows
        fine[2 * q + 1] = base[2 * q + 1] + wide_rows
        return carry

    lax.fori_loop(0, HALF // 2, body, 0)


def places():
    gx = lax.axis_index("gx")
    gy = lax.axis_index("gy")
    gz = lax.axis_index("gz_0") * 4 + lax.axis_index("gz_1")
    return gx, gy, gz


def widen(value):
    rows, lanes = value.shape
    if lanes == LANES:
        return value
    return jnp.concatenate([value, jnp.zeros((rows, LANES - lanes), jnp.float32)], axis=1)


def y_pack(parts, size):
    lane = iota((8, LANES), 1)
    tiles = [jnp.zeros((8, LANES), jnp.float32) for _ in range(-(-5 * size // LANES))]
    for k, part in enumerate(parts):
        start = k * size
        moved = roll(part, start % LANES, -1)
        for t in range(len(tiles)):
            a, b = max(start, t * LANES) - t * LANES, min(start + size, (t + 1) * LANES) - t * LANES
            if a < b:
                tiles[t] = jnp.where((lane >= a) & (lane < b), moved, tiles[t])
    return tiles


def y_value(tiles, k, size):
    start = k * size
    t = start // LANES
    value = tiles[t]
    if start + size > (t + 1) * LANES:
        value = jnp.where(iota(value.shape, 1) >= start - t * LANES, value, tiles[t + 1])
    return value


def y_start(k, size):
    return k * size % LANES


def y_unpack(tiles, k, size, to):
    return roll(y_value(tiles, k, size), to - y_start(k, size), -1)


def y_rows(at, size, y_even, y_odd):
    even_y = places()[1] % 2 == 0
    e, o = y_even[at], y_odd[at]
    ends = jnp.where(even_y, e, o), jnp.where(even_y, o, e)
    tiles = [
        jnp.concatenate([end[8 * t : 8 * t + 8] for end in ends], axis=0)
        for t in range(-(-5 * size // LANES))
    ]
    return [y_value(tiles, k, size) for k in range(5)]


def place_halves(stack, own, beside, size, y_even, y_odd):
    gx, _, _ = places()
    lane = iota((16, LANES), 1)
    in_low = (lane >= 8) & (lane < size + 8)
    in_high = (lane >= LANES // 2 + 8) & (lane < LANES // 2 + size + 8)

    def put(p, low, high, other, there):
        near_low = y_rows(p, size, y_even, y_odd)
        near_high = y_rows(other, size, y_even, y_odd)
        for k in range(5):
            stack[k, p, 0:size, :] = roll(low(k), 8, -1) + roll(high(k), LANES // 2 + 8, -1)
            start = y_start(k, size)
            second = jnp.where(in_high & there, roll(near_high[k], LANES // 2 + 8 - start, -1), 0.0)
            stack[k, p, size:, :] = jnp.where(in_low, roll(near_low[k], 8 - start, -1), second)

    def both(g, carry):
        for u in range(3):
            p = 3 * g + u
            put(p, lambda k: own(k, p), lambda k: own(k, p + HALF), p + HALF, True)
        return carry

    lax.fori_loop(0, (size - HALF) // 3, both, 0)

    def mixed(g, carry):
        for u in range(3):
            p = size - HALF + 3 * g + u
            j = 3 * g + u - 4 * gx
            there = (j >= 0) & (j < 8)
            at = jnp.clip(j, 0, 7)
            second = lambda k: jnp.where(there, beside(k, at), 0.0)
            put(p, lambda k: own(k, p), second, size + at, there)
        return carry

    lax.fori_loop(0, (2 * HALF - size) // 3, mixed, 0)


def each_group(size, group):
    gx = lax.axis_index("gx")

    def low(h, carry):
        for g in [5 * h + u for u in range(5)]:
            group(g, 3, 3 * g, 0)
        return carry

    def high(h, carry):
        for g in [3 * h + u for u in range(3)]:
            group(g + HALF // 3, 3, 3 * g, LANES // 2)
        return carry

    lax.fori_loop(0, HALF // 15, low, 0)
    lax.fori_loop(0, (size - HALF) // 9, high, 0)
    for q in range(3):
        first = size - HALF + 4 * gx + 3 * q
        group(size // 3 + q, min(3, 8 - 3 * q), first, LANES // 2)


def merge_halves(stack, size, z_even, z_odd, c_even, c_odd):
    even_z = places()[2] % 2 == 0
    lane = iota((size + 16, LANES), 1)

    def group(g, slots, first, base):
        even = jnp.concatenate([z_even[g], c_even[g]], axis=0)
        odd = jnp.concatenate([z_odd[g], c_odd[g]], axis=0)
        low, high = jnp.where(even_z, odd, even), jnp.where(even_z, even, odd)
        at_low = (lane >= base) & (lane < base + 8)
        at_high = (lane >= base + 56) & (lane < base + 64)
        for s in range(slots):
            for k in range(5):
                at = 40 * s + 8 * k
                v = stack[k, first + s]
                v = jnp.where(at_low, roll(low, base - at, -1), v)
                stack[k, first + s] = jnp.where(at_high, roll(high, base + 56 - at, -1), v)

    each_group(size, group)


def y_faces(values, size, at, y_even, y_odd):
    even_y = places()[1] % 2 == 0
    high = y_pack([v[size - 8 :] for v in values], size)
    low = y_pack([v[:8] for v in values], size)
    for t, (h, l) in enumerate(zip(high, low)):
        y_even[at, 8 * t : 8 * t + 8, :] = jnp.where(even_y, h, l)
        y_odd[at, 8 * t : 8 * t + 8, :] = jnp.where(even_y, l, h)


def z_faces(planes, size, starts=(0,) * 5):
    even_z = places()[2] % 2 == 0
    rows = planes[0][0].shape[0]
    lane = iota((rows, LANES), 1)
    top = jnp.zeros((rows, LANES), jnp.float32)
    bottom = top
    for s, values in enumerate(planes):
        for k, v in enumerate(values):
            at = 40 * s + 8 * k
            here = (lane >= at) & (lane < at + 8)
            top = jnp.where(here, roll(v, at - starts[k] - (size - 8), -1), top)
            bottom = jnp.where(here, roll(v, at - starts[k], -1), bottom)
    return jnp.where(even_z, top, bottom), jnp.where(even_z, bottom, top)


def y_sides(source, size, slots, keep, y_even, y_odd):
    even_y = places()[1] % 2 == 0
    lane = iota((16, LANES), 1)
    tiles = -(-5 * size // LANES)
    planes = []
    for s in range(slots):
        e, o = y_even[3 * source + s], y_odd[3 * source + s]
        ends = jnp.where(even_y, e, o), jnp.where(even_y, o, e)
        ends = [[end[8 * t : 8 * t + 8] for t in range(tiles)] for end in ends]
        values = []
        for k in range(5):
            v = jnp.concatenate([y_unpack(end, k, size, 0) for end in ends], axis=0)
            v = jnp.where(lane < size, v, 0.0)
            keep(k, s, v)
            values.append(v)
        planes.append(values)
    return planes


def merge_z(stack, size, z_even, z_odd):
    gx, _, gz = places()
    even_z = gz % 2 == 0
    lane = iota((size + 16, LANES), 1)

    def group(g, slots, first):
        low = jnp.where(even_z, z_odd[g], z_even[g])
        high = jnp.where(even_z, z_even[g], z_odd[g])
        for s in range(slots):
            for k in range(5):
                at = 40 * s + 8 * k
                v = stack[k, first + s]
                v = jnp.where(lane >= LANES - 8, roll(low, LANES - 8 - at, -1), v)
                here = (lane >= size) & (lane < size + 8)
                stack[k, first + s] = jnp.where(here, roll(high, size - at, -1), v)

    def body(h, carry):
        for g in (2 * h, 2 * h + 1):
            group(g, 3, 3 * g)
        return carry

    lax.fori_loop(0, size // 6, body, 0)
    for q in range(3):
        group(size // 3 + q, min(3, 8 - 3 * q), size + gx + 3 * q)


def partner(index, parity, count):
    if parity is None:
        return index
    other = index + 1 if index % 2 == parity else index - 1
    return other if 0 <= other < count else None


def swap(value, parity_y, parity_z):
    pairs = []
    for y in range(COUNT_Y):
        for z in range(COUNT_Z):
            to_y, to_z = partner(y, parity_y, COUNT_Y), partner(z, parity_z, COUNT_Z)
            if to_y is not None and to_z is not None:
                pairs.append((y * COUNT_Z + z, to_y * COUNT_Z + to_z))
    return lax.ppermute(value, YZ, pairs)


def swap_cores(value):
    return lax.ppermute(value, "gx", [(0, 1), (1, 0)])


def f32(*shape):
    return jax.ShapeDtypeStruct(shape, jnp.float32)


def near(*shape):
    return pltpu.VMEM(shape, jnp.float32)


def call(body, outs, ins, scratch, operands, limit, aliases={}):
    held = [
        pltpu.with_memory_space_constraint(v, pltpu.HBM if spec is far else pltpu.VMEM)
        for v, spec in zip(operands, ins)
    ]
    return pl.pallas_call(
        body,
        out_shape=outs,
        out_specs=[vmem] * len(outs),
        in_specs=ins,
        scratch_shapes=scratch,
        input_output_aliases=aliases,
        compiler_params=pltpu.CompilerParams(vmem_limit_bytes=limit * 2**20),
    )(*held)


def edge_kernel(right, faces, cells, out, sems):
    gx = lax.axis_index("gx")
    start = (1 - gx) * (SIZES[0] - WIDTH)
    part = pl.ds(start, WIDTH)
    copies = [
        pltpu.make_async_copy(right.at[part], out.at[0], sems.at[0]),
        pltpu.make_async_copy(faces.at[0, part], out.at[1], sems.at[1]),
        pltpu.make_async_copy(faces.at[1, part], out.at[2], sems.at[2]),
        pltpu.make_async_copy(faces.at[2, part], out.at[3], sems.at[3]),
        pltpu.make_async_copy(cells.at[part], out.at[4], sems.at[4]),
    ]
    for copy in copies:
        copy.start()
    for copy in copies:
        copy.wait()


def own_inputs(right, faces, cells):
    def own(k, i):
        if k == 0:
            return widen(right[i])
        return widen(cells[i] if k == 4 else faces[k - 1, i])

    return own


def pack_y_0_kernel(right, faces, cells, beside, y_even, y_odd):
    size = SIZES[0]
    own = own_inputs(right, faces, cells)

    def body(g, carry):
        for u in range(4):
            y_faces([own(k, 4 * g + u) for k in range(5)], size, 4 * g + u, y_even, y_odd)
        return carry

    lax.fori_loop(0, size // 4, body, 0)
    for j in range(8):
        y_faces([widen(beside[k, j]) for k in range(5)], size, size + j, y_even, y_odd)


def pack_z_0_kernel(right, faces, cells, beside, z_even, z_odd):
    size = SIZES[0]
    own = own_inputs(right, faces, cells)

    def body(h, carry):
        for u in range(4):
            g = 4 * h + u
            planes = [[own(k, 3 * g + s) for k in range(5)] for s in range(3)]
            z_even[g], z_odd[g] = z_faces(planes, size)
        return carry

    lax.fori_loop(0, size // 12, body, 0)
    for q in range(3):
        slots = range(min(3, 8 - 3 * q))
        planes = [[widen(beside[k, 3 * q + s]) for k in range(5)] for s in slots]
        g = size // 3 + q
        z_even[g], z_odd[g] = z_faces(planes, size)


def corner_0_kernel(y_even, y_odd, c_even, c_odd):
    size = SIZES[0]
    starts = [y_start(k, size) for k in range(5)]

    def group(g, slots):
        planes = [y_rows(3 * g + s, size, y_even, y_odd) for s in range(slots)]
        c_even[g], c_odd[g] = z_faces(planes, size, starts)

    def body(h, carry):
        for u in range(3):
            group(3 * h + u, 3)
        return carry

    lax.fori_loop(0, 6, body, 0)
    group(18, 2)


def place_0_kernel(right, faces, cells, beside, y_even, y_odd, stack):
    own = own_inputs(right, faces, cells)
    place_halves(stack, own, lambda k, j: widen(beside[k, j]), SIZES[0], y_even, y_odd)


def own_1_kernel(own, y_even, y_odd, z_even, z_odd):
    size = SIZES[1]

    def body(g, carry):
        planes = [[own[k, 3 * g + s] for k in range(5)] for s in range(3)]
        for s in range(3):
            y_faces(planes[s], size, 3 * g + s, y_even, y_odd)
        z_even[g], z_odd[g] = z_faces(planes, size)
        return carry

    lax.fori_loop(0, size // 3, body, 0)


def beside_1_kernel(beside, own_even, own_odd, y_even, y_odd):
    size = SIZES[1]
    y_even[0:size] = own_even[...]
    y_odd[0:size] = own_odd[...]
    for j in range(8):
        y_faces([beside[k, j] for k in range(5)], size, size + j, y_even, y_odd)


def fill_1_kernel(own, beside, own_even, own_odd, stack, z_even, z_odd):
    size = SIZES[1]
    gx = lax.axis_index("gx")
    z_even[0 : size // 3] = own_even[...]
    z_odd[0 : size // 3] = own_odd[...]

    def body(i, carry):
        for k in range(5):
            stack[k, i, 0:size, :] = own[k, i]
        return carry

    lax.fori_loop(0, size, body, 0)
    for q in range(3):
        slots, first = min(3, 8 - 3 * q), size + gx + 3 * q
        planes = [[beside[k, 3 * q + s] for k in range(5)] for s in range(slots)]
        for s in range(slots):
            for k in range(5):
                stack[k, first + s, 0:size, :] = planes[s][k]
        g = size // 3 + q
        z_even[g], z_odd[g] = z_faces(planes, size)
    empty = size + 8 * (1 - gx)
    for k in range(5):
        stack[k, empty] = jnp.zeros(stack.shape[2:], jnp.float32)


def side_1_kernel(filled, y_even, y_odd, own_even, own_odd, stack, z_even, z_odd):
    size = SIZES[1]
    gx = lax.axis_index("gx")
    z_even[:, 0:size, :] = own_even[...]
    z_odd[:, 0:size, :] = own_odd[...]
    sides = pl.ds(size, 16)

    def keep_at(first):
        def keep(k, s, v):
            stack[k, first + s, size : size + 16, :] = v

        return keep

    def body(h, carry):
        for g in (2 * h, 2 * h + 1):
            planes = y_sides(g, size, 3, keep_at(3 * g), y_even, y_odd)
            z_even[g, sides, :], z_odd[g, sides, :] = z_faces(planes, size)
        return carry

    lax.fori_loop(0, size // 6, body, 0)
    for q in range(3):
        slots, first = min(3, 8 - 3 * q), size + gx + 3 * q
        g = size // 3 + q
        planes = y_sides(g, size, slots, keep_at(first), y_even, y_odd)
        z_even[g, sides, :], z_odd[g, sides, :] = z_faces(planes, size)


def level_0_kernel(
    filled, z_even, z_odd, c_even, c_odd,
    coarse, coarse_edge, stack, iterate,
    update, rows, pairs,
):
    size = SIZES[0]
    gx = lax.axis_index("gx")
    merge_halves(stack, size, z_even, z_odd, c_even, c_odd)
    down(stack, iterate, update, 1.0, HALF, HALF, Halves)
    keep_remainder(stack, iterate, update, 1.0, HALF, HALF, Halves)

    def out(k, value):
        lane = iota(value.shape, -1)
        coarse[k, 0:15] = jnp.where(lane < 24, value, 0.0)
        second = roll(value[0:9], LANES // 2, -1)
        coarse[k, 15:24] = jnp.where(lane[0:9] < 24, second, 0.0)
        coarse_edge[k] = jnp.where(gx == 0, coarse[k, 16:24], coarse[k, 0:8])

    coarsen(stack, update, rows, pairs, out, HALF, size, LANES // 2, 8)


def level_1_kernel(
    filled, z_even, z_odd, held,
    coarse, stack, iterate,
    update, rows, pairs, made,
):
    size = SIZES[1]
    planes = size + 9
    merge_z(stack, size, z_even, z_odd)
    down(stack, iterate, update, 0.25, planes, planes, Wrapped)
    keep_remainder(stack, iterate, update, 0.25, planes, planes, Wrapped)

    def out(k, value):
        made[k] = value

    coarsen(stack, update, rows, pairs, out, size, size)
    for i in range(SIZES[2] // 2):
        line = made[0, 2 * i] + roll(made[0, 2 * i + 1], LANES // 2, -1)
        for h in range(2):
            for k in range(1, 5):
                line = line + roll(made[k, 2 * i + h], LANES // 2 * h + SIZES[2] * k, -1)
        coarse[i] = line


def level_2_kernel(
    mine, other, held,
    payload, stack, iterate,
    update, rows, pairs, made, lines,
):
    size = SIZES[2]
    planes = 2 * size + 1
    gx, gy, gz = places()
    even_y, even_z = gy % 2 == 0, gz % 2 == 0
    lane = iota((16, LANES), 1)
    bases = (0, size, LANES - size)
    half = size // 2
    for k in range(5):
        stack[k, 2 * size] = jnp.zeros(stack.shape[2:], jnp.float32)

    def body(i, carry):
        for core in range(2):

            def block(a, b):
                at = half * (3 * b + a) + i
                return jnp.where(gx == core, mine[at], other[at])

            columns = []
            for b in range(3):
                even, odd = block(1, b), block(2, b)
                columns.append(
                    (block(0, b), jnp.where(even_y, even, odd), jnp.where(even_y, odd, even))
                )
            columns = [columns[0]] + [
                [jnp.where(even_z, p, q) for p, q in zip(columns[c], columns[3 - c])] for c in (1, 2)
            ]
            for h in range(2):
                plane = size * core + 2 * i + h
                for k in range(5):
                    source = (LANES // 2) * h + size * k
                    stack[k, plane, 24:32, :] = jnp.zeros((8, LANES), jnp.float32)
                    for a, first in enumerate((0, size, 40 - size)):
                        line = jnp.zeros((16, LANES), jnp.float32)
                        for b, base in enumerate(bases):
                            here = (lane >= base) & (lane < base + size)
                            line = jnp.where(here, roll(columns[b][a], base - source, -1), line)
                        stack[k, plane, first : first + size, :] = line[:size]
        return carry

    lax.fori_loop(0, half, body, 0)
    weight = 0.0625
    iterate[2 * size] = jnp.zeros(iterate.shape[1:], jnp.float32)
    down(stack, iterate, update, weight, planes, 2 * size, Middle)
    keep_remainder(stack, iterate, update, weight, planes, 2 * size, Middle)

    def out(k, value):
        made[k * 96 : k * 96 + 96, :] = value.reshape(96, LANES)

    coarsen(stack, update, rows, pairs, out, 2 * size, size)
    line = jnp.zeros((60, LANES), jnp.float32)
    for y in range(6):
        line = line + roll(made[pl.ds(y, 60, stride=8), :], 6 * y, -1)
    lines[0:60, :] = line
    chunk = lines[0:20, :] + roll(lines[20:40, :], 40, -1) + roll(lines[40:60, :], 80, -1)
    chunk = jnp.concatenate([chunk, jnp.zeros((4, LANES), jnp.float32)], axis=0)

    def repeat(c, carry):
        payload[pl.ds(pl.multiple_of(c * CHUNK, 8), CHUNK), :] = chunk
        return carry

    lax.fori_loop(0, COLUMNS, repeat, 0)


def compact(value):
    row = iota(value.shape, -2)
    out = jnp.where(row == 0, value, 0.0)
    out = jnp.where(row == 1, roll(value, -1, -2), out)
    return jnp.where(row == 2, roll(value, -2, -2), out)


def bottom(source, faces, cells):
    weight = 0.25**4
    move = Columns(3)
    face_x, face_y, face_z = faces
    nothing = jnp.zeros((1,) + source.shape[1:], jnp.float32)

    def apply(v):
        flux_x = face_x * (v - jnp.concatenate([nothing, v[:-1]], axis=0))
        flux_y = face_y * (v - move.low_y(v))
        flux_z = face_z * (v - move.low_z(v))
        total = flux_x - jnp.concatenate([flux_x[1:], nothing], axis=0)
        total = total + (flux_y - move.up_y(flux_y)) + (flux_z - move.up_z(flux_z))
        return cells * v + weight * total

    def total_of(v):
        flat = jnp.sum(jnp.sum(v, axis=0), axis=0)
        one = jnp.sum(jnp.sum(flat, axis=0, keepdims=True), axis=1, keepdims=True)
        return jnp.broadcast_to(one, flat.shape)

    iterate = jnp.zeros_like(source)
    remainder = source
    search = source
    norm_now = total_of(remainder * remainder)
    for step in range(BOTTOM):
        applied = apply(search)
        size = norm_now / total_of(search * applied)
        iterate = iterate + size * search
        if step + 1 < BOTTOM:
            remainder = remainder - size * applied
            norm_next = total_of(remainder * remainder)
            search = remainder + (norm_next / norm_now) * search
            norm_now = norm_next
    return iterate


def rise_kernel(
    gathered, stack_2, base_2, stack_1, base_1, stack_0, base_0,
    solution_out, residual_out, sums,
    iterate_0, update_0, rows_0, spare_1,
    iterate_1, update_1, rows_1, spare_2,
    iterate_2, update_2, rows_2, spare_3,
    stack_3, iterate_3, update_3, turned, table, block_3,
):
    gx, gy, gz = places()

    stack_3[...] = jnp.zeros(stack_3.shape, jnp.float32)
    blank = jnp.zeros((LANES - COLUMNS, LANES), jnp.float32)
    for r in range(20):
        part = gathered[pl.ds(r, COLUMNS, stride=CHUNK), :]
        turned[...] = jnp.transpose(jnp.concatenate([part, blank], axis=0))
        for j in range(3):
            k, x = divmod(20 * j + r, 12)
            for y in range(6):
                stack_3[k, x, y, 0:6, :] = turned[40 * j + 6 * y : 40 * j + 6 * y + 6, :]
    move = Columns(6)
    weight = 0.25**3
    iterate_3[12] = jnp.zeros(iterate_3.shape[1:], jnp.float32)
    down(stack_3, iterate_3, update_3, weight, 13, 12, move)
    keep_remainder(stack_3, iterate_3, update_3, weight, 13, 12, move)

    def coarse(k, x_pair, y_pair, z_pair, scale):
        planes = []
        for x in range(6):
            read = (lambda i: update_3[i]) if k == 0 else (lambda i: stack_3[k, i])
            v = read(2 * x)
            if x_pair:
                v = v + read(2 * x + 1)
            lines = []
            for y in range(3):
                line = v[2 * y]
                if y_pair:
                    line = line + v[2 * y + 1]
                if z_pair:
                    line = line + roll(line, -1, -2)
                lines.append(scale * compact(line))
            planes.append(jnp.stack(lines))
        return jnp.stack(planes)

    lowest = bottom(
        coarse(0, True, True, True, 0.125),
        (
            coarse(1, False, True, True, 0.25),
            coarse(2, True, False, True, 0.25),
            coarse(3, True, True, False, 0.25),
        ),
        coarse(4, True, True, True, 0.125),
    )
    row = iota((8, LANES), 0)
    for x in range(6):
        for y in range(3):
            line = lowest[x, y]
            wide = jnp.where(row == 0, line, 0.0)
            for to in range(1, 6):
                wide = jnp.where(row == to, roll(line, to - to // 2, -2), wide)
            for a in range(2):
                for b in range(2):
                    iterate_3[2 * x + a, 2 * y + b] = iterate_3[2 * x + a, 2 * y + b] + wide
    up(stack_3, iterate_3, update_3, weight, 13, 12, move)

    low_rows = jnp.zeros((32, LANES), jnp.float32)
    for q in range(6):
        two = [iterate_3[2 * q + h].reshape(48, LANES) for h in range(2)]
        table[q] = jnp.transpose(jnp.concatenate(two + [low_rows], axis=0))
    block_3[...] = jnp.zeros(block_3.shape, jnp.float32)
    lane = iota((8, LANES), 1)

    def place(q, carry):
        for a, first in ((0, 0), (1, 6), (-1, 18)):
            lines = [jnp.zeros((8, LANES), jnp.float32) for _ in range(2)]
            for b, base in ((0, 0), (1, 6), (-1, LANES - 6)):
                y, z = gy + a, gz + b
                inside = (y >= 0) & (y < COUNT_Y) & (z >= 0) & (z < COUNT_Z)
                at = jnp.where(inside, y * COUNT_Z + z, 0)
                here = (lane >= base) & (lane < base + 6) & inside
                found = jnp.broadcast_to(table[q, pl.ds(at, 1), :], (8, LANES))
                for h in range(2):
                    for y_in in range(6):
                        moved = roll(found, base - 48 * h - 8 * y_in, -1)
                        lines[h] = jnp.where(here & (row == y_in), moved, lines[h])
            for h in range(2):
                block_3[2 * q + h, first : first + 6, :] = lines[h][0:6]
        return carry

    lax.fori_loop(0, 6, place, 0)

    spread(
        block_3, spare_3, rows_2, base_2, iterate_2,
        ((0, 12, 0), (18, 6, 28)),
        ((12, lambda i: i, lambda i: 2 * i),),
        24,
    )
    up(stack_2, iterate_2, update_2, 0.0625, 25, 24, Middle)

    size = SIZES[1]
    spread(
        iterate_2, spare_2, rows_1, base_1, iterate_1,
        ((0, 16, 0), (36, 4, 32)),
        (
            (12, lambda i: 12 * gx + i, lambda i: 2 * i),
            (4, lambda i: 12 - 4 * gx + i, lambda i: size + gx + 2 * i),
        ),
        size + 8 * (1 - gx),
    )
    up(stack_1, iterate_1, update_1, 0.25, size + 9, size + 9, Wrapped)

    size = SIZES[0]
    spread_halves(iterate_1, spare_1, rows_0, base_0, iterate_0, gx)
    up(stack_0, iterate_0, update_0, 1.0, HALF, HALF, Halves)
    iterate_0[HALF] = Halves.turn(iterate_0[0])
    inside = iota((size, LANES), 1)
    in_low = (inside >= 8) & (inside < 56)
    in_high = (inside >= 72) & (inside < 120)

    def use(i, v, remainder, carry):
        v, remainder = v[0:size], remainder[0:size]
        solution_out[i] = roll(v, -8, -1)[:, 0:size]
        residual_out[i] = roll(remainder, -8, -1)[:, 0:size]

        mask = in_low
        if i < size - HALF:
            solution_out[i + HALF] = roll(v, -72, -1)[:, 0:size]
            residual_out[i + HALF] = roll(remainder, -72, -1)[:, 0:size]
            mask = in_low | in_high
        mine = jnp.where(mask, remainder, 0.0)
        given = jnp.where(mask, stack_0[0, i, 0:size, :], 0.0)
        return carry[0] + mine * mine, carry[1] + given * given

    zero = jnp.zeros((size, LANES), jnp.float32)
    squares = stencil_pass(stack_0, iterate_0, 1.0, HALF, HALF, Halves, use, (zero, zero))
    ones = []
    for square in squares:
        one = jnp.sum(jnp.sum(square, axis=0, keepdims=True), axis=1, keepdims=True)
        ones.append(jnp.broadcast_to(one, (8, LANES)))
    sums[...] = jnp.where(lane == 0, ones[0], jnp.where(lane == 1, ones[1], 0.0))


def stack_kernel(*refs):
    out = refs[-1]
    for n, ref in enumerate(refs[:-1]):
        count = ref.shape[0]
        out[n * count : n * count + count] = ref[...]


def stacked(*parts):
    count, *rest = parts[0].shape
    return call(stack_kernel, [near(len(parts) * count, *rest)], [held_near] * 3, [], parts, 1)[0]


def shards(right, faces, cells):
    dma = pltpu.SemaphoreType.DMA
    edge = call(edge_kernel, [near(5, WIDTH, 48, 48)], [far] * 3, [dma((5,))],
        (right, faces, cells), 2)[0]
    beside = swap_cores(edge)
    given = (right, faces, cells, beside)
    outs = call(pack_y_0_kernel, [near(56, 16, LANES)] * 2, [held_near] * 4, [], given, 4)
    sides = [swap(v, parity, None) for parity, v in enumerate(outs)]
    outs = call(pack_z_0_kernel, [near(19, 48, LANES)] * 2, [held_near] * 4, [], given, 4)
    ends = [swap(v, None, parity) for parity, v in enumerate(outs)]
    outs = call(corner_0_kernel, [near(19, 16, LANES)] * 2, [held_near] * 2, [], sides, 4)
    corners = [swap(v, None, parity) for parity, v in enumerate(outs)]
    filled = call(place_0_kernel, [near(7, 31, 64, LANES)], [held_near] * 6, [],
        (*given, *sides), 4)[0]
    coarse, coarse_edge, stack_0, iterate_0 = call(
        level_0_kernel,
        [near(5, 24, 24, LANES), near(5, WIDTH, 24, LANES), near(7, 31, 64, LANES), near(31, 64, LANES)],
        [held_near] * 5,
        [near(31, 64, LANES), near(5, 64, LANES), near(5, 15, 24, LANES)],
        (filled, *ends, *corners),
        10,
        {0: 2},
    )
    beside = swap_cores(coarse_edge)
    y_shape, z_shape = near(32, 8, LANES), near(11, 24, LANES)
    *y_own, z_even, z_odd = call(own_1_kernel, [near(24, 8, LANES)] * 2 + [near(8, 24, LANES)] * 2,
        [held_near], [], (coarse,), 4)
    outs = call(beside_1_kernel, [y_shape] * 2, [held_near] * 3, [], (beside, *y_own), 4)
    sides = [swap(v, parity, None) for parity, v in enumerate(outs)]
    filled, *z_own = call(fill_1_kernel, [near(7, 34, 40, LANES), z_shape, z_shape],
        [held_near] * 4, [], (coarse, beside, z_even, z_odd), 4)
    filled, *outs = call(side_1_kernel, [near(7, 34, 40, LANES)] + [near(11, 40, LANES)] * 2,
        [held_near] * 5, [], (filled, *sides, *z_own), 4, {0: 0})
    z_sides = [swap(v, None, parity) for parity, v in enumerate(outs)]
    coarse, stack_1, iterate_1 = call(
        level_1_kernel,
        [near(6, 16, LANES), near(7, 34, 40, LANES), near(34, 40, LANES)],
        [held_near] * 4,
        [near(34, 40, LANES), near(5, 40, LANES), near(5, 12, 16, LANES), near(5, 12, 16, LANES)],
        (filled, *z_sides, stack_0),
        12,
        {0: 1},
    )
    column = stacked(coarse, *[swap(coarse, parity, None) for parity in (0, 1)])
    region = stacked(column, *[swap(column, None, parity) for parity in (0, 1)])
    other = swap_cores(region)
    payload, stack_2, iterate_2 = call(
        level_2_kernel,
        [near(COLUMNS * CHUNK, LANES), near(7, 26, 40, LANES), near(26, 40, LANES)],
        [held_near] * 3,
        [near(26, 40, LANES), near(5, 40, LANES), near(5, 12, 8, LANES), near(480, LANES), near(64, LANES)],
        (region, other, stack_0),
        12,
    )
    payload = payload.reshape(COLUMNS, CHUNK, LANES)
    gathered = lax.all_to_all(payload, YZ, 0, 0).reshape(COLUMNS * CHUNK, LANES)
    solved, residual, sums = call(
        rise_kernel,
        [f32(48, 48, 48), f32(48, 48, 48), f32(8, LANES)],
        [held_near] * 7,
        [
            near(31, 64, LANES), near(31, 64, LANES), near(64, LANES), near(33, 40, LANES),
            near(34, 40, LANES), near(34, 40, LANES), near(40, LANES), near(24, 40, LANES),
            near(26, 40, LANES), near(26, 40, LANES), near(40, LANES), near(12, 24, LANES),
            near(8, 14, 6, 8, LANES), near(14, 6, 8, LANES), near(14, 6, 8, LANES),
            near(LANES, LANES), near(6, LANES, LANES), near(12, 24, LANES),
        ],
        (gathered, stack_2, iterate_2, stack_1, iterate_1, stack_0, iterate_0),
        24,
    )
    each = jnp.broadcast_to(sums[0:1].reshape(1, 1, LANES), (128, 1, LANES))
    total = jnp.sum(lax.all_to_all(each, ALL, 0, 0), axis=(0, 1))
    return solved, residual, jnp.sqrt(total[0] / total[1])


def solution(mesh):
    torus = Mesh(
        mesh.devices.reshape(mesh.shape["gx"], mesh.shape["gy"], 4, 4), ("gx", "gy", "gz_0", "gz_1")
    )
    in_specs = (P("gx", "gy", GZ), P(None, "gx", "gy", GZ), P("gx", "gy", GZ))
    out_specs = (P("gx", "gy", GZ), P("gx", "gy", GZ), P())
    return jax.shard_map(
        shards, mesh=torus, in_specs=in_specs, out_specs=out_specs, check_vma=False
    )
```
